32 devices in a mesh: dp: 1 (over z), ty: 4 (over y), tx: 8 (over x, core).
Axes of the slice: x: 4, y: 4, z: 1, core: 2. Of those that a mesh axis runs over, the one named last changes fastest.
The devices are a block of a 4x4x8 slice.
Arguments:
- x_in: bfloat16 [4, 1024, 4096], P(('dp', 'ty'), None, 'tx')
- w_q: bfloat16 [4096, 4096], P('tx', 'ty')
- w_k: bfloat16 [4096, 4096], P('tx', 'ty')
- w_v: bfloat16 [4096, 4096], P('tx', 'ty')
- w_o: bfloat16 [4096, 4096], P('ty', 'tx')
- w_gate: bfloat16 [4096, 11008], P('tx', 'ty')
- w_up: bfloat16 [4096, 11008], P('tx', 'ty')
- w_down: bfloat16 [11008, 4096], P('ty', 'tx')
Outputs:
- output: bfloat16 [4, 1024, 4096], P(('dp', 'ty'), None, 'tx')
All inputs are finite; a program needn't handle non-finite values.
Results may differ from the reference program's by a relative error of at most 0.02.
Values are sent between devices in bfloat16 or wider.
A program may use at most 768 MiB of HBM per device.

```python
import jax
import jax.numpy as jnp
from jax import lax

NSEQ = 4
SEQ = 1024
D = 4096
FF = 11008
HEADS = 32

HEAD_DIM = D // HEADS
EPS = 1e-5
THETA = 10000.0


def setup_inputs(seed: int = 0, part: int = 0) -> dict:
    root_key = jax.random.key(seed)
    act_root, weight_root = jax.random.split(root_key)
    part_key = jax.random.fold_in(act_root, part)
    key_tok, key_scale, key_shift, key_slope, key_walk = jax.random.split(part_key, 5)
    tok_noise = jax.random.normal(key_tok, (NSEQ, SEQ, D), jnp.float32)
    tok_scale = jax.random.uniform(key_scale, (NSEQ, SEQ, 1), jnp.float32, 0.5, 2.0)
    tok_shift = 0.5 * jax.random.normal(key_shift, (NSEQ, SEQ, 1), jnp.float32)
    col_slope = jax.random.uniform(key_slope, (), jnp.float32, 1.0, 2.0)
    col_pos = jnp.arange(D, dtype=jnp.float32) / D - 0.5
    col_walk = jnp.cumsum(jax.random.normal(key_walk, (D,), jnp.float32)) * (1.5 * D ** -0.5)
    col_offset = 2.0 * col_slope * col_pos + col_walk
    x_in = (tok_scale * tok_noise + tok_shift + col_offset).astype(jnp.bfloat16)
    weight_keys = jax.random.split(weight_root, 7)

    def draw_weight(key_w, fan_in, fan_out, gain_mul):
        return (gain_mul * fan_in ** -0.5 * jax.random.normal(key_w, (fan_in, fan_out), jnp.float32)).astype(jnp.bfloat16)

    return {
        "x_in": x_in,
        "w_q": draw_weight(weight_keys[0], D, D, 1.5),
        "w_k": draw_weight(weight_keys[1], D, D, 1.5),
        "w_v": draw_weight(weight_keys[2], D, D, 1.0),
        "w_o": draw_weight(weight_keys[3], D, D, 2.5),
        "w_gate": draw_weight(weight_keys[4], D, FF, 1.0),
        "w_up": draw_weight(weight_keys[5], D, FF, 1.0),
        "w_down": draw_weight(weight_keys[6], FF, D, 2.0),
    }


def layer_norm(values_bf):
    values = values_bf.astype(jnp.float32)
    mean_val = jnp.mean(values, axis=-1, keepdims=True)
    var_val = jnp.mean(values * values, axis=-1, keepdims=True) - mean_val * mean_val
    return ((values - mean_val) * lax.rsqrt(var_val + EPS)).astype(jnp.bfloat16)


def rotary(heads_bf):
    seq_len = heads_bf.shape[1]
    half_dim = HEAD_DIM // 2
    inv_freq = THETA ** (-2.0 * jnp.arange(half_dim, dtype=jnp.float32) / HEAD_DIM)
    angles = jnp.arange(seq_len, dtype=jnp.float32)[:, None] * inv_freq[None, :]
    cos_t = jnp.cos(angles)[:, None, :]
    sin_t = jnp.sin(angles)[:, None, :]
    values = heads_bf.astype(jnp.float32)
    lower_half = values[..., :half_dim]
    upper_half = values[..., half_dim:]
    return jnp.concatenate([lower_half * cos_t - upper_half * sin_t, upper_half * cos_t + lower_half * sin_t], axis=-1).astype(jnp.bfloat16)


def causal_attention(q_heads, k_heads, v_heads):
    seq_len = q_heads.shape[1]
    q_block = min(seq_len, 128)
    key_pos = jnp.arange(seq_len)
    k_vals = k_heads.astype(jnp.float32)
    v_vals = v_heads.astype(jnp.float32)

    def one_block(block_idx, out_acc):
        q_start = block_idx * q_block
        q_blk = lax.dynamic_slice_in_dim(q_heads, q_start, q_block, axis=1).astype(jnp.float32)
        scores = jnp.einsum("nqhd,nkhd->nhqk", q_blk, k_vals) * HEAD_DIM ** -0.5
        q_pos = q_start + jnp.arange(q_block)
        allowed = q_pos[:, None] >= key_pos[None, :]
        scores = jnp.where(allowed, scores, -1e30)
        prob_blk = jax.nn.softmax(scores, axis=-1).astype(jnp.bfloat16).astype(jnp.float32)
        blk_out = jnp.einsum("nhqk,nkhd->nqhd", prob_blk, v_vals).astype(jnp.bfloat16)
        return lax.dynamic_update_slice_in_dim(out_acc, blk_out, q_start, axis=1)

    return lax.fori_loop(0, seq_len // q_block, one_block, jnp.zeros_like(q_heads))


def project(rows_bf, weight):
    return jnp.dot(rows_bf, weight, preferred_element_type=jnp.float32).astype(jnp.bfloat16)


def reference(x_in, w_q, w_k, w_v, w_o, w_gate, w_up, w_down):
    n_seqs, seq_len, d_model = x_in.shape
    head_shape = (n_seqs, seq_len, HEADS, HEAD_DIM)
    x_rows = x_in.reshape(n_seqs * seq_len, d_model)
    normed = layer_norm(x_rows)
    q_heads = rotary(project(normed, w_q).reshape(head_shape))
    k_heads = rotary(project(normed, w_k).reshape(head_shape))
    v_heads = project(normed, w_v).reshape(head_shape)
    attn_heads = causal_attention(q_heads, k_heads, v_heads)
    attn_out = project(attn_heads.reshape(n_seqs * seq_len, d_model), w_o)
    resid_h = (x_rows.astype(jnp.float32) + attn_out.astype(jnp.float32)).astype(jnp.bfloat16)
    normed_mlp = layer_norm(resid_h)
    gate_val = project(normed_mlp, w_gate)
    up_val = project(normed_mlp, w_up)
    act_val = (jax.nn.silu(gate_val.astype(jnp.float32)) * up_val.astype(jnp.float32)).astype(jnp.bfloat16)
    mlp_out = project(act_val, w_down)
    y_out = (resid_h.astype(jnp.float32) + mlp_out.astype(jnp.float32)).astype(jnp.bfloat16)
    return y_out.reshape(n_seqs, seq_len, d_model)
```

```python
import functools

import jax
import jax.numpy as jnp
from jax import lax
from jax.experimental import pallas as pl
from jax.experimental.pallas import tpu as pltpu
from jax.sharding import PartitionSpec as P

HEAD_DIM = 128
EPS = 1e-5
THETA = 10000.0
MESH = pl.DeviceIdType.MESH
F32 = jnp.float32
BF16 = jnp.bfloat16
NX = 4
NJ = 4
NCH = 16
STAGES = 4
VMEM_LIMIT = 67_043_328


def rem(a, b):
    return lax.rem(a, jnp.int32(b))


def div(a, b):
    return lax.div(a, jnp.int32(b))


def al(v, m):
    return pl.multiple_of(v, m)


def remote(src, dst, ssem, rsem, dev):
    return pltpu.make_async_remote_copy(src_ref=src, dst_ref=dst, send_sem=ssem, recv_sem=rsem, device_id=dev, device_id_type=MESH)


def chunk_of(n):
    is_c = div(n, 12)
    is_a = div(15 - n, 12)
    is_b = 1 - is_a - is_c
    j = is_a * n + is_b * (div(n + 12, 2) - 8) + is_c * (n - 12)
    r = is_b * (3 - 2 * rem(n, 2)) + 2 * is_c
    return r, j


class Place:
    def __init__(self):
        tx, ty = lax.axis_index("tx"), lax.axis_index("ty")
        self.x, self.c, self.y = div(tx, 2), rem(tx, 2), ty
        x, c, y = self.x, self.c, self.y
        self.xr, self.xl, self.xo = rem(x + 1, NX), rem(x + 3, NX), rem(x + 2, NX)
        self.yu, self.yd, self.yo = rem(y + 1, NX), rem(y + 3, NX), rem(y + 2, NX)
        self.right = {"tx": self.xr * 2 + c, "ty": y}
        self.left = {"tx": self.xl * 2 + c, "ty": y}
        self.up = {"tx": tx, "ty": self.yu}
        self.down = {"tx": tx, "ty": self.yd}
        self.partner = {"tx": x * 2 + 1 - c, "ty": y}

    def barrier(self):
        sem = pltpu.get_barrier_semaphore()
        for dev in (self.right, self.left, self.up, self.down, self.partner):
            pl.semaphore_signal(sem, inc=1, device_id=dev, device_id_type=MESH)
        pl.semaphore_wait(sem, 5)


class Gather:
    def __init__(self, at, src, xg, kc, ch, sx, rx, sy, ry):
        self.at, self.src, self.xg, self.kc, self.ch, self.h = at, src, xg, kc, ch, ch // 2
        self.sx, self.rx, self.sy, self.ry = sx, rx, sy, ry

    def cols(self, x):
        return pl.ds(al(x * self.kc, 128), self.kc)

    def keep_own(self, j):
        self.xg[self.at.y, j, :, self.cols(self.at.x)] = self.src[j]

    def xcopy(self, kind, j):
        at, h, ch = self.at, self.h, self.ch
        if kind < 2:
            src, dst = self.src.at[j], self.xg.at[at.y, j, :, self.cols(at.x)]
        elif kind == 2:
            src = dst = self.xg.at[at.y, j, pl.ds(0, h), self.cols(at.xl)]
        else:
            src = dst = self.xg.at[at.y, j, pl.ds(h, ch - h), self.cols(at.xr)]
        return remote(src, dst, self.sx.at[kind, j], self.rx.at[kind, j], at.left if kind % 2 else at.right)

    def xwait(self, kind, j):
        at, h, ch = self.at, self.h, self.ch
        dst = (
            lambda: self.xg.at[at.y, j, :, self.cols(at.xl)],
            lambda: self.xg.at[at.y, j, :, self.cols(at.xr)],
            lambda: self.xg.at[at.y, j, pl.ds(0, h), self.cols(at.xo)],
            lambda: self.xg.at[at.y, j, pl.ds(h, ch - h), self.cols(at.xo)],
        )[kind]()
        remote(dst, dst, self.sx.at[kind, j], self.rx.at[kind, j], at.right).wait_recv()

    def ycopy(self, kind, j):
        at, h, ch = self.at, self.h, self.ch
        if kind < 2:
            ref = self.xg.at[at.y, j]
        elif kind == 2:
            ref = self.xg.at[at.yd, j, pl.ds(0, h)]
        else:
            ref = self.xg.at[at.yu, j, pl.ds(h, ch - h)]
        return remote(ref, ref, self.sy.at[kind, j], self.ry.at[kind, j], at.down if kind % 2 else at.up)

    def ywait(self, kind, j):
        at, h, ch = self.at, self.h, self.ch
        dst = (
            lambda: self.xg.at[at.yd, j],
            lambda: self.xg.at[at.yu, j],
            lambda: self.xg.at[at.yo, j, pl.ds(0, h)],
            lambda: self.xg.at[at.yo, j, pl.ds(h, ch - h)],
        )[kind]()
        remote(dst, dst, self.sy.at[kind, j], self.ry.at[kind, j], at.up).wait_recv()

    def full(self, j):
        self.xcopy(0, j).start()
        self.xcopy(1, j).start()

    def pass_on(self, j):
        self.xwait(0, j)
        self.xwait(1, j)
        self.xcopy(2, j).start()
        self.xcopy(3, j).start()

    def finish(self, j):
        self.xwait(2, j)
        self.xwait(3, j)
        self.xcopy(2, j).wait_send()
        self.xcopy(3, j).wait_send()
        width = self.xg.shape[-1]
        rows = 8

        def body(i, carry):
            at_rows = pl.ds(al(i * rows, rows), rows)
            v = self.xg[self.at.y, j, at_rows, :].astype(F32)
            mean = jnp.sum(v, axis=-1, keepdims=True) / width
            var = jnp.sum(v * v, axis=-1, keepdims=True) / width - mean * mean
            self.xg[self.at.y, j, at_rows, :] = ((v - mean) * lax.rsqrt(var + EPS)).astype(BF16)
            return carry

        lax.fori_loop(0, self.ch // rows, body, 0)
        self.ycopy(0, j).start()
        self.ycopy(1, j).start()

    def arrive(self, n):
        _, j = chunk_of(n)

        @pl.when(n < 12)
        def _():
            @pl.when(rem(n, 2) == 0)
            def _():
                self.ywait(0, j)
                self.ycopy(2, j).start()

            @pl.when(rem(n, 2) == 1)
            def _():
                self.ywait(1, j)
                self.ycopy(3, j).start()

        @pl.when(n >= 12)
        def _():
            self.ywait(2, j)
            self.ywait(3, j)

    def drain(self):
        for j in range(NJ):
            self.xcopy(0, j).wait_send()
            self.xcopy(1, j).wait_send()
            for kind in range(4):
                self.ycopy(kind, j).wait_send()


class Reduce:
    def __init__(self, at, zb, ya, yb, yfd, yfu, ss, rs):
        self.at, self.zb, self.ya, self.yb, self.yfd, self.yfu, self.ss, self.rs = at, zb, ya, yb, yfd, yfu, ss, rs
        self.ch = zb.shape[2]
        self.h = self.ch // 2

    def copy(self, kind, j):
        at, h, ch = self.at, self.h, self.ch
        src, dst = (
            lambda: (self.zb.at[2, j, pl.ds(0, h)], self.ya.at[j]),
            lambda: (self.zb.at[2, j, pl.ds(h, ch - h)], self.yb.at[j]),
            lambda: (self.zb.at[1, j], self.yfd.at[j]),
            lambda: (self.zb.at[3, j], self.yfu.at[j]),
        )[kind]()
        return remote(src, dst, self.ss.at[kind, j], self.rs.at[kind, j], at.down if kind % 2 else at.up)

    def wait(self, kind, j):
        self.copy(kind, j).wait_recv()

    def halves(self, j):
        self.copy(0, j).start()
        self.copy(1, j).start()

    def middle(self, j):
        h = self.h
        self.wait(0, j)
        self.zb[1, j, 0:h] = (self.zb[1, j, 0:h].astype(F32) + self.ya[j].astype(F32)).astype(BF16)
        self.copy(2, j).start()
        self.wait(1, j)
        self.zb[3, j, h:] = (self.zb[3, j, h:].astype(F32) + self.yb[j].astype(F32)).astype(BF16)
        self.copy(3, j).start()

    def total(self, j):
        self.wait(2, j)
        self.wait(3, j)
        return self.zb[0, j].astype(F32) + self.yfd[j].astype(F32) + self.yfu[j].astype(F32)

    def drain(self):
        for j in range(NJ):
            for kind in range(4):
                self.copy(kind, j).wait_send()


def attention_kernel(
    x_ref, cos_ref, sin_ref, wq, wk, wv, wo, wg_t, wu_t, wdn,
    h_ref, w_all,
    xc, xg, wb, wrel, wob, qkv, kvo, kvp, og, zb, ya, yb, yfd, yfu, own, drel_r, drel_l,
    sx, rx, sy, ry, sd, rd, swd, rwd, swo, rwo, swf, rwf, swp, rwp, lw, so, ro, skv, rkv, sog, rog, syr, ryr,
    lg, sw, rw, swx, rwx, swy, rwy, swz, rwz,
):
    at = Place()
    x, c, y = at.x, at.c, at.y
    ch, kc, h = xc.shape[1], xc.shape[2], xc.shape[1] // 2
    kd = wq.shape[0]
    hc = wb.shape[1] // 3
    fc = w_all.shape[1]
    f_r = drel_r.shape[1]
    gather = Gather(at, xc, xg, kc, ch, sx, rx, sy, ry)
    reduce = Reduce(at, zb, ya, yb, yfd, yfu, syr, ryr)
    weights = (wq, wk, wv)
    my_rows = lambda xx: al((2 * xx + c) * kd, 128)
    half_cols = lambda core: pl.ds(al(core * kd, 128), kd)

    def head_cols(xx):
        return pl.ds(al(xx * hc, 128), hc)

    def w_direct(d, i):
        to, dev = (at.xl, at.left) if d else (at.xr, at.right)
        return remote(weights[i].at[:, head_cols(to)], wb.at[pl.ds(my_rows(x), kd), pl.ds(i * hc, hc)], swd.at[d, i], rwd.at[d, i], dev)

    def w_direct_wait(d, i):
        dst = wb.at[pl.ds(my_rows(at.xr if d else at.xl), kd), pl.ds(i * hc, hc)]
        remote(dst, dst, swd.at[d, i], rwd.at[d, i], at.right).wait_recv()

    def w_opp(d, i):
        rows = pl.ds(d * (kd // 2), kd // 2)
        return remote(weights[i].at[rows, head_cols(at.xo)], wrel.at[d, :, pl.ds(i * hc, hc)], swo.at[d, i], rwo.at[d, i], at.left if d else at.right)

    def w_fwd(d):
        src_x = at.xr if d else at.xl
        dst = wb.at[pl.ds(al(my_rows(src_x) + d * (kd // 2), 128), kd // 2)]
        return remote(wrel.at[d], dst, swf.at[d], rwf.at[d], at.left if d else at.right)

    def w_fwd_wait(d):
        dst = wb.at[pl.ds(al(my_rows(at.xo) + d * (kd // 2), 128), kd // 2)]
        remote(dst, dst, swf.at[d], rwf.at[d], at.right).wait_recv()

    def w_own_pair(i):
        return remote(weights[i].at[:, head_cols(x)], wb.at[pl.ds(my_rows(x), kd), pl.ds(i * hc, hc)], swp.at[i], rwp.at[i], at.partner)

    def w_pair(k):
        src = wb.at[pl.ds(my_rows((at.xl, at.xr, at.xo)[k]), kd)]
        return remote(src, src, swp.at[3 + k], rwp.at[3 + k], at.partner)

    def w_pair_wait(k):
        other = lambda xx: al((2 * xx + 1 - c) * kd, 128)
        if k < 3:
            dst = wb.at[pl.ds(other(x), kd), pl.ds(k * hc, hc)]
        else:
            dst = wb.at[pl.ds(other((at.xl, at.xr, at.xo)[k - 3]), kd)]
        remote(dst, dst, swp.at[k], rwp.at[k], at.partner).wait_recv()

    def w_own_local(i):
        return pltpu.make_async_copy(weights[i].at[:, head_cols(x)], wb.at[pl.ds(my_rows(x), kd), pl.ds(i * hc, hc)], lw.at[i])

    wo_local = pltpu.make_async_copy(wo, wob.at[:, half_cols(c)], lw.at[3])
    wo_pair = remote(wo, wob.at[:, half_cols(c)], so.at[0], ro.at[0], at.partner)

    mlp_weights = (wg_t, wu_t, wdn)
    parts = ((0, f_r), (f_r, fc - f_r))

    def d_cols(xx, core):
        return pl.ds(al((2 * xx + core) * kd, 128), kd)

    def d_direct(m, d, p):
        to, dev = (at.xl, at.left) if d else (at.xr, at.right)
        off, size = parts[p]
        src = mlp_weights[m].at[pl.ds(al(to * fc + off, 8), size)]
        return remote(src, w_all.at[m, pl.ds(off, size), d_cols(x, c)], sw.at[m, d, p], rw.at[m, d, p], dev)

    def d_direct_wait(m, d, p):
        off, size = parts[p]
        dst = w_all.at[m, pl.ds(off, size), d_cols(at.xr if d else at.xl, c)]
        remote(dst, dst, sw.at[m, d, p], rw.at[m, d, p], at.right).wait_recv()

    def d_opp(m, d):
        off, size = parts[d]
        src = mlp_weights[m].at[pl.ds(al(at.xo * fc + off, 8), size)]
        return remote(src, (drel_r, drel_l)[d].at[m], swx.at[m, d], rwx.at[m, d], at.left if d else at.right)

    def d_fwd(m, d):
        off, size = parts[d]
        src_x = at.xr if d else at.xl
        dst = w_all.at[m, pl.ds(off, size), d_cols(src_x, c)]
        return remote((drel_r, drel_l)[d].at[m], dst, swy.at[m, d], rwy.at[m, d], at.left if d else at.right)

    def d_fwd_wait(m, d):
        off, size = parts[d]
        dst = w_all.at[m, pl.ds(off, size), d_cols(at.xo, c)]
        remote(dst, dst, swy.at[m, d], rwy.at[m, d], at.right).wait_recv()

    def d_in(m):
        return pltpu.make_async_copy(mlp_weights[m].at[pl.ds(al(x * fc, 8), fc)], own.at[m], lg.at[0, m])

    def d_out(m):
        return pltpu.make_async_copy(own.at[m], w_all.at[m, :, d_cols(x, c)], lg.at[1, m])

    def d_pair(m, k):
        dst = w_all.at[m, :, d_cols((at.xl, at.xr, at.xo, x)[k], c)]
        return remote(own.at[m] if k == 3 else dst, dst, swz.at[m, k], rwz.at[m, k], at.partner)

    def d_pair_wait(m, k):
        dst = w_all.at[m, :, d_cols((at.xl, at.xr, at.xo, x)[k], 1 - c)]
        remote(dst, dst, swz.at[m, k], rwz.at[m, k], at.partner).wait_recv()

    def d_pairs(m):
        for d in range(2):
            for p in range(2):
                d_direct_wait(m, d, p)
            d_pair(m, d).start()
        for d in range(2):
            d_fwd_wait(m, d)
        d_pair(m, 2).start()

    def d_turn(m):
        for d in range(2):
            d_opp(m, d).wait_recv()
            d_fwd(m, d).start()

    for i in range(3):
        w_own_local(i).start()
    wo_local.start()
    for m in range(3):
        d_in(m).start()

    def x_rows(j, core):
        return pl.ds(al((2 * j + core) * ch, 8), ch)

    def x_pair(j):
        return remote(x_ref.at[x_rows(j, 1 - c)], xc.at[j, :, half_cols(c)], sd.at[j], rd.at[j], at.partner)

    def x_pair_wait(j):
        dst = xc.at[j, :, half_cols(1 - c)]
        remote(dst, dst, sd.at[j], rd.at[j], at.partner).wait_recv()

    for j in range(NJ):
        xc[j, :, half_cols(c)] = x_ref[x_rows(j, c), :]
    at.barrier()
    for j in range(NJ):
        x_pair(j).start()
    for i in range(3):
        w_own_pair(i).start()
    wo_pair.start()
    for j in range(2):
        x_pair_wait(j)
        gather.full(j)
        gather.keep_own(j)
    gather.pass_on(0)
    for j in range(2, NJ):
        x_pair_wait(j)
        gather.full(j)
        gather.keep_own(j)
        gather.pass_on(j - 1)
        gather.finish(j - 2)
    for d in range(2):
        for i in range(3):
            w_opp(d, i).start()
    gather.pass_on(NJ - 1)
    for d in range(2):
        for i in range(3):
            w_direct(d, i).start()
    gather.finish(NJ - 2)
    gather.finish(NJ - 1)
    for d in range(2):
        for i in range(3):
            w_opp(d, i).wait_recv()
        w_fwd(d).start()
    for m in range(3):
        d_in(m).wait()
        d_out(m).start()
        d_pair(m, 3).start()
    for i in range(3):
        w_own_local(i).wait()
    wo_local.wait()
    for d in range(2):
        for i in range(3):
            w_direct_wait(d, i)
        w_pair(d).start()
    for d in range(2):
        w_fwd_wait(d)
    w_pair(2).start()
    for k in range(6):
        w_pair_wait(k)
    wo_pair.wait_recv()

    def kv_copy(s, j, n):
        return remote(kvo.at[s, j], kvp.at[s, j], skv.at[n], rkv.at[n], at.partner)

    def og_copy(kind, n):
        cols = lambda xx: pl.ds(al(xx * hc, 128), hc)
        if kind < 2:
            ref = og.at[n, :, cols(x)]
        elif kind == 2:
            ref = og.at[n, pl.ds(0, h), cols(at.xl)]
        else:
            ref = og.at[n, pl.ds(h, ch - h), cols(at.xr)]
        return remote(ref, ref, sog.at[kind, n], rog.at[kind, n], at.left if kind % 2 else at.right)

    def og_wait(kind, n):
        cols = lambda xx: pl.ds(al(xx * hc, 128), hc)
        dst = (
            lambda: og.at[n, :, cols(at.xl)],
            lambda: og.at[n, :, cols(at.xr)],
            lambda: og.at[n, pl.ds(0, h), cols(at.xo)],
            lambda: og.at[n, pl.ds(h, ch - h), cols(at.xo)],
        )[kind]()
        remote(dst, dst, sog.at[kind, n], rog.at[kind, n], at.right).wait_recv()

    def project(n):
        r, j = chunk_of(n)
        s = rem(y + r, NX)

        def body(i, carry):
            cols = pl.ds(al(i * hc, 128), hc)
            qkv[rem(n, 2), :, cols] = jnp.dot(xg[s, j], wb[:, cols], preferred_element_type=F32).astype(BF16)
            return carry

        lax.fori_loop(0, 3, body, 0)
        rows = pl.ds(al((2 * j + c) * ch, 8), ch)
        cos_t, sin_t = cos_ref[rows, :], sin_ref[rows, :]

        def turned(col):
            v = qkv[rem(n, 2), :, col : col + HEAD_DIM].astype(F32)
            return (v * cos_t + pltpu.roll(v, HEAD_DIM // 2, axis=1) * sin_t).astype(BF16)

        for col in range(0, hc, HEAD_DIM):
            qkv[rem(n, 2), :, col : col + HEAD_DIM] = turned(col)
        for col in range(0, hc, HEAD_DIM):
            kvo[s, j, :, col : col + HEAD_DIM] = turned(hc + col)
        kvo[s, j, :, hc:] = qkv[rem(n, 2), :, 2 * hc :]
        kv_copy(s, j, n).start()

    def attend(n):
        r, j = chunk_of(n)
        s = rem(y + r, NX)
        kv_copy(s, j, n).wait_recv()

        def one(jj):
            keys = (jj + 1) * ch
            iq = lax.broadcasted_iota(jnp.int32, (ch, keys), 0) + jj * ch
            ik = lax.broadcasted_iota(jnp.int32, (ch, keys), 1)
            own_ok = iq >= ik
            par_ok = ik < (jj + c) * ch
            contract = (((1,), (1,)), ((), ()))
            for head in range(hc // HEAD_DIM):
                lo = head * HEAD_DIM
                q = qkv[rem(n, 2), :, lo : lo + HEAD_DIM]
                k_own = kvo[s, 0 : jj + 1, :, lo : lo + HEAD_DIM].reshape(keys, HEAD_DIM)
                k_par = kvp[s, 0 : jj + 1, :, lo : lo + HEAD_DIM].reshape(keys, HEAD_DIM)
                s_own = lax.dot_general(q, k_own, contract, preferred_element_type=F32) * HEAD_DIM**-0.5
                s_par = lax.dot_general(q, k_par, contract, preferred_element_type=F32) * HEAD_DIM**-0.5
                s_own = jnp.where(own_ok, s_own, -1e30)
                s_par = jnp.where(par_ok, s_par, -1e30)
                top = jnp.maximum(jnp.max(s_own, axis=1, keepdims=True), jnp.max(s_par, axis=1, keepdims=True))
                e_own, e_par = jnp.exp(s_own - top), jnp.exp(s_par - top)
                inv = 1.0 / (jnp.sum(e_own, axis=1, keepdims=True) + jnp.sum(e_par, axis=1, keepdims=True))
                v_own = kvo[s, 0 : jj + 1, :, hc + lo : hc + lo + HEAD_DIM].reshape(keys, HEAD_DIM)
                v_par = kvp[s, 0 : jj + 1, :, hc + lo : hc + lo + HEAD_DIM].reshape(keys, HEAD_DIM)
                out = jnp.dot((e_own * inv).astype(BF16), v_own, preferred_element_type=F32)
                out += jnp.dot((e_par * inv).astype(BF16), v_par, preferred_element_type=F32)
                og[n, :, pl.ds(al(x * hc + lo, 128), HEAD_DIM)] = out.astype(BF16)

        for jj in range(NJ):
            pl.when(j == jj)(functools.partial(one, jj))
        og_copy(0, n).start()
        og_copy(1, n).start()

    def pass_o(n):
        og_wait(0, n)
        og_copy(2, n).start()
        og_wait(1, n)
        og_copy(3, n).start()

    def out_project(n):
        r, j = chunk_of(n)
        og_wait(2, n)
        og_wait(3, n)

        def body(i, carry):
            cols = pl.ds(al(i * 256, 128), 256)
            zb[r, j, :, cols] = jnp.dot(og[n], wob[:, cols], preferred_element_type=F32).astype(BF16)
            return carry

        lax.fori_loop(0, kc // 256, body, 0)

        @pl.when(n >= 12)
        def _():
            reduce.halves(j)

    events = {}
    for m in range(3):
        events[4 * m] = lambda m=m: [d_direct(m, d, 0).start() for d in range(2)]
        events[4 * m + 1] = lambda m=m: [d_opp(m, d).start() for d in range(2)]
        events[4 * m + 2] = lambda m=m: [d_direct(m, d, 1).start() for d in range(2)]
        events[4 * m + 3] = functools.partial(d_turn, m)
        events[(12, 15, 19)[m]] = functools.partial(d_pairs, m)

    def tick(n, carry):
        @pl.when(n < NCH)
        def _():
            @pl.when(n >= 4)
            def _():
                gather.arrive(n)

            project(n)

        @pl.when(jnp.logical_and(n >= 1, n < NCH + 1))
        def _():
            attend(n - 1)

        @pl.when(jnp.logical_and(n >= 2, n < NCH + 2))
        def _():
            pass_o(n - 2)

        @pl.when(jnp.logical_and(n >= 3, n < NCH + 3))
        def _():
            out_project(n - 3)

        @pl.when(jnp.logical_and(n >= 16, n < NCH + 4))
        def _():
            reduce.middle(n - 16)

        @pl.when(n >= 17)
        def _():
            j = n - 17
            attn = reduce.total(j).astype(BF16)
            h_ref[j] = (xc[j].astype(F32) + attn.astype(F32)).astype(BF16)

        for when, event in events.items():

            @pl.when(n == when)
            def _(event=event):
                event()

        return carry

    lax.fori_loop(0, NCH + 5, tick, 0)

    for m in range(3):
        for k in range(4):
            d_pair_wait(m, k)
        d_out(m).wait()
    for j in range(NJ):
        x_pair(j).wait_send()
    gather.drain()
    reduce.drain()
    wo_pair.wait_send()
    for k in range(3):
        w_own_pair(k).wait_send()
        w_pair(k).wait_send()
    for d in range(2):
        for i in range(3):
            w_direct(d, i).wait_send()
            w_opp(d, i).wait_send()
        w_fwd(d).wait_send()
    for m in range(3):
        for k in range(4):
            d_pair(m, k).wait_send()
        for d in range(2):
            for p in range(2):
                d_direct(m, d, p).wait_send()
            d_opp(m, d).wait_send()
            d_fwd(m, d).wait_send()

    def drain_chunk(n, carry):
        r, j = chunk_of(n)
        kv_copy(rem(y + r, NX), j, n).wait_send()
        for kind in range(4):
            og_copy(kind, n).wait_send()
        return carry

    lax.fori_loop(0, NCH, drain_chunk, 0)


def mlp_kernel(
    h_ref, w_hbm, y_ref,
    xg, wt, act, pp, rsa, rsb, rsl, rsr, zb, ya, yb, yfd, yfu, yst,
    sx, rx, sy, ry, sr, rr, syr, ryr, sd, rd, lw,
):
    at = Place()
    x, c, y = at.x, at.c, at.y
    ch, kc, h = h_ref.shape[1], h_ref.shape[2], h_ref.shape[1] // 2
    width = xg.shape[-1]
    kd = kc // 2
    fc, fp = w_hbm.shape[1], wt.shape[1]
    gather = Gather(at, h_ref, xg, kc, ch, sx, rx, sy, ry)
    reduce = Reduce(at, zb, ya, yb, yfd, yfu, syr, ryr)

    def w_in(m):
        return pltpu.make_async_copy(w_hbm.at[m], wt.at[m, pl.ds(0, fc)], lw.at[m])

    for m in range(3):
        w_in(m).start()
    for m in range(3):
        wt[m, fc:, :] = jnp.zeros((fp - fc, width), BF16)
    at.barrier()
    for j in range(2):
        gather.full(j)
    for j in range(NJ):
        gather.keep_own(j)
    gather.pass_on(0)

    def silu_mul(g, u):
        g, u = g.astype(BF16).astype(F32), u.astype(BF16).astype(F32)
        return g / (1.0 + jnp.exp(-g)) * u

    def compute(n):
        r, j = chunk_of(n)
        s = rem(y + r, NX)
        slot = rem(n, STAGES)

        def columns(i, carry):
            rows = pl.ds(al(i * 256, 8), 256)
            g = lax.dot_general(xg[s, j], wt[0, rows, :], (((1,), (1,)), ((), ())), preferred_element_type=F32)
            u = lax.dot_general(xg[s, j], wt[1, rows, :], (((1,), (1,)), ((), ())), preferred_element_type=F32)
            act[:, pl.ds(al(i * 256, 128), 256)] = silu_mul(g, u).astype(BF16)
            return carry

        lax.fori_loop(0, fp // 256, columns, 0)
        per = kc // 256

        def down(i, carry):
            q, k = div(i, per), rem(i, per)
            out = jnp.dot(act[...], wt[2, :, pl.ds(al(i * 256, 128), 256)], preferred_element_type=F32)
            pp[slot, q, :, pl.ds(al(k * 256, 128), 256)] = out.astype(BF16)
            return carry

        lax.fori_loop(0, width // 256, down, 0)

    def rs_copy(kind, n):
        slot = rem(n, STAGES)
        src, dst = (
            lambda: (pp.at[slot, at.xo, pl.ds(0, h)], rsa.at[n]),
            lambda: (pp.at[slot, at.xo, pl.ds(h, ch - h)], rsb.at[n]),
            lambda: (pp.at[slot, at.xr], rsl.at[n]),
            lambda: (pp.at[slot, at.xl], rsr.at[n]),
        )[kind]()
        return remote(src, dst, sr.at[kind, n], rr.at[kind, n], at.left if kind % 2 else at.right)

    def rs_second(n):
        slot = rem(n, STAGES)
        rs_copy(0, n).wait_recv()
        pp[slot, at.xr, 0:h] = (pp[slot, at.xr, 0:h].astype(F32) + rsa[n].astype(F32)).astype(BF16)
        rs_copy(2, n).start()
        rs_copy(1, n).wait_recv()
        pp[slot, at.xl, h:] = (pp[slot, at.xl, h:].astype(F32) + rsb[n].astype(F32)).astype(BF16)
        rs_copy(3, n).start()

    def rs_third(n):
        r, j = chunk_of(n)
        slot = rem(n, STAGES)
        rs_copy(2, n).wait_recv()
        rs_copy(3, n).wait_recv()
        zb[r, j] = (pp[slot, x].astype(F32) + rsl[n].astype(F32) + rsr[n].astype(F32)).astype(BF16)

        @pl.when(n >= 12)
        def _():
            reduce.halves(j)

    def rs_sent(n):
        for kind in range(4):
            rs_copy(kind, n).wait_send()

    def y_rows(j, core):
        return pl.ds(al((2 * j + core) * ch, 8), ch)

    def y_copy(j):
        return remote(yst.at[1 - c, j], y_ref.at[y_rows(j, c)], sd.at[j], rd.at[j], at.partner)

    def y_wait(j):
        dst = y_ref.at[y_rows(j, 1 - c)]
        remote(dst, dst, sd.at[j], rd.at[j], at.partner).wait_recv()

    def tick(n, carry):
        @pl.when(n < 2)
        def _():
            gather.full(n + 2)

        @pl.when(n < 3)
        def _():
            gather.pass_on(n + 1)

        @pl.when(n < 4)
        def _():
            gather.finish(n)

        @pl.when(n == 0)
        def _():
            for m in range(3):
                w_in(m).wait()

        @pl.when(n < NCH)
        def _():
            @pl.when(n >= 4)
            def _():
                gather.arrive(n)

            @pl.when(n >= STAGES)
            def _():
                rs_sent(n - STAGES)

            compute(n)
            rs_copy(0, n).start()
            rs_copy(1, n).start()

        @pl.when(jnp.logical_and(n >= 1, n < NCH + 1))
        def _():
            rs_second(n - 1)

        @pl.when(jnp.logical_and(n >= 2, n < NCH + 2))
        def _():
            rs_third(n - 2)

        @pl.when(jnp.logical_and(n >= 15, n < NCH + 3))
        def _():
            reduce.middle(n - 15)

        @pl.when(n >= 16)
        def _():
            j = n - 16
            mlp = reduce.total(j).astype(BF16)
            out = (h_ref[j].astype(F32) + mlp.astype(F32)).astype(BF16)
            yst[0, j] = out[:, :kd]
            yst[1, j] = out[:, kd:]
            y_copy(j).start()
            y_ref[y_rows(j, c), :] = yst[c, j]

        return carry

    lax.fori_loop(0, NCH + 4, tick, 0)
    for n in range(NCH - STAGES, NCH):
        rs_sent(n)
    gather.drain()
    reduce.drain()
    for j in range(NJ):
        y_copy(j).wait_send()
        y_wait(j)


def vmem(*shape, dtype=BF16):
    return pltpu.VMEM(shape, dtype)


def sems(*shape):
    return pltpu.SemaphoreType.DMA(shape)


def solution(mesh):
    assert mesh.shape["tx"] == 2 * NX and mesh.shape["ty"] == NX
    act_spec = P(("dp", "ty"), None, "tx")
    col_spec = P("tx", "ty")
    row_spec = P("ty", "tx")
    any_spec = pl.BlockSpec(memory_space=pl.ANY)
    vmem_spec = pl.BlockSpec(memory_space=pltpu.VMEM)

    def layer(x_blk, w_q, w_k, w_v, w_o, w_gate, w_up, w_down):
        _, seq, kd = x_blk.shape
        kc, width = 2 * kd, 2 * NX * kd
        ch = seq // (2 * NJ)
        h = ch // 2
        row_heads = w_q.shape[1]
        hc = row_heads // NX
        fc = w_down.shape[0] // NX
        assert hc % HEAD_DIM == 0
        fp = (fc + 255) // 256 * 256
        f_r = (fc // 2 + 15) // 16 * 16

        half = HEAD_DIM // 2
        inv_freq = THETA ** (-2.0 * jnp.arange(half, dtype=F32) / HEAD_DIM)
        angles = jnp.arange(seq, dtype=F32)[:, None] * inv_freq[None, :]
        cos_t, sin_t = jnp.cos(angles), jnp.sin(angles)
        cos_t = jnp.concatenate([cos_t, cos_t], axis=1)
        sin_t = jnp.concatenate([-sin_t, sin_t], axis=1)

        reduce_scratch = [vmem(NX, NJ, ch, kc), vmem(NJ, h, kc), vmem(NJ, ch - h, kc), vmem(NJ, ch, kc), vmem(NJ, ch, kc)]
        h_blk, w_all = pl.pallas_call(
            attention_kernel,
            out_shape=(
                jax.ShapeDtypeStruct((NJ, ch, kc), BF16),
                jax.ShapeDtypeStruct((3, fc, width), BF16),
            ),
            in_specs=[vmem_spec] * 3 + [any_spec] * 7,
            out_specs=(vmem_spec, any_spec),
            scratch_shapes=[
                vmem(NJ, ch, kc), vmem(NX, NJ, ch, width), vmem(width, 3 * hc), vmem(2, kd // 2, 3 * hc), vmem(row_heads, kc),
                vmem(2, ch, 3 * hc), vmem(NX, NJ, ch, 2 * hc), vmem(NX, NJ, ch, 2 * hc), vmem(NCH, ch, row_heads),
                *reduce_scratch,
                vmem(3, fc, kd), vmem(3, f_r, kd), vmem(3, fc - f_r, kd),
                sems(4, NJ), sems(4, NJ), sems(4, NJ), sems(4, NJ), sems(NJ), sems(NJ),
                sems(2, 3), sems(2, 3), sems(2, 3), sems(2, 3), sems(2), sems(2), sems(6), sems(6), sems(4), sems(1), sems(1),
                sems(NCH), sems(NCH), sems(4, NCH), sems(4, NCH), sems(4, NJ), sems(4, NJ),
                sems(2, 3), sems(3, 2, 2), sems(3, 2, 2), sems(3, 2), sems(3, 2), sems(3, 2), sems(3, 2), sems(3, 4), sems(3, 4),
            ],
            compiler_params=pltpu.CompilerParams(collective_id=0, has_side_effects=True, vmem_limit_bytes=VMEM_LIMIT),
            name="attention_part",
        )(x_blk[0], cos_t, sin_t, w_q, w_k, w_v, w_o, w_gate.T, w_up.T, w_down)

        y_blk = pl.pallas_call(
            mlp_kernel,
            out_shape=jax.ShapeDtypeStruct((seq, kd), BF16),
            in_specs=[vmem_spec, any_spec],
            out_specs=vmem_spec,
            scratch_shapes=[
                vmem(NX, NJ, ch, width), vmem(3, fp, width), vmem(ch, fp), vmem(STAGES, NX, ch, kc),
                vmem(NCH, h, kc), vmem(NCH, ch - h, kc), vmem(NCH, ch, kc), vmem(NCH, ch, kc),
                *reduce_scratch, vmem(2, NJ, ch, kd),
                sems(4, NJ), sems(4, NJ), sems(4, NJ), sems(4, NJ), sems(4, NCH), sems(4, NCH), sems(4, NJ), sems(4, NJ),
                sems(NJ), sems(NJ), sems(3),
            ],
            compiler_params=pltpu.CompilerParams(collective_id=1, has_side_effects=True, vmem_limit_bytes=VMEM_LIMIT),
            name="mlp_part",
        )(h_blk, w_all)
        return y_blk[None]

    return jax.shard_map(
        layer,
        mesh=mesh,
        in_specs=(act_spec, col_spec, col_spec, col_spec, row_spec, col_spec, col_spec, row_spec),
        out_specs=act_spec,
        check_vma=False,
    )
```

```python
import functools

import jax
import jax.numpy as jnp
from jax import lax
from jax.experimental import pallas as pl
from jax.experimental.pallas import tpu as pltpu
from jax.sharding import PartitionSpec as P

HEAD_DIM = 128
EPS = 1e-5
THETA = 10000.0
MESH = pl.DeviceIdType.MESH
F32 = jnp.float32
BF16 = jnp.bfloat16
NX = 4
NJ = 4
NCH = 16
STAGES = 4
VMEM_LIMIT = 67_043_328


def rem(a, b):
    return lax.rem(a, jnp.int32(b))


def div(a, b):
    return lax.div(a, jnp.int32(b))


def al(v, m):
    return pl.multiple_of(v, m)


def remote(src, dst, ssem, rsem, dev):
    return pltpu.make_async_remote_copy(src_ref=src, dst_ref=dst, send_sem=ssem, recv_sem=rsem, device_id=dev, device_id_type=MESH)


def chunk_of(n):
    is_c = div(n, 12)
    is_a = div(15 - n, 12)
    is_b = 1 - is_a - is_c
    j = is_a * n + is_b * (div(n + 12, 2) - 8) + is_c * (n - 12)
    r = is_b * (3 - 2 * rem(n, 2)) + 2 * is_c
    return r, j


def mlp_chunk_of(n):
    r, j = chunk_of(n + 1)
    own = div(n, NCH - 1) + div(17 - n, 15)
    return (1 - own) * r, (1 - own) * j + div(17 - n, 15) * n + div(n, NCH - 1) * (NJ - 1)


class Place:
    def __init__(self):
        tx, ty = lax.axis_index("tx"), lax.axis_index("ty")
        self.x, self.c, self.y = div(tx, 2), rem(tx, 2), ty
        x, c, y = self.x, self.c, self.y
        self.xr, self.xl, self.xo = rem(x + 1, NX), rem(x + 3, NX), rem(x + 2, NX)
        self.yu, self.yd, self.yo = rem(y + 1, NX), rem(y + 3, NX), rem(y + 2, NX)
        self.right = {"tx": self.xr * 2 + c, "ty": y}
        self.left = {"tx": self.xl * 2 + c, "ty": y}
        self.up = {"tx": tx, "ty": self.yu}
        self.down = {"tx": tx, "ty": self.yd}
        self.partner = {"tx": x * 2 + 1 - c, "ty": y}

    def barrier(self):
        sem = pltpu.get_barrier_semaphore()
        for dev in (self.right, self.left, self.up, self.down, self.partner):
            pl.semaphore_signal(sem, inc=1, device_id=dev, device_id_type=MESH)
        pl.semaphore_wait(sem, 5)


class Gather:
    def __init__(self, at, src, xg, kc, ch, sx, rx, sy, ry, syh, ryh):
        self.at, self.src, self.xg, self.kc, self.ch, self.h = at, src, xg, kc, ch, ch // 2
        self.sx, self.rx, self.sy, self.ry, self.syh, self.ryh = sx, rx, sy, ry, syh, ryh

    def cols(self, x):
        return pl.ds(al(x * self.kc, 128), self.kc)

    def unit(self, u):
        return (0, u * self.h, self.h) if u < 2 else (u - 1, 0, self.ch)

    def keep_own(self, j):
        self.xg[self.at.y, j, :, self.cols(self.at.x)] = self.src[j]

    def xcopy(self, kind, u):
        at = self.at
        j, lo, n = self.unit(u)
        if kind < 2:
            rows = pl.ds(lo, n)
            src, dst = self.src.at[j, rows], self.xg.at[at.y, j, rows, self.cols(at.x)]
        elif kind == 2:
            src = dst = self.xg.at[at.y, j, pl.ds(lo, n // 2), self.cols(at.xl)]
        else:
            src = dst = self.xg.at[at.y, j, pl.ds(lo + n // 2, n // 2), self.cols(at.xr)]
        return remote(src, dst, self.sx.at[kind, u], self.rx.at[kind, u], at.left if kind % 2 else at.right)

    def xwait(self, kind, u):
        at = self.at
        j, lo, n = self.unit(u)
        dst = (
            lambda: self.xg.at[at.y, j, pl.ds(lo, n), self.cols(at.xl)],
            lambda: self.xg.at[at.y, j, pl.ds(lo, n), self.cols(at.xr)],
            lambda: self.xg.at[at.y, j, pl.ds(lo, n // 2), self.cols(at.xo)],
            lambda: self.xg.at[at.y, j, pl.ds(lo + n // 2, n // 2), self.cols(at.xo)],
        )[kind]()
        remote(dst, dst, self.sx.at[kind, u], self.rx.at[kind, u], at.right).wait_recv()

    def ycopy(self, d, u):
        j, lo, n = self.unit(u)
        ref = self.xg.at[self.at.y, j, pl.ds(lo, n)]
        return remote(ref, ref, self.sy.at[d, u], self.ry.at[d, u], self.at.down if d else self.at.up)

    def ywait(self, d, j):
        at, h = self.at, self.h
        s = at.yu if d else at.yd

        @pl.when(j == 0)
        def _():
            for u in range(2):
                dst = self.xg.at[s, 0, pl.ds(u * h, h)]
                remote(dst, dst, self.sy.at[d, u], self.ry.at[d, u], at.up).wait_recv()

        @pl.when(j > 0)
        def _():
            dst = self.xg.at[s, j]
            remote(dst, dst, self.sy.at[d, j + 1], self.ry.at[d, j + 1], at.up).wait_recv()

    def yhalf(self, d, j):
        at, h = self.at, self.h
        ref = self.xg.at[at.yu if d else at.yd, j, pl.ds(d * h, h)]
        return remote(ref, ref, self.syh.at[d, j], self.ryh.at[d, j], at.down if d else at.up)

    def yhalf_wait(self, d, j):
        dst = self.xg.at[self.at.yo, j, pl.ds(d * self.h, self.h)]
        remote(dst, dst, self.syh.at[d, j], self.ryh.at[d, j], self.at.up).wait_recv()

    def full(self, u):
        self.xcopy(0, u).start()
        self.xcopy(1, u).start()

    def pass_on(self, u):
        self.xwait(0, u)
        self.xcopy(2, u).start()
        self.xwait(1, u)
        self.xcopy(3, u).start()

    def finish(self, u):
        self.xwait(2, u)
        self.xwait(3, u)
        self.xcopy(2, u).wait_send()
        self.xcopy(3, u).wait_send()
        width = self.xg.shape[-1]
        j, lo, n = self.unit(u)
        rows = 8

        def body(i, carry):
            at_rows = pl.ds(al(lo + i * rows, rows), rows)
            v = self.xg[self.at.y, j, at_rows, :].astype(F32)
            mean = jnp.sum(v, axis=-1, keepdims=True) / width
            var = jnp.sum(v * v, axis=-1, keepdims=True) / width - mean * mean
            self.xg[self.at.y, j, at_rows, :] = ((v - mean) * lax.rsqrt(var + EPS)).astype(BF16)
            return carry

        lax.fori_loop(0, n // rows, body, 0)
        self.ycopy(0, u).start()
        self.ycopy(1, u).start()

    def arrive(self, r, j):
        @pl.when(r == 3)
        def _():
            self.ywait(0, j)
            self.yhalf(0, j).start()

        @pl.when(r == 1)
        def _():
            self.ywait(1, j)
            self.yhalf(1, j).start()

        @pl.when(r == 2)
        def _():
            self.yhalf_wait(0, j)
            self.yhalf_wait(1, j)

    def drain(self):
        for d in range(2):
            for u in range(NJ + 1):
                self.xcopy(d, u).wait_send()
                self.ycopy(d, u).wait_send()
            for j in range(NJ):
                self.yhalf(d, j).wait_send()


class Reduce:
    def __init__(self, at, zb, ya, yb, yfd, yfu, ss, rs):
        self.at, self.zb, self.ya, self.yb, self.yfd, self.yfu, self.ss, self.rs = at, zb, ya, yb, yfd, yfu, ss, rs
        self.ch = zb.shape[2]
        self.h = self.ch // 2

    def copy(self, kind, j):
        at, h, ch = self.at, self.h, self.ch
        src, dst = (
            lambda: (self.zb.at[2, j, pl.ds(0, h)], self.ya.at[j]),
            lambda: (self.zb.at[2, j, pl.ds(h, ch - h)], self.yb.at[j]),
            lambda: (self.zb.at[1, j], self.yfd.at[j]),
            lambda: (self.zb.at[3, j], self.yfu.at[j]),
        )[kind]()
        return remote(src, dst, self.ss.at[kind, j], self.rs.at[kind, j], at.down if kind % 2 else at.up)

    def wait(self, kind, j):
        self.copy(kind, j).wait_recv()

    def halves(self, j):
        self.copy(0, j).start()
        self.copy(1, j).start()

    def middle(self, j):
        h = self.h
        self.wait(0, j)
        self.zb[1, j, 0:h] = (self.zb[1, j, 0:h].astype(F32) + self.ya[j].astype(F32)).astype(BF16)
        self.copy(2, j).start()
        self.wait(1, j)
        self.zb[3, j, h:] = (self.zb[3, j, h:].astype(F32) + self.yb[j].astype(F32)).astype(BF16)
        self.copy(3, j).start()

    def total(self, j):
        self.wait(2, j)
        self.wait(3, j)
        return self.zb[0, j].astype(F32) + self.yfd[j].astype(F32) + self.yfu[j].astype(F32)

    def drain(self):
        for j in range(NJ):
            for kind in range(4):
                self.copy(kind, j).wait_send()


def attention_kernel(
    x_ref, cos_ref, sin_ref, wq, wk, wv, wo, wg_t, wu_t, wdn,
    h_ref, w_all,
    xc, xg, wb, wrel, wob, qkv, kvo, kvp, og, zb, ya, yb, yfd, yfu, own, drel_r, drel_l,
    sx, rx, sy, ry, syh, ryh, sd, rd, swd, rwd, swo, rwo, swf, rwf, swp, rwp, lw, so, ro, skv, rkv, sog, rog, syr, ryr,
    lg, sw, rw, swx, rwx, swy, rwy, swz, rwz,
):
    at = Place()
    x, c, y = at.x, at.c, at.y
    ch, kc, h = xc.shape[1], xc.shape[2], xc.shape[1] // 2
    kd = wq.shape[0]
    hc = wb.shape[1] // 3
    fc = w_all.shape[1]
    f_r = drel_r.shape[1]
    gather = Gather(at, xc, xg, kc, ch, sx, rx, sy, ry, syh, ryh)
    reduce = Reduce(at, zb, ya, yb, yfd, yfu, syr, ryr)
    weights = (wq, wk, wv)
    my_rows = lambda xx: al((2 * xx + c) * kd, 128)
    half_cols = lambda core: pl.ds(al(core * kd, 128), kd)

    def head_cols(xx):
        return pl.ds(al(xx * hc, 128), hc)

    def w_direct(d, i):
        to, dev = (at.xl, at.left) if d else (at.xr, at.right)
        return remote(weights[i].at[:, head_cols(to)], wb.at[pl.ds(my_rows(x), kd), pl.ds(i * hc, hc)], swd.at[d, i], rwd.at[d, i], dev)

    def w_direct_wait(d, i):
        dst = wb.at[pl.ds(my_rows(at.xr if d else at.xl), kd), pl.ds(i * hc, hc)]
        remote(dst, dst, swd.at[d, i], rwd.at[d, i], at.right).wait_recv()

    def w_opp(d, i):
        rows = pl.ds(d * (kd // 2), kd // 2)
        return remote(weights[i].at[rows, head_cols(at.xo)], wrel.at[d, :, pl.ds(i * hc, hc)], swo.at[d, i], rwo.at[d, i], at.left if d else at.right)

    def w_fwd(d):
        src_x = at.xr if d else at.xl
        dst = wb.at[pl.ds(al(my_rows(src_x) + d * (kd // 2), 128), kd // 2)]
        return remote(wrel.at[d], dst, swf.at[d], rwf.at[d], at.left if d else at.right)

    def w_fwd_wait(d):
        dst = wb.at[pl.ds(al(my_rows(at.xo) + d * (kd // 2), 128), kd // 2)]
        remote(dst, dst, swf.at[d], rwf.at[d], at.right).wait_recv()

    def w_own_pair(i):
        return remote(weights[i].at[:, head_cols(x)], wb.at[pl.ds(my_rows(x), kd), pl.ds(i * hc, hc)], swp.at[i], rwp.at[i], at.partner)

    def w_pair(k):
        src = wb.at[pl.ds(my_rows((at.xl, at.xr, at.xo)[k]), kd)]
        return remote(src, src, swp.at[3 + k], rwp.at[3 + k], at.partner)

    def w_pair_wait(k):
        other = lambda xx: al((2 * xx + 1 - c) * kd, 128)
        if k < 3:
            dst = wb.at[pl.ds(other(x), kd), pl.ds(k * hc, hc)]
        else:
            dst = wb.at[pl.ds(other((at.xl, at.xr, at.xo)[k - 3]), kd)]
        remote(dst, dst, swp.at[k], rwp.at[k], at.partner).wait_recv()

    def w_own_local(i):
        return pltpu.make_async_copy(weights[i].at[:, head_cols(x)], wb.at[pl.ds(my_rows(x), kd), pl.ds(i * hc, hc)], lw.at[i])

    wo_local = pltpu.make_async_copy(wo, wob.at[:, half_cols(c)], lw.at[3])
    wo_pair = remote(wo, wob.at[:, half_cols(c)], so.at[0], ro.at[0], at.partner)

    mlp_weights = (wg_t, wu_t, wdn)
    parts = ((0, f_r), (f_r, fc - f_r))

    def d_cols(xx, core):
        return pl.ds(al((2 * xx + core) * kd, 128), kd)

    def d_direct(m, d, p):
        to, dev = (at.xl, at.left) if d else (at.xr, at.right)
        off, size = parts[p]
        src = mlp_weights[m].at[pl.ds(al(to * fc + off, 8), size)]
        return remote(src, w_all.at[m, pl.ds(off, size), d_cols(x, c)], sw.at[m, d, p], rw.at[m, d, p], dev)

    def d_direct_wait(m, d, p):
        off, size = parts[p]
        dst = w_all.at[m, pl.ds(off, size), d_cols(at.xr if d else at.xl, c)]
        remote(dst, dst, sw.at[m, d, p], rw.at[m, d, p], at.right).wait_recv()

    def d_opp(m, d):
        off, size = parts[d]
        src = mlp_weights[m].at[pl.ds(al(at.xo * fc + off, 8), size)]
        return remote(src, (drel_r, drel_l)[d].at[m], swx.at[m, d], rwx.at[m, d], at.left if d else at.right)

    def d_fwd(m, d):
        off, size = parts[d]
        src_x = at.xr if d else at.xl
        dst = w_all.at[m, pl.ds(off, size), d_cols(src_x, c)]
        return remote((drel_r, drel_l)[d].at[m], dst, swy.at[m, d], rwy.at[m, d], at.left if d else at.right)

    def d_fwd_wait(m, d):
        off, size = parts[d]
        dst = w_all.at[m, pl.ds(off, size), d_cols(at.xo, c)]
        remote(dst, dst, swy.at[m, d], rwy.at[m, d], at.right).wait_recv()

    def d_in(m):
        return pltpu.make_async_copy(mlp_weights[m].at[pl.ds(al(x * fc, 8), fc)], own.at[m], lg.at[0, m])

    def d_out(m):
        return pltpu.make_async_copy(own.at[m], w_all.at[m, :, d_cols(x, c)], lg.at[1, m])

    def d_pair(m, k):
        dst = w_all.at[m, :, d_cols((at.xl, at.xr, at.xo, x)[k], c)]
        return remote(own.at[m] if k == 3 else dst, dst, swz.at[m, k], rwz.at[m, k], at.partner)

    def d_pair_wait(m, k):
        dst = w_all.at[m, :, d_cols((at.xl, at.xr, at.xo, x)[k], 1 - c)]
        remote(dst, dst, swz.at[m, k], rwz.at[m, k], at.partner).wait_recv()

    def d_pairs(m):
        for d in range(2):
            for p in range(2):
                d_direct_wait(m, d, p)
            d_pair(m, d).start()
        for d in range(2):
            d_fwd_wait(m, d)
        d_pair(m, 2).start()

    def d_turn(m):
        for d in range(2):
            d_opp(m, d).wait_recv()
            d_fwd(m, d).start()

    events = {}
    starts = (-1, 0, 3, 5, 7, 9, 11, 13, 15, 17, 17, 18)
    for m in range(3):
        steps = (
            lambda m=m: [d_direct(m, d, 0).start() for d in range(2)],
            lambda m=m: [d_opp(m, d).start() for d in range(2)],
            lambda m=m: [d_direct(m, d, 1).start() for d in range(2)],
            functools.partial(d_turn, m),
        )
        for k, step in enumerate(steps):
            events.setdefault(starts[4 * m + k], []).append(step)
        events.setdefault((14, 17, 20)[m], []).append(functools.partial(d_pairs, m))

    for i in range(3):
        w_own_local(i).start()
    wo_local.start()
    for m in range(3):
        d_in(m).start()

    def x_rows(j, core):
        return pl.ds(al((2 * j + core) * ch, 8), ch)

    def x_pair(j):
        return remote(x_ref.at[x_rows(j, 1 - c)], xc.at[j, :, half_cols(c)], sd.at[j], rd.at[j], at.partner)

    def x_pair_wait(j):
        dst = xc.at[j, :, half_cols(1 - c)]
        remote(dst, dst, sd.at[j], rd.at[j], at.partner).wait_recv()

    for j in range(NJ):
        xc[j, :, half_cols(c)] = x_ref[x_rows(j, c), :]
    at.barrier()
    for j in range(NJ):
        x_pair(j).start()
    for i in range(3):
        w_own_pair(i).start()
    wo_pair.start()

    def full(u):
        j = max(u - 1, 0)
        if u != 1:
            x_pair_wait(j)
        gather.full(u)

    full(0)
    full(1)
    gather.keep_own(0)
    gather.pass_on(0)
    full(2)
    gather.pass_on(1)
    gather.keep_own(1)
    gather.finish(0)
    gather.finish(1)
    full(3)
    gather.pass_on(2)
    gather.keep_own(2)
    gather.finish(2)
    full(4)
    gather.pass_on(3)
    gather.keep_own(3)
    for d in range(2):
        for i in range(3):
            w_opp(d, i).start()
    gather.finish(3)
    gather.pass_on(4)
    for d in range(2):
        for i in range(3):
            w_direct(d, i).start()
    gather.finish(4)
    for d in range(2):
        for i in range(3):
            w_opp(d, i).wait_recv()
        w_fwd(d).start()
    for event in events.pop(-1):
        event()
    for m in range(3):
        d_in(m).wait()
        d_out(m).start()
        d_pair(m, 3).start()
    for i in range(3):
        w_own_local(i).wait()
    wo_local.wait()
    for d in range(2):
        for i in range(3):
            w_direct_wait(d, i)
        w_pair(d).start()
    for d in range(2):
        w_fwd_wait(d)
    w_pair(2).start()
    for k in range(6):
        w_pair_wait(k)
    wo_pair.wait_recv()

    def kv_copy(s, j, n):
        return remote(kvo.at[s, j], kvp.at[s, j], skv.at[n], rkv.at[n], at.partner)

    def og_copy(kind, n):
        cols = lambda xx: pl.ds(al(xx * hc, 128), hc)
        if kind < 2:
            ref = og.at[n, :, cols(x)]
        elif kind == 2:
            ref = og.at[n, pl.ds(0, h), cols(at.xl)]
        else:
            ref = og.at[n, pl.ds(h, ch - h), cols(at.xr)]
        return remote(ref, ref, sog.at[kind, n], rog.at[kind, n], at.left if kind % 2 else at.right)

    def og_wait(kind, n):
        cols = lambda xx: pl.ds(al(xx * hc, 128), hc)
        dst = (
            lambda: og.at[n, :, cols(at.xl)],
            lambda: og.at[n, :, cols(at.xr)],
            lambda: og.at[n, pl.ds(0, h), cols(at.xo)],
            lambda: og.at[n, pl.ds(h, ch - h), cols(at.xo)],
        )[kind]()
        remote(dst, dst, sog.at[kind, n], rog.at[kind, n], at.right).wait_recv()

    def project(n):
        r, j = chunk_of(n)
        s = rem(y + r, NX)

        def body(i, carry):
            cols = pl.ds(al(i * hc, 128), hc)
            qkv[rem(n, 2), :, cols] = jnp.dot(xg[s, j], wb[:, cols], preferred_element_type=F32).astype(BF16)
            return carry

        lax.fori_loop(0, 3, body, 0)
        rows = pl.ds(al((2 * j + c) * ch, 8), ch)
        cos_t, sin_t = cos_ref[rows, :], sin_ref[rows, :]

        def turned(col):
            v = qkv[rem(n, 2), :, col : col + HEAD_DIM].astype(F32)
            return (v * cos_t + pltpu.roll(v, HEAD_DIM // 2, axis=1) * sin_t).astype(BF16)

        for col in range(0, hc, HEAD_DIM):
            qkv[rem(n, 2), :, col : col + HEAD_DIM] = turned(col)
        for col in range(0, hc, HEAD_DIM):
            kvo[s, j, :, col : col + HEAD_DIM] = turned(hc + col)
        kvo[s, j, :, hc:] = qkv[rem(n, 2), :, 2 * hc :]
        kv_copy(s, j, n).start()

    def attend(n):
        r, j = chunk_of(n)
        s = rem(y + r, NX)
        kv_copy(s, j, n).wait_recv()

        def one(jj):
            keys = (jj + 1) * ch
            iq = lax.broadcasted_iota(jnp.int32, (ch, keys), 0) + jj * ch
            ik = lax.broadcasted_iota(jnp.int32, (ch, keys), 1)
            own_ok = iq >= ik
            par_ok = ik < (jj + c) * ch
            contract = (((1,), (1,)), ((), ()))
            for head in range(hc // HEAD_DIM):
                lo = head * HEAD_DIM
                q = qkv[rem(n, 2), :, lo : lo + HEAD_DIM]
                k_own = kvo[s, 0 : jj + 1, :, lo : lo + HEAD_DIM].reshape(keys, HEAD_DIM)
                k_par = kvp[s, 0 : jj + 1, :, lo : lo + HEAD_DIM].reshape(keys, HEAD_DIM)
                s_own = lax.dot_general(q, k_own, contract, preferred_element_type=F32) * HEAD_DIM**-0.5
                s_par = lax.dot_general(q, k_par, contract, preferred_element_type=F32) * HEAD_DIM**-0.5
                s_own = jnp.where(own_ok, s_own, -1e30)
                s_par = jnp.where(par_ok, s_par, -1e30)
                top = jnp.maximum(jnp.max(s_own, axis=1, keepdims=True), jnp.max(s_par, axis=1, keepdims=True))
                e_own, e_par = jnp.exp(s_own - top), jnp.exp(s_par - top)
                inv = 1.0 / (jnp.sum(e_own, axis=1, keepdims=True) + jnp.sum(e_par, axis=1, keepdims=True))
                v_own = kvo[s, 0 : jj + 1, :, hc + lo : hc + lo + HEAD_DIM].reshape(keys, HEAD_DIM)
                v_par = kvp[s, 0 : jj + 1, :, hc + lo : hc + lo + HEAD_DIM].reshape(keys, HEAD_DIM)
                out = jnp.dot((e_own * inv).astype(BF16), v_own, preferred_element_type=F32)
                out += jnp.dot((e_par * inv).astype(BF16), v_par, preferred_element_type=F32)
                og[n, :, pl.ds(al(x * hc + lo, 128), HEAD_DIM)] = out.astype(BF16)

        for jj in range(NJ):
            pl.when(j == jj)(functools.partial(one, jj))
        og_copy(0, n).start()
        og_copy(1, n).start()

    def pass_o(n):
        og_wait(0, n)
        og_copy(2, n).start()
        og_wait(1, n)
        og_copy(3, n).start()

    def out_project(n):
        r, j = chunk_of(n)
        og_wait(2, n)
        og_wait(3, n)

        def body(i, carry):
            cols = pl.ds(al(i * 256, 128), 256)
            zb[r, j, :, cols] = jnp.dot(og[n], wob[:, cols], preferred_element_type=F32).astype(BF16)
            return carry

        lax.fori_loop(0, kc // 256, body, 0)

        @pl.when(n >= 12)
        def _():
            reduce.halves(j)

    def tick(n, carry):
        @pl.when(n < NCH)
        def _():
            @pl.when(n >= 4)
            def _():
                gather.arrive(*chunk_of(n))

            project(n)

        @pl.when(jnp.logical_and(n >= 2, n < NCH + 2))
        def _():
            pass_o(n - 2)

        @pl.when(jnp.logical_and(n >= 4, n < NCH + 4))
        def _():
            out_project(n - 4)

        @pl.when(n < NCH)
        def _():
            attend(n)

        @pl.when(jnp.logical_and(n >= 17, n < NCH + 5))
        def _():
            reduce.middle(n - 17)

        @pl.when(n >= 18)
        def _():
            j = n - 18
            attn = reduce.total(j).astype(BF16)
            h_ref[j] = (xc[j].astype(F32) + attn.astype(F32)).astype(BF16)

        for when, steps in events.items():

            @pl.when(n == when)
            def _(steps=steps):
                for step in steps:
                    step()

        return carry

    lax.fori_loop(0, NCH + 6, tick, 0)

    for m in range(3):
        for k in range(4):
            d_pair_wait(m, k)
        d_out(m).wait()
    for j in range(NJ):
        x_pair(j).wait_send()
    gather.drain()
    reduce.drain()
    wo_pair.wait_send()
    for k in range(3):
        w_own_pair(k).wait_send()
        w_pair(k).wait_send()
    for d in range(2):
        for i in range(3):
            w_direct(d, i).wait_send()
            w_opp(d, i).wait_send()
        w_fwd(d).wait_send()
    for m in range(3):
        for k in range(4):
            d_pair(m, k).wait_send()
        for d in range(2):
            for p in range(2):
                d_direct(m, d, p).wait_send()
            d_opp(m, d).wait_send()
            d_fwd(m, d).wait_send()

    def drain_chunk(n, carry):
        r, j = chunk_of(n)
        kv_copy(rem(y + r, NX), j, n).wait_send()
        for kind in range(4):
            og_copy(kind, n).wait_send()
        return carry

    lax.fori_loop(0, NCH, drain_chunk, 0)


def mlp_kernel(
    h_ref, w_hbm, y_ref,
    xg, wt, act, pp, rsa, rsb, rsl, rsr, zb, ya, yb, yfd, yfu, yst,
    sx, rx, sy, ry, syh, ryh, sr, rr, syr, ryr, sd, rd, lw,
):
    at = Place()
    x, c, y = at.x, at.c, at.y
    ch, kc, h = h_ref.shape[1], h_ref.shape[2], h_ref.shape[1] // 2
    width = xg.shape[-1]
    kd = kc // 2
    fc, fp = w_hbm.shape[1], wt.shape[1]
    gather = Gather(at, h_ref, xg, kc, ch, sx, rx, sy, ry, syh, ryh)
    reduce = Reduce(at, zb, ya, yb, yfd, yfu, syr, ryr)

    def w_in(m):
        return pltpu.make_async_copy(w_hbm.at[m], wt.at[m, pl.ds(0, fc)], lw.at[m])

    for m in range(3):
        w_in(m).start()
    for m in range(3):
        wt[m, fc:, :] = jnp.zeros((fp - fc, width), BF16)
    at.barrier()
    gather.full(0)
    gather.full(1)
    for j in range(NJ):
        gather.keep_own(j)
    gather.pass_on(0)
    gather.full(2)
    gather.pass_on(1)
    gather.finish(0)
    gather.finish(1)
    gather.full(3)
    gather.pass_on(2)

    def silu_mul(g, u):
        g, u = g.astype(BF16).astype(F32), u.astype(BF16).astype(F32)
        return g / (1.0 + jnp.exp(-g)) * u

    def compute(n):
        r, j = mlp_chunk_of(n)
        s = rem(y + r, NX)
        slot = rem(n, STAGES)

        def columns(i, carry):
            rows = pl.ds(al(i * 256, 8), 256)
            g = lax.dot_general(xg[s, j], wt[0, rows, :], (((1,), (1,)), ((), ())), preferred_element_type=F32)
            u = lax.dot_general(xg[s, j], wt[1, rows, :], (((1,), (1,)), ((), ())), preferred_element_type=F32)
            act[:, pl.ds(al(i * 256, 128), 256)] = silu_mul(g, u).astype(BF16)
            return carry

        lax.fori_loop(0, fp // 256, columns, 0)
        per = kc // 256

        def down(i, carry):
            q, k = div(i, per), rem(i, per)
            out = jnp.dot(act[...], wt[2, :, pl.ds(al(i * 256, 128), 256)], preferred_element_type=F32)
            pp[slot, q, :, pl.ds(al(k * 256, 128), 256)] = out.astype(BF16)
            return carry

        lax.fori_loop(0, width // 256, down, 0)

    def rs_copy(kind, n):
        slot = rem(n, STAGES)
        src, dst = (
            lambda: (pp.at[slot, at.xo, pl.ds(0, h)], rsa.at[n]),
            lambda: (pp.at[slot, at.xo, pl.ds(h, ch - h)], rsb.at[n]),
            lambda: (pp.at[slot, at.xr], rsl.at[n]),
            lambda: (pp.at[slot, at.xl], rsr.at[n]),
        )[kind]()
        return remote(src, dst, sr.at[kind, n], rr.at[kind, n], at.left if kind % 2 else at.right)

    def rs_second(n):
        slot = rem(n, STAGES)
        rs_copy(0, n).wait_recv()
        pp[slot, at.xr, 0:h] = (pp[slot, at.xr, 0:h].astype(F32) + rsa[n].astype(F32)).astype(BF16)
        rs_copy(2, n).start()
        rs_copy(1, n).wait_recv()
        pp[slot, at.xl, h:] = (pp[slot, at.xl, h:].astype(F32) + rsb[n].astype(F32)).astype(BF16)
        rs_copy(3, n).start()

    def rs_third(n):
        r, j = mlp_chunk_of(n)
        slot = rem(n, STAGES)
        rs_copy(2, n).wait_recv()
        rs_copy(3, n).wait_recv()
        zb[r, j] = (pp[slot, x].astype(F32) + rsl[n].astype(F32) + rsr[n].astype(F32)).astype(BF16)

        @pl.when(r == 2)
        def _():
            reduce.halves(j)

    def rs_sent(n):
        for kind in range(4):
            rs_copy(kind, n).wait_send()

    def y_rows(j, core):
        return pl.ds(al((2 * j + core) * ch, 8), ch)

    def y_copy(j):
        return remote(yst.at[1 - c, j], y_ref.at[y_rows(j, c)], sd.at[j], rd.at[j], at.partner)

    def y_wait(j):
        dst = y_ref.at[y_rows(j, 1 - c)]
        remote(dst, dst, sd.at[j], rd.at[j], at.partner).wait_recv()

    def tick(n, carry):
        @pl.when(n == 0)
        def _():
            for m in range(3):
                w_in(m).wait()

        @pl.when(n == 1)
        def _():
            gather.finish(2)
            gather.full(4)
            gather.pass_on(3)

        @pl.when(n == 2)
        def _():
            gather.finish(3)
            gather.pass_on(4)

        @pl.when(n == 3)
        def _():
            gather.finish(4)

        @pl.when(n < NCH)
        def _():
            @pl.when(jnp.logical_and(n >= 3, n < NCH - 1))
            def _():
                gather.arrive(*mlp_chunk_of(n))

            @pl.when(n >= STAGES)
            def _():
                rs_sent(n - STAGES)

            compute(n)
            rs_copy(0, n).start()
            rs_copy(1, n).start()

        @pl.when(jnp.logical_and(n >= 1, n < NCH + 1))
        def _():
            rs_second(n - 1)

        @pl.when(jnp.logical_and(n >= 2, n < NCH + 2))
        def _():
            rs_third(n - 2)

        @pl.when(jnp.logical_and(n >= 14, n < NCH + 2))
        def _():
            reduce.middle(n - 14)

        @pl.when(n >= 15)
        def _():
            j = n - 15
            mlp = reduce.total(j).astype(BF16)
            out = (h_ref[j].astype(F32) + mlp.astype(F32)).astype(BF16)
            yst[0, j] = out[:, :kd]
            yst[1, j] = out[:, kd:]
            y_copy(j).start()
            y_ref[y_rows(j, c), :] = yst[c, j]

        return carry

    lax.fori_loop(0, NCH + 3, tick, 0)
    for n in range(NCH - STAGES, NCH):
        rs_sent(n)
    gather.drain()
    reduce.drain()
    for j in range(NJ):
        y_copy(j).wait_send()
        y_wait(j)


def vmem(*shape, dtype=BF16):
    return pltpu.VMEM(shape, dtype)


def sems(*shape):
    return pltpu.SemaphoreType.DMA(shape)


def solution(mesh):
    assert mesh.shape["tx"] == 2 * NX and mesh.shape["ty"] == NX
    act_spec = P(("dp", "ty"), None, "tx")
    col_spec = P("tx", "ty")
    row_spec = P("ty", "tx")
    any_spec = pl.BlockSpec(memory_space=pl.ANY)
    vmem_spec = pl.BlockSpec(memory_space=pltpu.VMEM)

    def layer(x_blk, w_q, w_k, w_v, w_o, w_gate, w_up, w_down):
        _, seq, kd = x_blk.shape
        kc, width = 2 * kd, 2 * NX * kd
        ch = seq // (2 * NJ)
        h = ch // 2
        row_heads = w_q.shape[1]
        hc = row_heads // NX
        fc = w_down.shape[0] // NX
        assert hc % HEAD_DIM == 0
        fp = (fc + 255) // 256 * 256
        f_r = (fc // 2 + 15) // 16 * 16

        half = HEAD_DIM // 2
        inv_freq = THETA ** (-2.0 * jnp.arange(half, dtype=F32) / HEAD_DIM)
        angles = jnp.arange(seq, dtype=F32)[:, None] * inv_freq[None, :]
        cos_t, sin_t = jnp.cos(angles), jnp.sin(angles)
        cos_t = jnp.concatenate([cos_t, cos_t], axis=1)
        sin_t = jnp.concatenate([-sin_t, sin_t], axis=1)

        units = NJ + 1
        gather_sems = [sems(4, units), sems(4, units), sems(2, units), sems(2, units), sems(2, NJ), sems(2, NJ)]
        reduce_scratch = [vmem(NX, NJ, ch, kc), vmem(NJ, h, kc), vmem(NJ, ch - h, kc), vmem(NJ, ch, kc), vmem(NJ, ch, kc)]
        h_blk, w_all = pl.pallas_call(
            attention_kernel,
            out_shape=(
                jax.ShapeDtypeStruct((NJ, ch, kc), BF16),
                jax.ShapeDtypeStruct((3, fc, width), BF16),
            ),
            in_specs=[vmem_spec] * 3 + [any_spec] * 7,
            out_specs=(vmem_spec, any_spec),
            scratch_shapes=[
                vmem(NJ, ch, kc), vmem(NX, NJ, ch, width), vmem(width, 3 * hc), vmem(2, kd // 2, 3 * hc), vmem(row_heads, kc),
                vmem(2, ch, 3 * hc), vmem(NX, NJ, ch, 2 * hc), vmem(NX, NJ, ch, 2 * hc), vmem(NCH, ch, row_heads),
                *reduce_scratch,
                vmem(3, fc, kd), vmem(3, f_r, kd), vmem(3, fc - f_r, kd),
                *gather_sems, sems(NJ), sems(NJ),
                sems(2, 3), sems(2, 3), sems(2, 3), sems(2, 3), sems(2), sems(2), sems(6), sems(6), sems(4), sems(1), sems(1),
                sems(NCH), sems(NCH), sems(4, NCH), sems(4, NCH), sems(4, NJ), sems(4, NJ),
                sems(2, 3), sems(3, 2, 2), sems(3, 2, 2), sems(3, 2), sems(3, 2), sems(3, 2), sems(3, 2), sems(3, 4), sems(3, 4),
            ],
            compiler_params=pltpu.CompilerParams(collective_id=0, has_side_effects=True, vmem_limit_bytes=VMEM_LIMIT),
            name="attention_part",
        )(x_blk[0], cos_t, sin_t, w_q, w_k, w_v, w_o, w_gate.T, w_up.T, w_down)

        y_blk = pl.pallas_call(
            mlp_kernel,
            out_shape=jax.ShapeDtypeStruct((seq, kd), BF16),
            in_specs=[vmem_spec, any_spec],
            out_specs=vmem_spec,
            scratch_shapes=[
                vmem(NX, NJ, ch, width), vmem(3, fp, width), vmem(ch, fp), vmem(STAGES, NX, ch, kc),
                vmem(NCH, h, kc), vmem(NCH, ch - h, kc), vmem(NCH, ch, kc), vmem(NCH, ch, kc),
                *reduce_scratch, vmem(2, NJ, ch, kd),
                *gather_sems, sems(4, NCH), sems(4, NCH), sems(4, NJ), sems(4, NJ),
                sems(NJ), sems(NJ), sems(3),
            ],
            compiler_params=pltpu.CompilerParams(collective_id=1, has_side_effects=True, vmem_limit_bytes=VMEM_LIMIT),
            name="mlp_part",
        )(h_blk, w_all)
        return y_blk[None]

    return jax.shard_map(
        layer,
        mesh=mesh,
        in_specs=(act_spec, col_spec, col_spec, col_spec, row_spec, col_spec, col_spec, row_spec),
        out_specs=act_spec,
        check_vma=False,
    )
```

```python
import functools

import jax
import jax.numpy as jnp
from jax import lax
from jax.experimental import pallas as pl
from jax.experimental.pallas import tpu as pltpu
from jax.sharding import PartitionSpec as P

HEAD_DIM = 128
EPS = 1e-5
THETA = 10000.0
MESH = pl.DeviceIdType.MESH
F32 = jnp.float32
BF16 = jnp.bfloat16
NX = 4
NJ = 4
NCH = 16
VMEM_LIMIT = 67_043_328


def rem(a, b):
    return lax.rem(a, jnp.int32(b))


def div(a, b):
    return lax.div(a, jnp.int32(b))


def al(v, m):
    return pl.multiple_of(v, m)


def remote(src, dst, ssem, rsem, dev):
    return pltpu.make_async_remote_copy(src_ref=src, dst_ref=dst, send_sem=ssem, recv_sem=rsem, device_id=dev, device_id_type=MESH)


def chunk_of(n):
    is_c = div(n, 12)
    is_a = div(15 - n, 12)
    is_b = 1 - is_a - is_c
    j = is_a * n + is_b * (div(n + 12, 2) - 8) + is_c * (n - 12)
    r = is_b * (3 - 2 * rem(n, 2)) + 2 * is_c
    return r, j


MLP_STEPS = (
    ("XF", 0, 1), ("XF", 0, 2), ("YR", 0), ("XF", 0, 0), ("XH", 0, 1), ("YRH", 0), ("XF", 0, 3), ("XH", 0, 2), ("XH", 0, 0),
    ("N", 0, 1), ("XF", 2, 0), ("XH", 0, 3), ("N", 0, 2), ("G", 0, 1), ("N", 0, 0), ("G", 0, 0), ("N", 0, 3), ("G", 0, 2),
    ("YH", 1), ("XH", 2, 0), ("P", 0, 1), ("P", 0, 0), ("XF", 1, 0), ("P", 0, 2), ("N", 2, 0), ("X", 0, 1), ("XF", 3, 0),
    ("X", 0, 0), ("XF", 0, 4), ("YH", 2), ("G", 3, 1), ("G", 1, 1), ("XH", 3, 0), ("XH", 1, 0), ("X", 0, 2), ("XH", 0, 4),
    ("P", 3, 1), ("P", 1, 1), ("N", 3, 0), ("G", 3, 0), ("N", 1, 0), ("G", 1, 0), ("N", 0, 4), ("G", 0, 3), ("G", 2, 0),
    ("P", 3, 0), ("YH", 3), ("G", 1, 2), ("G", 3, 2), ("G", 2, 1), ("P", 1, 0), ("P", 0, 3), ("X", 1, 1), ("X", 3, 1),
    ("P", 2, 0), ("X", 3, 0), ("P", 1, 2), ("P", 3, 2), ("P", 2, 1), ("YH", 4), ("G", 1, 3), ("G", 3, 3), ("X", 1, 0),
    ("X", 2, 0), ("X", 0, 3), ("X", 3, 2), ("G", 2, 2), ("X", 2, 1), ("P", 1, 3), ("X", 1, 2), ("P", 3, 3), ("G", 2, 3),
    ("M", 0), ("P", 2, 2), ("X", 1, 3), ("M", 1), ("X", 3, 3), ("P", 2, 3), ("T", 0), ("X", 2, 2), ("X", 2, 3), ("T", 1),
    ("M", 2), ("M", 3), ("T", 2), ("T", 3),
)


class Place:
    def __init__(self):
        tx, ty = lax.axis_index("tx"), lax.axis_index("ty")
        self.x, self.c, self.y = div(tx, 2), rem(tx, 2), ty
        x, c, y = self.x, self.c, self.y
        self.xr, self.xl, self.xo = rem(x + 1, NX), rem(x + 3, NX), rem(x + 2, NX)
        self.yu, self.yd, self.yo = rem(y + 1, NX), rem(y + 3, NX), rem(y + 2, NX)
        self.right = {"tx": self.xr * 2 + c, "ty": y}
        self.left = {"tx": self.xl * 2 + c, "ty": y}
        self.up = {"tx": tx, "ty": self.yu}
        self.down = {"tx": tx, "ty": self.yd}
        self.partner = {"tx": x * 2 + 1 - c, "ty": y}

    def barrier(self):
        sem = pltpu.get_barrier_semaphore()
        for dev in (self.right, self.left, self.up, self.down, self.partner):
            pl.semaphore_signal(sem, inc=1, device_id=dev, device_id_type=MESH)
        pl.semaphore_wait(sem, 5)


class Gather:
    def __init__(self, at, src, xg, kc, ch, sx, rx, sy, ry, syh, ryh):
        self.at, self.src, self.xg, self.kc, self.ch, self.h = at, src, xg, kc, ch, ch // 2
        self.sx, self.rx, self.sy, self.ry, self.syh, self.ryh = sx, rx, sy, ry, syh, ryh

    def cols(self, x):
        return pl.ds(al(x * self.kc, 128), self.kc)

    def unit(self, u):
        return (0, u * self.h, self.h) if u < 2 else (u - 1, 0, self.ch)

    def keep_own(self, j):
        self.xg[self.at.y, j, :, self.cols(self.at.x)] = self.src[j]

    def xcopy(self, kind, u):
        at = self.at
        j, lo, n = self.unit(u)
        if kind < 2:
            rows = pl.ds(lo, n)
            src, dst = self.src.at[j, rows], self.xg.at[at.y, j, rows, self.cols(at.x)]
        elif kind == 2:
            src = dst = self.xg.at[at.y, j, pl.ds(lo, n // 2), self.cols(at.xl)]
        else:
            src = dst = self.xg.at[at.y, j, pl.ds(lo + n // 2, n // 2), self.cols(at.xr)]
        return remote(src, dst, self.sx.at[kind, u], self.rx.at[kind, u], at.left if kind % 2 else at.right)

    def xwait(self, kind, u):
        at = self.at
        j, lo, n = self.unit(u)
        dst = (
            lambda: self.xg.at[at.y, j, pl.ds(lo, n), self.cols(at.xl)],
            lambda: self.xg.at[at.y, j, pl.ds(lo, n), self.cols(at.xr)],
            lambda: self.xg.at[at.y, j, pl.ds(lo, n // 2), self.cols(at.xo)],
            lambda: self.xg.at[at.y, j, pl.ds(lo + n // 2, n // 2), self.cols(at.xo)],
        )[kind]()
        remote(dst, dst, self.sx.at[kind, u], self.rx.at[kind, u], at.right).wait_recv()

    def ycopy(self, d, u):
        j, lo, n = self.unit(u)
        ref = self.xg.at[self.at.y, j, pl.ds(lo, n)]
        return remote(ref, ref, self.sy.at[d, u], self.ry.at[d, u], self.at.down if d else self.at.up)

    def ywait(self, d, j):
        at, h = self.at, self.h
        s = at.yu if d else at.yd

        @pl.when(j == 0)
        def _():
            for u in range(2):
                dst = self.xg.at[s, 0, pl.ds(u * h, h)]
                remote(dst, dst, self.sy.at[d, u], self.ry.at[d, u], at.up).wait_recv()

        @pl.when(j > 0)
        def _():
            dst = self.xg.at[s, j]
            remote(dst, dst, self.sy.at[d, j + 1], self.ry.at[d, j + 1], at.up).wait_recv()

    def yhalf(self, d, j):
        at, h = self.at, self.h
        ref = self.xg.at[at.yu if d else at.yd, j, pl.ds(d * h, h)]
        return remote(ref, ref, self.syh.at[d, j], self.ryh.at[d, j], at.down if d else at.up)

    def yhalf_wait(self, d, j):
        dst = self.xg.at[self.at.yo, j, pl.ds(d * self.h, self.h)]
        remote(dst, dst, self.syh.at[d, j], self.ryh.at[d, j], self.at.up).wait_recv()

    def full(self, u):
        self.xcopy(0, u).start()
        self.xcopy(1, u).start()

    def pass_on(self, u):
        self.xwait(0, u)
        self.xcopy(2, u).start()
        self.xwait(1, u)
        self.xcopy(3, u).start()

    def finish(self, u):
        self.xwait(2, u)
        self.xwait(3, u)
        self.xcopy(2, u).wait_send()
        self.xcopy(3, u).wait_send()
        width = self.xg.shape[-1]
        j, lo, n = self.unit(u)
        rows = 8

        def body(i, carry):
            at_rows = pl.ds(al(lo + i * rows, rows), rows)
            v = self.xg[self.at.y, j, at_rows, :].astype(F32)
            mean = jnp.sum(v, axis=-1, keepdims=True) / width
            var = jnp.sum(v * v, axis=-1, keepdims=True) / width - mean * mean
            self.xg[self.at.y, j, at_rows, :] = ((v - mean) * lax.rsqrt(var + EPS)).astype(BF16)
            return carry

        lax.fori_loop(0, n // rows, body, 0)
        self.ycopy(0, u).start()
        self.ycopy(1, u).start()

    def arrive(self, r, j):
        @pl.when(r == 3)
        def _():
            self.ywait(0, j)
            self.yhalf(0, j).start()

        @pl.when(r == 1)
        def _():
            self.ywait(1, j)
            self.yhalf(1, j).start()

        @pl.when(r == 2)
        def _():
            self.yhalf_wait(0, j)
            self.yhalf_wait(1, j)

    def drain(self):
        for d in range(2):
            for u in range(NJ + 1):
                self.xcopy(d, u).wait_send()
                self.ycopy(d, u).wait_send()
            for j in range(NJ):
                self.yhalf(d, j).wait_send()


class Spread:
    def __init__(self, at, src, xg, units, sx, rx, sy, ry, syh, ryh):
        self.at, self.src, self.xg, self.units, self.kc = at, src, xg, units, src.shape[2]
        self.sx, self.rx, self.sy, self.ry, self.syh, self.ryh = sx, rx, sy, ry, syh, ryh
        pairs = [(r, u) for u, unit in enumerate(units) for r in ((0, 3, 1, 2) if unit[3] else (0,))]
        self.index = {pair: i for i, pair in enumerate(pairs)}
        self.seqs = (at.y, at.yu, at.yo, at.yd)

    def cols(self, x):
        return pl.ds(al(x * self.kc, 128), self.kc)

    def keep_own(self):
        for j in range(NJ):
            self.xg[self.at.y, j, :, self.cols(self.at.x)] = self.src[j]

    def xcopy(self, kind, r, u):
        at, s = self.at, self.seqs[r]
        j, lo, n, _ = self.units[u]
        i = self.index[r, u]
        if kind < 2:
            dst = self.xg.at[s, j, pl.ds(lo, n), self.cols(at.x)]
            src = self.src.at[j, pl.ds(lo, n)] if r == 0 else dst
        elif kind == 2:
            src = dst = self.xg.at[s, j, pl.ds(lo, n // 2), self.cols(at.xl)]
        else:
            src = dst = self.xg.at[s, j, pl.ds(lo + n // 2, n // 2), self.cols(at.xr)]
        return remote(src, dst, self.sx.at[kind, i], self.rx.at[kind, i], at.left if kind % 2 else at.right)

    def xwait(self, kind, r, u):
        at = self.at
        j, lo, n, _ = self.units[u]
        i = self.index[r, u]
        x = (at.xl, at.xr, at.xo, at.xo)[kind]
        rows = (pl.ds(lo, n), pl.ds(lo, n), pl.ds(lo, n // 2), pl.ds(lo + n // 2, n // 2))[kind]
        dst = self.xg.at[self.seqs[r], j, rows, self.cols(x)]
        remote(dst, dst, self.sx.at[kind, i], self.rx.at[kind, i], at.right).wait_recv()

    def yref(self, s, u, lo, n):
        j, _, _, first = self.units[u]
        rows = pl.ds(lo, n)
        return self.xg.at[s, j, rows, self.cols(self.at.x)] if first else self.xg.at[s, j, rows]

    def ycopy(self, d, u):
        j, lo, n, first = self.units[u]
        dst = self.yref(self.at.y, u, lo, n)
        src = self.src.at[j, pl.ds(lo, n)] if first else dst
        return remote(src, dst, self.sy.at[d, u], self.ry.at[d, u], self.at.down if d else self.at.up)

    def ywait(self, d, u):
        _, lo, n, _ = self.units[u]
        dst = self.yref(self.at.yu if d else self.at.yd, u, lo, n)
        remote(dst, dst, self.sy.at[d, u], self.ry.at[d, u], self.at.up).wait_recv()

    def yhalf(self, d, u):
        _, lo, n, _ = self.units[u]
        ref = self.yref(self.at.yu if d else self.at.yd, u, lo + d * (n // 2), n // 2)
        return remote(ref, ref, self.syh.at[d, u], self.ryh.at[d, u], self.at.down if d else self.at.up)

    def yhalf_wait(self, d, u):
        _, lo, n, _ = self.units[u]
        dst = self.yref(self.at.yo, u, lo + d * (n // 2), n // 2)
        remote(dst, dst, self.syh.at[d, u], self.ryh.at[d, u], self.at.up).wait_recv()

    def YR(self, u):
        for d in range(2):
            self.ycopy(d, u).start()

    def YH(self, u):
        for d in range(2):
            self.ywait(d, u)
            self.yhalf(d, u).start()

    YRH = YH

    def XF(self, r, u):
        if r == 2:
            for d in range(2):
                self.yhalf_wait(d, u)
        for kind in range(2):
            self.xcopy(kind, r, u).start()

    def XH(self, r, u):
        for kind in range(2):
            self.xwait(kind, r, u)
            self.xcopy(kind + 2, r, u).start()

    def N(self, r, u):
        j, lo, n, first = self.units[u]
        for kind in (2, 3):
            self.xwait(kind, r, u)
            self.xcopy(kind, r, u).wait_send()
        if r:
            for kind in range(2):
                self.xcopy(kind, r, u).wait_send()
        if r % 2:
            self.yhalf(0 if r == 3 else 1, u).wait_send()
        width, rows, s = self.xg.shape[-1], 8, self.seqs[r]

        def body(i, carry):
            at_rows = pl.ds(al(lo + i * rows, rows), rows)
            v = self.xg[s, j, at_rows, :].astype(F32)
            mean = jnp.sum(v, axis=-1, keepdims=True) / width
            var = jnp.sum(v * v, axis=-1, keepdims=True) / width - mean * mean
            self.xg[s, j, at_rows, :] = ((v - mean) * lax.rsqrt(var + EPS)).astype(BF16)
            return carry

        lax.fori_loop(0, n // rows, body, 0)
        if not first:
            self.YR(u)

    def chunk_wait(self, r, j):
        if r == 2:
            for u, unit in enumerate(self.units):
                if unit[0] == j and not unit[3]:
                    for d in range(2):
                        self.yhalf_wait(d, u)

    def drain(self):
        for u, unit in enumerate(self.units):
            for d in range(2):
                self.xcopy(d, 0, u).wait_send()
                self.ycopy(d, u).wait_send()
                if not unit[3]:
                    self.yhalf(d, u).wait_send()


class Reduce:
    def __init__(self, at, zb, ya, yb, yfd, yfu, ss, rs):
        self.at, self.zb, self.ya, self.yb, self.yfd, self.yfu, self.ss, self.rs = at, zb, ya, yb, yfd, yfu, ss, rs
        self.ch = zb.shape[2]
        self.h = self.ch // 2

    def copy(self, kind, j):
        at, h, ch = self.at, self.h, self.ch
        src, dst = (
            lambda: (self.zb.at[2, j, pl.ds(0, h)], self.ya.at[j]),
            lambda: (self.zb.at[2, j, pl.ds(h, ch - h)], self.yb.at[j]),
            lambda: (self.zb.at[1, j], self.yfd.at[j]),
            lambda: (self.zb.at[3, j], self.yfu.at[j]),
        )[kind]()
        return remote(src, dst, self.ss.at[kind, j], self.rs.at[kind, j], at.down if kind % 2 else at.up)

    def wait(self, kind, j):
        self.copy(kind, j).wait_recv()

    def halves(self, j):
        self.copy(0, j).start()
        self.copy(1, j).start()

    def middle(self, j):
        h = self.h
        self.wait(0, j)
        self.zb[1, j, 0:h] = (self.zb[1, j, 0:h].astype(F32) + self.ya[j].astype(F32)).astype(BF16)
        self.copy(2, j).start()
        self.wait(1, j)
        self.zb[3, j, h:] = (self.zb[3, j, h:].astype(F32) + self.yb[j].astype(F32)).astype(BF16)
        self.copy(3, j).start()

    def total(self, j):
        self.wait(2, j)
        self.wait(3, j)
        return self.zb[0, j].astype(F32) + self.yfd[j].astype(F32) + self.yfu[j].astype(F32)

    def drain(self):
        for j in range(NJ):
            for kind in range(4):
                self.copy(kind, j).wait_send()


def attention_kernel(
    x_ref, cos_ref, sin_ref, wq, wk, wv, wo, wg_t, wu_t,
    h_ref, w_all,
    xc, xg, wb, wrel, wob, qkv, kvo, kvp, og, zb, ya, yb, yfd, yfu, own, drel_r, drel_l,
    sx, rx, sy, ry, syh, ryh, sd, rd, swd, rwd, swo, rwo, swf, rwf, swp, rwp, lw, so, ro, skv, rkv, sog, rog, syr, ryr,
    lg, sw, rw, swx, rwx, swy, rwy, swz, rwz,
):
    at = Place()
    x, c, y = at.x, at.c, at.y
    ch, kc, h = xc.shape[1], xc.shape[2], xc.shape[1] // 2
    kd = wq.shape[0]
    hc = wb.shape[1] // 3
    fc = w_all.shape[1]
    f_r = drel_r.shape[1]
    gather = Gather(at, xc, xg, kc, ch, sx, rx, sy, ry, syh, ryh)
    reduce = Reduce(at, zb, ya, yb, yfd, yfu, syr, ryr)
    weights = (wq, wk, wv)
    my_rows = lambda xx: al((2 * xx + c) * kd, 128)
    half_cols = lambda core: pl.ds(al(core * kd, 128), kd)

    def head_cols(xx):
        return pl.ds(al(xx * hc, 128), hc)

    def w_direct(d, i):
        to, dev = (at.xl, at.left) if d else (at.xr, at.right)
        return remote(weights[i].at[:, head_cols(to)], wb.at[pl.ds(my_rows(x), kd), pl.ds(i * hc, hc)], swd.at[d, i], rwd.at[d, i], dev)

    def w_direct_wait(d, i):
        dst = wb.at[pl.ds(my_rows(at.xr if d else at.xl), kd), pl.ds(i * hc, hc)]
        remote(dst, dst, swd.at[d, i], rwd.at[d, i], at.right).wait_recv()

    def w_opp(d, i):
        rows = pl.ds(d * (kd // 2), kd // 2)
        return remote(weights[i].at[rows, head_cols(at.xo)], wrel.at[d, :, pl.ds(i * hc, hc)], swo.at[d, i], rwo.at[d, i], at.left if d else at.right)

    def w_fwd(d):
        src_x = at.xr if d else at.xl
        dst = wb.at[pl.ds(al(my_rows(src_x) + d * (kd // 2), 128), kd // 2)]
        return remote(wrel.at[d], dst, swf.at[d], rwf.at[d], at.left if d else at.right)

    def w_fwd_wait(d):
        dst = wb.at[pl.ds(al(my_rows(at.xo) + d * (kd // 2), 128), kd // 2)]
        remote(dst, dst, swf.at[d], rwf.at[d], at.right).wait_recv()

    def w_own_pair(i):
        return remote(weights[i].at[:, head_cols(x)], wb.at[pl.ds(my_rows(x), kd), pl.ds(i * hc, hc)], swp.at[i], rwp.at[i], at.partner)

    def w_pair(k):
        src = wb.at[pl.ds(my_rows((at.xl, at.xr, at.xo)[k]), kd)]
        return remote(src, src, swp.at[3 + k], rwp.at[3 + k], at.partner)

    def w_pair_wait(k):
        other = lambda xx: al((2 * xx + 1 - c) * kd, 128)
        if k < 3:
            dst = wb.at[pl.ds(other(x), kd), pl.ds(k * hc, hc)]
        else:
            dst = wb.at[pl.ds(other((at.xl, at.xr, at.xo)[k - 3]), kd)]
        remote(dst, dst, swp.at[k], rwp.at[k], at.partner).wait_recv()

    def w_own_local(i):
        return pltpu.make_async_copy(weights[i].at[:, head_cols(x)], wb.at[pl.ds(my_rows(x), kd), pl.ds(i * hc, hc)], lw.at[i])

    wo_local = pltpu.make_async_copy(wo, wob.at[:, half_cols(c)], lw.at[3])
    wo_pair = remote(wo, wob.at[:, half_cols(c)], so.at[0], ro.at[0], at.partner)

    mlp_weights = (wg_t, wu_t)
    parts = ((0, f_r), (f_r, fc - f_r))

    def d_cols(xx, core):
        return pl.ds(al((2 * xx + core) * kd, 128), kd)

    def d_direct(m, d, p):
        to, dev = (at.xl, at.left) if d else (at.xr, at.right)
        off, size = parts[p]
        src = mlp_weights[m].at[pl.ds(al(to * fc + off, 8), size)]
        return remote(src, w_all.at[m, pl.ds(off, size), d_cols(x, c)], sw.at[m, d, p], rw.at[m, d, p], dev)

    def d_direct_wait(m, d, p):
        off, size = parts[p]
        dst = w_all.at[m, pl.ds(off, size), d_cols(at.xr if d else at.xl, c)]
        remote(dst, dst, sw.at[m, d, p], rw.at[m, d, p], at.right).wait_recv()

    def d_opp(m, d):
        off, size = parts[d]
        src = mlp_weights[m].at[pl.ds(al(at.xo * fc + off, 8), size)]
        return remote(src, (drel_r, drel_l)[d].at[m], swx.at[m, d], rwx.at[m, d], at.left if d else at.right)

    def d_fwd(m, d):
        off, size = parts[d]
        src_x = at.xr if d else at.xl
        dst = w_all.at[m, pl.ds(off, size), d_cols(src_x, c)]
        return remote((drel_r, drel_l)[d].at[m], dst, swy.at[m, d], rwy.at[m, d], at.left if d else at.right)

    def d_fwd_wait(m, d):
        off, size = parts[d]
        dst = w_all.at[m, pl.ds(off, size), d_cols(at.xo, c)]
        remote(dst, dst, swy.at[m, d], rwy.at[m, d], at.right).wait_recv()

    def d_in(m):
        return pltpu.make_async_copy(mlp_weights[m].at[pl.ds(al(x * fc, 8), fc)], own.at[m], lg.at[0, m])

    def d_out(m):
        return pltpu.make_async_copy(own.at[m], w_all.at[m, :, d_cols(x, c)], lg.at[1, m])

    def d_pair(m, k):
        dst = w_all.at[m, :, d_cols((at.xl, at.xr, at.xo, x)[k], c)]
        return remote(own.at[m] if k == 3 else dst, dst, swz.at[m, k], rwz.at[m, k], at.partner)

    def d_pair_wait(m, k):
        dst = w_all.at[m, :, d_cols((at.xl, at.xr, at.xo, x)[k], 1 - c)]
        remote(dst, dst, swz.at[m, k], rwz.at[m, k], at.partner).wait_recv()

    def d_pairs(m):
        for d in range(2):
            for p in range(2):
                d_direct_wait(m, d, p)
            d_pair(m, d).start()
        for d in range(2):
            d_fwd_wait(m, d)
        d_pair(m, 2).start()

    def d_turn(m):
        for d in range(2):
            d_opp(m, d).wait_recv()
            d_fwd(m, d).start()

    events = {}
    starts = (-1, 0, 3, 6, 8, 10, 13, 15)
    for m in range(2):
        steps = (
            lambda m=m: [d_direct(m, d, 0).start() for d in range(2)],
            lambda m=m: [d_opp(m, d).start() for d in range(2)],
            lambda m=m: [d_direct(m, d, 1).start() for d in range(2)],
            functools.partial(d_turn, m),
        )
        for k, step in enumerate(steps):
            events.setdefault(starts[4 * m + k], []).append(step)
        events.setdefault((15, 19)[m], []).append(functools.partial(d_pairs, m))

    for i in range(3):
        w_own_local(i).start()
    wo_local.start()
    for m in range(2):
        d_in(m).start()

    def x_rows(j, core):
        return pl.ds(al((2 * j + core) * ch, 8), ch)

    def x_pair(j):
        return remote(x_ref.at[x_rows(j, 1 - c)], xc.at[j, :, half_cols(c)], sd.at[j], rd.at[j], at.partner)

    def x_pair_wait(j):
        dst = xc.at[j, :, half_cols(1 - c)]
        remote(dst, dst, sd.at[j], rd.at[j], at.partner).wait_recv()

    for j in range(NJ):
        xc[j, :, half_cols(c)] = x_ref[x_rows(j, c), :]
    at.barrier()
    for j in range(NJ):
        x_pair(j).start()
    for i in range(3):
        w_own_pair(i).start()
    wo_pair.start()

    def full(u):
        j = max(u - 1, 0)
        if u != 1:
            x_pair_wait(j)
        gather.full(u)

    full(0)
    full(1)
    gather.keep_own(0)
    gather.pass_on(0)
    full(2)
    gather.pass_on(1)
    gather.keep_own(1)
    gather.finish(0)
    gather.finish(1)
    full(3)
    gather.pass_on(2)
    gather.keep_own(2)
    gather.finish(2)
    full(4)
    gather.pass_on(3)
    gather.keep_own(3)
    for d in range(2):
        for i in range(3):
            w_opp(d, i).start()
    gather.finish(3)
    gather.pass_on(4)
    for d in range(2):
        for i in range(3):
            w_direct(d, i).start()
    gather.finish(4)
    for d in range(2):
        for i in range(3):
            w_opp(d, i).wait_recv()
        w_fwd(d).start()
    for event in events.pop(-1):
        event()
    for m in range(2):
        d_in(m).wait()
        d_out(m).start()
        d_pair(m, 3).start()
    for i in range(3):
        w_own_local(i).wait()
    wo_local.wait()
    for d in range(2):
        for i in range(3):
            w_direct_wait(d, i)
        w_pair(d).start()
    for d in range(2):
        w_fwd_wait(d)
    w_pair(2).start()
    for k in range(6):
        w_pair_wait(k)
    wo_pair.wait_recv()

    def kv_copy(s, j, n):
        return remote(kvo.at[s, j], kvp.at[s, j], skv.at[n], rkv.at[n], at.partner)

    def og_copy(kind, n):
        cols = lambda xx: pl.ds(al(xx * hc, 128), hc)
        if kind < 2:
            ref = og.at[n, :, cols(x)]
        elif kind == 2:
            ref = og.at[n, pl.ds(0, h), cols(at.xl)]
        else:
            ref = og.at[n, pl.ds(h, ch - h), cols(at.xr)]
        return remote(ref, ref, sog.at[kind, n], rog.at[kind, n], at.left if kind % 2 else at.right)

    def og_wait(kind, n):
        cols = lambda xx: pl.ds(al(xx * hc, 128), hc)
        dst = (
            lambda: og.at[n, :, cols(at.xl)],
            lambda: og.at[n, :, cols(at.xr)],
            lambda: og.at[n, pl.ds(0, h), cols(at.xo)],
            lambda: og.at[n, pl.ds(h, ch - h), cols(at.xo)],
        )[kind]()
        remote(dst, dst, sog.at[kind, n], rog.at[kind, n], at.right).wait_recv()

    def project(n):
        r, j = chunk_of(n)
        s = rem(y + r, NX)

        def body(i, carry):
            cols = pl.ds(al(i * hc, 128), hc)
            qkv[rem(n, 2), :, cols] = jnp.dot(xg[s, j], wb[:, cols], preferred_element_type=F32).astype(BF16)
            return carry

        lax.fori_loop(0, 3, body, 0)
        rows = pl.ds(al((2 * j + c) * ch, 8), ch)
        cos_t, sin_t = cos_ref[rows, :], sin_ref[rows, :]

        def turned(col):
            v = qkv[rem(n, 2), :, col : col + HEAD_DIM].astype(F32)
            return (v * cos_t + pltpu.roll(v, HEAD_DIM // 2, axis=1) * sin_t).astype(BF16)

        for col in range(0, hc, HEAD_DIM):
            qkv[rem(n, 2), :, col : col + HEAD_DIM] = turned(col)
        for col in range(0, hc, HEAD_DIM):
            kvo[s, j, :, col : col + HEAD_DIM] = turned(hc + col)
        kvo[s, j, :, hc:] = qkv[rem(n, 2), :, 2 * hc :]
        kv_copy(s, j, n).start()

    def attend(n):
        r, j = chunk_of(n)
        s = rem(y + r, NX)
        kv_copy(s, j, n).wait_recv()

        def one(jj):
            keys = (jj + 1) * ch
            iq = lax.broadcasted_iota(jnp.int32, (ch, keys), 0) + jj * ch
            ik = lax.broadcasted_iota(jnp.int32, (ch, keys), 1)
            own_ok = iq >= ik
            par_ok = ik < (jj + c) * ch
            contract = (((1,), (1,)), ((), ()))
            for head in range(hc // HEAD_DIM):
                lo = head * HEAD_DIM
                q = qkv[rem(n, 2), :, lo : lo + HEAD_DIM]
                k_own = kvo[s, 0 : jj + 1, :, lo : lo + HEAD_DIM].reshape(keys, HEAD_DIM)
                k_par = kvp[s, 0 : jj + 1, :, lo : lo + HEAD_DIM].reshape(keys, HEAD_DIM)
                s_own = lax.dot_general(q, k_own, contract, preferred_element_type=F32) * HEAD_DIM**-0.5
                s_par = lax.dot_general(q, k_par, contract, preferred_element_type=F32) * HEAD_DIM**-0.5
                s_own = jnp.where(own_ok, s_own, -1e30)
                s_par = jnp.where(par_ok, s_par, -1e30)
                top = jnp.maximum(jnp.max(s_own, axis=1, keepdims=True), jnp.max(s_par, axis=1, keepdims=True))
                e_own, e_par = jnp.exp(s_own - top), jnp.exp(s_par - top)
                inv = 1.0 / (jnp.sum(e_own, axis=1, keepdims=True) + jnp.sum(e_par, axis=1, keepdims=True))
                v_own = kvo[s, 0 : jj + 1, :, hc + lo : hc + lo + HEAD_DIM].reshape(keys, HEAD_DIM)
                v_par = kvp[s, 0 : jj + 1, :, hc + lo : hc + lo + HEAD_DIM].reshape(keys, HEAD_DIM)
                out = jnp.dot((e_own * inv).astype(BF16), v_own, preferred_element_type=F32)
                out += jnp.dot((e_par * inv).astype(BF16), v_par, preferred_element_type=F32)
                og[n, :, pl.ds(al(x * hc + lo, 128), HEAD_DIM)] = out.astype(BF16)

        for jj in range(NJ):
            pl.when(j == jj)(functools.partial(one, jj))
        og_copy(0, n).start()
        og_copy(1, n).start()

    def pass_o(n):
        og_wait(0, n)
        og_copy(2, n).start()
        og_wait(1, n)
        og_copy(3, n).start()

    def out_project(n):
        r, j = chunk_of(n)
        og_wait(2, n)
        og_wait(3, n)

        def body(i, carry):
            cols = pl.ds(al(i * 256, 128), 256)
            zb[r, j, :, cols] = jnp.dot(og[n], wob[:, cols], preferred_element_type=F32).astype(BF16)
            return carry

        lax.fori_loop(0, kc // 256, body, 0)

        @pl.when(n >= 12)
        def _():
            reduce.halves(j)

    def tick(n, carry):
        @pl.when(n < NCH)
        def _():
            @pl.when(n >= 4)
            def _():
                gather.arrive(*chunk_of(n))

            project(n)

        @pl.when(jnp.logical_and(n >= 2, n < NCH + 2))
        def _():
            pass_o(n - 2)

        @pl.when(jnp.logical_and(n >= 4, n < NCH + 4))
        def _():
            out_project(n - 4)

        @pl.when(n < NCH)
        def _():
            attend(n)

        @pl.when(jnp.logical_and(n >= 17, n < NCH + 5))
        def _():
            reduce.middle(n - 17)

        @pl.when(n >= 18)
        def _():
            j = n - 18
            attn = reduce.total(j).astype(BF16)
            h_ref[j] = (xc[j].astype(F32) + attn.astype(F32)).astype(BF16)

        for when, steps in events.items():

            @pl.when(n == when)
            def _(steps=steps):
                for step in steps:
                    step()

        return carry

    lax.fori_loop(0, NCH + 6, tick, 0)

    for m in range(2):
        for k in range(4):
            d_pair_wait(m, k)
        d_out(m).wait()
    for j in range(NJ):
        x_pair(j).wait_send()
    gather.drain()
    reduce.drain()
    wo_pair.wait_send()
    for k in range(3):
        w_own_pair(k).wait_send()
        w_pair(k).wait_send()
    for d in range(2):
        for i in range(3):
            w_direct(d, i).wait_send()
            w_opp(d, i).wait_send()
        w_fwd(d).wait_send()
    for m in range(2):
        for k in range(4):
            d_pair(m, k).wait_send()
        for d in range(2):
            for p in range(2):
                d_direct(m, d, p).wait_send()
            d_opp(m, d).wait_send()
            d_fwd(m, d).wait_send()

    def drain_chunk(n, carry):
        r, j = chunk_of(n)
        kv_copy(rem(y + r, NX), j, n).wait_send()
        for kind in range(4):
            og_copy(kind, n).wait_send()
        return carry

    lax.fori_loop(0, NCH, drain_chunk, 0)


def mlp_kernel(
    units, h_ref, w_hbm, wdn, y_ref,
    xg, wt, wd, ag, zb, ya, yb, yfd, yfu, yst,
    sx, rx, sy, ry, syh, ryh, sa, ra, syr, ryr, sd, rd, lw, lwd, swd, rwd,
):
    at = Place()
    x, c, y = at.x, at.c, at.y
    ch, kc, h = h_ref.shape[1], h_ref.shape[2], h_ref.shape[1] // 2
    width = xg.shape[-1]
    kd = kc // 2
    fc, tiles = w_hbm.shape[1], wt.shape[0]
    fp = tiles * 128
    gather = Spread(at, h_ref, xg, units, sx, rx, sy, ry, syh, ryh)
    reduce = Reduce(at, zb, ya, yb, yfd, yfu, syr, ryr)

    def w_in(m, i):
        n = min(128, fc - i * 128)
        return pltpu.make_async_copy(w_hbm.at[m, pl.ds(i * 128, n)], wt.at[i, pl.ds(m * 128, n)], lw.at[m, i])

    def d_own(q):
        return pltpu.make_async_copy(wdn.at[pl.ds(q * fc, fc)], wd.at[pl.ds(q * fp, fc), pl.ds(al(c * kd, 128), kd)], lwd.at[q])

    def d_pair(q):
        dst = wd.at[pl.ds(q * fp, fc), pl.ds(al(c * kd, 128), kd)]
        return remote(wdn.at[pl.ds(q * fc, fc)], dst, swd.at[q], rwd.at[q], at.partner)

    def d_pair_wait(q):
        dst = wd.at[pl.ds(q * fp, fc), pl.ds(al((1 - c) * kd, 128), kd)]
        remote(dst, dst, swd.at[q], rwd.at[q], at.partner).wait_recv()

    for m in range(2):
        for i in range(tiles):
            w_in(m, i).start()
    for q in range(NX):
        d_own(q).start()
    rest = fc - (tiles - 1) * 128
    if rest < 128:
        for m in range(2):
            wt[tiles - 1, m * 128 + rest : (m + 1) * 128, :] = jnp.zeros((128 - rest, width), BF16)
        for q in range(NX):
            wd[q * fp + fc : (q + 1) * fp, :] = jnp.zeros((fp - fc, kc), BF16)
    at.barrier()
    for q in range(NX):
        d_pair(q).start()

    def a_cols(xx):
        return pl.ds(al(xx * fp, 128), fp)

    def a_copy(kind, n):
        if kind < 2:
            ref = ag.at[n, :, a_cols(x)]
        elif kind == 2:
            ref = ag.at[n, pl.ds(0, h), a_cols(at.xl)]
        else:
            ref = ag.at[n, pl.ds(h, ch - h), a_cols(at.xr)]
        return remote(ref, ref, sa.at[kind, n], ra.at[kind, n], at.left if kind % 2 else at.right)

    def a_wait(kind, n):
        xx = (at.xl, at.xr, at.xo, at.xo)[kind]
        rows = (pl.ds(0, ch), pl.ds(0, ch), pl.ds(0, h), pl.ds(h, ch - h))[kind]
        dst = ag.at[n, rows, a_cols(xx)]
        remote(dst, dst, sa.at[kind, n], ra.at[kind, n], at.right).wait_recv()

    def G(r, j):
        gather.chunk_wait(r, j)
        s, n = gather.seqs[r], r * NJ + j

        def columns(i, carry):
            out = lax.dot_general(xg[s, j], wt[i], (((1,), (1,)), ((), ())), preferred_element_type=F32)
            g, u = out[:, :128].astype(BF16).astype(F32), out[:, 128:].astype(BF16).astype(F32)
            ag[n, :, pl.ds(al(x * fp + i * 128, 128), 128)] = (g / (1.0 + jnp.exp(-g)) * u).astype(BF16)
            return carry

        lax.fori_loop(0, tiles, columns, 0)
        for kind in range(2):
            a_copy(kind, n).start()

    def P(r, j):
        n = r * NJ + j
        for kind in range(2):
            a_wait(kind, n)
            a_copy(kind + 2, n).start()

    def X(r, j):
        n = r * NJ + j
        for kind in (2, 3):
            a_wait(kind, n)

        def columns(i, carry):
            cols = pl.ds(al(i * 256, 128), 256)
            zb[r, j, :, cols] = jnp.dot(ag[n], wd[:, cols], preferred_element_type=F32).astype(BF16)
            return carry

        lax.fori_loop(0, kc // 256, columns, 0)
        if r == 2:
            reduce.halves(j)

    def y_rows(j, core):
        return pl.ds(al((2 * j + core) * ch, 8), ch)

    def y_copy(j):
        return remote(yst.at[1 - c, j], y_ref.at[y_rows(j, c)], sd.at[j], rd.at[j], at.partner)

    def y_wait(j):
        dst = y_ref.at[y_rows(j, 1 - c)]
        remote(dst, dst, sd.at[j], rd.at[j], at.partner).wait_recv()

    def T(j):
        mlp = reduce.total(j).astype(BF16)
        out = (h_ref[j].astype(F32) + mlp.astype(F32)).astype(BF16)
        yst[0, j] = out[:, :kd]
        yst[1, j] = out[:, kd:]
        y_copy(j).start()
        y_ref[y_rows(j, c), :] = yst[c, j]

    ops = {"G": G, "P": P, "X": X, "M": reduce.middle, "T": T}
    for name in ("YR", "YRH", "YH", "XF", "XH", "N"):
        ops[name] = getattr(gather, name)
    waits = {
        "N": gather.keep_own,
        "G": lambda: [w_in(m, i).wait() for m in range(2) for i in range(tiles)],
        "X": lambda: [(d_own(q).wait(), d_pair_wait(q)) for q in range(NX)],
    }
    for step in MLP_STEPS:
        if step[0] in waits:
            waits.pop(step[0])()
        ops[step[0]](*step[1:])

    gather.drain()
    reduce.drain()
    for q in range(NX):
        d_pair(q).wait_send()
    for n in range(NCH):
        for kind in range(4):
            a_copy(kind, n).wait_send()
    for j in range(NJ):
        y_copy(j).wait_send()
        y_wait(j)


def vmem(*shape, dtype=BF16):
    return pltpu.VMEM(shape, dtype)


def sems(*shape):
    return pltpu.SemaphoreType.DMA(shape)


def solution(mesh):
    assert mesh.shape["tx"] == 2 * NX and mesh.shape["ty"] == NX
    act_spec = P(("dp", "ty"), None, "tx")
    col_spec = P("tx", "ty")
    row_spec = P("ty", "tx")
    any_spec = pl.BlockSpec(memory_space=pl.ANY)
    vmem_spec = pl.BlockSpec(memory_space=pltpu.VMEM)

    def layer(x_blk, w_q, w_k, w_v, w_o, w_gate, w_up, w_down):
        _, seq, kd = x_blk.shape
        kc, width = 2 * kd, 2 * NX * kd
        ch = seq // (2 * NJ)
        h = ch // 2
        row_heads = w_q.shape[1]
        hc = row_heads // NX
        fc = w_down.shape[0] // NX
        assert hc % HEAD_DIM == 0
        tiles = (fc + 127) // 128
        f_r = (fc // 2 + 15) // 16 * 16

        half = HEAD_DIM // 2
        inv_freq = THETA ** (-2.0 * jnp.arange(half, dtype=F32) / HEAD_DIM)
        angles = jnp.arange(seq, dtype=F32)[:, None] * inv_freq[None, :]
        cos_t, sin_t = jnp.cos(angles), jnp.sin(angles)
        cos_t = jnp.concatenate([cos_t, cos_t], axis=1)
        sin_t = jnp.concatenate([-sin_t, sin_t], axis=1)

        units = NJ + 1
        gather_sems = [sems(4, units), sems(4, units), sems(2, units), sems(2, units), sems(2, NJ), sems(2, NJ)]
        reduce_scratch = [vmem(NX, NJ, ch, kc), vmem(NJ, h, kc), vmem(NJ, ch - h, kc), vmem(NJ, ch, kc), vmem(NJ, ch, kc)]
        h_blk, w_all = pl.pallas_call(
            attention_kernel,
            out_shape=(
                jax.ShapeDtypeStruct((NJ, ch, kc), BF16),
                jax.ShapeDtypeStruct((2, fc, width), BF16),
            ),
            in_specs=[vmem_spec] * 3 + [any_spec] * 6,
            out_specs=(vmem_spec, any_spec),
            scratch_shapes=[
                vmem(NJ, ch, kc), vmem(NX, NJ, ch, width), vmem(width, 3 * hc), vmem(2, kd // 2, 3 * hc), vmem(row_heads, kc),
                vmem(2, ch, 3 * hc), vmem(NX, NJ, ch, 2 * hc), vmem(NX, NJ, ch, 2 * hc), vmem(NCH, ch, row_heads),
                *reduce_scratch,
                vmem(2, fc, kd), vmem(2, f_r, kd), vmem(2, fc - f_r, kd),
                *gather_sems, sems(NJ), sems(NJ),
                sems(2, 3), sems(2, 3), sems(2, 3), sems(2, 3), sems(2), sems(2), sems(6), sems(6), sems(4), sems(1), sems(1),
                sems(NCH), sems(NCH), sems(4, NCH), sems(4, NCH), sems(4, NJ), sems(4, NJ),
                sems(2, 2), sems(2, 2, 2), sems(2, 2, 2), sems(2, 2), sems(2, 2), sems(2, 2), sems(2, 2), sems(2, 4), sems(2, 4),
            ],
            compiler_params=pltpu.CompilerParams(collective_id=0, has_side_effects=True, vmem_limit_bytes=VMEM_LIMIT),
            name="attention_part",
        )(x_blk[0], cos_t, sin_t, w_q, w_k, w_v, w_o, w_gate.T, w_up.T)

        units = ((0, 0, h, 1), (0, h, h, 0)) + tuple((j, 0, ch, 0) for j in range(1, NJ))
        n_u, n_x = len(units), len(units) + 3
        y_blk = pl.pallas_call(
            functools.partial(mlp_kernel, units),
            out_shape=jax.ShapeDtypeStruct((seq, kd), BF16),
            in_specs=[vmem_spec, any_spec, any_spec],
            out_specs=vmem_spec,
            scratch_shapes=[
                vmem(NX, NJ, ch, width), vmem(tiles, 256, width), vmem(NX * tiles * 128, kc), vmem(NCH, ch, NX * tiles * 128),
                *reduce_scratch, vmem(2, NJ, ch, kd),
                sems(4, n_x), sems(4, n_x), sems(2, n_u), sems(2, n_u), sems(2, n_u), sems(2, n_u),
                sems(4, NCH), sems(4, NCH), sems(4, NJ), sems(4, NJ), sems(NJ), sems(NJ),
                sems(2, tiles), sems(NX), sems(NX), sems(NX),
            ],
            compiler_params=pltpu.CompilerParams(collective_id=1, has_side_effects=True, vmem_limit_bytes=VMEM_LIMIT),
            name="mlp_part",
        )(h_blk, w_all, w_down)
        return y_blk[None]

    return jax.shard_map(
        layer,
        mesh=mesh,
        in_specs=(act_spec, col_spec, col_spec, col_spec, row_spec, col_spec, col_spec, row_spec),
        out_specs=act_spec,
        check_vma=False,
    )
```

```python
import functools

import jax
import jax.numpy as jnp
from jax import lax
from jax.experimental import pallas as pl
from jax.experimental.pallas import tpu as pltpu
from jax.sharding import PartitionSpec as P

HEAD_DIM = 128
EPS = 1e-5
THETA = 10000.0
MESH = pl.DeviceIdType.MESH
F32 = jnp.float32
BF16 = jnp.bfloat16
NX = 4
NJ = 4
NCH = 16
VMEM_LIMIT = 67_043_328


def rem(a, b):
    return lax.rem(a, jnp.int32(b))


def div(a, b):
    return lax.div(a, jnp.int32(b))


def al(v, m):
    return pl.multiple_of(v, m)


def remote(src, dst, ssem, rsem, dev):
    return pltpu.make_async_remote_copy(src_ref=src, dst_ref=dst, send_sem=ssem, recv_sem=rsem, device_id=dev, device_id_type=MESH)


ATTENTION_STEPS = (
    ("S", "b", 1, 1), ("WA", 0), ("XP", 2), ("XE", 3), ("S", "b", 0, 0), ("XP", 3), ("S", "b", 1, 0), ("XP", 0), ("WOP",),
    ("XE", 0), ("WP", 0), ("O", "b", 1), ("ST", 3), ("WA", 1), ("ST", 0), ("S", "b", 0, 1), ("XP", 1), ("O", "b", 0),
    ("XE", 1), ("N", 3), ("WP", 1), ("XE", 2), ("XE", 4), ("ST", 1), ("YH", 3), ("G", 3, 2), ("G", 1, 2), ("O", "a", 1),
    ("N", 1), ("F", "a", 0), ("F", "a", 1), ("ST", 2), ("G", 2, 2), ("S", "a", 1, 0), ("N", 0), ("G", 0, 0), ("YH", 1),
    ("N", 2), ("S", "a", 0, 1), ("S", "a", 1, 1), ("ST", 4), ("YH", 0), ("R", 3, 2), ("O", "a", 0), ("F", "b", 1), ("N", 4),
    ("G", 1, 0), ("G", 3, 0), ("G", 0, 3), ("R", 2, 2), ("G", 2, 0), ("R", 1, 2), ("R", 3, 0), ("YH", 2), ("G", 1, 1),
    ("R", 1, 0), ("R", 0, 3), ("A", 3, 0), ("YH", 4), ("R", 2, 0), ("G", 1, 3), ("G", 3, 1), ("G", 2, 1), ("A", 1, 0),
    ("A", 2, 0), ("R", 3, 1), ("G", 3, 3), ("A", 3, 1), ("G", 2, 3), ("P", 2, 0), ("R", 1, 1), ("P", 1, 0), ("R", 2, 1),
    ("R", 1, 3), ("A", 2, 1), ("R", 0, 0), ("A", 2, 2), ("A", 3, 2), ("P", 3, 0), ("R", 3, 3), ("A", 1, 1), ("R", 2, 3),
    ("P", 2, 1), ("DP", 1), ("X", 2, 0), ("A", 2, 3), ("X", 1, 0), ("A", 1, 2), ("A", 3, 3), ("P", 3, 2), ("A", 1, 3),
    ("P", 3, 1), ("X", 2, 1), ("X", 3, 0), ("P", 1, 2), ("P", 2, 2), ("P", 2, 3), ("P", 1, 1), ("M", 0), ("P", 3, 3),
    ("G", 0, 1), ("G", 0, 2), ("X", 2, 2), ("X", 3, 1), ("P", 1, 3), ("X", 1, 1), ("M", 1), ("S", "a", 0, 0), ("A", 0, 0),
    ("X", 3, 2), ("X", 1, 2), ("F", "b", 0), ("R", 0, 2), ("X", 2, 3), ("M", 2), ("X", 1, 3), ("R", 0, 1), ("A", 0, 1),
    ("A", 0, 2), ("X", 3, 3), ("M", 3), ("A", 0, 3), ("DP", 0), ("P", 0, 0), ("P", 0, 1), ("P", 0, 2), ("P", 0, 3),
    ("X", 0, 0), ("T", 0), ("X", 0, 1), ("X", 0, 2), ("T", 1), ("T", 2), ("X", 0, 3), ("T", 3),
)
MLP_STEPS = (
    ("XF", 0, 1), ("YR", 0), ("XH", 0, 1), ("XF", 0, 2), ("YRH", 0), ("N", 0, 1), ("XH", 0, 2), ("XF", 3, 0), ("XF", 0, 0),
    ("XF", 0, 3), ("N", 0, 2), ("XF", 1, 0), ("XH", 0, 3), ("XH", 0, 0), ("XH", 3, 0), ("XF", 0, 4), ("N", 0, 3), ("G", 0, 1),
    ("XF", 2, 0), ("N", 3, 0), ("XH", 1, 0), ("YH", 2), ("YH", 1), ("N", 0, 0), ("G", 1, 1), ("G", 3, 0), ("XH", 0, 4),
    ("G", 0, 0), ("N", 1, 0), ("G", 3, 1), ("P", 3, 0), ("N", 0, 4), ("G", 1, 0), ("G", 0, 2), ("YH", 3), ("XH", 2, 0),
    ("G", 3, 2), ("G", 2, 1), ("G", 1, 2), ("P", 1, 1), ("G", 0, 3), ("P", 1, 2), ("X", 1, 1), ("P", 3, 1), ("P", 0, 2),
    ("P", 2, 1), ("N", 2, 0), ("G", 2, 0), ("YH", 4), ("X", 3, 0), ("G", 3, 3), ("X", 2, 1), ("G", 1, 3), ("X", 3, 1),
    ("P", 2, 0), ("P", 3, 2), ("P", 1, 0), ("G", 2, 2), ("X", 2, 0), ("G", 2, 3), ("M", 1), ("X", 1, 0), ("P", 2, 2),
    ("X", 3, 2), ("M", 0), ("P", 2, 3), ("P", 1, 3), ("P", 3, 3), ("P", 0, 1), ("X", 0, 2), ("X", 2, 2), ("X", 1, 2),
    ("X", 2, 3), ("M", 2), ("X", 3, 3), ("X", 0, 1), ("P", 0, 3), ("X", 1, 3), ("P", 0, 0), ("M", 3), ("T", 2), ("X", 0, 3),
    ("T", 1), ("X", 0, 0), ("T", 0), ("T", 3),
)


class Place:
    def __init__(self):
        tx, ty = lax.axis_index("tx"), lax.axis_index("ty")
        self.x, self.c, self.y = div(tx, 2), rem(tx, 2), ty
        x, c, y = self.x, self.c, self.y
        self.xr, self.xl, self.xo = rem(x + 1, NX), rem(x + 3, NX), rem(x + 2, NX)
        self.yu, self.yd, self.yo = rem(y + 1, NX), rem(y + 3, NX), rem(y + 2, NX)
        self.right = {"tx": self.xr * 2 + c, "ty": y}
        self.left = {"tx": self.xl * 2 + c, "ty": y}
        self.up = {"tx": tx, "ty": self.yu}
        self.down = {"tx": tx, "ty": self.yd}
        self.partner = {"tx": x * 2 + 1 - c, "ty": y}
        self.xa, self.xb = x + 1 - 2 * rem(x, 2), rem(x + 3 + 2 * rem(x, 2), NX)
        self.pa, self.pb = {"tx": self.xa * 2 + c, "ty": y}, {"tx": self.xb * 2 + c, "ty": y}

    def barrier(self):
        sem = pltpu.get_barrier_semaphore()
        for dev in (self.right, self.left, self.up, self.down, self.partner):
            pl.semaphore_signal(sem, inc=1, device_id=dev, device_id_type=MESH)
        pl.semaphore_wait(sem, 5)


class Spread:
    def __init__(self, at, src, xg, units, sx, rx, sy, ry, syh, ryh):
        self.at, self.src, self.xg, self.units, self.kc = at, src, xg, units, src.shape[2]
        self.sx, self.rx, self.sy, self.ry, self.syh, self.ryh = sx, rx, sy, ry, syh, ryh
        pairs = [(r, u) for u, unit in enumerate(units) for r in ((0, 3, 1, 2) if unit[3] else (0,))]
        self.index = {pair: i for i, pair in enumerate(pairs)}
        self.seqs = (at.y, at.yu, at.yo, at.yd)

    def cols(self, x):
        return pl.ds(al(x * self.kc, 128), self.kc)

    def keep_own(self):
        for j in range(NJ):
            self.xg[self.at.y, j, :, self.cols(self.at.x)] = self.src[j]

    def xcopy(self, kind, r, u):
        at, s = self.at, self.seqs[r]
        j, lo, n, _ = self.units[u]
        i = self.index[r, u]
        if kind < 2:
            dst = self.xg.at[s, j, pl.ds(lo, n), self.cols(at.x)]
            src = self.src.at[j, pl.ds(lo, n)] if r == 0 else dst
        elif kind == 2:
            src = dst = self.xg.at[s, j, pl.ds(lo, n // 2), self.cols(at.xl)]
        else:
            src = dst = self.xg.at[s, j, pl.ds(lo + n // 2, n // 2), self.cols(at.xr)]
        return remote(src, dst, self.sx.at[kind, i], self.rx.at[kind, i], at.left if kind % 2 else at.right)

    def xwait(self, kind, r, u):
        at = self.at
        j, lo, n, _ = self.units[u]
        i = self.index[r, u]
        x = (at.xl, at.xr, at.xo, at.xo)[kind]
        rows = (pl.ds(lo, n), pl.ds(lo, n), pl.ds(lo, n // 2), pl.ds(lo + n // 2, n // 2))[kind]
        dst = self.xg.at[self.seqs[r], j, rows, self.cols(x)]
        remote(dst, dst, self.sx.at[kind, i], self.rx.at[kind, i], at.right).wait_recv()

    def yref(self, s, u, lo, n):
        j, _, _, first = self.units[u]
        rows = pl.ds(lo, n)
        return self.xg.at[s, j, rows, self.cols(self.at.x)] if first else self.xg.at[s, j, rows]

    def ycopy(self, d, u):
        j, lo, n, first = self.units[u]
        dst = self.yref(self.at.y, u, lo, n)
        src = self.src.at[j, pl.ds(lo, n)] if first else dst
        return remote(src, dst, self.sy.at[d, u], self.ry.at[d, u], self.at.down if d else self.at.up)

    def ywait(self, d, u):
        _, lo, n, _ = self.units[u]
        dst = self.yref(self.at.yu if d else self.at.yd, u, lo, n)
        remote(dst, dst, self.sy.at[d, u], self.ry.at[d, u], self.at.up).wait_recv()

    def yhalf(self, d, u):
        _, lo, n, _ = self.units[u]
        ref = self.yref(self.at.yu if d else self.at.yd, u, lo + d * (n // 2), n // 2)
        return remote(ref, ref, self.syh.at[d, u], self.ryh.at[d, u], self.at.down if d else self.at.up)

    def yhalf_wait(self, d, u):
        _, lo, n, _ = self.units[u]
        dst = self.yref(self.at.yo, u, lo + d * (n // 2), n // 2)
        remote(dst, dst, self.syh.at[d, u], self.ryh.at[d, u], self.at.up).wait_recv()

    def YR(self, u):
        for d in range(2):
            self.ycopy(d, u).start()

    def YH(self, u):
        for d in range(2):
            self.ywait(d, u)
            self.yhalf(d, u).start()

    YRH = YH

    def XF(self, r, u):
        if r == 2:
            for d in range(2):
                self.yhalf_wait(d, u)
        for kind in range(2):
            self.xcopy(kind, r, u).start()

    def XH(self, r, u):
        for kind in range(2):
            self.xwait(kind, r, u)
            self.xcopy(kind + 2, r, u).start()

    def N(self, r, u):
        j, lo, n, first = self.units[u]
        for kind in (2, 3):
            self.xwait(kind, r, u)
            self.xcopy(kind, r, u).wait_send()
        if r:
            for kind in range(2):
                self.xcopy(kind, r, u).wait_send()
        if r % 2:
            self.yhalf(0 if r == 3 else 1, u).wait_send()
        width, rows, s = self.xg.shape[-1], 8, self.seqs[r]

        def body(i, carry):
            at_rows = pl.ds(al(lo + i * rows, rows), rows)
            v = self.xg[s, j, at_rows, :].astype(F32)
            mean = jnp.sum(v, axis=-1, keepdims=True) / width
            var = jnp.sum(v * v, axis=-1, keepdims=True) / width - mean * mean
            self.xg[s, j, at_rows, :] = ((v - mean) * lax.rsqrt(var + EPS)).astype(BF16)
            return carry

        lax.fori_loop(0, n // rows, body, 0)
        if not first:
            self.YR(u)

    def chunk_wait(self, r, j):
        if r == 2:
            for u, unit in enumerate(self.units):
                if unit[0] == j and not unit[3]:
                    for d in range(2):
                        self.yhalf_wait(d, u)

    def drain(self):
        for u, unit in enumerate(self.units):
            for d in range(2):
                self.xcopy(d, 0, u).wait_send()
                self.ycopy(d, u).wait_send()
                if not unit[3]:
                    self.yhalf(d, u).wait_send()


class Reduce:
    def __init__(self, at, zb, ya, yb, yfd, yfu, ss, rs):
        self.at, self.zb, self.ya, self.yb, self.yfd, self.yfu, self.ss, self.rs = at, zb, ya, yb, yfd, yfu, ss, rs
        self.ch = zb.shape[2]
        self.h = self.ch // 2

    def copy(self, kind, j):
        at, h, ch = self.at, self.h, self.ch
        src, dst = (
            lambda: (self.zb.at[2, j, pl.ds(0, h)], self.ya.at[j]),
            lambda: (self.zb.at[2, j, pl.ds(h, ch - h)], self.yb.at[j]),
            lambda: (self.zb.at[1, j], self.yfd.at[j]),
            lambda: (self.zb.at[3, j], self.yfu.at[j]),
        )[kind]()
        return remote(src, dst, self.ss.at[kind, j], self.rs.at[kind, j], at.down if kind % 2 else at.up)

    def wait(self, kind, j):
        self.copy(kind, j).wait_recv()

    def halves(self, j):
        self.copy(0, j).start()
        self.copy(1, j).start()

    def middle(self, j):
        h = self.h
        self.wait(0, j)
        self.zb[1, j, 0:h] = (self.zb[1, j, 0:h].astype(F32) + self.ya[j].astype(F32)).astype(BF16)
        self.copy(2, j).start()
        self.wait(1, j)
        self.zb[3, j, h:] = (self.zb[3, j, h:].astype(F32) + self.yb[j].astype(F32)).astype(BF16)
        self.copy(3, j).start()

    def total(self, j):
        self.wait(2, j)
        self.wait(3, j)
        return self.zb[0, j].astype(F32) + self.yfd[j].astype(F32) + self.yfu[j].astype(F32)

    def drain(self):
        for j in range(NJ):
            for kind in range(4):
                self.copy(kind, j).wait_send()


def attention_kernel(
    units, x_ref, cos_ref, sin_ref, wq, wk, wv, wo, wg_t, wu_t,
    h_ref, w_all,
    xc, xg, st_own, st_in, wb, wob, part, precv, qb, kvo, kvp, og, zb, ya, yb, yfd, yfu, own, drel_a, drel_b,
    sxe, rxe, sst, rst, sy, ry, syh, ryh, sd, rd, swa, rwa, swo, rwo, swp, rwp, lw, so, ro, spr, rpr, skv, rkv, sog, rog, syr, ryr,
    lg, sds, rds, sdo, rdo, sdf, rdf, sdp, rdp,
):
    at = Place()
    x, c, y = at.x, at.c, at.y
    ch, kc, h = xc.shape[1], xc.shape[2], xc.shape[1] // 2
    kd = wq.shape[0]
    hc = qb.shape[2]
    fc, f_a = w_all.shape[1], drel_a.shape[1]
    width = 2 * xg.shape[3]
    kh = div(x, 2)
    ng = rem(div(x + 1, 2), 2)
    gather = Spread(at, xc, xg, units, None, None, sy, ry, syh, ryh)
    reduce = Reduce(at, zb, ya, yb, yfd, yfu, syr, ryr)
    weights = (wq, wk, wv)

    def half_cols(core):
        return pl.ds(al(core * kd, 128), kd)

    def x_rows(j, core):
        return pl.ds(al((2 * j + core) * ch, 8), ch)

    def x_pair(j):
        return remote(x_ref.at[x_rows(j, 1 - c)], xc.at[j, :, half_cols(c)], sd.at[j], rd.at[j], at.partner)

    def pair_cols(xx):
        return pl.ds(al(rem(xx, 2) * kc, 128), kc)

    def xe_copy(u, xx):
        j, lo, n, _ = units[u]
        rows = pl.ds(lo, n)
        return remote(xc.at[j, rows], xg.at[y, j, rows, pair_cols(xx)], sxe.at[u], rxe.at[u], at.pa)

    def st_copy(u):
        j, lo, n, _ = units[u]
        rows = pl.ds(lo, n)
        return remote(st_own.at[j, rows], st_in.at[j, rows], sst.at[u], rst.at[u], at.pb)

    def XP(j):
        x_pair(j).start()

    def XE(u):
        j, lo, n, _ = units[u]
        if lo == 0:
            dst = xc.at[j, :, half_cols(1 - c)]
            remote(dst, dst, sd.at[j], rd.at[j], at.partner).wait_recv()
        xe_copy(u, x).start()
        xg[y, j, lo : lo + n, pair_cols(x)] = xc[j, lo : lo + n]

    def ST(u):
        j, lo, n, _ = units[u]
        xe_copy(u, at.xa).wait_recv()
        lane = lax.broadcasted_iota(jnp.int32, (8, 128), 1)

        def body(i, carry):
            rows = pl.ds(al(lo + i * 8, 8), 8)
            v = xg[y, j, rows, :].astype(F32)
            total, square = jnp.sum(v, axis=-1, keepdims=True), jnp.sum(v * v, axis=-1, keepdims=True)
            st_own[j, rows, :] = jnp.where(lane < 64, total, square)
            return carry

        lax.fori_loop(0, n // 8, body, 0)
        st_copy(u).start()

    def N(u):
        j, lo, n, _ = units[u]
        st_copy(u).wait_recv()

        def body(i, carry):
            rows = pl.ds(al(lo + i * 8, 8), 8)
            moments = (st_own[j, rows, :] + st_in[j, rows, :]) / width
            mean = moments[:, 0:1]
            var = moments[:, 64:65] - mean * mean
            v = xg[y, j, rows, :].astype(F32)
            xg[y, j, rows, :] = ((v - mean) * lax.rsqrt(var + EPS)).astype(BF16)
            return carry

        lax.fori_loop(0, n // 8, body, 0)
        gather.YR(u)

    def w_rows(xx, core):
        return pl.ds(al(rem(xx, 2) * kc + core * kd, 128), kd)

    def w_part(group, half, i):
        return weights[i].at[:, pl.ds(al((2 * group + half) * hc, 128), hc)]

    def w_cols(half, i):
        return pl.ds(half * 3 * hc + i * hc, hc)

    def wa_copy(half, i, xx):
        return remote(w_part(1 - ng, half, i), wb.at[w_rows(xx, c), w_cols(half, i)], swa.at[half, i], rwa.at[half, i], at.pa)

    def wo_copy(half, i, core):
        return remote(w_part(ng, half, i), wb.at[w_rows(x, core), w_cols(half, i)], swo.at[half, i], rwo.at[half, i], at.partner)

    def w_local(half, i):
        return pltpu.make_async_copy(w_part(ng, half, i), wb.at[w_rows(x, c), w_cols(half, i)], lw.at[half, i])

    def wp_copy(half, core):
        ref = wb.at[w_rows(at.xa, core), pl.ds(half * 3 * hc, 3 * hc)]
        return remote(ref, ref, swp.at[half], rwp.at[half], at.partner)

    o_local = pltpu.make_async_copy(wo, wob.at[:, half_cols(c)], lw.at[2, 0])
    o_pair = remote(wo, wob.at[:, half_cols(c)], so.at[0], ro.at[0], at.partner)
    pieces = [(half, i) for half in range(2) for i in range(3)]

    def WOP():
        for half, i in pieces:
            wo_copy(half, i, c).start()
        o_pair.start()

    def WA(half):
        for i in range(3):
            wa_copy(half, i, x).start()

    def WP(half):
        for i in range(3):
            wa_copy(half, i, at.xa).wait_recv()
        wp_copy(half, c).start()

    def w_ready():
        for half, i in pieces:
            w_local(half, i).wait()
            wo_copy(half, i, 1 - c).wait_recv()
        for half in range(2):
            wp_copy(half, 1 - c).wait_recv()
        for m in range(2):
            d_in(m).wait()
            d_out(m).start()
            d_pair(m, 3, c).start()

    def o_ready():
        o_local.wait()
        dst = wob.at[:, half_cols(1 - c)]
        remote(dst, dst, so.at[0], ro.at[0], at.partner).wait_recv()

    mlp_weights = (wg_t, wu_t)
    parts = ((0, f_a), (f_a, fc - f_a))

    def d_src(m, xx, p):
        return mlp_weights[m].at[pl.ds(al(xx * fc + parts[p][0], 8), parts[p][1])]

    def d_dst(m, xx, p):
        return w_all.at[m, pl.ds(*parts[p]), pl.ds(al((2 * xx + c) * kd, 128), kd)]

    def s_copy(d, m, p, xx):
        to, dev = ((at.xa, at.pa), (at.xb, at.pb))[d]
        return remote(d_src(m, to, p), d_dst(m, xx, p), sds.at[d, m, p], rds.at[d, m, p], dev)

    def o_copy(d, m):
        return remote(d_src(m, at.xo, d), (drel_a, drel_b)[d].at[m], sdo.at[d, m], rdo.at[d, m], (at.pa, at.pb)[d])

    def f_copy(d, m, xx):
        return remote((drel_a, drel_b)[d].at[m], d_dst(m, xx, d), sdf.at[d, m], rdf.at[d, m], (at.pb, at.pa)[d])

    def d_in(m):
        return pltpu.make_async_copy(mlp_weights[m].at[pl.ds(al(x * fc, 8), fc)], own.at[m], lg.at[0, m])

    def d_all(m, xx, core):
        return w_all.at[m, :, pl.ds(al((2 * xx + core) * kd, 128), kd)]

    def d_out(m):
        return pltpu.make_async_copy(own.at[m], d_all(m, x, c), lg.at[1, m])

    def d_pair(m, k, core):
        dst = d_all(m, (at.xa, at.xb, at.xo, x)[k], core)
        return remote(own.at[m] if k == 3 else dst, dst, sdp.at[m, k], rdp.at[m, k], at.partner)

    def S(link, m, p):
        s_copy("ab".index(link), m, p, x).start()

    def O(link, m):
        o_copy("ab".index(link), m).start()

    def F(link, m):
        d = "ba".index(link)
        o_copy(d, m).wait_recv()
        f_copy(d, m, (at.xa, at.xb)[d]).start()

    def DP(m):
        for d in range(2):
            for p in range(2):
                s_copy(d, m, p, (at.xa, at.xb)[d]).wait_recv()
            f_copy(d, m, at.xo).wait_recv()
        for k in range(3):
            d_pair(m, k, c).start()

    def pr_copy(n):
        src = part.at[n, :, pl.ds(al((1 - kh) * 3 * hc, 128), 3 * hc)]
        return remote(src, precv.at[n], spr.at[n], rpr.at[n], at.pb)

    def G(r, j):
        gather.chunk_wait(r, j)
        s, n = gather.seqs[r], r * NJ + j

        def columns(i, carry):
            cols = pl.ds(al(i * 256, 128), 256)
            part[n, :, cols] = jnp.dot(xg[s, j], wb[:, cols], preferred_element_type=F32).astype(BF16)
            return carry

        lax.fori_loop(0, wb.shape[1] // 256, columns, 0)
        pr_copy(n).start()

    def kv_copy(r, j):
        s, n = gather.seqs[r], r * NJ + j
        return remote(kvo.at[s, j], kvp.at[s, j], skv.at[n], rkv.at[n], at.partner)

    def R(r, j):
        s, n = gather.seqs[r], r * NJ + j
        pr_copy(n).wait_recv()
        rows = pl.ds(al((2 * j + c) * ch, 8), ch)
        cos_t, sin_t = cos_ref[rows, :], sin_ref[rows, :]

        def total(col, size):
            mine = part[n, :, pl.ds(al(kh * 3 * hc + col, 128), size)]
            return (mine.astype(F32) + precv[n, :, col : col + size].astype(F32)).astype(BF16)

        def turned(col):
            v = total(col, HEAD_DIM).astype(F32)
            return (v * cos_t + pltpu.roll(v, HEAD_DIM // 2, axis=1) * sin_t).astype(BF16)

        for col in range(0, hc, HEAD_DIM):
            qb[n, :, col : col + HEAD_DIM] = turned(col)
            kvo[s, j, :, col : col + HEAD_DIM] = turned(hc + col)
        kvo[s, j, :, hc:] = total(2 * hc, hc)
        kv_copy(r, j).start()

    def o_cols(xx):
        return pl.ds(al((2 * rem(div(xx + 1, 2), 2) + div(xx, 2)) * hc, 128), hc)

    def og_copy(kind, n):
        if kind < 2:
            ref = og.at[n, :, o_cols(x)]
        elif kind == 2:
            ref = og.at[n, pl.ds(0, h), o_cols(at.xa)]
        else:
            ref = og.at[n, pl.ds(h, ch - h), o_cols(at.xb)]
        return remote(ref, ref, sog.at[kind, n], rog.at[kind, n], at.pa if kind in (0, 3) else at.pb)

    def og_wait(kind, n):
        xx = (at.xa, at.xb, at.xo, at.xo)[kind]
        rows = (pl.ds(0, ch), pl.ds(0, ch), pl.ds(0, h), pl.ds(h, ch - h))[kind]
        dst = og.at[n, rows, o_cols(xx)]
        remote(dst, dst, sog.at[kind, n], rog.at[kind, n], at.pa).wait_recv()

    def A(r, j):
        s, n = gather.seqs[r], r * NJ + j
        kv_copy(r, j).wait_recv()
        keys = (j + 1) * ch
        iq = lax.broadcasted_iota(jnp.int32, (ch, keys), 0) + j * ch
        ik = lax.broadcasted_iota(jnp.int32, (ch, keys), 1)
        own_ok = iq >= ik
        par_ok = ik < (j + c) * ch
        contract = (((1,), (1,)), ((), ()))
        first = (2 * ng + kh) * hc
        for lo in range(0, hc, HEAD_DIM):
            q = qb[n, :, lo : lo + HEAD_DIM]
            k_own = kvo[s, 0 : j + 1, :, lo : lo + HEAD_DIM].reshape(keys, HEAD_DIM)
            k_par = kvp[s, 0 : j + 1, :, lo : lo + HEAD_DIM].reshape(keys, HEAD_DIM)
            s_own = lax.dot_general(q, k_own, contract, preferred_element_type=F32) * HEAD_DIM**-0.5
            s_par = lax.dot_general(q, k_par, contract, preferred_element_type=F32) * HEAD_DIM**-0.5
            s_own = jnp.where(own_ok, s_own, -1e30)
            s_par = jnp.where(par_ok, s_par, -1e30)
            top = jnp.maximum(jnp.max(s_own, axis=1, keepdims=True), jnp.max(s_par, axis=1, keepdims=True))
            e_own, e_par = jnp.exp(s_own - top), jnp.exp(s_par - top)
            inv = 1.0 / (jnp.sum(e_own, axis=1, keepdims=True) + jnp.sum(e_par, axis=1, keepdims=True))
            v_own = kvo[s, 0 : j + 1, :, hc + lo : hc + lo + HEAD_DIM].reshape(keys, HEAD_DIM)
            v_par = kvp[s, 0 : j + 1, :, hc + lo : hc + lo + HEAD_DIM].reshape(keys, HEAD_DIM)
            out = jnp.dot((e_own * inv).astype(BF16), v_own, preferred_element_type=F32)
            out += jnp.dot((e_par * inv).astype(BF16), v_par, preferred_element_type=F32)
            og[n, :, pl.ds(al(first + lo, 128), HEAD_DIM)] = out.astype(BF16)
        og_copy(0, n).start()
        og_copy(1, n).start()

    def P(r, j):
        n = r * NJ + j
        for kind in range(2):
            og_wait(kind, n)
            og_copy(kind + 2, n).start()

    def X(r, j):
        n = r * NJ + j
        og_wait(2, n)
        og_wait(3, n)

        def columns(i, carry):
            cols = pl.ds(al(i * 256, 128), 256)
            zb[r, j, :, cols] = jnp.dot(og[n], wob[:, cols], preferred_element_type=F32).astype(BF16)
            return carry

        lax.fori_loop(0, kc // 256, columns, 0)
        if r == 2:
            reduce.halves(j)

    def T(j):
        attn = reduce.total(j).astype(BF16)
        h_ref[j] = (xc[j].astype(F32) + attn.astype(F32)).astype(BF16)

    for half, i in pieces:
        w_local(half, i).start()
    o_local.start()
    for m in range(2):
        d_in(m).start()
    for j in range(NJ):
        xc[j, :, half_cols(c)] = x_ref[x_rows(j, c), :]
    at.barrier()
    ops = {
        "XP": XP, "WOP": WOP, "XE": XE, "ST": ST, "N": N, "YH": gather.YH, "WA": WA, "WP": WP, "S": S, "O": O, "F": F, "DP": DP,
        "G": G, "R": R, "A": A, "P": P, "X": X, "M": reduce.middle, "T": T,
    }
    waits = {"G": w_ready, "X": o_ready}
    for step in ATTENTION_STEPS:
        if step[0] in waits:
            waits.pop(step[0])()
        ops[step[0]](*step[1:])

    for m in range(2):
        for k in range(4):
            d_pair(m, k, 1 - c).wait_recv()
            d_pair(m, k, c).wait_send()
        d_out(m).wait()
        for d in range(2):
            for p in range(2):
                s_copy(d, m, p, x).wait_send()
            o_copy(d, m).wait_send()
            f_copy(d, m, x).wait_send()
    for j in range(NJ):
        x_pair(j).wait_send()
    for u in range(len(units)):
        xe_copy(u, x).wait_send()
        st_copy(u).wait_send()
        for d in range(2):
            gather.ycopy(d, u).wait_send()
            gather.yhalf(d, u).wait_send()
    reduce.drain()
    o_pair.wait_send()
    for half, i in pieces:
        wa_copy(half, i, x).wait_send()
        wo_copy(half, i, c).wait_send()
    for half in range(2):
        wp_copy(half, c).wait_send()

    def chunk_sent(n, carry):
        pr_copy(n).wait_send()
        remote(kvo.at[0, 0], kvp.at[0, 0], skv.at[n], rkv.at[n], at.partner).wait_send()
        for kind in range(4):
            og_copy(kind, n).wait_send()
        return carry

    lax.fori_loop(0, NCH, chunk_sent, 0)


def mlp_kernel(
    units, h_ref, w_hbm, wdn, y_ref,
    xg, wt, wd, ag, acc, zb, ya, yb, yfd, yfu, yst,
    sx, rx, sy, ry, syh, ryh, sa, ra, syr, ryr, sd, rd, lw, lwd, swd, rwd,
):
    at = Place()
    x, c, y = at.x, at.c, at.y
    ch, kc, h = h_ref.shape[1], h_ref.shape[2], h_ref.shape[1] // 2
    width = xg.shape[-1]
    kd = kc // 2
    fc, tiles = w_hbm.shape[1], wt.shape[0]
    fp = tiles * 128
    gather = Spread(at, h_ref, xg, units, sx, rx, sy, ry, syh, ryh)
    reduce = Reduce(at, zb, ya, yb, yfd, yfu, syr, ryr)

    def w_in(m, i):
        n = min(128, fc - i * 128)
        return pltpu.make_async_copy(w_hbm.at[m, pl.ds(i * 128, n)], wt.at[i, pl.ds(m * 128, n)], lw.at[m, i])

    def d_own(q):
        return pltpu.make_async_copy(wdn.at[pl.ds(q * fc, fc)], wd.at[pl.ds(q * fp, fc), pl.ds(al(c * kd, 128), kd)], lwd.at[q])

    def d_pair(q):
        dst = wd.at[pl.ds(q * fp, fc), pl.ds(al(c * kd, 128), kd)]
        return remote(wdn.at[pl.ds(q * fc, fc)], dst, swd.at[q], rwd.at[q], at.partner)

    def d_pair_wait(q):
        dst = wd.at[pl.ds(q * fp, fc), pl.ds(al((1 - c) * kd, 128), kd)]
        remote(dst, dst, swd.at[q], rwd.at[q], at.partner).wait_recv()

    for m in range(2):
        for i in range(tiles):
            w_in(m, i).start()
    for q in range(NX):
        d_own(q).start()
    rest = fc - (tiles - 1) * 128
    if rest < 128:
        for m in range(2):
            wt[tiles - 1, m * 128 + rest : (m + 1) * 128, :] = jnp.zeros((128 - rest, width), BF16)
        for q in range(NX):
            wd[q * fp + fc : (q + 1) * fp, :] = jnp.zeros((fp - fc, kc), BF16)
    at.barrier()
    for q in range(NX):
        d_pair(q).start()

    def a_cols(xx):
        return pl.ds(al(xx * fp, 128), fp)

    def a_copy(kind, n):
        if kind < 2:
            ref = ag.at[n, :, a_cols(x)]
        elif kind == 2:
            ref = ag.at[n, pl.ds(0, h), a_cols(at.xl)]
        else:
            ref = ag.at[n, pl.ds(h, ch - h), a_cols(at.xr)]
        return remote(ref, ref, sa.at[kind, n], ra.at[kind, n], at.left if kind % 2 else at.right)

    def a_wait(kind, n):
        xx = (at.xl, at.xr, at.xo, at.xo)[kind]
        rows = (pl.ds(0, ch), pl.ds(0, ch), pl.ds(0, h), pl.ds(h, ch - h))[kind]
        dst = ag.at[n, rows, a_cols(xx)]
        remote(dst, dst, sa.at[kind, n], ra.at[kind, n], at.right).wait_recv()

    def G(r, j):
        gather.chunk_wait(r, j)
        s, n = gather.seqs[r], r * NJ + j

        def columns(i, carry):
            acc[...] = jnp.zeros_like(acc)

            def depth(k, carry):
                cols = pl.ds(al(k * (width // 2), 128), width // 2)
                acc[...] += lax.dot_general(xg[s, j, :, cols], wt[i, :, cols], (((1,), (1,)), ((), ())), preferred_element_type=F32)
                return carry

            lax.fori_loop(0, 2, depth, 0)
            out = acc[...]
            g, u = out[:, :128].astype(BF16).astype(F32), out[:, 128:].astype(BF16).astype(F32)
            ag[n, :, pl.ds(al(x * fp + i * 128, 128), 128)] = (g / (1.0 + jnp.exp(-g)) * u).astype(BF16)
            return carry

        lax.fori_loop(0, tiles, columns, 0)
        for kind in range(2):
            a_copy(kind, n).start()

    def P(r, j):
        n = r * NJ + j
        for kind in range(2):
            a_wait(kind, n)
            a_copy(kind + 2, n).start()

    def X(r, j):
        n = r * NJ + j
        for kind in (2, 3):
            a_wait(kind, n)

        def columns(i, carry):
            cols = pl.ds(al(i * 256, 128), 256)
            acc[...] = jnp.zeros_like(acc)

            def depth(k, carry):
                part = pl.ds(al(k * 2 * fp, 128), 2 * fp)
                acc[...] += jnp.dot(ag[n, :, part], wd[part, cols], preferred_element_type=F32)
                return carry

            lax.fori_loop(0, 2, depth, 0)
            zb[r, j, :, cols] = acc[...].astype(BF16)
            return carry

        lax.fori_loop(0, kc // 256, columns, 0)
        if r == 2:
            reduce.halves(j)

    def y_rows(j, core):
        return pl.ds(al((2 * j + core) * ch, 8), ch)

    def y_copy(j):
        return remote(yst.at[1 - c, j], y_ref.at[y_rows(j, c)], sd.at[j], rd.at[j], at.partner)

    def y_wait(j):
        dst = y_ref.at[y_rows(j, 1 - c)]
        remote(dst, dst, sd.at[j], rd.at[j], at.partner).wait_recv()

    def T(j):
        mlp = reduce.total(j).astype(BF16)
        out = (h_ref[j].astype(F32) + mlp.astype(F32)).astype(BF16)
        yst[0, j] = out[:, :kd]
        yst[1, j] = out[:, kd:]
        y_copy(j).start()
        y_ref[y_rows(j, c), :] = yst[c, j]

    ops = {"G": G, "P": P, "X": X, "M": reduce.middle, "T": T}
    for name in ("YR", "YRH", "YH", "XF", "XH", "N"):
        ops[name] = getattr(gather, name)
    waits = {
        "N": gather.keep_own,
        "G": lambda: [w_in(m, i).wait() for m in range(2) for i in range(tiles)],
        "X": lambda: [(d_own(q).wait(), d_pair_wait(q)) for q in range(NX)],
    }
    for step in MLP_STEPS:
        if step[0] in waits:
            waits.pop(step[0])()
        ops[step[0]](*step[1:])

    gather.drain()
    reduce.drain()
    for q in range(NX):
        d_pair(q).wait_send()

    def chunk_sent(n, carry):
        for kind in range(4):
            a_copy(kind, n).wait_send()
        return carry

    lax.fori_loop(0, NCH, chunk_sent, 0)
    for j in range(NJ):
        y_copy(j).wait_send()
        y_wait(j)


def vmem(*shape, dtype=BF16):
    return pltpu.VMEM(shape, dtype)


def sems(*shape):
    return pltpu.SemaphoreType.DMA(shape)


def solution(mesh):
    assert mesh.shape["tx"] == 2 * NX and mesh.shape["ty"] == NX
    act_spec = P(("dp", "ty"), None, "tx")
    col_spec = P("tx", "ty")
    row_spec = P("ty", "tx")
    any_spec = pl.BlockSpec(memory_space=pl.ANY)
    vmem_spec = pl.BlockSpec(memory_space=pltpu.VMEM)

    def layer(x_blk, w_q, w_k, w_v, w_o, w_gate, w_up, w_down):
        _, seq, kd = x_blk.shape
        kc, width = 2 * kd, 2 * NX * kd
        ch = seq // (2 * NJ)
        h = ch // 2
        row_heads = w_q.shape[1]
        hc = row_heads // NX
        fc = w_down.shape[0] // NX
        assert hc % HEAD_DIM == 0
        tiles = (fc + 127) // 128
        f_a = (fc // 2 + 15) // 16 * 16

        half = HEAD_DIM // 2
        inv_freq = THETA ** (-2.0 * jnp.arange(half, dtype=F32) / HEAD_DIM)
        angles = jnp.arange(seq, dtype=F32)[:, None] * inv_freq[None, :]
        cos_t, sin_t = jnp.cos(angles), jnp.sin(angles)
        cos_t = jnp.concatenate([cos_t, cos_t], axis=1)
        sin_t = jnp.concatenate([-sin_t, sin_t], axis=1)

        reduce_scratch = [vmem(NX, NJ, ch, kc), vmem(NJ, h, kc), vmem(NJ, ch - h, kc), vmem(NJ, ch, kc), vmem(NJ, ch, kc)]
        units = ((0, 0, h, 0), (0, h, h, 0)) + tuple((j, 0, ch, 0) for j in range(1, NJ))
        n_u = len(units)
        h_blk, w_all = pl.pallas_call(
            functools.partial(attention_kernel, units),
            out_shape=(jax.ShapeDtypeStruct((NJ, ch, kc), BF16), jax.ShapeDtypeStruct((2, fc, width), BF16)),
            in_specs=[vmem_spec] * 3 + [any_spec] * 6,
            out_specs=(vmem_spec, any_spec),
            scratch_shapes=[
                vmem(NJ, ch, kc), vmem(NX, NJ, ch, 2 * kc), vmem(NJ, ch, 128, dtype=F32), vmem(NJ, ch, 128, dtype=F32),
                vmem(2 * kc, 6 * hc), vmem(row_heads, kc), vmem(NCH, ch, 6 * hc), vmem(NCH, ch, 3 * hc), vmem(NCH, ch, hc),
                vmem(NX, NJ, ch, 2 * hc), vmem(NX, NJ, ch, 2 * hc), vmem(NCH, ch, row_heads), *reduce_scratch,
                vmem(2, fc, kd), vmem(2, f_a, kd), vmem(2, fc - f_a, kd),
                sems(n_u), sems(n_u), sems(n_u), sems(n_u), sems(2, n_u), sems(2, n_u), sems(2, n_u), sems(2, n_u),
                sems(NJ), sems(NJ), sems(2, 3), sems(2, 3), sems(2, 3), sems(2, 3), sems(2), sems(2), sems(3, 3), sems(1), sems(1),
                sems(NCH), sems(NCH), sems(NCH), sems(NCH), sems(4, NCH), sems(4, NCH), sems(4, NJ), sems(4, NJ),
                sems(2, 2), sems(2, 2, 2), sems(2, 2, 2), sems(2, 2), sems(2, 2), sems(2, 2), sems(2, 2), sems(2, 4), sems(2, 4),
            ],
            compiler_params=pltpu.CompilerParams(collective_id=0, has_side_effects=True, vmem_limit_bytes=VMEM_LIMIT),
            name="attention_part",
        )(x_blk[0], cos_t, sin_t, w_q, w_k, w_v, w_o, w_gate.T, w_up.T)

        units = ((0, 0, h, 1), (0, h, h, 0)) + tuple((j, 0, ch, 0) for j in range(1, NJ))
        n_x = n_u + 3
        y_blk = pl.pallas_call(
            functools.partial(mlp_kernel, units),
            out_shape=jax.ShapeDtypeStruct((seq, kd), BF16),
            in_specs=[vmem_spec, any_spec, any_spec],
            out_specs=vmem_spec,
            scratch_shapes=[
                vmem(NX, NJ, ch, width), vmem(tiles, 256, width), vmem(NX * tiles * 128, kc), vmem(NCH, ch, NX * tiles * 128),
                vmem(ch, 256, dtype=F32),
                *reduce_scratch, vmem(2, NJ, ch, kd),
                sems(4, n_x), sems(4, n_x), sems(2, n_u), sems(2, n_u), sems(2, n_u), sems(2, n_u),
                sems(4, NCH), sems(4, NCH), sems(4, NJ), sems(4, NJ), sems(NJ), sems(NJ),
                sems(2, tiles), sems(NX), sems(NX), sems(NX),
            ],
            compiler_params=pltpu.CompilerParams(collective_id=1, has_side_effects=True, vmem_limit_bytes=VMEM_LIMIT),
            name="mlp_part",
        )(h_blk, w_all, w_down)
        return y_blk[None]

    return jax.shard_map(
        layer,
        mesh=mesh,
        in_specs=(act_spec, col_spec, col_spec, col_spec, row_spec, col_spec, col_spec, row_spec),
        out_specs=act_spec,
        check_vma=False,
    )
```

```python
import functools

import jax
import jax.numpy as jnp
from jax import lax
from jax.experimental import pallas as pl
from jax.experimental.pallas import tpu as pltpu
from jax.sharding import PartitionSpec as P

HEAD_DIM = 128
EPS = 1e-5
THETA = 10000.0
MESH = pl.DeviceIdType.MESH
F32 = jnp.float32
BF16 = jnp.bfloat16
NX = 4
NJ = 4
NCH = 16
VMEM_LIMIT = 67_043_328


def rem(a, b):
    return lax.rem(a, jnp.int32(b))


def div(a, b):
    return lax.div(a, jnp.int32(b))


def al(v, m):
    return pl.multiple_of(v, m)


def remote(src, dst, ssem, rsem, dev):
    return pltpu.make_async_remote_copy(src_ref=src, dst_ref=dst, send_sem=ssem, recv_sem=rsem, device_id=dev, device_id_type=MESH)


ATTENTION_STEPS = (
    ("S", "b", 1, 1), ("WA", 0), ("XP", 2), ("XE", 3), ("S", "b", 0, 0), ("XP", 3), ("S", "b", 1, 0), ("XP", 0), ("WOP",),
    ("XE", 0), ("WP", 0), ("O", "b", 1), ("ST", 3), ("WA", 1), ("ST", 0), ("S", "b", 0, 1), ("XP", 1), ("O", "b", 0),
    ("XE", 1), ("N", 3), ("WP", 1), ("XE", 2), ("XE", 4), ("ST", 1), ("YH", 3), ("G", 3, 2), ("G", 1, 2), ("O", "a", 1),
    ("N", 1), ("F", "a", 0), ("F", "a", 1), ("ST", 2), ("G", 2, 2), ("S", "a", 1, 0), ("N", 0), ("G", 0, 0), ("YH", 1),
    ("N", 2), ("S", "a", 0, 1), ("S", "a", 1, 1), ("ST", 4), ("YH", 0), ("R", 3, 2), ("O", "a", 0), ("F", "b", 1), ("N", 4),
    ("G", 1, 0), ("G", 3, 0), ("G", 0, 3), ("R", 2, 2), ("G", 2, 0), ("R", 1, 2), ("R", 3, 0), ("YH", 2), ("G", 1, 1),
    ("R", 1, 0), ("R", 0, 3), ("A", 3, 0), ("YH", 4), ("R", 2, 0), ("G", 1, 3), ("G", 3, 1), ("G", 2, 1), ("A", 1, 0),
    ("A", 2, 0), ("R", 3, 1), ("G", 3, 3), ("A", 3, 1), ("G", 2, 3), ("P", 2, 0), ("R", 1, 1), ("P", 1, 0), ("R", 2, 1),
    ("R", 1, 3), ("A", 2, 1), ("R", 0, 0), ("A", 2, 2), ("A", 3, 2), ("P", 3, 0), ("R", 3, 3), ("A", 1, 1), ("R", 2, 3),
    ("P", 2, 1), ("DP", 1), ("X", 2, 0), ("A", 2, 3), ("X", 1, 0), ("A", 1, 2), ("A", 3, 3), ("P", 3, 2), ("A", 1, 3),
    ("P", 3, 1), ("X", 2, 1), ("X", 3, 0), ("P", 1, 2), ("P", 2, 2), ("P", 2, 3), ("P", 1, 1), ("M", 0), ("P", 3, 3),
    ("G", 0, 1), ("G", 0, 2), ("X", 2, 2), ("X", 3, 1), ("P", 1, 3), ("X", 1, 1), ("M", 1), ("S", "a", 0, 0), ("A", 0, 0),
    ("X", 3, 2), ("X", 1, 2), ("F", "b", 0), ("R", 0, 2), ("X", 2, 3), ("M", 2), ("X", 1, 3), ("R", 0, 1), ("A", 0, 1),
    ("A", 0, 2), ("X", 3, 3), ("M", 3), ("A", 0, 3), ("DP", 0), ("P", 0, 0), ("P", 0, 1), ("P", 0, 2), ("P", 0, 3),
    ("X", 0, 0), ("T", 0), ("X", 0, 1), ("X", 0, 2), ("T", 1), ("T", 2), ("X", 0, 3), ("T", 3),
)
MLP_STEPS = (
    ("XF", 0, 1), ("XF", 0, 2), ("YR", 0), ("XH", 0, 1), ("YRH", 0), ("XH", 0, 2), ("XF", 3, 0), ("XF", 0, 3), ("N", 0, 1),
    ("XF", 2, 0), ("N", 0, 2), ("YH", 1), ("XH", 0, 3), ("XF", 0, 4), ("WT", 0), ("XH", 2, 0), ("XF", 1, 0), ("WT", 1),
    ("XH", 3, 0), ("WT", 2), ("N", 0, 3), ("YH", 2), ("XF", 0, 0), ("N", 3, 0), ("XH", 1, 0), ("WT", 3), ("XH", 0, 4),
    ("N", 2, 0), ("G", 3, 1), ("N", 1, 0), ("G", 3, 0), ("XH", 0, 0), ("G", 2, 0), ("G", 1, 0), ("YH", 3), ("P", 3, 0),
    ("G", 1, 1), ("P", 3, 1), ("G", 1, 2), ("G", 2, 1), ("G", 0, 2), ("N", 0, 4), ("P", 1, 2), ("P", 2, 1), ("P", 1, 0),
    ("G", 2, 2), ("P", 1, 1), ("G", 3, 2), ("G", 0, 1), ("P", 2, 0), ("P", 0, 2), ("X", 3, 1), ("X", 3, 0), ("P", 2, 2),
    ("X", 1, 0), ("X", 2, 1), ("YH", 4), ("G", 1, 3), ("X", 1, 1), ("G", 3, 3), ("N", 0, 0), ("X", 2, 0), ("P", 3, 2),
    ("M", 1), ("X", 2, 2), ("G", 2, 3), ("M", 0), ("P", 1, 3), ("P", 3, 3), ("X", 3, 2), ("X", 1, 2), ("M", 2), ("P", 2, 3),
    ("G", 0, 0), ("G", 0, 3), ("X", 2, 3), ("P", 0, 1), ("P", 0, 0), ("X", 1, 3), ("X", 3, 3), ("M", 3), ("P", 0, 3),
    ("X", 0, 2), ("T", 2), ("X", 0, 1), ("T", 1), ("X", 0, 0), ("T", 0), ("X", 0, 3), ("T", 3),
)


class Place:
    def __init__(self):
        tx, ty = lax.axis_index("tx"), lax.axis_index("ty")
        self.x, self.c, self.y = div(tx, 2), rem(tx, 2), ty
        x, c, y = self.x, self.c, self.y
        self.xr, self.xl, self.xo = rem(x + 1, NX), rem(x + 3, NX), rem(x + 2, NX)
        self.yu, self.yd, self.yo = rem(y + 1, NX), rem(y + 3, NX), rem(y + 2, NX)
        self.right = {"tx": self.xr * 2 + c, "ty": y}
        self.left = {"tx": self.xl * 2 + c, "ty": y}
        self.up = {"tx": tx, "ty": self.yu}
        self.down = {"tx": tx, "ty": self.yd}
        self.partner = {"tx": x * 2 + 1 - c, "ty": y}
        self.xa, self.xb = x + 1 - 2 * rem(x, 2), rem(x + 3 + 2 * rem(x, 2), NX)
        self.pa, self.pb = {"tx": self.xa * 2 + c, "ty": y}, {"tx": self.xb * 2 + c, "ty": y}

    def barrier(self):
        sem = pltpu.get_barrier_semaphore()
        for dev in (self.right, self.left, self.up, self.down, self.partner):
            pl.semaphore_signal(sem, inc=1, device_id=dev, device_id_type=MESH)
        pl.semaphore_wait(sem, 5)


class Spread:
    def __init__(self, at, src, xg, units, sx, rx, sy, ry, syh, ryh):
        self.at, self.src, self.xg, self.units, self.kc = at, src, xg, units, src.shape[2]
        self.sx, self.rx, self.sy, self.ry, self.syh, self.ryh = sx, rx, sy, ry, syh, ryh
        pairs = [(r, u) for u, unit in enumerate(units) for r in ((0, 3, 1, 2) if unit[3] else (0,))]
        self.index = {pair: i for i, pair in enumerate(pairs)}
        self.seqs = (at.y, at.yu, at.yo, at.yd)

    def cols(self, x):
        return pl.ds(al(x * self.kc, 128), self.kc)

    def keep_own(self):
        for j in range(NJ):
            self.xg[self.at.y, j, :, self.cols(self.at.x)] = self.src[j]

    def xcopy(self, kind, r, u):
        at, s = self.at, self.seqs[r]
        j, lo, n, _ = self.units[u]
        i = self.index[r, u]
        if kind < 2:
            dst = self.xg.at[s, j, pl.ds(lo, n), self.cols(at.x)]
            src = self.src.at[j, pl.ds(lo, n)] if r == 0 else dst
        elif kind == 2:
            src = dst = self.xg.at[s, j, pl.ds(lo, n // 2), self.cols(at.xl)]
        else:
            src = dst = self.xg.at[s, j, pl.ds(lo + n // 2, n // 2), self.cols(at.xr)]
        return remote(src, dst, self.sx.at[kind, i], self.rx.at[kind, i], at.left if kind % 2 else at.right)

    def xwait(self, kind, r, u):
        at = self.at
        j, lo, n, _ = self.units[u]
        i = self.index[r, u]
        x = (at.xl, at.xr, at.xo, at.xo)[kind]
        rows = (pl.ds(lo, n), pl.ds(lo, n), pl.ds(lo, n // 2), pl.ds(lo + n // 2, n // 2))[kind]
        dst = self.xg.at[self.seqs[r], j, rows, self.cols(x)]
        remote(dst, dst, self.sx.at[kind, i], self.rx.at[kind, i], at.right).wait_recv()

    def yref(self, s, u, lo, n):
        j, _, _, first = self.units[u]
        rows = pl.ds(lo, n)
        return self.xg.at[s, j, rows, self.cols(self.at.x)] if first else self.xg.at[s, j, rows]

    def ycopy(self, d, u):
        j, lo, n, first = self.units[u]
        dst = self.yref(self.at.y, u, lo, n)
        src = self.src.at[j, pl.ds(lo, n)] if first else dst
        return remote(src, dst, self.sy.at[d, u], self.ry.at[d, u], self.at.down if d else self.at.up)

    def ywait(self, d, u):
        _, lo, n, _ = self.units[u]
        dst = self.yref(self.at.yu if d else self.at.yd, u, lo, n)
        remote(dst, dst, self.sy.at[d, u], self.ry.at[d, u], self.at.up).wait_recv()

    def yhalf(self, d, u):
        _, lo, n, _ = self.units[u]
        ref = self.yref(self.at.yu if d else self.at.yd, u, lo + d * (n // 2), n // 2)
        return remote(ref, ref, self.syh.at[d, u], self.ryh.at[d, u], self.at.down if d else self.at.up)

    def yhalf_wait(self, d, u):
        _, lo, n, _ = self.units[u]
        dst = self.yref(self.at.yo, u, lo + d * (n // 2), n // 2)
        remote(dst, dst, self.syh.at[d, u], self.ryh.at[d, u], self.at.up).wait_recv()

    def YR(self, u):
        for d in range(2):
            self.ycopy(d, u).start()

    def YH(self, u):
        for d in range(2):
            self.ywait(d, u)
            self.yhalf(d, u).start()

    YRH = YH

    def XF(self, r, u):
        if r == 2:
            for d in range(2):
                self.yhalf_wait(d, u)
        for kind in range(2):
            self.xcopy(kind, r, u).start()

    def XH(self, r, u):
        for kind in range(2):
            self.xwait(kind, r, u)
            self.xcopy(kind + 2, r, u).start()

    def N(self, r, u):
        j, lo, n, first = self.units[u]
        for kind in (2, 3):
            self.xwait(kind, r, u)
            self.xcopy(kind, r, u).wait_send()
        if r:
            for kind in range(2):
                self.xcopy(kind, r, u).wait_send()
        if r % 2:
            self.yhalf(0 if r == 3 else 1, u).wait_send()
        width, rows, s = self.xg.shape[-1], 8, self.seqs[r]

        def body(i, carry):
            at_rows = pl.ds(al(lo + i * rows, rows), rows)
            v = self.xg[s, j, at_rows, :].astype(F32)
            mean = jnp.sum(v, axis=-1, keepdims=True) / width
            var = jnp.sum(v * v, axis=-1, keepdims=True) / width - mean * mean
            self.xg[s, j, at_rows, :] = ((v - mean) * lax.rsqrt(var + EPS)).astype(BF16)
            return carry

        lax.fori_loop(0, n // rows, body, 0)
        if not first:
            self.YR(u)

    def chunk_wait(self, r, j):
        if r == 2:
            for u, unit in enumerate(self.units):
                if unit[0] == j and not unit[3]:
                    for d in range(2):
                        self.yhalf_wait(d, u)

    def drain(self):
        for u, unit in enumerate(self.units):
            for d in range(2):
                self.xcopy(d, 0, u).wait_send()
                self.ycopy(d, u).wait_send()
                if not unit[3]:
                    self.yhalf(d, u).wait_send()


class Reduce:
    def __init__(self, at, zb, ya, yb, yfd, yfu, ss, rs):
        self.at, self.zb, self.ya, self.yb, self.yfd, self.yfu, self.ss, self.rs = at, zb, ya, yb, yfd, yfu, ss, rs
        self.ch = zb.shape[2]
        self.h = self.ch // 2

    def copy(self, kind, j):
        at, h, ch = self.at, self.h, self.ch
        src, dst = (
            lambda: (self.zb.at[2, j, pl.ds(0, h)], self.ya.at[j]),
            lambda: (self.zb.at[2, j, pl.ds(h, ch - h)], self.yb.at[j]),
            lambda: (self.zb.at[1, j], self.yfd.at[j]),
            lambda: (self.zb.at[3, j], self.yfu.at[j]),
        )[kind]()
        return remote(src, dst, self.ss.at[kind, j], self.rs.at[kind, j], at.down if kind % 2 else at.up)

    def wait(self, kind, j):
        self.copy(kind, j).wait_recv()

    def halves(self, j):
        self.copy(0, j).start()
        self.copy(1, j).start()

    def middle(self, j):
        h = self.h
        self.wait(0, j)
        self.zb[1, j, 0:h] = (self.zb[1, j, 0:h].astype(F32) + self.ya[j].astype(F32)).astype(BF16)
        self.copy(2, j).start()
        self.wait(1, j)
        self.zb[3, j, h:] = (self.zb[3, j, h:].astype(F32) + self.yb[j].astype(F32)).astype(BF16)
        self.copy(3, j).start()

    def total(self, j):
        self.wait(2, j)
        self.wait(3, j)
        return self.zb[0, j].astype(F32) + self.yfd[j].astype(F32) + self.yfu[j].astype(F32)

    def drain(self):
        for j in range(NJ):
            for kind in range(4):
                self.copy(kind, j).wait_send()


def attention_kernel(
    units, x_ref, cos_ref, sin_ref, wq, wk, wv, wo, wg_t, wu_t,
    h_ref, w_all,
    xc, xg, st_own, st_in, wb, wob, part, precv, qb, kvo, kvp, og, zb, ya, yb, yfd, yfu, own, drel_a, drel_b,
    sxe, rxe, sst, rst, sy, ry, syh, ryh, sd, rd, swa, rwa, swo, rwo, swp, rwp, lw, so, ro, spr, rpr, skv, rkv, sog, rog, syr, ryr,
    lg, sds, rds, sdo, rdo, sdf, rdf, sdp, rdp,
):
    at = Place()
    x, c, y = at.x, at.c, at.y
    ch, kc, h = xc.shape[1], xc.shape[2], xc.shape[1] // 2
    kd = wq.shape[0]
    hc = qb.shape[2]
    fc, f_a = w_all.shape[1], drel_a.shape[1]
    width = 2 * xg.shape[3]
    kh = div(x, 2)
    ng = rem(div(x + 1, 2), 2)
    gather = Spread(at, xc, xg, units, None, None, sy, ry, syh, ryh)
    reduce = Reduce(at, zb, ya, yb, yfd, yfu, syr, ryr)
    weights = (wq, wk, wv)

    def half_cols(core):
        return pl.ds(al(core * kd, 128), kd)

    def x_rows(j, core):
        return pl.ds(al((2 * j + core) * ch, 8), ch)

    def x_pair(j):
        return remote(x_ref.at[x_rows(j, 1 - c)], xc.at[j, :, half_cols(c)], sd.at[j], rd.at[j], at.partner)

    def pair_cols(xx):
        return pl.ds(al(rem(xx, 2) * kc, 128), kc)

    def xe_copy(u, xx):
        j, lo, n, _ = units[u]
        rows = pl.ds(lo, n)
        return remote(xc.at[j, rows], xg.at[y, j, rows, pair_cols(xx)], sxe.at[u], rxe.at[u], at.pa)

    def st_copy(u):
        j, lo, n, _ = units[u]
        rows = pl.ds(lo, n)
        return remote(st_own.at[j, rows], st_in.at[j, rows], sst.at[u], rst.at[u], at.pb)

    def XP(j):
        x_pair(j).start()

    def XE(u):
        j, lo, n, _ = units[u]
        if lo == 0:
            dst = xc.at[j, :, half_cols(1 - c)]
            remote(dst, dst, sd.at[j], rd.at[j], at.partner).wait_recv()
        xe_copy(u, x).start()
        xg[y, j, lo : lo + n, pair_cols(x)] = xc[j, lo : lo + n]

    def ST(u):
        j, lo, n, _ = units[u]
        xe_copy(u, at.xa).wait_recv()
        lane = lax.broadcasted_iota(jnp.int32, (8, 128), 1)

        def body(i, carry):
            rows = pl.ds(al(lo + i * 8, 8), 8)
            v = xg[y, j, rows, :].astype(F32)
            total, square = jnp.sum(v, axis=-1, keepdims=True), jnp.sum(v * v, axis=-1, keepdims=True)
            st_own[j, rows, :] = jnp.where(lane < 64, total, square)
            return carry

        lax.fori_loop(0, n // 8, body, 0)
        st_copy(u).start()

    def N(u):
        j, lo, n, _ = units[u]
        st_copy(u).wait_recv()

        def body(i, carry):
            rows = pl.ds(al(lo + i * 8, 8), 8)
            moments = (st_own[j, rows, :] + st_in[j, rows, :]) / width
            mean = moments[:, 0:1]
            var = moments[:, 64:65] - mean * mean
            v = xg[y, j, rows, :].astype(F32)
            xg[y, j, rows, :] = ((v - mean) * lax.rsqrt(var + EPS)).astype(BF16)
            return carry

        lax.fori_loop(0, n // 8, body, 0)
        gather.YR(u)

    def w_rows(xx, core):
        return pl.ds(al(rem(xx, 2) * kc + core * kd, 128), kd)

    def w_part(group, half, i):
        return weights[i].at[:, pl.ds(al((2 * group + half) * hc, 128), hc)]

    def w_cols(half, i):
        return pl.ds(half * 3 * hc + i * hc, hc)

    def wa_copy(half, i, xx):
        return remote(w_part(1 - ng, half, i), wb.at[w_rows(xx, c), w_cols(half, i)], swa.at[half, i], rwa.at[half, i], at.pa)

    def wo_copy(half, i, core):
        return remote(w_part(ng, half, i), wb.at[w_rows(x, core), w_cols(half, i)], swo.at[half, i], rwo.at[half, i], at.partner)

    def w_local(half, i):
        return pltpu.make_async_copy(w_part(ng, half, i), wb.at[w_rows(x, c), w_cols(half, i)], lw.at[half, i])

    def wp_copy(half, core):
        ref = wb.at[w_rows(at.xa, core), pl.ds(half * 3 * hc, 3 * hc)]
        return remote(ref, ref, swp.at[half], rwp.at[half], at.partner)

    o_local = pltpu.make_async_copy(wo, wob.at[:, half_cols(c)], lw.at[2, 0])
    o_pair = remote(wo, wob.at[:, half_cols(c)], so.at[0], ro.at[0], at.partner)
    pieces = [(half, i) for half in range(2) for i in range(3)]

    def WOP():
        for half, i in pieces:
            wo_copy(half, i, c).start()
        o_pair.start()

    def WA(half):
        for i in range(3):
            wa_copy(half, i, x).start()

    def WP(half):
        for i in range(3):
            wa_copy(half, i, at.xa).wait_recv()
        wp_copy(half, c).start()

    def w_ready():
        for half, i in pieces:
            w_local(half, i).wait()
            wo_copy(half, i, 1 - c).wait_recv()
        for half in range(2):
            wp_copy(half, 1 - c).wait_recv()
        for m in range(2):
            d_in(m).wait()
            d_out(m).start()
            d_pair(m, 3, c).start()

    def o_ready():
        o_local.wait()
        dst = wob.at[:, half_cols(1 - c)]
        remote(dst, dst, so.at[0], ro.at[0], at.partner).wait_recv()

    mlp_weights = (wg_t, wu_t)
    parts = ((0, f_a), (f_a, fc - f_a))

    def d_src(m, xx, p):
        return mlp_weights[m].at[pl.ds(al(xx * fc + parts[p][0], 8), parts[p][1])]

    def d_dst(m, xx, p):
        return w_all.at[m, pl.ds(*parts[p]), pl.ds(al((2 * xx + c) * kd, 128), kd)]

    def s_copy(d, m, p, xx):
        to, dev = ((at.xa, at.pa), (at.xb, at.pb))[d]
        return remote(d_src(m, to, p), d_dst(m, xx, p), sds.at[d, m, p], rds.at[d, m, p], dev)

    def o_copy(d, m):
        return remote(d_src(m, at.xo, d), (drel_a, drel_b)[d].at[m], sdo.at[d, m], rdo.at[d, m], (at.pa, at.pb)[d])

    def f_copy(d, m, xx):
        return remote((drel_a, drel_b)[d].at[m], d_dst(m, xx, d), sdf.at[d, m], rdf.at[d, m], (at.pb, at.pa)[d])

    def d_in(m):
        return pltpu.make_async_copy(mlp_weights[m].at[pl.ds(al(x * fc, 8), fc)], own.at[m], lg.at[0, m])

    def d_all(m, xx, core):
        return w_all.at[m, :, pl.ds(al((2 * xx + core) * kd, 128), kd)]

    def d_out(m):
        return pltpu.make_async_copy(own.at[m], d_all(m, x, c), lg.at[1, m])

    def d_pair(m, k, core):
        dst = d_all(m, (at.xa, at.xb, at.xo, x)[k], core)
        return remote(own.at[m] if k == 3 else dst, dst, sdp.at[m, k], rdp.at[m, k], at.partner)

    def S(link, m, p):
        s_copy("ab".index(link), m, p, x).start()

    def O(link, m):
        o_copy("ab".index(link), m).start()

    def F(link, m):
        d = "ba".index(link)
        o_copy(d, m).wait_recv()
        f_copy(d, m, (at.xa, at.xb)[d]).start()

    def DP(m):
        for d in range(2):
            for p in range(2):
                s_copy(d, m, p, (at.xa, at.xb)[d]).wait_recv()
            f_copy(d, m, at.xo).wait_recv()
        for k in range(3):
            d_pair(m, k, c).start()

    def pr_copy(n):
        src = part.at[n, :, pl.ds(al((1 - kh) * 3 * hc, 128), 3 * hc)]
        return remote(src, precv.at[n], spr.at[n], rpr.at[n], at.pb)

    def G(r, j):
        gather.chunk_wait(r, j)
        s, n = gather.seqs[r], r * NJ + j

        def columns(i, carry):
            cols = pl.ds(al(i * 256, 128), 256)
            part[n, :, cols] = jnp.dot(xg[s, j], wb[:, cols], preferred_element_type=F32).astype(BF16)
            return carry

        lax.fori_loop(0, wb.shape[1] // 256, columns, 0)
        pr_copy(n).start()

    def kv_copy(r, j):
        s, n = gather.seqs[r], r * NJ + j
        return remote(kvo.at[s, j], kvp.at[s, j], skv.at[n], rkv.at[n], at.partner)

    def R(r, j):
        s, n = gather.seqs[r], r * NJ + j
        pr_copy(n).wait_recv()
        rows = pl.ds(al((2 * j + c) * ch, 8), ch)
        cos_t, sin_t = cos_ref[rows, :], sin_ref[rows, :]

        def total(col, size):
            mine = part[n, :, pl.ds(al(kh * 3 * hc + col, 128), size)]
            return (mine.astype(F32) + precv[n, :, col : col + size].astype(F32)).astype(BF16)

        def turned(col):
            v = total(col, HEAD_DIM).astype(F32)
            return (v * cos_t + pltpu.roll(v, HEAD_DIM // 2, axis=1) * sin_t).astype(BF16)

        for col in range(0, hc, HEAD_DIM):
            qb[n, :, col : col + HEAD_DIM] = turned(col)
            kvo[s, j, :, col : col + HEAD_DIM] = turned(hc + col)
        kvo[s, j, :, hc:] = total(2 * hc, hc)
        kv_copy(r, j).start()

    def o_cols(xx):
        return pl.ds(al((2 * rem(div(xx + 1, 2), 2) + div(xx, 2)) * hc, 128), hc)

    def og_copy(kind, n):
        if kind < 2:
            ref = og.at[n, :, o_cols(x)]
        elif kind == 2:
            ref = og.at[n, pl.ds(0, h), o_cols(at.xa)]
        else:
            ref = og.at[n, pl.ds(h, ch - h), o_cols(at.xb)]
        return remote(ref, ref, sog.at[kind, n], rog.at[kind, n], at.pa if kind in (0, 3) else at.pb)

    def og_wait(kind, n):
        xx = (at.xa, at.xb, at.xo, at.xo)[kind]
        rows = (pl.ds(0, ch), pl.ds(0, ch), pl.ds(0, h), pl.ds(h, ch - h))[kind]
        dst = og.at[n, rows, o_cols(xx)]
        remote(dst, dst, sog.at[kind, n], rog.at[kind, n], at.pa).wait_recv()

    def A(r, j):
        s, n = gather.seqs[r], r * NJ + j
        kv_copy(r, j).wait_recv()
        keys = (j + 1) * ch
        iq = lax.broadcasted_iota(jnp.int32, (ch, keys), 0) + j * ch
        ik = lax.broadcasted_iota(jnp.int32, (ch, keys), 1)
        own_ok = iq >= ik
        par_ok = ik < (j + c) * ch
        contract = (((1,), (1,)), ((), ()))
        first = (2 * ng + kh) * hc
        for lo in range(0, hc, HEAD_DIM):
            q = qb[n, :, lo : lo + HEAD_DIM]
            k_own = kvo[s, 0 : j + 1, :, lo : lo + HEAD_DIM].reshape(keys, HEAD_DIM)
            k_par = kvp[s, 0 : j + 1, :, lo : lo + HEAD_DIM].reshape(keys, HEAD_DIM)
            s_own = lax.dot_general(q, k_own, contract, preferred_element_type=F32) * HEAD_DIM**-0.5
            s_par = lax.dot_general(q, k_par, contract, preferred_element_type=F32) * HEAD_DIM**-0.5
            s_own = jnp.where(own_ok, s_own, -1e30)
            s_par = jnp.where(par_ok, s_par, -1e30)
            top = jnp.maximum(jnp.max(s_own, axis=1, keepdims=True), jnp.max(s_par, axis=1, keepdims=True))
            e_own, e_par = jnp.exp(s_own - top), jnp.exp(s_par - top)
            inv = 1.0 / (jnp.sum(e_own, axis=1, keepdims=True) + jnp.sum(e_par, axis=1, keepdims=True))
            v_own = kvo[s, 0 : j + 1, :, hc + lo : hc + lo + HEAD_DIM].reshape(keys, HEAD_DIM)
            v_par = kvp[s, 0 : j + 1, :, hc + lo : hc + lo + HEAD_DIM].reshape(keys, HEAD_DIM)
            out = jnp.dot((e_own * inv).astype(BF16), v_own, preferred_element_type=F32)
            out += jnp.dot((e_par * inv).astype(BF16), v_par, preferred_element_type=F32)
            og[n, :, pl.ds(al(first + lo, 128), HEAD_DIM)] = out.astype(BF16)
        og_copy(0, n).start()
        og_copy(1, n).start()

    def P(r, j):
        n = r * NJ + j
        for kind in range(2):
            og_wait(kind, n)
            og_copy(kind + 2, n).start()

    def X(r, j):
        n = r * NJ + j
        og_wait(2, n)
        og_wait(3, n)

        def columns(i, carry):
            cols = pl.ds(al(i * 256, 128), 256)
            zb[r, j, :, cols] = jnp.dot(og[n], wob[:, cols], preferred_element_type=F32).astype(BF16)
            return carry

        lax.fori_loop(0, kc // 256, columns, 0)
        if r == 2:
            reduce.halves(j)

    def T(j):
        attn = reduce.total(j).astype(BF16)
        h_ref[j] = (xc[j].astype(F32) + attn.astype(F32)).astype(BF16)

    for half, i in pieces:
        w_local(half, i).start()
    o_local.start()
    for m in range(2):
        d_in(m).start()
    for j in range(NJ):
        xc[j, :, half_cols(c)] = x_ref[x_rows(j, c), :]
    at.barrier()
    ops = {
        "XP": XP, "WOP": WOP, "XE": XE, "ST": ST, "N": N, "YH": gather.YH, "WA": WA, "WP": WP, "S": S, "O": O, "F": F, "DP": DP,
        "G": G, "R": R, "A": A, "P": P, "X": X, "M": reduce.middle, "T": T,
    }
    waits = {"G": w_ready, "X": o_ready}
    for step in ATTENTION_STEPS:
        if step[0] in waits:
            waits.pop(step[0])()
        ops[step[0]](*step[1:])

    for m in range(2):
        for k in range(4):
            d_pair(m, k, 1 - c).wait_recv()
            d_pair(m, k, c).wait_send()
        d_out(m).wait()
        for d in range(2):
            for p in range(2):
                s_copy(d, m, p, x).wait_send()
            o_copy(d, m).wait_send()
            f_copy(d, m, x).wait_send()
    for j in range(NJ):
        x_pair(j).wait_send()
    for u in range(len(units)):
        xe_copy(u, x).wait_send()
        st_copy(u).wait_send()
        for d in range(2):
            gather.ycopy(d, u).wait_send()
            gather.yhalf(d, u).wait_send()
    reduce.drain()
    o_pair.wait_send()
    for half, i in pieces:
        wa_copy(half, i, x).wait_send()
        wo_copy(half, i, c).wait_send()
    for half in range(2):
        wp_copy(half, c).wait_send()

    def chunk_sent(n, carry):
        pr_copy(n).wait_send()
        remote(kvo.at[0, 0], kvp.at[0, 0], skv.at[n], rkv.at[n], at.partner).wait_send()
        for kind in range(4):
            og_copy(kind, n).wait_send()
        return carry

    lax.fori_loop(0, NCH, chunk_sent, 0)


def mlp_kernel(
    units, h_ref, w_hbm, wdn, y_ref,
    xg, wt, raw, wd, ag, acc, zb, ya, yb, yfd, yfu, yst,
    sx, rx, sy, ry, syh, ryh, sa, ra, syr, ryr, sd, rd, lw, lwd, swd, rwd,
):
    at = Place()
    x, c, y = at.x, at.c, at.y
    ch, kc, h = h_ref.shape[1], h_ref.shape[2], h_ref.shape[1] // 2
    width = xg.shape[-1]
    kd = kc // 2
    fc, tiles = w_hbm.shape[1], wt.shape[1] // 256
    fp = tiles * 128
    blocks, slots = 2 * tiles, raw.shape[0]
    gather = Spread(at, h_ref, xg, units, sx, rx, sy, ry, syh, ryh)
    reduce = Reduce(at, zb, ya, yb, yfd, yfu, syr, ryr)

    def w_in(q):
        i, m = q // 2, q % 2
        n = min(128, fc - i * 128)
        return pltpu.make_async_copy(w_hbm.at[m, pl.ds(i * 128, n)], raw.at[q % slots, pl.ds(0, n)], lw.at[q])

    def WT(g):
        for q in range(g * blocks // 4, (g + 1) * blocks // 4):
            i, m, slot = q // 2, q % 2, q % slots
            w_in(q).wait()
            if fc < (i + 1) * 128:
                raw[slot, fc - i * 128 :, :] = jnp.zeros(((i + 1) * 128 - fc, width), BF16)

            def turn(k, carry, slot=slot, q=q):
                part = pl.ds(al(k * (width // 4), 128), width // 4)
                wt[part, q * 128 : (q + 1) * 128] = raw[slot, :, part].T
                return carry

            lax.fori_loop(0, 4, turn, 0)
            if q + slots < blocks:
                w_in(q + slots).start()

    def d_own(q):
        return pltpu.make_async_copy(wdn.at[pl.ds(q * fc, fc)], wd.at[pl.ds(q * fp, fc), pl.ds(al(c * kd, 128), kd)], lwd.at[q])

    def d_pair(q):
        dst = wd.at[pl.ds(q * fp, fc), pl.ds(al(c * kd, 128), kd)]
        return remote(wdn.at[pl.ds(q * fc, fc)], dst, swd.at[q], rwd.at[q], at.partner)

    def d_pair_wait(q):
        dst = wd.at[pl.ds(q * fp, fc), pl.ds(al((1 - c) * kd, 128), kd)]
        remote(dst, dst, swd.at[q], rwd.at[q], at.partner).wait_recv()

    for q in range(slots):
        w_in(q).start()
    for q in range(NX):
        d_own(q).start()
        if fc < fp:
            wd[q * fp + fc : (q + 1) * fp, :] = jnp.zeros((fp - fc, kc), BF16)
    at.barrier()
    for q in range(NX):
        d_pair(q).start()

    def a_cols(xx):
        return pl.ds(al(xx * fp, 128), fp)

    def a_copy(kind, n):
        if kind < 2:
            ref = ag.at[n, :, a_cols(x)]
        elif kind == 2:
            ref = ag.at[n, pl.ds(0, h), a_cols(at.xl)]
        else:
            ref = ag.at[n, pl.ds(h, ch - h), a_cols(at.xr)]
        return remote(ref, ref, sa.at[kind, n], ra.at[kind, n], at.left if kind % 2 else at.right)

    def a_wait(kind, n):
        xx = (at.xl, at.xr, at.xo, at.xo)[kind]
        rows = (pl.ds(0, ch), pl.ds(0, ch), pl.ds(0, h), pl.ds(h, ch - h))[kind]
        dst = ag.at[n, rows, a_cols(xx)]
        remote(dst, dst, sa.at[kind, n], ra.at[kind, n], at.right).wait_recv()

    def G(r, j):
        gather.chunk_wait(r, j)
        s, n = gather.seqs[r], r * NJ + j

        def columns(i, carry):
            acc[...] = jnp.zeros_like(acc)
            cols = pl.ds(al(i * 256, 128), 256)

            def depth(k, carry):
                part = pl.ds(al(k * (width // 2), 128), width // 2)
                acc[...] += jnp.dot(xg[s, j, :, part], wt[part, cols], preferred_element_type=F32)
                return carry

            lax.fori_loop(0, 2, depth, 0)
            out = acc[...]
            g, u = out[:, :128].astype(BF16).astype(F32), out[:, 128:].astype(BF16).astype(F32)
            ag[n, :, pl.ds(al(x * fp + i * 128, 128), 128)] = (g / (1.0 + jnp.exp(-g)) * u).astype(BF16)
            return carry

        lax.fori_loop(0, tiles, columns, 0)
        for kind in range(2):
            a_copy(kind, n).start()

    def P(r, j):
        n = r * NJ + j
        for kind in range(2):
            a_wait(kind, n)
            a_copy(kind + 2, n).start()

    def X(r, j):
        n = r * NJ + j
        for kind in (2, 3):
            a_wait(kind, n)

        def columns(i, carry):
            cols = pl.ds(al(i * 256, 128), 256)
            acc[...] = jnp.zeros_like(acc)

            def depth(k, carry):
                part = pl.ds(al(k * 2 * fp, 128), 2 * fp)
                acc[...] += jnp.dot(ag[n, :, part], wd[part, cols], preferred_element_type=F32)
                return carry

            lax.fori_loop(0, 2, depth, 0)
            zb[r, j, :, cols] = acc[...].astype(BF16)
            return carry

        lax.fori_loop(0, kc // 256, columns, 0)
        if r == 2:
            reduce.halves(j)

    def y_rows(j, core):
        return pl.ds(al((2 * j + core) * ch, 8), ch)

    def y_copy(j):
        return remote(yst.at[1 - c, j], y_ref.at[y_rows(j, c)], sd.at[j], rd.at[j], at.partner)

    def y_wait(j):
        dst = y_ref.at[y_rows(j, 1 - c)]
        remote(dst, dst, sd.at[j], rd.at[j], at.partner).wait_recv()

    def T(j):
        mlp = reduce.total(j).astype(BF16)
        out = (h_ref[j].astype(F32) + mlp.astype(F32)).astype(BF16)
        yst[0, j] = out[:, :kd]
        yst[1, j] = out[:, kd:]
        y_copy(j).start()
        y_ref[y_rows(j, c), :] = yst[c, j]

    ops = {"G": G, "P": P, "X": X, "M": reduce.middle, "T": T, "WT": WT}
    for name in ("YR", "YRH", "YH", "XF", "XH", "N"):
        ops[name] = getattr(gather, name)
    waits = {
        "N": gather.keep_own,
        "X": lambda: [(d_own(q).wait(), d_pair_wait(q)) for q in range(NX)],
    }
    for step in MLP_STEPS:
        if step[0] in waits:
            waits.pop(step[0])()
        ops[step[0]](*step[1:])

    gather.drain()
    reduce.drain()
    for q in range(NX):
        d_pair(q).wait_send()

    def chunk_sent(n, carry):
        for kind in range(4):
            a_copy(kind, n).wait_send()
        return carry

    lax.fori_loop(0, NCH, chunk_sent, 0)
    for j in range(NJ):
        y_copy(j).wait_send()
        y_wait(j)


def vmem(*shape, dtype=BF16):
    return pltpu.VMEM(shape, dtype)


def sems(*shape):
    return pltpu.SemaphoreType.DMA(shape)


def solution(mesh):
    assert mesh.shape["tx"] == 2 * NX and mesh.shape["ty"] == NX
    act_spec = P(("dp", "ty"), None, "tx")
    col_spec = P("tx", "ty")
    row_spec = P("ty", "tx")
    any_spec = pl.BlockSpec(memory_space=pl.ANY)
    vmem_spec = pl.BlockSpec(memory_space=pltpu.VMEM)

    def layer(x_blk, w_q, w_k, w_v, w_o, w_gate, w_up, w_down):
        _, seq, kd = x_blk.shape
        kc, width = 2 * kd, 2 * NX * kd
        ch = seq // (2 * NJ)
        h = ch // 2
        row_heads = w_q.shape[1]
        hc = row_heads // NX
        fc = w_down.shape[0] // NX
        assert hc % HEAD_DIM == 0
        tiles = (fc + 127) // 128
        f_a = (fc // 2 + 15) // 16 * 16

        half = HEAD_DIM // 2
        inv_freq = THETA ** (-2.0 * jnp.arange(half, dtype=F32) / HEAD_DIM)
        angles = jnp.arange(seq, dtype=F32)[:, None] * inv_freq[None, :]
        cos_t, sin_t = jnp.cos(angles), jnp.sin(angles)
        cos_t = jnp.concatenate([cos_t, cos_t], axis=1)
        sin_t = jnp.concatenate([-sin_t, sin_t], axis=1)

        reduce_scratch = [vmem(NX, NJ, ch, kc), vmem(NJ, h, kc), vmem(NJ, ch - h, kc), vmem(NJ, ch, kc), vmem(NJ, ch, kc)]
        units = ((0, 0, h, 0), (0, h, h, 0)) + tuple((j, 0, ch, 0) for j in range(1, NJ))
        n_u = len(units)
        h_blk, w_all = pl.pallas_call(
            functools.partial(attention_kernel, units),
            out_shape=(jax.ShapeDtypeStruct((NJ, ch, kc), BF16), jax.ShapeDtypeStruct((2, fc, width), BF16)),
            in_specs=[vmem_spec] * 3 + [any_spec] * 6,
            out_specs=(vmem_spec, any_spec),
            scratch_shapes=[
                vmem(NJ, ch, kc), vmem(NX, NJ, ch, 2 * kc), vmem(NJ, ch, 128, dtype=F32), vmem(NJ, ch, 128, dtype=F32),
                vmem(2 * kc, 6 * hc), vmem(row_heads, kc), vmem(NCH, ch, 6 * hc), vmem(NCH, ch, 3 * hc), vmem(NCH, ch, hc),
                vmem(NX, NJ, ch, 2 * hc), vmem(NX, NJ, ch, 2 * hc), vmem(NCH, ch, row_heads), *reduce_scratch,
                vmem(2, fc, kd), vmem(2, f_a, kd), vmem(2, fc - f_a, kd),
                sems(n_u), sems(n_u), sems(n_u), sems(n_u), sems(2, n_u), sems(2, n_u), sems(2, n_u), sems(2, n_u),
                sems(NJ), sems(NJ), sems(2, 3), sems(2, 3), sems(2, 3), sems(2, 3), sems(2), sems(2), sems(3, 3), sems(1), sems(1),
                sems(NCH), sems(NCH), sems(NCH), sems(NCH), sems(4, NCH), sems(4, NCH), sems(4, NJ), sems(4, NJ),
                sems(2, 2), sems(2, 2, 2), sems(2, 2, 2), sems(2, 2), sems(2, 2), sems(2, 2), sems(2, 2), sems(2, 4), sems(2, 4),
            ],
            compiler_params=pltpu.CompilerParams(collective_id=0, has_side_effects=True, vmem_limit_bytes=VMEM_LIMIT),
            name="attention_part",
        )(x_blk[0], cos_t, sin_t, w_q, w_k, w_v, w_o, w_gate.T, w_up.T)

        first = ch * 3 // 4
        units = ((0, 0, first, 1), (0, first, ch - first, 0)) + tuple((j, 0, ch, 0) for j in range(1, NJ))
        n_x = n_u + 3
        y_blk = pl.pallas_call(
            functools.partial(mlp_kernel, units),
            out_shape=jax.ShapeDtypeStruct((seq, kd), BF16),
            in_specs=[vmem_spec, any_spec, any_spec],
            out_specs=vmem_spec,
            scratch_shapes=[
                vmem(NX, NJ, ch, width), vmem(width, tiles * 256), vmem(3, 128, width), vmem(NX * tiles * 128, kc), vmem(NCH, ch, NX * tiles * 128),
                vmem(ch, 256, dtype=F32),
                *reduce_scratch, vmem(2, NJ, ch, kd),
                sems(4, n_x), sems(4, n_x), sems(2, n_u), sems(2, n_u), sems(2, n_u), sems(2, n_u),
                sems(4, NCH), sems(4, NCH), sems(4, NJ), sems(4, NJ), sems(NJ), sems(NJ),
                sems(2 * tiles), sems(NX), sems(NX), sems(NX),
            ],
            compiler_params=pltpu.CompilerParams(collective_id=1, has_side_effects=True, vmem_limit_bytes=VMEM_LIMIT),
            name="mlp_part",
        )(h_blk, w_all, w_down)
        return y_blk[None]

    return jax.shard_map(
        layer,
        mesh=mesh,
        in_specs=(act_spec, col_spec, col_spec, col_spec, row_spec, col_spec, col_spec, row_spec),
        out_specs=act_spec,
        check_vma=False,
    )
```

```python
import functools

import jax
import jax.numpy as jnp
import numpy as np
from jax import lax
from jax.experimental import pallas as pl
from jax.experimental.pallas import tpu as pltpu
from jax.sharding import PartitionSpec as P

HEAD_DIM = 128
EPS = 1e-5
THETA = 10000.0
MESH = pl.DeviceIdType.MESH
F32 = jnp.float32
BF16 = jnp.bfloat16
NX = 4
NJ = 4
NCH = 16
VMEM_LIMIT = 67_043_328


def rem(a, b):
    return lax.rem(a, jnp.int32(b))


def div(a, b):
    return lax.div(a, jnp.int32(b))


def al(v, m):
    return pl.multiple_of(v, m)


def remote(src, dst, ssem, rsem, dev):
    return pltpu.make_async_remote_copy(src_ref=src, dst_ref=dst, send_sem=ssem, recv_sem=rsem, device_id=dev, device_id_type=MESH)


ATTENTION_STEPS = (
    ("XP", 2), ("O", "b", 0), ("S", "b", 1, 1), ("XE", 3), ("WA", 0), ("XP", 3), ("WA", 1), ("WOP",), ("XP", 0), ("XE", 0),
    ("ST", 3), ("S", "b", 1, 0), ("N", 3), ("S", "b", 0, 0), ("XP", 1), ("S", "b", 0, 1), ("XE", 1), ("XE", 2), ("O", "b", 1),
    ("WP", 0), ("WP", 1), ("YH", 3), ("ST", 0), ("G", 1, 2), ("O", "a", 1), ("XE", 4), ("N", 0), ("ST", 1), ("G", 3, 2),
    ("F", "a", 0), ("G", 2, 2), ("ST", 2), ("N", 1), ("S", "a", 1, 0), ("G", 0, 0), ("YH", 0), ("F", "b", 1), ("YH", 1),
    ("R", 1, 2), ("F", "a", 1), ("G", 1, 0), ("N", 2), ("ST", 4), ("G", 2, 0), ("G", 3, 0), ("YH", 2), ("O", "a", 0),
    ("R", 2, 2), ("N", 4), ("G", 0, 3), ("G", 3, 1), ("R", 1, 0), ("R", 2, 0), ("G", 1, 1), ("R", 3, 0), ("G", 2, 1),
    ("S", "a", 0, 1), ("A", 1, 0), ("YH", 4), ("S", "a", 1, 1), ("G", 1, 3), ("R", 3, 1), ("R", 2, 1), ("R", 0, 0),
    ("A", 3, 0), ("R", 1, 1), ("R", 3, 2), ("A", 2, 0), ("A", 2, 1), ("P", 1, 0), ("G", 2, 3), ("A", 1, 1), ("A", 3, 1),
    ("P", 2, 0), ("A", 2, 2), ("P", 2, 1), ("G", 3, 3), ("DP", 1), ("R", 2, 3), ("R", 1, 3), ("A", 3, 2), ("P", 3, 1),
    ("X", 1, 0), ("P", 3, 0), ("X", 2, 0), ("P", 2, 2), ("A", 2, 3), ("A", 1, 2), ("X", 2, 1), ("G", 0, 2), ("P", 1, 1),
    ("R", 3, 3), ("P", 3, 2), ("X", 2, 2), ("X", 3, 0), ("M", 0), ("P", 2, 3), ("A", 3, 3), ("X", 3, 1), ("P", 1, 2),
    ("A", 1, 3), ("G", 0, 1), ("X", 1, 1), ("M", 1), ("S", "a", 0, 0), ("X", 1, 2), ("X", 2, 3), ("R", 0, 2), ("F", "b", 0),
    ("X", 3, 2), ("R", 0, 3), ("P", 3, 3), ("P", 1, 3), ("R", 0, 1), ("A", 0, 0), ("A", 0, 1), ("M", 2), ("A", 0, 2),
    ("A", 0, 3), ("X", 3, 3), ("X", 1, 3), ("M", 3), ("DP", 0), ("P", 0, 0), ("P", 0, 1), ("P", 0, 2), ("P", 0, 3),
    ("X", 0, 0), ("T", 0), ("X", 0, 1), ("X", 0, 2), ("T", 1), ("T", 2), ("X", 0, 3), ("T", 3),
)
MLP_STEPS = (
    ("YR", 0), ("XF", 0, 1), ("XF", 0, 3), ("XH", 0, 1), ("XF", 0, 2), ("WT", 0), ("YRH", 0), ("XH", 0, 3), ("WT", 1),
    ("XF", 0, 0), ("N", 0, 1), ("XH", 0, 2), ("XF", 0, 4), ("XF", 0, 5), ("WT", 2), ("N", 0, 3), ("N", 0, 2), ("XF", 2, 0),
    ("XH", 0, 0), ("XH", 0, 4), ("YH", 1), ("YH", 3), ("XH", 2, 0), ("XF", 3, 0), ("XF", 1, 0), ("YH", 2), ("WT", 3),
    ("XH", 0, 5), ("N", 0, 4), ("G", 0, 1), ("G", 3, 1), ("N", 0, 5), ("XH", 3, 0), ("N", 0, 0), ("G", 1, 1), ("G", 2, 1),
    ("P", 3, 1), ("XH", 1, 0), ("P", 1, 1), ("P", 2, 1), ("G", 0, 3), ("N", 2, 0), ("G", 2, 0), ("G", 0, 0), ("N", 1, 0),
    ("N", 3, 0), ("YH", 4), ("G", 1, 2), ("G", 1, 0), ("X", 3, 1), ("G", 3, 2), ("X", 1, 1), ("G", 3, 0), ("P", 0, 1),
    ("YH", 5), ("P", 2, 0), ("G", 1, 3), ("X", 2, 1), ("G", 3, 3), ("P", 3, 0), ("X", 2, 0), ("G", 2, 2), ("P", 1, 0),
    ("X", 3, 0), ("P", 1, 2), ("P", 2, 2), ("G", 2, 3), ("M", 1), ("X", 1, 0), ("P", 3, 2), ("X", 2, 2), ("X", 0, 1),
    ("P", 2, 3), ("P", 1, 3), ("M", 0), ("G", 0, 2), ("P", 3, 3), ("X", 1, 2), ("X", 2, 3), ("X", 3, 2), ("M", 2), ("P", 0, 3),
    ("X", 1, 3), ("T", 1), ("P", 0, 2), ("P", 0, 0), ("X", 3, 3), ("M", 3), ("X", 0, 3), ("X", 0, 0), ("X", 0, 2), ("T", 2),
    ("T", 0), ("T", 3),
)


class Place:
    def __init__(self):
        tx, ty = lax.axis_index("tx"), lax.axis_index("ty")
        self.x, self.c, self.y = div(tx, 2), rem(tx, 2), ty
        x, c, y = self.x, self.c, self.y
        self.xr, self.xl, self.xo = rem(x + 1, NX), rem(x + 3, NX), rem(x + 2, NX)
        self.yu, self.yd, self.yo = rem(y + 1, NX), rem(y + 3, NX), rem(y + 2, NX)
        self.right = {"tx": self.xr * 2 + c, "ty": y}
        self.left = {"tx": self.xl * 2 + c, "ty": y}
        self.up = {"tx": tx, "ty": self.yu}
        self.down = {"tx": tx, "ty": self.yd}
        self.partner = {"tx": x * 2 + 1 - c, "ty": y}
        self.xa, self.xb = x + 1 - 2 * rem(x, 2), rem(x + 3 + 2 * rem(x, 2), NX)
        self.pa, self.pb = {"tx": self.xa * 2 + c, "ty": y}, {"tx": self.xb * 2 + c, "ty": y}

    def barrier(self):
        sem = pltpu.get_barrier_semaphore()
        for dev in (self.right, self.left, self.up, self.down, self.partner):
            pl.semaphore_signal(sem, inc=1, device_id=dev, device_id_type=MESH)
        pl.semaphore_wait(sem, 5)


class Spread:
    def __init__(self, at, src, xg, units, sx, rx, sy, ry, syh, ryh):
        self.at, self.src, self.xg, self.units, self.kc = at, src, xg, units, src.shape[2]
        self.sx, self.rx, self.sy, self.ry, self.syh, self.ryh = sx, rx, sy, ry, syh, ryh
        pairs = [(r, u) for u, unit in enumerate(units) for r in ((0, 3, 1, 2) if unit[3] else (0,))]
        self.index = {pair: i for i, pair in enumerate(pairs)}
        self.seqs = (at.y, at.yu, at.yo, at.yd)

    def cols(self, x):
        return pl.ds(al(x * self.kc, 128), self.kc)

    def keep_own(self):
        for j in range(NJ):
            self.xg[self.at.y, j, :, self.cols(self.at.x)] = self.src[j]

    def xcopy(self, kind, r, u):
        at, s = self.at, self.seqs[r]
        j, lo, n, _ = self.units[u]
        i = self.index[r, u]
        if kind < 2:
            dst = self.xg.at[s, j, pl.ds(lo, n), self.cols(at.x)]
            src = self.src.at[j, pl.ds(lo, n)] if r == 0 else dst
        elif kind == 2:
            src = dst = self.xg.at[s, j, pl.ds(lo, n // 2), self.cols(at.xl)]
        else:
            src = dst = self.xg.at[s, j, pl.ds(lo + n // 2, n // 2), self.cols(at.xr)]
        return remote(src, dst, self.sx.at[kind, i], self.rx.at[kind, i], at.left if kind % 2 else at.right)

    def xwait(self, kind, r, u):
        at = self.at
        j, lo, n, _ = self.units[u]
        i = self.index[r, u]
        x = (at.xl, at.xr, at.xo, at.xo)[kind]
        rows = (pl.ds(lo, n), pl.ds(lo, n), pl.ds(lo, n // 2), pl.ds(lo + n // 2, n // 2))[kind]
        dst = self.xg.at[self.seqs[r], j, rows, self.cols(x)]
        remote(dst, dst, self.sx.at[kind, i], self.rx.at[kind, i], at.right).wait_recv()

    def yref(self, s, u, lo, n):
        j, _, _, first = self.units[u]
        rows = pl.ds(lo, n)
        return self.xg.at[s, j, rows, self.cols(self.at.x)] if first else self.xg.at[s, j, rows]

    def ycopy(self, d, u):
        j, lo, n, first = self.units[u]
        dst = self.yref(self.at.y, u, lo, n)
        src = self.src.at[j, pl.ds(lo, n)] if first else dst
        return remote(src, dst, self.sy.at[d, u], self.ry.at[d, u], self.at.down if d else self.at.up)

    def ywait(self, d, u):
        _, lo, n, _ = self.units[u]
        dst = self.yref(self.at.yu if d else self.at.yd, u, lo, n)
        remote(dst, dst, self.sy.at[d, u], self.ry.at[d, u], self.at.up).wait_recv()

    def yhalf(self, d, u):
        _, lo, n, _ = self.units[u]
        ref = self.yref(self.at.yu if d else self.at.yd, u, lo + d * (n // 2), n // 2)
        return remote(ref, ref, self.syh.at[d, u], self.ryh.at[d, u], self.at.down if d else self.at.up)

    def yhalf_wait(self, d, u):
        _, lo, n, _ = self.units[u]
        dst = self.yref(self.at.yo, u, lo + d * (n // 2), n // 2)
        remote(dst, dst, self.syh.at[d, u], self.ryh.at[d, u], self.at.up).wait_recv()

    def YR(self, u):
        for d in range(2):
            self.ycopy(d, u).start()

    def YH(self, u):
        for d in range(2):
            self.ywait(d, u)
            self.yhalf(d, u).start()

    YRH = YH

    def XF(self, r, u):
        if r == 2:
            for d in range(2):
                self.yhalf_wait(d, u)
        for kind in range(2):
            self.xcopy(kind, r, u).start()

    def XH(self, r, u):
        for kind in range(2):
            self.xwait(kind, r, u)
            self.xcopy(kind + 2, r, u).start()

    def N(self, r, u):
        j, lo, n, first = self.units[u]
        for kind in (2, 3):
            self.xwait(kind, r, u)
            self.xcopy(kind, r, u).wait_send()
        if r:
            for kind in range(2):
                self.xcopy(kind, r, u).wait_send()
        if r % 2:
            self.yhalf(0 if r == 3 else 1, u).wait_send()
        width, rows, s = self.xg.shape[-1], 8, self.seqs[r]

        def body(i, carry):
            at_rows = pl.ds(al(lo + i * rows, rows), rows)
            v = self.xg[s, j, at_rows, :].astype(F32)
            mean = jnp.sum(v, axis=-1, keepdims=True) / width
            var = jnp.sum(v * v, axis=-1, keepdims=True) / width - mean * mean
            self.xg[s, j, at_rows, :] = ((v - mean) * lax.rsqrt(var + EPS)).astype(BF16)
            return carry

        lax.fori_loop(0, n // rows, body, 0)
        if not first:
            self.YR(u)

    def chunk_wait(self, r, j):
        if r == 2:
            for u, unit in enumerate(self.units):
                if unit[0] == j and not unit[3]:
                    for d in range(2):
                        self.yhalf_wait(d, u)

    def drain(self):
        for u, unit in enumerate(self.units):
            for d in range(2):
                self.xcopy(d, 0, u).wait_send()
                self.ycopy(d, u).wait_send()
                if not unit[3]:
                    self.yhalf(d, u).wait_send()


class Reduce:
    def __init__(self, at, zb, ya, yb, yfd, yfu, ss, rs):
        self.at, self.zb, self.ya, self.yb, self.yfd, self.yfu, self.ss, self.rs = at, zb, ya, yb, yfd, yfu, ss, rs
        self.ch = zb.shape[2]
        self.h = self.ch // 2

    def copy(self, kind, j):
        at, h, ch = self.at, self.h, self.ch
        src, dst = (
            lambda: (self.zb.at[2, j, pl.ds(0, h)], self.ya.at[j]),
            lambda: (self.zb.at[2, j, pl.ds(h, ch - h)], self.yb.at[j]),
            lambda: (self.zb.at[1, j], self.yfd.at[j]),
            lambda: (self.zb.at[3, j], self.yfu.at[j]),
        )[kind]()
        return remote(src, dst, self.ss.at[kind, j], self.rs.at[kind, j], at.down if kind % 2 else at.up)

    def wait(self, kind, j):
        self.copy(kind, j).wait_recv()

    def halves(self, j):
        self.copy(0, j).start()
        self.copy(1, j).start()

    def middle(self, j):
        h = self.h
        self.wait(0, j)
        self.zb[1, j, 0:h] = (self.zb[1, j, 0:h].astype(F32) + self.ya[j].astype(F32)).astype(BF16)
        self.copy(2, j).start()
        self.wait(1, j)
        self.zb[3, j, h:] = (self.zb[3, j, h:].astype(F32) + self.yb[j].astype(F32)).astype(BF16)
        self.copy(3, j).start()

    def total(self, j):
        self.wait(2, j)
        self.wait(3, j)
        return self.zb[0, j].astype(F32) + self.yfd[j].astype(F32) + self.yfu[j].astype(F32)

    def drain(self):
        for j in range(NJ):
            for kind in range(4):
                self.copy(kind, j).wait_send()


def attention_kernel(
    units, x_ref, turn_ref, base_ref, wq, wk, wv, wo, wg_t, wu_t,
    h_ref, w_all,
    xc, xg, cos_all, sin_all, st_own, st_in, wb, wob, part, precv, qb, kvo, kvp, og, zb, ya, yb, yfd, yfu, own, drel_a, drel_b,
    sxe, rxe, sst, rst, sy, ry, syh, ryh, sd, rd, swa, rwa, swo, rwo, swp, rwp, lw, so, ro, spr, rpr, skv, rkv, sog, rog, syr, ryr,
    lg, sds, rds, sdo, rdo, sdf, rdf, sdp, rdp,
):
    at = Place()
    x, c, y = at.x, at.c, at.y
    ch, kc = xc.shape[1], xc.shape[2]
    kd = wq.shape[0]
    hc = qb.shape[2]
    fc, f_a = w_all.shape[1], drel_a.shape[1]
    width = 2 * xg.shape[3]
    kh = div(x, 2)
    ng = rem(div(x + 1, 2), 2)
    gather = Spread(at, xc, xg, units, None, None, sy, ry, syh, ryh)
    reduce = Reduce(at, zb, ya, yb, yfd, yfu, syr, ryr)
    weights = (wq, wk, wv)

    def half_cols(core):
        return pl.ds(al(core * kd, 128), kd)

    def x_rows(j, core):
        return pl.ds(al((2 * j + core) * ch, 8), ch)

    def x_pair(j):
        return remote(x_ref.at[x_rows(j, 1 - c)], xc.at[j, :, half_cols(c)], sd.at[j], rd.at[j], at.partner)

    def pair_cols(xx):
        return pl.ds(al(rem(xx, 2) * kc, 128), kc)

    def xe_copy(u, xx):
        j, lo, n, _ = units[u]
        rows = pl.ds(lo, n)
        return remote(xc.at[j, rows], xg.at[y, j, rows, pair_cols(xx)], sxe.at[u], rxe.at[u], at.pa)

    def st_copy(u):
        j, lo, n, _ = units[u]
        rows = pl.ds(lo // 4, n // 4)
        return remote(st_own.at[j, rows], st_in.at[j, rows], sst.at[u], rst.at[u], at.pb)

    def XP(j):
        x_pair(j).start()

    def XE(u):
        j, lo, n, _ = units[u]
        if lo == 0:
            dst = xc.at[j, :, half_cols(1 - c)]
            remote(dst, dst, sd.at[j], rd.at[j], at.partner).wait_recv()
        xe_copy(u, x).start()
        xg[y, j, lo : lo + n, pair_cols(x)] = xc[j, lo : lo + n]

    def ST(u):
        j, lo, n, _ = units[u]
        xe_copy(u, at.xa).wait_recv()
        lane = lax.broadcasted_iota(jnp.int32, (8, 128), 1)

        def body(i, carry):
            packed = jnp.zeros((8, 128), F32)
            for g in range(4):
                v = xg[y, j, pl.ds(al(lo + g * (n // 4) + i * 8, 8), 8), :].astype(F32)
                total, square = jnp.sum(v, axis=-1, keepdims=True), jnp.sum(v * v, axis=-1, keepdims=True)
                packed = jnp.where(lane // 32 == g, jnp.where(lane % 32 < 16, total, square), packed)
            st_own[j, pl.ds(al(lo // 4 + i * 8, 8), 8), :] = packed
            return carry

        lax.fori_loop(0, n // 32, body, 0)
        st_copy(u).start()

    def N(u):
        j, lo, n, _ = units[u]
        st_copy(u).wait_recv()

        def body(i, carry):
            at_rows = pl.ds(al(lo // 4 + i * 8, 8), 8)
            moments = (st_own[j, at_rows, :] + st_in[j, at_rows, :]) / width
            for g in range(4):
                rows = pl.ds(al(lo + g * (n // 4) + i * 8, 8), 8)
                mean = moments[:, 32 * g : 32 * g + 1]
                var = moments[:, 32 * g + 16 : 32 * g + 17] - mean * mean
                v = xg[y, j, rows, :].astype(F32)
                xg[y, j, rows, :] = ((v - mean) * lax.rsqrt(var + EPS)).astype(BF16)
            return carry

        lax.fori_loop(0, n // 32, body, 0)
        gather.YR(u)

    def w_rows(xx, core):
        return pl.ds(al(rem(xx, 2) * kc + core * kd, 128), kd)

    def w_part(group, half, i):
        return weights[i].at[:, pl.ds(al((2 * group + half) * hc, 128), hc)]

    def w_cols(half, i):
        return pl.ds(half * 3 * hc + i * hc, hc)

    def wa_copy(half, i, xx):
        return remote(w_part(1 - ng, half, i), wb.at[w_rows(xx, c), w_cols(half, i)], swa.at[half, i], rwa.at[half, i], at.pa)

    def wo_copy(half, i, core):
        return remote(w_part(ng, half, i), wb.at[w_rows(x, core), w_cols(half, i)], swo.at[half, i], rwo.at[half, i], at.partner)

    def w_local(half, i):
        return pltpu.make_async_copy(w_part(ng, half, i), wb.at[w_rows(x, c), w_cols(half, i)], lw.at[half, i])

    def wp_copy(half, core):
        ref = wb.at[w_rows(at.xa, core), pl.ds(half * 3 * hc, 3 * hc)]
        return remote(ref, ref, swp.at[half], rwp.at[half], at.partner)

    o_local = pltpu.make_async_copy(wo, wob.at[:, half_cols(c)], lw.at[2, 0])
    o_pair = remote(wo, wob.at[:, half_cols(c)], so.at[0], ro.at[0], at.partner)
    pieces = [(half, i) for half in range(2) for i in range(3)]

    def WOP():
        for half, i in pieces:
            wo_copy(half, i, c).start()
        o_pair.start()

    def WA(half):
        for i in range(3):
            wa_copy(half, i, x).start()

    def WP(half):
        for i in range(3):
            wa_copy(half, i, at.xa).wait_recv()
        wp_copy(half, c).start()

    def w_ready():
        for half, i in pieces:
            w_local(half, i).wait()
            wo_copy(half, i, 1 - c).wait_recv()
        for half in range(2):
            wp_copy(half, 1 - c).wait_recv()
        for m in range(2):
            d_in(m).wait()
            d_out(m).start()
            d_pair(m, 3, c).start()

    def o_ready():
        o_local.wait()
        dst = wob.at[:, half_cols(1 - c)]
        remote(dst, dst, so.at[0], ro.at[0], at.partner).wait_recv()

    mlp_weights = (wg_t, wu_t)
    parts = ((0, f_a), (f_a, fc - f_a))

    def d_src(m, xx, p):
        return mlp_weights[m].at[pl.ds(al(xx * fc + parts[p][0], 8), parts[p][1])]

    def d_dst(m, xx, p):
        return w_all.at[m, pl.ds(*parts[p]), pl.ds(al((2 * xx + c) * kd, 128), kd)]

    def s_copy(d, m, p, xx):
        to, dev = ((at.xa, at.pa), (at.xb, at.pb))[d]
        return remote(d_src(m, to, p), d_dst(m, xx, p), sds.at[d, m, p], rds.at[d, m, p], dev)

    def o_copy(d, m):
        return remote(d_src(m, at.xo, d), (drel_a, drel_b)[d].at[m], sdo.at[d, m], rdo.at[d, m], (at.pa, at.pb)[d])

    def f_copy(d, m, xx):
        return remote((drel_a, drel_b)[d].at[m], d_dst(m, xx, d), sdf.at[d, m], rdf.at[d, m], (at.pb, at.pa)[d])

    def d_in(m):
        return pltpu.make_async_copy(mlp_weights[m].at[pl.ds(al(x * fc, 8), fc)], own.at[m], lg.at[0, m])

    def d_all(m, xx, core):
        return w_all.at[m, :, pl.ds(al((2 * xx + core) * kd, 128), kd)]

    def d_out(m):
        return pltpu.make_async_copy(own.at[m], d_all(m, x, c), lg.at[1, m])

    def d_pair(m, k, core):
        dst = d_all(m, (at.xa, at.xb, at.xo, x)[k], core)
        return remote(own.at[m] if k == 3 else dst, dst, sdp.at[m, k], rdp.at[m, k], at.partner)

    def S(link, m, p):
        s_copy("ab".index(link), m, p, x).start()

    def O(link, m):
        o_copy("ab".index(link), m).start()

    def F(link, m):
        d = "ba".index(link)
        o_copy(d, m).wait_recv()
        f_copy(d, m, (at.xa, at.xb)[d]).start()

    def DP(m):
        for d in range(2):
            for p in range(2):
                s_copy(d, m, p, (at.xa, at.xb)[d]).wait_recv()
            f_copy(d, m, at.xo).wait_recv()
        for k in range(3):
            d_pair(m, k, c).start()

    def pr_copy(n):
        src = part.at[n, :, pl.ds(al((1 - kh) * 3 * hc, 128), 3 * hc)]
        return remote(src, precv.at[n], spr.at[n], rpr.at[n], at.pb)

    def G(r, j):
        gather.chunk_wait(r, j)
        s, n = gather.seqs[r], r * NJ + j

        def columns(i, carry):
            cols = pl.ds(al(i * 256, 128), 256)
            part[n, :, cols] = jnp.dot(xg[s, j], wb[:, cols], preferred_element_type=F32).astype(BF16)
            return carry

        lax.fori_loop(0, wb.shape[1] // 256, columns, 0)
        pr_copy(n).start()

    def kv_copy(r, j):
        s, n = gather.seqs[r], r * NJ + j
        return remote(kvo.at[s, j], kvp.at[s, j], skv.at[n], rkv.at[n], at.partner)

    def R(r, j):
        s, n = gather.seqs[r], r * NJ + j
        pr_copy(n).wait_recv()
        cos_t, sin_t = cos_all[j], sin_all[j]

        def total(col, size):
            mine = part[n, :, pl.ds(al(kh * 3 * hc + col, 128), size)]
            return (mine.astype(F32) + precv[n, :, col : col + size].astype(F32)).astype(BF16)

        def turned(col):
            v = total(col, HEAD_DIM).astype(F32)
            return (v * cos_t + pltpu.roll(v, HEAD_DIM // 2, axis=1) * sin_t).astype(BF16)

        for col in range(0, hc, HEAD_DIM):
            qb[n, :, col : col + HEAD_DIM] = turned(col)
            kvo[s, j, :, col : col + HEAD_DIM] = turned(hc + col)
        kvo[s, j, :, hc:] = total(2 * hc, hc)
        kv_copy(r, j).start()

    def o_cols(xx):
        return pl.ds(al((2 * rem(div(xx + 1, 2), 2) + div(xx, 2)) * hc, 128), hc)

    cut = ch // 8

    def og_copy(kind, n):
        if kind < 2:
            ref = og.at[n, :, o_cols(x)]
        elif kind == 2:
            ref = og.at[n, pl.ds(0, cut), o_cols(at.xa)]
        else:
            ref = og.at[n, pl.ds(cut, ch - cut), o_cols(at.xb)]
        return remote(ref, ref, sog.at[kind, n], rog.at[kind, n], at.pa if kind in (0, 3) else at.pb)

    def og_wait(kind, n):
        xx = (at.xa, at.xb, at.xo, at.xo)[kind]
        rows = (pl.ds(0, ch), pl.ds(0, ch), pl.ds(0, cut), pl.ds(cut, ch - cut))[kind]
        dst = og.at[n, rows, o_cols(xx)]
        remote(dst, dst, sog.at[kind, n], rog.at[kind, n], at.pa).wait_recv()

    def A(r, j):
        s, n = gather.seqs[r], r * NJ + j
        kv_copy(r, j).wait_recv()
        keys = (j + 1) * ch
        iq = lax.broadcasted_iota(jnp.int32, (ch, keys), 0) + j * ch
        ik = lax.broadcasted_iota(jnp.int32, (ch, keys), 1)
        own_ok = iq >= ik
        par_ok = ik < (j + c) * ch
        contract = (((1,), (1,)), ((), ()))
        first = (2 * ng + kh) * hc

        def head(i, carry):
            cols = pl.ds(al(i * HEAD_DIM, 128), HEAD_DIM)
            v_cols = pl.ds(al(hc + i * HEAD_DIM, 128), HEAD_DIM)
            q = qb[n, :, cols]
            k_own = kvo[s, 0 : j + 1, :, cols].reshape(keys, HEAD_DIM)
            k_par = kvp[s, 0 : j + 1, :, cols].reshape(keys, HEAD_DIM)
            s_own = lax.dot_general(q, k_own, contract, preferred_element_type=F32) * HEAD_DIM**-0.5
            s_par = lax.dot_general(q, k_par, contract, preferred_element_type=F32) * HEAD_DIM**-0.5
            s_own = jnp.where(own_ok, s_own, -1e30)
            s_par = jnp.where(par_ok, s_par, -1e30)
            top = jnp.maximum(jnp.max(s_own, axis=1, keepdims=True), jnp.max(s_par, axis=1, keepdims=True))
            e_own, e_par = jnp.exp(s_own - top), jnp.exp(s_par - top)
            inv = 1.0 / (jnp.sum(e_own, axis=1, keepdims=True) + jnp.sum(e_par, axis=1, keepdims=True))
            v_own = kvo[s, 0 : j + 1, :, v_cols].reshape(keys, HEAD_DIM)
            v_par = kvp[s, 0 : j + 1, :, v_cols].reshape(keys, HEAD_DIM)
            out = jnp.dot((e_own * inv).astype(BF16), v_own, preferred_element_type=F32)
            out += jnp.dot((e_par * inv).astype(BF16), v_par, preferred_element_type=F32)
            og[n, :, pl.ds(al(first + i * HEAD_DIM, 128), HEAD_DIM)] = out.astype(BF16)
            return carry

        lax.fori_loop(0, hc // HEAD_DIM, head, 0)
        og_copy(0, n).start()
        og_copy(1, n).start()

    def P(r, j):
        n = r * NJ + j
        for kind in range(2):
            og_wait(kind, n)
            og_copy(kind + 2, n).start()

    def X(r, j):
        n = r * NJ + j
        og_wait(2, n)
        og_wait(3, n)

        def columns(i, carry):
            cols = pl.ds(al(i * 256, 128), 256)
            zb[r, j, :, cols] = jnp.dot(og[n], wob[:, cols], preferred_element_type=F32).astype(BF16)
            return carry

        lax.fori_loop(0, kc // 256, columns, 0)
        if r == 2:
            reduce.halves(j)

    def T(j):
        attn = reduce.total(j).astype(BF16)
        h_ref[j] = (xc[j].astype(F32) + attn.astype(F32)).astype(BF16)

    for half, i in pieces:
        w_local(half, i).start()
    o_local.start()
    for m in range(2):
        d_in(m).start()
    for j in range(NJ):
        xc[j, :, half_cols(c)] = x_ref[x_rows(j, c), :]
    at.barrier()

    def angles():
        lane = lax.broadcasted_iota(jnp.int32, (ch, HEAD_DIM), 1)
        for j in range(NJ):
            base_cos, base_sin = base_ref[0, pl.ds(2 * j + c, 1), :], base_ref[1, pl.ds(2 * j + c, 1), :]
            cos_all[j] = base_cos * turn_ref[0] - base_sin * turn_ref[1]
            sine = base_sin * turn_ref[0] + base_cos * turn_ref[1]
            sin_all[j] = jnp.where(lane < HEAD_DIM // 2, -sine, sine)

    ops = {
        "XP": XP, "WOP": WOP, "XE": XE, "ST": ST, "N": N, "YH": gather.YH, "WA": WA, "WP": WP, "S": S, "O": O, "F": F, "DP": DP,
        "G": G, "R": R, "A": A, "P": P, "X": X, "M": reduce.middle, "T": T,
    }
    waits = {"G": w_ready, "X": o_ready, "WP": angles}
    for step in ATTENTION_STEPS:
        if step[0] in waits:
            waits.pop(step[0])()
        ops[step[0]](*step[1:])

    for m in range(2):
        for k in range(4):
            d_pair(m, k, 1 - c).wait_recv()
            d_pair(m, k, c).wait_send()
        d_out(m).wait()
        for d in range(2):
            for p in range(2):
                s_copy(d, m, p, x).wait_send()
            o_copy(d, m).wait_send()
            f_copy(d, m, x).wait_send()
    for j in range(NJ):
        x_pair(j).wait_send()
    for u in range(len(units)):
        xe_copy(u, x).wait_send()
        st_copy(u).wait_send()
        for d in range(2):
            gather.ycopy(d, u).wait_send()
            gather.yhalf(d, u).wait_send()
    reduce.drain()
    o_pair.wait_send()
    for half, i in pieces:
        wa_copy(half, i, x).wait_send()
        wo_copy(half, i, c).wait_send()
    for half in range(2):
        wp_copy(half, c).wait_send()

    def chunk_sent(n, carry):
        pr_copy(n).wait_send()
        remote(kvo.at[0, 0], kvp.at[0, 0], skv.at[n], rkv.at[n], at.partner).wait_send()
        for kind in range(4):
            og_copy(kind, n).wait_send()
        return carry

    lax.fori_loop(0, NCH, chunk_sent, 0)


def mlp_kernel(
    units, h_ref, w_hbm, wdn, y_ref,
    xg, wt, raw, wd, wr, ag, ar, act, acc, zb, ya, yb, yfd, yfu, yst,
    sx, rx, sy, ry, syh, ryh, sa, ra, syr, ryr, sd, rd, lw, lwd, swd, rwd,
):
    at = Place()
    x, c, y = at.x, at.c, at.y
    ch, kc, h = h_ref.shape[1], h_ref.shape[2], h_ref.shape[1] // 2
    width = xg.shape[-1]
    kd = kc // 2
    fc, tiles = w_hbm.shape[1], wt.shape[1] // 256
    fm = (tiles - 1) * 128
    fr = fc - fm
    blocks, slots = 2 * tiles, raw.shape[0]
    gather = Spread(at, h_ref, xg, units, sx, rx, sy, ry, syh, ryh)
    reduce = Reduce(at, zb, ya, yb, yfd, yfu, syr, ryr)

    def w_in(q):
        i, m = q // 2, q % 2
        n = min(128, fc - i * 128)
        return pltpu.make_async_copy(w_hbm.at[m, pl.ds(i * 128, n)], raw.at[q % slots, pl.ds(0, n)], lw.at[q])

    def WT(g):
        for q in range(g * blocks // 4, (g + 1) * blocks // 4):
            i, m, slot = q // 2, q % 2, q % slots
            w_in(q).wait()
            if fc < (i + 1) * 128:
                raw[slot, fc - i * 128 :, :] = jnp.zeros(((i + 1) * 128 - fc, width), BF16)

            def turn(k, carry, slot=slot, q=q):
                part = pl.ds(al(k * (width // 4), 128), width // 4)
                wt[part, q * 128 : (q + 1) * 128] = raw[slot, :, part].T
                return carry

            lax.fori_loop(0, 4, turn, 0)
            if q + slots < blocks:
                w_in(q + slots).start()

    def d_refs(q, core):
        cols = pl.ds(al(core * kd, 128), kd)
        main, rest = wdn.at[pl.ds(q * fc, fm)], wdn.at[pl.ds(q * fc + fm, fr)]
        return (main, wd.at[pl.ds(q * fm, fm), cols]), (rest, wr.at[pl.ds(q * 128, fr), cols])

    def d_own(q, k):
        src, dst = d_refs(q, c)[k]
        return pltpu.make_async_copy(src, dst, lwd.at[q, k])

    def d_pair(q, k, core):
        src, dst = d_refs(q, core)[k]
        return remote(src, dst, swd.at[q, k], rwd.at[q, k], at.partner)

    quarters = [(q, k) for q in range(NX) for k in range(2)]
    for q in range(slots):
        w_in(q).start()
    for q, k in quarters:
        d_own(q, k).start()
    for q in range(NX):
        wr[q * 128 + fr : (q + 1) * 128, :] = jnp.zeros((128 - fr, kc), BF16)
    at.barrier()
    for q, k in quarters:
        d_pair(q, k, c).start()

    def a_refs(kind, n, xx):
        main, rest = pl.ds(al(xx * fm, 128), fm), pl.ds(al(xx * 128, 128), 128)
        if kind < 2:
            return ag.at[n, :, main], ar.at[n, :, rest]
        lo = (kind - 2) * h
        return ag.at[n, pl.ds(lo, h), main], ar.at[n, pl.ds(lo // 2, h // 2), rest]

    def a_copies(kind, n):
        refs = a_refs(kind, n, (x, x, at.xl, at.xr)[kind])
        return [remote(v, v, sa.at[kind, n, k], ra.at[kind, n, k], at.left if kind % 2 else at.right) for k, v in enumerate(refs)]

    def a_wait(kind, n):
        for k, v in enumerate(a_refs(kind, n, (at.xl, at.xr, at.xo, at.xo)[kind])):
            remote(v, v, sa.at[kind, n, k], ra.at[kind, n, k], at.right).wait_recv()

    def a_start(kind, n):
        for copy in a_copies(kind, n):
            copy.start()

    def G(r, j):
        gather.chunk_wait(r, j)
        s, n = gather.seqs[r], r * NJ + j

        def columns(i, carry):
            acc[...] = jnp.zeros_like(acc)
            cols = pl.ds(al(i * 256, 128), 256)

            def depth(k, carry):
                part = pl.ds(al(k * (width // 2), 128), width // 2)
                acc[...] += jnp.dot(xg[s, j, :, part], wt[part, cols], preferred_element_type=F32)
                return carry

            lax.fori_loop(0, 2, depth, 0)
            out = acc[...]
            g, u = out[:, :128].astype(BF16).astype(F32), out[:, 128:].astype(BF16).astype(F32)
            act[:, pl.ds(al(i * 128, 128), 128)] = (g / (1.0 + jnp.exp(-g)) * u).astype(BF16)
            return carry

        lax.fori_loop(0, tiles, columns, 0)
        ag[n, :, pl.ds(al(x * fm, 128), fm)] = act[:, :fm]
        below = pltpu.roll(act[h:, fm:].astype(F32), 64, axis=1)
        ar[n, :, pl.ds(al(x * 128, 128), 128)] = (act[:h, fm:].astype(F32) + below).astype(BF16)
        for kind in range(2):
            a_start(kind, n)

    def P(r, j):
        n = r * NJ + j
        for kind in range(2):
            a_wait(kind, n)
            a_start(kind + 2, n)

    def X(r, j):
        n = r * NJ + j
        for kind in (2, 3):
            a_wait(kind, n)
        for q in range(NX):
            cols = pl.ds(q * 128, 128)
            act[0:h, cols] = ar[n, :, cols]
            act[h:, cols] = pltpu.roll(ar[n, :, cols].astype(F32), 64, axis=1).astype(BF16)

        def columns(i, carry):
            cols = pl.ds(al(i * 256, 128), 256)
            acc[...] = jnp.dot(act[:, : NX * 128], wr[:, cols], preferred_element_type=F32)

            def depth(k, carry):
                part = pl.ds(al(k * 2 * fm, 128), 2 * fm)
                acc[...] += jnp.dot(ag[n, :, part], wd[part, cols], preferred_element_type=F32)
                return carry

            lax.fori_loop(0, 2, depth, 0)
            zb[r, j, :, cols] = acc[...].astype(BF16)
            return carry

        lax.fori_loop(0, kc // 256, columns, 0)
        if r == 2:
            reduce.halves(j)

    def y_rows(j, core):
        return pl.ds(al((2 * j + core) * ch, 8), ch)

    def y_copy(j):
        return remote(yst.at[1 - c, j], y_ref.at[y_rows(j, c)], sd.at[j], rd.at[j], at.partner)

    def y_wait(j):
        dst = y_ref.at[y_rows(j, 1 - c)]
        remote(dst, dst, sd.at[j], rd.at[j], at.partner).wait_recv()

    def T(j):
        mlp = reduce.total(j).astype(BF16)
        out = (h_ref[j].astype(F32) + mlp.astype(F32)).astype(BF16)
        yst[0, j] = out[:, :kd]
        yst[1, j] = out[:, kd:]
        y_copy(j).start()
        y_ref[y_rows(j, c), :] = yst[c, j]

    ops = {"G": G, "P": P, "X": X, "M": reduce.middle, "T": T, "WT": WT}
    for name in ("YR", "YRH", "YH", "XF", "XH", "N"):
        ops[name] = getattr(gather, name)
    waits = {
        "N": gather.keep_own,
        "X": lambda: [(d_own(q, k).wait(), d_pair(q, k, 1 - c).wait_recv()) for q, k in quarters],
    }
    for step in MLP_STEPS:
        if step[0] in waits:
            waits.pop(step[0])()
        ops[step[0]](*step[1:])

    gather.drain()
    reduce.drain()
    for q, k in quarters:
        d_pair(q, k, c).wait_send()

    def chunk_sent(n, carry):
        for kind in range(4):
            for copy in a_copies(kind, n):
                copy.wait_send()
        return carry

    lax.fori_loop(0, NCH, chunk_sent, 0)
    for j in range(NJ):
        y_copy(j).wait_send()
        y_wait(j)


def vmem(*shape, dtype=BF16):
    return pltpu.VMEM(shape, dtype)


def sems(*shape):
    return pltpu.SemaphoreType.DMA(shape)


def solution(mesh):
    assert mesh.shape["tx"] == 2 * NX and mesh.shape["ty"] == NX
    act_spec = P(("dp", "ty"), None, "tx")
    col_spec = P("tx", "ty")
    row_spec = P("ty", "tx")
    any_spec = pl.BlockSpec(memory_space=pl.ANY)
    vmem_spec = pl.BlockSpec(memory_space=pltpu.VMEM)

    def layer(x_blk, w_q, w_k, w_v, w_o, w_gate, w_up, w_down):
        _, seq, kd = x_blk.shape
        kc, width = 2 * kd, 2 * NX * kd
        ch = seq // (2 * NJ)
        h = ch // 2
        row_heads = w_q.shape[1]
        hc = row_heads // NX
        fc = w_down.shape[0] // NX
        assert hc % HEAD_DIM == 0
        tiles = (fc + 127) // 128
        f_a = (fc // 2 + 15) // 16 * 16

        inv_freq = THETA ** (-2.0 * np.arange(HEAD_DIM // 2) / HEAD_DIM)
        inv_freq = np.concatenate([inv_freq, inv_freq])
        turn = np.arange(ch)[:, None] * inv_freq
        base = np.arange(2 * NJ)[:, None] * ch * inv_freq
        turn = jnp.asarray(np.stack([np.cos(turn), np.sin(turn)]), F32)
        base = jnp.asarray(np.stack([np.cos(base), np.sin(base)]), F32)

        reduce_scratch = [vmem(NX, NJ, ch, kc), vmem(NJ, h, kc), vmem(NJ, ch - h, kc), vmem(NJ, ch, kc), vmem(NJ, ch, kc)]
        units = ((0, 0, h, 0), (0, h, h, 0)) + tuple((j, 0, ch, 0) for j in range(1, NJ))
        n_u = len(units)
        h_blk, w_all = pl.pallas_call(
            functools.partial(attention_kernel, units),
            out_shape=(jax.ShapeDtypeStruct((NJ, ch, kc), BF16), jax.ShapeDtypeStruct((2, fc, width), BF16)),
            in_specs=[vmem_spec] * 3 + [any_spec] * 6,
            out_specs=(vmem_spec, any_spec),
            scratch_shapes=[
                vmem(NJ, ch, kc), vmem(NX, NJ, ch, 2 * kc), vmem(NJ, ch, HEAD_DIM, dtype=F32), vmem(NJ, ch, HEAD_DIM, dtype=F32),
                vmem(NJ, ch // 4, 128, dtype=F32), vmem(NJ, ch // 4, 128, dtype=F32),
                vmem(2 * kc, 6 * hc), vmem(row_heads, kc), vmem(NCH, ch, 6 * hc), vmem(NCH, ch, 3 * hc), vmem(NCH, ch, hc),
                vmem(NX, NJ, ch, 2 * hc), vmem(NX, NJ, ch, 2 * hc), vmem(NCH, ch, row_heads), *reduce_scratch,
                vmem(2, fc, kd), vmem(2, f_a, kd), vmem(2, fc - f_a, kd),
                sems(n_u), sems(n_u), sems(n_u), sems(n_u), sems(2, n_u), sems(2, n_u), sems(2, n_u), sems(2, n_u),
                sems(NJ), sems(NJ), sems(2, 3), sems(2, 3), sems(2, 3), sems(2, 3), sems(2), sems(2), sems(3, 3), sems(1), sems(1),
                sems(NCH), sems(NCH), sems(NCH), sems(NCH), sems(4, NCH), sems(4, NCH), sems(4, NJ), sems(4, NJ),
                sems(2, 2), sems(2, 2, 2), sems(2, 2, 2), sems(2, 2), sems(2, 2), sems(2, 2), sems(2, 2), sems(2, 4), sems(2, 4),
            ],
            compiler_params=pltpu.CompilerParams(collective_id=0, has_side_effects=True, vmem_limit_bytes=VMEM_LIMIT),
            name="attention_part",
        )(x_blk[0], turn, base, w_q, w_k, w_v, w_o, w_gate.T, w_up.T)

        first = ch * 3 // 4
        units = ((0, 0, first, 1), (0, first, ch - first, 0), (1, 0, h, 0), (1, h, h, 0)) + tuple((j, 0, ch, 0) for j in range(2, NJ))
        n_u, n_x = len(units), len(units) + 3
        y_blk = pl.pallas_call(
            functools.partial(mlp_kernel, units),
            out_shape=jax.ShapeDtypeStruct((seq, kd), BF16),
            in_specs=[vmem_spec, any_spec, any_spec],
            out_specs=vmem_spec,
            scratch_shapes=[
                vmem(NX, NJ, ch, width), vmem(width, tiles * 256), vmem(3, 128, width),
                vmem(NX * (tiles - 1) * 128, kc), vmem(NX * 128, kc), vmem(NCH, ch, NX * (tiles - 1) * 128), vmem(NCH, h, NX * 128),
                vmem(ch, tiles * 128),
                vmem(ch, 256, dtype=F32),
                *reduce_scratch, vmem(2, NJ, ch, kd),
                sems(4, n_x), sems(4, n_x), sems(2, n_u), sems(2, n_u), sems(2, n_u), sems(2, n_u),
                sems(4, NCH, 2), sems(4, NCH, 2), sems(4, NJ), sems(4, NJ), sems(NJ), sems(NJ),
                sems(2 * tiles), sems(NX, 2), sems(NX, 2), sems(NX, 2),
            ],
            compiler_params=pltpu.CompilerParams(collective_id=1, has_side_effects=True, vmem_limit_bytes=VMEM_LIMIT),
            name="mlp_part",
        )(h_blk, w_all, w_down)
        return y_blk[None]

    return jax.shard_map(
        layer,
        mesh=mesh,
        in_specs=(act_spec, col_spec, col_spec, col_spec, row_spec, col_spec, col_spec, row_spec),
        out_specs=act_spec,
        check_vma=False,
    )
```

```python
import functools

import jax
import jax.numpy as jnp
import numpy as np
from jax import lax
from jax.experimental import pallas as pl
from jax.experimental.pallas import tpu as pltpu
from jax.sharding import PartitionSpec as P

HEAD_DIM = 128
EPS = 1e-5
THETA = 10000.0
MESH = pl.DeviceIdType.MESH
F32 = jnp.float32
BF16 = jnp.bfloat16
NX = 4
NJ = 4
NCH = 16
VMEM_LIMIT = 67_043_328
GROUPS = (((0, 0), (0, 1)), ((0, 2), (0, 3)), *(((3, j), (1, j)) for j in range(NJ)), *(((2, j),) for j in range(NJ)))


def rem(a, b):
    return lax.rem(a, jnp.int32(b))


def div(a, b):
    return lax.div(a, jnp.int32(b))


def al(v, m):
    return pl.multiple_of(v, m)


def remote(src, dst, ssem, rsem, dev):
    return pltpu.make_async_remote_copy(src_ref=src, dst_ref=dst, send_sem=ssem, recv_sem=rsem, device_id=dev, device_id_type=MESH)


ATTENTION_STEPS = (
    ("XP", 2), ("XP", 0), ("S", "b", 0, 0), ("XE", 3), ("XP", 1), ("WA", 0), ("S", "b", 0, 1), ("ST", 3), ("O", "b", 1),
    ("N", 3), ("O", "b", 0), ("XP", 3), ("WA", 1), ("XE", 0), ("WOP",), ("S", "b", 1, 0), ("WP", 0), ("XE", 1), ("XE", 2),
    ("YH", 3), ("S", "b", 1, 1), ("WP", 1), ("O", "a", 1), ("S", "a", 1, 0), ("ST", 0), ("G", 8), ("ST", 1), ("N", 0),
    ("G", 4), ("N", 1), ("YH", 0), ("ST", 2), ("XE", 4), ("F", "a", 0), ("F", "b", 1), ("O", "a", 0), ("YH", 1), ("F", "a", 1),
    ("N", 2), ("G", 2), ("ST", 4), ("G", 6), ("YH", 2), ("G", 3), ("S", "a", 1, 1), ("N", 4), ("G", 7), ("R", 6), ("R", 2),
    ("G", 1), ("R", 3), ("R", 7), ("YH", 4), ("R", 8), ("A", 2), ("A", 6), ("A", 7), ("A", 8), ("R", 4), ("G", 9),
    ("S", "a", 0, 1), ("P", 2), ("R", 1), ("G", 5), ("P", 8), ("P", 6), ("DP", 1), ("P", 7), ("A", 3), ("A", 4), ("R", 9),
    ("A", 9), ("G", 0), ("X", 8), ("R", 5), ("X", 6), ("P", 3), ("X", 7), ("A", 5), ("P", 9), ("P", 4), ("X", 2),
    ("S", "a", 0, 0), ("M", 0), ("F", "b", 0), ("X", 3), ("M", 1), ("P", 5), ("R", 0), ("X", 9), ("X", 4), ("M", 2), ("A", 0),
    ("A", 1), ("X", 5), ("M", 3), ("DP", 0), ("P", 0), ("P", 1), ("X", 0), ("T", 1), ("T", 0), ("X", 1), ("T", 2), ("T", 3),
)
MLP_STEPS = (
    ("YR", 0), ("XF", 0, 1), ("XF", 0, 3), ("WT", 0), ("XH", 0, 1), ("XF", 0, 2), ("YRH", 0), ("XH", 0, 3), ("XF", 0, 5),
    ("N", 0, 1), ("N", 0, 3), ("XH", 0, 2), ("XF", 0, 4), ("N", 0, 2), ("XF", 2, 0), ("XF", 3, 0), ("XF", 0, 0), ("XH", 3, 0),
    ("XH", 2, 0), ("XH", 0, 4), ("WT", 1), ("YH", 1), ("XF", 1, 0), ("WT", 2), ("WT", 3), ("XH", 0, 5), ("YH", 3), ("YH", 2),
    ("G", 3), ("N", 3, 0), ("N", 0, 4), ("XH", 0, 0), ("N", 0, 5), ("G", 7), ("N", 2, 0), ("G", 6), ("N", 0, 0), ("XH", 1, 0),
    ("P", 3), ("G", 0), ("G", 1), ("P", 7), ("N", 1, 0), ("X", 3), ("G", 2), ("P", 6), ("YH", 4), ("G", 4), ("YH", 5),
    ("X", 7), ("G", 5), ("X", 6), ("G", 8), ("P", 2), ("P", 8), ("G", 9), ("M", 1), ("P", 4), ("X", 8), ("X", 2), ("P", 9),
    ("M", 0), ("P", 5), ("P", 0), ("P", 1), ("X", 9), ("X", 4), ("M", 2), ("X", 5), ("M", 3), ("X", 0), ("T", 0), ("X", 1),
    ("T", 1), ("T", 2), ("T", 3),
)


class Place:
    def __init__(self):
        tx, ty = lax.axis_index("tx"), lax.axis_index("ty")
        self.x, self.c, self.y = div(tx, 2), rem(tx, 2), ty
        x, c, y = self.x, self.c, self.y
        self.xr, self.xl, self.xo = rem(x + 1, NX), rem(x + 3, NX), rem(x + 2, NX)
        self.yu, self.yd, self.yo = rem(y + 1, NX), rem(y + 3, NX), rem(y + 2, NX)
        self.right = {"tx": self.xr * 2 + c, "ty": y}
        self.left = {"tx": self.xl * 2 + c, "ty": y}
        self.up = {"tx": tx, "ty": self.yu}
        self.down = {"tx": tx, "ty": self.yd}
        self.partner = {"tx": x * 2 + 1 - c, "ty": y}
        self.xa, self.xb = x + 1 - 2 * rem(x, 2), rem(x + 3 + 2 * rem(x, 2), NX)
        self.pa, self.pb = {"tx": self.xa * 2 + c, "ty": y}, {"tx": self.xb * 2 + c, "ty": y}

    def barrier(self):
        sem = pltpu.get_barrier_semaphore()
        for dev in (self.right, self.left, self.up, self.down, self.partner):
            pl.semaphore_signal(sem, inc=1, device_id=dev, device_id_type=MESH)
        pl.semaphore_wait(sem, 5)


class Spread:
    def __init__(self, at, src, xg, units, sums, sx, rx, sy, ry, syh, ryh):
        self.sums = sums
        self.at, self.src, self.xg, self.units, self.kc = at, src, xg, units, src.shape[2]
        self.sx, self.rx, self.sy, self.ry, self.syh, self.ryh = sx, rx, sy, ry, syh, ryh
        pairs = [(r, u) for u, unit in enumerate(units) for r in ((0, 3, 1, 2) if unit[3] else (0,))]
        self.index = {pair: i for i, pair in enumerate(pairs)}
        self.seqs = (at.y, at.yu, at.yo, at.yd)

    def cols(self, x):
        return pl.ds(al(x * self.kc, 128), self.kc)

    def keep_own(self):
        for j in range(NJ):
            self.xg[self.at.y, j, :, self.cols(self.at.x)] = self.src[j]

    def xcopy(self, kind, r, u):
        at, s = self.at, self.seqs[r]
        j, lo, n, _ = self.units[u]
        i = self.index[r, u]
        if kind < 2:
            dst = self.xg.at[s, j, pl.ds(lo, n), self.cols(at.x)]
            src = self.src.at[j, pl.ds(lo, n)] if r == 0 else dst
        elif kind == 2:
            src = dst = self.xg.at[s, j, pl.ds(lo, n // 2), self.cols(at.xl)]
        else:
            src = dst = self.xg.at[s, j, pl.ds(lo + n // 2, n // 2), self.cols(at.xr)]
        return remote(src, dst, self.sx.at[kind, i], self.rx.at[kind, i], at.left if kind % 2 else at.right)

    def xwait(self, kind, r, u):
        at = self.at
        j, lo, n, _ = self.units[u]
        i = self.index[r, u]
        x = (at.xl, at.xr, at.xo, at.xo)[kind]
        rows = (pl.ds(lo, n), pl.ds(lo, n), pl.ds(lo, n // 2), pl.ds(lo + n // 2, n // 2))[kind]
        dst = self.xg.at[self.seqs[r], j, rows, self.cols(x)]
        remote(dst, dst, self.sx.at[kind, i], self.rx.at[kind, i], at.right).wait_recv()

    def yref(self, s, u, lo, n):
        j, _, _, first = self.units[u]
        rows = pl.ds(lo, n)
        return self.xg.at[s, j, rows, self.cols(self.at.x)] if first else self.xg.at[s, j, rows]

    def ycopy(self, d, u):
        j, lo, n, first = self.units[u]
        dst = self.yref(self.at.y, u, lo, n)
        src = self.src.at[j, pl.ds(lo, n)] if first else dst
        return remote(src, dst, self.sy.at[d, u], self.ry.at[d, u], self.at.down if d else self.at.up)

    def ywait(self, d, u):
        _, lo, n, _ = self.units[u]
        dst = self.yref(self.at.yu if d else self.at.yd, u, lo, n)
        remote(dst, dst, self.sy.at[d, u], self.ry.at[d, u], self.at.up).wait_recv()

    def yhalf(self, d, u):
        _, lo, n, _ = self.units[u]
        ref = self.yref(self.at.yu if d else self.at.yd, u, lo + d * (n // 2), n // 2)
        return remote(ref, ref, self.syh.at[d, u], self.ryh.at[d, u], self.at.down if d else self.at.up)

    def yhalf_wait(self, d, u):
        _, lo, n, _ = self.units[u]
        dst = self.yref(self.at.yo, u, lo + d * (n // 2), n // 2)
        remote(dst, dst, self.syh.at[d, u], self.ryh.at[d, u], self.at.up).wait_recv()

    def YR(self, u):
        for d in range(2):
            self.ycopy(d, u).start()

    def YH(self, u):
        for d in range(2):
            self.ywait(d, u)
            self.yhalf(d, u).start()

    YRH = YH

    def XF(self, r, u):
        if r == 2:
            for d in range(2):
                self.yhalf_wait(d, u)
        for kind in range(2):
            self.xcopy(kind, r, u).start()

    def XH(self, r, u):
        for kind in range(2):
            self.xwait(kind, r, u)
            self.xcopy(kind + 2, r, u).start()

    def N(self, r, u):
        j, lo, n, first = self.units[u]
        for kind in (2, 3):
            self.xwait(kind, r, u)
            self.xcopy(kind, r, u).wait_send()
        if r:
            for kind in range(2):
                self.xcopy(kind, r, u).wait_send()
        if r % 2:
            self.yhalf(0 if r == 3 else 1, u).wait_send()
        width, ref = self.xg.shape[-1], self.xg.at[self.seqs[r], j]
        s1, s2 = self.sums
        lane_sums(ref, lo, n, s1, s2)
        mean = jnp.sum(s1[0:n, :], axis=-1, keepdims=True) / width
        var = jnp.sum(s2[0:n, :], axis=-1, keepdims=True) / width - mean * mean
        s1[0:n, :] = jnp.broadcast_to(mean, (n, 128))
        s2[0:n, :] = jnp.broadcast_to(lax.rsqrt(var + EPS), (n, 128))
        scale_rows(ref, lo, n, s1, s2)
        if not first:
            self.YR(u)

    def chunk_wait(self, r, j):
        if r == 2:
            for u, unit in enumerate(self.units):
                if unit[0] == j and not unit[3]:
                    for d in range(2):
                        self.yhalf_wait(d, u)

    def drain(self):
        for u, unit in enumerate(self.units):
            for d in range(2):
                self.xcopy(d, 0, u).wait_send()
                self.ycopy(d, u).wait_send()
                if not unit[3]:
                    self.yhalf(d, u).wait_send()


def rows_of(refs):
    return refs[0][...] if len(refs) == 1 else jnp.concatenate([ref[...] for ref in refs], axis=0)


def product(refs, weight, depth, n_cols, done, wide=True):
    step = 512 if wide and len(refs) == 1 and n_cols % 512 == 0 else 256

    def columns(i, carry):
        out = jnp.dot(rows_of(refs), weight[0:depth, pl.ds(al(i * step, 128), step)], preferred_element_type=F32)
        done(i * step, step, out)
        return carry

    lax.fori_loop(0, n_cols // step, columns, 0)


def lane_sums(ref, lo, n, s1, s2):
    width, rows, wide = ref.shape[-1], 32, 512

    def some_rows(i, carry):
        def some_columns(k, sums):
            a, b = sums
            v = ref[pl.ds(al(lo + i * rows, 8), rows), pl.ds(al(k * wide, 128), wide)].astype(F32)
            for c in range(0, wide, 128):
                part = v[:, c : c + 128]
                a, b = a + part, b + part * part
            return a, b

        zero = jnp.zeros((rows, 128), F32)
        a, b = lax.fori_loop(0, width // wide, some_columns, (zero, zero))
        s1[pl.ds(al(i * rows, 8), rows), :] = a
        s2[pl.ds(al(i * rows, 8), rows), :] = b
        return carry

    lax.fori_loop(0, n // rows, some_rows, 0)


def scale_rows(ref, lo, n, means, scales):
    width, rows, wide = ref.shape[-1], 32, 512

    def some_rows(i, carry):
        mean, scale = (t[pl.ds(al(i * rows, 8), rows), :] for t in (means, scales))

        def some_columns(k, carry):
            at_rows = pl.ds(al(lo + i * rows, 8), rows)
            for c in range(0, wide, 128):
                cols = pl.ds(al(k * wide + c, 128), 128)
                ref[at_rows, cols] = ((ref[at_rows, cols].astype(F32) - mean) * scale).astype(BF16)
            return carry

        lax.fori_loop(0, width // wide, some_columns, 0)
        return carry

    lax.fori_loop(0, n // rows, some_rows, 0)


class Reduce:
    def __init__(self, at, zb, ya, yb, yfd, yfu, ss, rs):
        self.at, self.zb, self.ya, self.yb, self.yfd, self.yfu, self.ss, self.rs = at, zb, ya, yb, yfd, yfu, ss, rs
        self.ch = zb.shape[2]
        self.h = self.ch // 2

    def copy(self, kind, j):
        at, h, ch = self.at, self.h, self.ch
        src, dst = (
            lambda: (self.zb.at[2, j, pl.ds(0, h)], self.ya.at[j]),
            lambda: (self.zb.at[2, j, pl.ds(h, ch - h)], self.yb.at[j]),
            lambda: (self.zb.at[1, j], self.yfd.at[j]),
            lambda: (self.zb.at[3, j], self.yfu.at[j]),
        )[kind]()
        return remote(src, dst, self.ss.at[kind, j], self.rs.at[kind, j], at.down if kind % 2 else at.up)

    def wait(self, kind, j):
        self.copy(kind, j).wait_recv()

    def halves(self, j):
        self.copy(0, j).start()
        self.copy(1, j).start()

    def middle(self, j):
        h = self.h
        self.wait(0, j)
        self.zb[1, j, 0:h] = (self.zb[1, j, 0:h].astype(F32) + self.ya[j].astype(F32)).astype(BF16)
        self.copy(2, j).start()
        self.wait(1, j)
        self.zb[3, j, h:] = (self.zb[3, j, h:].astype(F32) + self.yb[j].astype(F32)).astype(BF16)
        self.copy(3, j).start()

    def total(self, j):
        self.wait(2, j)
        self.wait(3, j)
        return self.zb[0, j].astype(F32) + self.yfd[j].astype(F32) + self.yfu[j].astype(F32)

    def drain(self):
        for j in range(NJ):
            for kind in range(4):
                self.copy(kind, j).wait_send()


def attention_kernel(
    units, x_ref, turn_ref, base_ref, wq, wk, wv, wo, wg_t, wu_t,
    h_ref, w_all,
    xc, xg, cos_all, sin_all, st_own, st_in, s1, s2, wb, wob, part, precv, qb, kvo, kvp, og, zb, ya, yb, yfd, yfu, own, drel_a, drel_b,
    sxe, rxe, sst, rst, sy, ry, syh, ryh, sd, rd, swa, rwa, swo, rwo, swp, rwp, lw, so, ro, spr, rpr, skv, rkv, sog, rog, syr, ryr,
    lg, sds, rds, sdo, rdo, sdf, rdf, sdp, rdp,
):
    at = Place()
    x, c, y = at.x, at.c, at.y
    ch, kc = xc.shape[1], xc.shape[2]
    kd = wq.shape[0]
    hc = qb.shape[2]
    fc, f_a = w_all.shape[1], drel_a.shape[1]
    width = 2 * xg.shape[3]
    kh = div(x, 2)
    ng = rem(div(x + 1, 2), 2)
    gather = Spread(at, xc, xg, units, (s1, s2), None, None, sy, ry, syh, ryh)
    reduce = Reduce(at, zb, ya, yb, yfd, yfu, syr, ryr)
    weights = (wq, wk, wv)

    def half_cols(core):
        return pl.ds(al(core * kd, 128), kd)

    def x_rows(j, core):
        return pl.ds(al((2 * j + core) * ch, 8), ch)

    def x_pair(j):
        return remote(x_ref.at[x_rows(j, 1 - c)], xc.at[j, :, half_cols(c)], sd.at[j], rd.at[j], at.partner)

    def pair_cols(xx):
        return pl.ds(al(rem(xx, 2) * kc, 128), kc)

    def xe_copy(u, xx):
        j, lo, n, _ = units[u]
        rows = pl.ds(lo, n)
        return remote(xc.at[j, rows], xg.at[y, j, rows, pair_cols(xx)], sxe.at[u], rxe.at[u], at.pa)

    def st_copy(u):
        j, lo, n, _ = units[u]
        rows = pl.ds(lo // 4, n // 4)
        return remote(st_own.at[j, rows], st_in.at[j, rows], sst.at[u], rst.at[u], at.pb)

    def XP(j):
        x_pair(j).start()

    def XE(u):
        j, lo, n, _ = units[u]
        if lo == 0:
            dst = xc.at[j, :, half_cols(1 - c)]
            remote(dst, dst, sd.at[j], rd.at[j], at.partner).wait_recv()
        xe_copy(u, x).start()
        xg[y, j, lo : lo + n, pair_cols(x)] = xc[j, lo : lo + n]

    def ST(u):
        j, lo, n, _ = units[u]
        xe_copy(u, at.xa).wait_recv()
        quarter = n // 4
        lane = lax.broadcasted_iota(jnp.int32, (quarter, 128), 1)
        lane_sums(xg.at[y, j], lo, n, s1, s2)
        packed = jnp.zeros((quarter, 128), F32)
        for g in range(4):
            rows = pl.ds(g * quarter, quarter)
            total, square = (jnp.sum(t[rows, :], axis=-1, keepdims=True) for t in (s1, s2))
            packed = jnp.where(lane // 32 == g, jnp.where(lane % 32 < 16, total, square), packed)
        st_own[j, lo // 4 : lo // 4 + quarter, :] = packed
        st_copy(u).start()

    def N(u):
        j, lo, n, _ = units[u]
        st_copy(u).wait_recv()
        quarter = n // 4
        at_rows = slice(lo // 4, lo // 4 + quarter)
        moments = (st_own[j, at_rows, :] + st_in[j, at_rows, :]) / width
        for g in range(4):
            mean = moments[:, 32 * g : 32 * g + 1]
            var = moments[:, 32 * g + 16 : 32 * g + 17] - mean * mean
            rows = pl.ds(g * quarter, quarter)
            s1[rows, :] = jnp.broadcast_to(mean, (quarter, 128))
            s2[rows, :] = jnp.broadcast_to(lax.rsqrt(var + EPS), (quarter, 128))
        scale_rows(xg.at[y, j], lo, n, s1, s2)
        gather.YR(u)

    def w_rows(xx, core):
        return pl.ds(al(rem(xx, 2) * kc + core * kd, 128), kd)

    def w_part(group, half, i):
        return weights[i].at[:, pl.ds(al((2 * group + half) * hc, 128), hc)]

    def w_cols(half, i):
        return pl.ds(half * 3 * hc + i * hc, hc)

    def wa_copy(half, i, xx):
        return remote(w_part(1 - ng, half, i), wb.at[w_rows(xx, c), w_cols(half, i)], swa.at[half, i], rwa.at[half, i], at.pa)

    def wo_copy(half, i, core):
        return remote(w_part(ng, half, i), wb.at[w_rows(x, core), w_cols(half, i)], swo.at[half, i], rwo.at[half, i], at.partner)

    def w_local(half, i):
        return pltpu.make_async_copy(w_part(ng, half, i), wb.at[w_rows(x, c), w_cols(half, i)], lw.at[half, i])

    def wp_copy(half, core):
        ref = wb.at[w_rows(at.xa, core), pl.ds(half * 3 * hc, 3 * hc)]
        return remote(ref, ref, swp.at[half], rwp.at[half], at.partner)

    o_local = pltpu.make_async_copy(wo, wob.at[:, half_cols(c)], lw.at[2, 0])
    o_pair = remote(wo, wob.at[:, half_cols(c)], so.at[0], ro.at[0], at.partner)
    pieces = [(half, i) for half in range(2) for i in range(3)]

    def WOP():
        for half, i in pieces:
            wo_copy(half, i, c).start()
        o_pair.start()

    def WA(half):
        for i in range(3):
            wa_copy(half, i, x).start()

    def WP(half):
        for i in range(3):
            wa_copy(half, i, at.xa).wait_recv()
        wp_copy(half, c).start()

    def w_ready():
        for half, i in pieces:
            w_local(half, i).wait()
            wo_copy(half, i, 1 - c).wait_recv()
        for half in range(2):
            wp_copy(half, 1 - c).wait_recv()
        for m in range(2):
            d_in(m).wait()
            d_out(m).start()
            d_pair(m, 3, c).start()

    def o_ready():
        o_local.wait()
        dst = wob.at[:, half_cols(1 - c)]
        remote(dst, dst, so.at[0], ro.at[0], at.partner).wait_recv()

    mlp_weights = (wg_t, wu_t)
    parts = ((0, f_a), (f_a, fc - f_a))

    def d_src(m, xx, p):
        return mlp_weights[m].at[pl.ds(al(xx * fc + parts[p][0], 8), parts[p][1])]

    def d_dst(m, xx, p):
        return w_all.at[m, pl.ds(*parts[p]), pl.ds(al((2 * xx + c) * kd, 128), kd)]

    def s_copy(d, m, p, xx):
        to, dev = ((at.xa, at.pa), (at.xb, at.pb))[d]
        return remote(d_src(m, to, p), d_dst(m, xx, p), sds.at[d, m, p], rds.at[d, m, p], dev)

    def o_copy(d, m):
        return remote(d_src(m, at.xo, d), (drel_a, drel_b)[d].at[m], sdo.at[d, m], rdo.at[d, m], (at.pa, at.pb)[d])

    def f_copy(d, m, xx):
        return remote((drel_a, drel_b)[d].at[m], d_dst(m, xx, d), sdf.at[d, m], rdf.at[d, m], (at.pb, at.pa)[d])

    def d_in(m):
        return pltpu.make_async_copy(mlp_weights[m].at[pl.ds(al(x * fc, 8), fc)], own.at[m], lg.at[0, m])

    def d_all(m, xx, core):
        return w_all.at[m, :, pl.ds(al((2 * xx + core) * kd, 128), kd)]

    def d_out(m):
        return pltpu.make_async_copy(own.at[m], d_all(m, x, c), lg.at[1, m])

    def d_pair(m, k, core):
        dst = d_all(m, (at.xa, at.xb, at.xo, x)[k], core)
        return remote(own.at[m] if k == 3 else dst, dst, sdp.at[m, k], rdp.at[m, k], at.partner)

    def S(link, m, p):
        s_copy("ab".index(link), m, p, x).start()

    def O(link, m):
        o_copy("ab".index(link), m).start()

    def F(link, m):
        d = "ba".index(link)
        o_copy(d, m).wait_recv()
        f_copy(d, m, (at.xa, at.xb)[d]).start()

    def DP(m):
        for d in range(2):
            for p in range(2):
                s_copy(d, m, p, (at.xa, at.xb)[d]).wait_recv()
            f_copy(d, m, at.xo).wait_recv()
        for k in range(3):
            d_pair(m, k, c).start()

    def pr_copy(n):
        src = part.at[n, :, pl.ds(al((1 - kh) * 3 * hc, 128), 3 * hc)]
        return remote(src, precv.at[n], spr.at[n], rpr.at[n], at.pb)

    def G(g):
        for r, j in GROUPS[g]:
            gather.chunk_wait(r, j)

        def done(col, size, out):
            for i, (r, j) in enumerate(GROUPS[g]):
                part[r * NJ + j, :, pl.ds(al(col, 128), size)] = out[i * ch : (i + 1) * ch].astype(BF16)

        product([xg.at[gather.seqs[r], j] for r, j in GROUPS[g]], wb, wb.shape[0], wb.shape[1], done)
        for r, j in GROUPS[g]:
            pr_copy(r * NJ + j).start()

    def kv_copy(r, j):
        s, n = gather.seqs[r], r * NJ + j
        return remote(kvo.at[s, j], kvp.at[s, j], skv.at[n], rkv.at[n], at.partner)

    def rotate(r, j):
        s, n = gather.seqs[r], r * NJ + j
        pr_copy(n).wait_recv()
        cos_t, sin_t = cos_all[j], sin_all[j]

        def total(col, size):
            mine = part[n, :, pl.ds(al(kh * 3 * hc + col, 128), size)]
            return (mine.astype(F32) + precv[n, :, col : col + size].astype(F32)).astype(BF16)

        def turned(col):
            v = total(col, HEAD_DIM).astype(F32)
            return (v * cos_t + pltpu.roll(v, HEAD_DIM // 2, axis=1) * sin_t).astype(BF16)

        for col in range(0, hc, HEAD_DIM):
            qb[n, :, col : col + HEAD_DIM] = turned(col)
            kvo[s, j, :, col : col + HEAD_DIM] = turned(hc + col)
        kvo[s, j, :, hc:] = total(2 * hc, hc)
        kv_copy(r, j).start()

    def R(g):
        for r, j in GROUPS[g]:
            rotate(r, j)

    def o_cols(xx):
        return pl.ds(al((2 * rem(div(xx + 1, 2), 2) + div(xx, 2)) * hc, 128), hc)

    cut = ch // 8

    def og_copy(kind, n):
        if kind < 2:
            ref = og.at[n, :, o_cols(x)]
        elif kind == 2:
            ref = og.at[n, pl.ds(0, cut), o_cols(at.xa)]
        else:
            ref = og.at[n, pl.ds(cut, ch - cut), o_cols(at.xb)]
        return remote(ref, ref, sog.at[kind, n], rog.at[kind, n], at.pa if kind in (0, 3) else at.pb)

    def og_wait(kind, n):
        xx = (at.xa, at.xb, at.xo, at.xo)[kind]
        rows = (pl.ds(0, ch), pl.ds(0, ch), pl.ds(0, cut), pl.ds(cut, ch - cut))[kind]
        dst = og.at[n, rows, o_cols(xx)]
        remote(dst, dst, sog.at[kind, n], rog.at[kind, n], at.pa).wait_recv()

    def attend(r, j, i):
        s, n = gather.seqs[r], r * NJ + j
        keys = (j + 1) * ch
        iq = lax.broadcasted_iota(jnp.int32, (ch, keys), 0) + j * ch
        ik = lax.broadcasted_iota(jnp.int32, (ch, keys), 1)
        own_ok = iq >= ik
        par_ok = ik < (j + c) * ch
        contract = (((1,), (1,)), ((), ()))
        cols = pl.ds(al(i * HEAD_DIM, 128), HEAD_DIM)
        v_cols = pl.ds(al(hc + i * HEAD_DIM, 128), HEAD_DIM)
        q = qb[n, :, cols]
        k_own = kvo[s, 0 : j + 1, :, cols].reshape(keys, HEAD_DIM)
        k_par = kvp[s, 0 : j + 1, :, cols].reshape(keys, HEAD_DIM)
        s_own = lax.dot_general(q, k_own, contract, preferred_element_type=F32) * HEAD_DIM**-0.5
        s_par = lax.dot_general(q, k_par, contract, preferred_element_type=F32) * HEAD_DIM**-0.5
        s_own = jnp.where(own_ok, s_own, -1e30)
        s_par = jnp.where(par_ok, s_par, -1e30)
        top = jnp.maximum(jnp.max(s_own, axis=1, keepdims=True), jnp.max(s_par, axis=1, keepdims=True))
        e_own, e_par = jnp.exp(s_own - top), jnp.exp(s_par - top)
        inv = 1.0 / (jnp.sum(e_own, axis=1, keepdims=True) + jnp.sum(e_par, axis=1, keepdims=True))
        v_own = kvo[s, 0 : j + 1, :, v_cols].reshape(keys, HEAD_DIM)
        v_par = kvp[s, 0 : j + 1, :, v_cols].reshape(keys, HEAD_DIM)
        out = jnp.dot((e_own * inv).astype(BF16), v_own, preferred_element_type=F32)
        out += jnp.dot((e_par * inv).astype(BF16), v_par, preferred_element_type=F32)
        og[n, :, pl.ds(al((2 * ng + kh) * hc + i * HEAD_DIM, 128), HEAD_DIM)] = out.astype(BF16)

    def A(g):
        for r, j in GROUPS[g]:
            kv_copy(r, j).wait_recv()

        def head(i, carry):
            for r, j in GROUPS[g]:
                attend(r, j, i)
            return carry

        lax.fori_loop(0, hc // HEAD_DIM, head, 0)
        for r, j in GROUPS[g]:
            og_copy(0, r * NJ + j).start()
            og_copy(1, r * NJ + j).start()

    def P(g):
        for r, j in GROUPS[g]:
            for kind in range(2):
                og_wait(kind, r * NJ + j)
                og_copy(kind + 2, r * NJ + j).start()

    def X(g):
        for r, j in GROUPS[g]:
            og_wait(2, r * NJ + j)
            og_wait(3, r * NJ + j)

        def done(col, size, out):
            for i, (r, j) in enumerate(GROUPS[g]):
                zb[r, j, :, pl.ds(al(col, 128), size)] = out[i * ch : (i + 1) * ch].astype(BF16)

        product([og.at[r * NJ + j] for r, j in GROUPS[g]], wob, wob.shape[0], kc, done)
        for r, j in GROUPS[g]:
            if r == 2:
                reduce.halves(j)

    def T(j):
        attn = reduce.total(j).astype(BF16)
        h_ref[j] = (xc[j].astype(F32) + attn.astype(F32)).astype(BF16)

    for half, i in pieces:
        w_local(half, i).start()
    o_local.start()
    for m in range(2):
        d_in(m).start()
    for j in range(NJ):
        xc[j, :, half_cols(c)] = x_ref[x_rows(j, c), :]
    at.barrier()

    def angles():
        lane = lax.broadcasted_iota(jnp.int32, (ch, HEAD_DIM), 1)
        for j in range(NJ):
            base_cos, base_sin = base_ref[0, pl.ds(2 * j + c, 1), :], base_ref[1, pl.ds(2 * j + c, 1), :]
            cos_all[j] = base_cos * turn_ref[0] - base_sin * turn_ref[1]
            sine = base_sin * turn_ref[0] + base_cos * turn_ref[1]
            sin_all[j] = jnp.where(lane < HEAD_DIM // 2, -sine, sine)

    ops = {
        "XP": XP, "WOP": WOP, "XE": XE, "ST": ST, "N": N, "YH": gather.YH, "WA": WA, "WP": WP, "S": S, "O": O, "F": F, "DP": DP,
        "G": G, "R": R, "A": A, "P": P, "X": X, "M": reduce.middle, "T": T,
    }
    waits = {"G": w_ready, "X": o_ready, "WP": angles}
    for step in ATTENTION_STEPS:
        if step[0] in waits:
            waits.pop(step[0])()
        ops[step[0]](*step[1:])

    for m in range(2):
        for k in range(4):
            d_pair(m, k, 1 - c).wait_recv()
            d_pair(m, k, c).wait_send()
        d_out(m).wait()
        for d in range(2):
            for p in range(2):
                s_copy(d, m, p, x).wait_send()
            o_copy(d, m).wait_send()
            f_copy(d, m, x).wait_send()
    for j in range(NJ):
        x_pair(j).wait_send()
    for u in range(len(units)):
        xe_copy(u, x).wait_send()
        st_copy(u).wait_send()
        for d in range(2):
            gather.ycopy(d, u).wait_send()
            gather.yhalf(d, u).wait_send()
    reduce.drain()
    o_pair.wait_send()
    for half, i in pieces:
        wa_copy(half, i, x).wait_send()
        wo_copy(half, i, c).wait_send()
    for half in range(2):
        wp_copy(half, c).wait_send()

    def chunk_sent(n, carry):
        pr_copy(n).wait_send()
        remote(kvo.at[0, 0], kvp.at[0, 0], skv.at[n], rkv.at[n], at.partner).wait_send()
        for kind in range(4):
            og_copy(kind, n).wait_send()
        return carry

    lax.fori_loop(0, NCH, chunk_sent, 0)


def mlp_kernel(
    units, h_ref, w_hbm, wdn, y_ref,
    xg, wt, raw, wd, ag, ar, act, s1, s2, zb, ya, yb, yfd, yfu, yst,
    sx, rx, sy, ry, syh, ryh, sa, ra, syr, ryr, sd, rd, lw, lwd, swd, rwd,
):
    at = Place()
    x, c, y = at.x, at.c, at.y
    ch, kc, h = h_ref.shape[1], h_ref.shape[2], h_ref.shape[1] // 2
    width = xg.shape[-1]
    kd = kc // 2
    fc, tiles = w_hbm.shape[1], wt.shape[1] // 256
    fm = (tiles - 1) * 128
    fr = fc - fm
    blocks, slots = 2 * tiles, raw.shape[0]
    gather = Spread(at, h_ref, xg, units, (s1, s2), sx, rx, sy, ry, syh, ryh)
    reduce = Reduce(at, zb, ya, yb, yfd, yfu, syr, ryr)

    def w_in(q):
        i, m = q // 2, q % 2
        n = min(128, fc - i * 128)
        return pltpu.make_async_copy(w_hbm.at[m, pl.ds(i * 128, n)], raw.at[q % slots, pl.ds(0, n)], lw.at[q])

    def WT(g):
        for q in range(g * blocks // 4, (g + 1) * blocks // 4):
            i, m, slot = q // 2, q % 2, q % slots
            w_in(q).wait()
            if fc < (i + 1) * 128:
                raw[slot, fc - i * 128 :, :] = jnp.zeros(((i + 1) * 128 - fc, width), BF16)

            def turn(k, carry, slot=slot, q=q):
                part = pl.ds(al(k * (width // 4), 128), width // 4)
                wt[part, q * 128 : (q + 1) * 128] = raw[slot, :, part].T
                return carry

            lax.fori_loop(0, 4, turn, 0)
            if q + slots < blocks:
                w_in(q + slots).start()

    def d_refs(q, core):
        cols = pl.ds(al(core * kd, 128), kd)
        main, rest = wdn.at[pl.ds(q * fc, fm)], wdn.at[pl.ds(q * fc + fm, fr)]
        return (main, wd.at[pl.ds(q * fm, fm), cols]), (rest, wd.at[pl.ds(NX * fm + q * 128, fr), cols])

    def d_own(q, k):
        src, dst = d_refs(q, c)[k]
        return pltpu.make_async_copy(src, dst, lwd.at[q, k])

    def d_pair(q, k, core):
        src, dst = d_refs(q, core)[k]
        return remote(src, dst, swd.at[q, k], rwd.at[q, k], at.partner)

    quarters = [(q, k) for q in range(NX) for k in range(2)]
    for q in range(slots):
        w_in(q).start()
    for q, k in quarters:
        d_own(q, k).start()
    for q in range(NX):
        wd[NX * fm + q * 128 + fr : NX * fm + (q + 1) * 128, :] = jnp.zeros((128 - fr, kc), BF16)
    at.barrier()
    for q, k in quarters:
        d_pair(q, k, c).start()

    def a_refs(kind, n, xx):
        main, rest = pl.ds(al(xx * fm, 128), fm), pl.ds(al(xx * 128, 128), 128)
        if kind < 2:
            return ag.at[n, :, main], ar.at[n, :, rest]
        lo = (kind - 2) * h
        return ag.at[n, pl.ds(lo, h), main], ar.at[n, pl.ds(lo // 2, h // 2), rest]

    def a_copies(kind, n):
        refs = a_refs(kind, n, (x, x, at.xl, at.xr)[kind])
        return [remote(v, v, sa.at[kind, n, k], ra.at[kind, n, k], at.left if kind % 2 else at.right) for k, v in enumerate(refs)]

    def a_wait(kind, n):
        for k, v in enumerate(a_refs(kind, n, (at.xl, at.xr, at.xo, at.xo)[kind])):
            remote(v, v, sa.at[kind, n, k], ra.at[kind, n, k], at.right).wait_recv()

    def a_start(kind, n):
        for copy in a_copies(kind, n):
            copy.start()

    def G(g):
        for r, j in GROUPS[g]:
            gather.chunk_wait(r, j)

        def done(col, size, out):
            for k in range(0, size, 256):
                gate, up = out[:, k : k + 128].astype(BF16).astype(F32), out[:, k + 128 : k + 256].astype(BF16).astype(F32)
                value = (gate / (1.0 + jnp.exp(-gate)) * up).astype(BF16)
                act[0 : value.shape[0], pl.ds(al(div(col + k, 2), 128), 128)] = value

        product([xg.at[gather.seqs[r], j] for r, j in GROUPS[g]], wt, width, wt.shape[1], done)
        for i, (r, j) in enumerate(GROUPS[g]):
            n, lo = r * NJ + j, i * ch
            ag[n, :, pl.ds(al(x * fm, 128), fm)] = act[lo : lo + ch, :fm]
            below = pltpu.roll(act[lo + h : lo + ch, fm:].astype(F32), 64, axis=1)
            ar[n, :, pl.ds(al(x * 128, 128), 128)] = (act[lo : lo + h, fm:].astype(F32) + below).astype(BF16)
            for kind in range(2):
                a_start(kind, n)

    def P(g):
        for r, j in GROUPS[g]:
            for kind in range(2):
                a_wait(kind, r * NJ + j)
                a_start(kind + 2, r * NJ + j)

    def X(g):
        for r, j in GROUPS[g]:
            n = r * NJ + j
            for kind in (2, 3):
                a_wait(kind, n)
            for q in range(NX):
                cols = pl.ds(NX * fm + q * 128, 128)
                rest = ar[n, :, q * 128 : (q + 1) * 128]
                ag[n, 0:h, cols] = rest
                ag[n, h:, cols] = pltpu.roll(rest.astype(F32), 64, axis=1).astype(BF16)

        def done(col, size, out):
            for i, (r, j) in enumerate(GROUPS[g]):
                zb[r, j, :, pl.ds(al(col, 128), size)] = out[i * ch : (i + 1) * ch].astype(BF16)

        product([ag.at[r * NJ + j] for r, j in GROUPS[g]], wd, wd.shape[0], kc, done, wide=False)
        for r, j in GROUPS[g]:
            if r == 2:
                reduce.halves(j)

    def y_rows(j, core):
        return pl.ds(al((2 * j + core) * ch, 8), ch)

    def y_copy(j):
        return remote(yst.at[1 - c, j], y_ref.at[y_rows(j, c)], sd.at[j], rd.at[j], at.partner)

    def y_wait(j):
        dst = y_ref.at[y_rows(j, 1 - c)]
        remote(dst, dst, sd.at[j], rd.at[j], at.partner).wait_recv()

    def T(j):
        mlp = reduce.total(j).astype(BF16)
        out = (h_ref[j].astype(F32) + mlp.astype(F32)).astype(BF16)
        yst[0, j] = out[:, :kd]
        yst[1, j] = out[:, kd:]
        y_copy(j).start()
        y_ref[y_rows(j, c), :] = yst[c, j]

    ops = {"G": G, "P": P, "X": X, "M": reduce.middle, "T": T, "WT": WT}
    for name in ("YR", "YRH", "YH", "XF", "XH", "N"):
        ops[name] = getattr(gather, name)
    waits = {
        "N": gather.keep_own,
        "X": lambda: [(d_own(q, k).wait(), d_pair(q, k, 1 - c).wait_recv()) for q, k in quarters],
    }
    for step in MLP_STEPS:
        if step[0] in waits:
            waits.pop(step[0])()
        ops[step[0]](*step[1:])

    gather.drain()
    reduce.drain()
    for q, k in quarters:
        d_pair(q, k, c).wait_send()

    def chunk_sent(n, carry):
        for kind in range(4):
            for copy in a_copies(kind, n):
                copy.wait_send()
        return carry

    lax.fori_loop(0, NCH, chunk_sent, 0)
    for j in range(NJ):
        y_copy(j).wait_send()
        y_wait(j)


def vmem(*shape, dtype=BF16):
    return pltpu.VMEM(shape, dtype)


def sems(*shape):
    return pltpu.SemaphoreType.DMA(shape)


def solution(mesh):
    assert mesh.shape["tx"] == 2 * NX and mesh.shape["ty"] == NX
    act_spec = P(("dp", "ty"), None, "tx")
    col_spec = P("tx", "ty")
    row_spec = P("ty", "tx")
    any_spec = pl.BlockSpec(memory_space=pl.ANY)
    vmem_spec = pl.BlockSpec(memory_space=pltpu.VMEM)

    def layer(x_blk, w_q, w_k, w_v, w_o, w_gate, w_up, w_down):
        _, seq, kd = x_blk.shape
        kc, width = 2 * kd, 2 * NX * kd
        ch = seq // (2 * NJ)
        h = ch // 2
        row_heads = w_q.shape[1]
        hc = row_heads // NX
        fc = w_down.shape[0] // NX
        assert hc % HEAD_DIM == 0
        tiles = (fc + 127) // 128
        f_a = (fc // 2 + 15) // 16 * 16

        inv_freq = THETA ** (-2.0 * np.arange(HEAD_DIM // 2) / HEAD_DIM)
        inv_freq = np.concatenate([inv_freq, inv_freq])
        turn = np.arange(ch)[:, None] * inv_freq
        base = np.arange(2 * NJ)[:, None] * ch * inv_freq
        turn = jnp.asarray(np.stack([np.cos(turn), np.sin(turn)]), F32)
        base = jnp.asarray(np.stack([np.cos(base), np.sin(base)]), F32)

        reduce_scratch = [vmem(NX, NJ, ch, kc), vmem(NJ, h, kc), vmem(NJ, ch - h, kc), vmem(NJ, ch, kc), vmem(NJ, ch, kc)]
        units = ((0, 0, h, 0), (0, h, h, 0)) + tuple((j, 0, ch, 0) for j in range(1, NJ))
        n_u = len(units)
        h_blk, w_all = pl.pallas_call(
            functools.partial(attention_kernel, units),
            out_shape=(jax.ShapeDtypeStruct((NJ, ch, kc), BF16), jax.ShapeDtypeStruct((2, fc, width), BF16)),
            in_specs=[vmem_spec] * 3 + [any_spec] * 6,
            out_specs=(vmem_spec, any_spec),
            scratch_shapes=[
                vmem(NJ, ch, kc), vmem(NX, NJ, ch, 2 * kc), vmem(NJ, ch, HEAD_DIM, dtype=F32), vmem(NJ, ch, HEAD_DIM, dtype=F32),
                vmem(NJ, ch // 4, 128, dtype=F32), vmem(NJ, ch // 4, 128, dtype=F32), vmem(ch, 128, dtype=F32), vmem(ch, 128, dtype=F32),
                vmem(2 * kc, 6 * hc), vmem(row_heads, kc), vmem(NCH, ch, 6 * hc), vmem(NCH, ch, 3 * hc), vmem(NCH, ch, hc),
                vmem(NX, NJ, ch, 2 * hc), vmem(NX, NJ, ch, 2 * hc), vmem(NCH, ch, row_heads), *reduce_scratch,
                vmem(2, fc, kd), vmem(2, f_a, kd), vmem(2, fc - f_a, kd),
                sems(n_u), sems(n_u), sems(n_u), sems(n_u), sems(2, n_u), sems(2, n_u), sems(2, n_u), sems(2, n_u),
                sems(NJ), sems(NJ), sems(2, 3), sems(2, 3), sems(2, 3), sems(2, 3), sems(2), sems(2), sems(3, 3), sems(1), sems(1),
                sems(NCH), sems(NCH), sems(NCH), sems(NCH), sems(4, NCH), sems(4, NCH), sems(4, NJ), sems(4, NJ),
                sems(2, 2), sems(2, 2, 2), sems(2, 2, 2), sems(2, 2), sems(2, 2), sems(2, 2), sems(2, 2), sems(2, 4), sems(2, 4),
            ],
            compiler_params=pltpu.CompilerParams(collective_id=0, has_side_effects=True, vmem_limit_bytes=VMEM_LIMIT),
            name="attention_part",
        )(x_blk[0], turn, base, w_q, w_k, w_v, w_o, w_gate.T, w_up.T)

        first = ch * 3 // 4 // 32 * 32
        units = ((0, 0, first, 1), (0, first, ch - first, 0), (1, 0, h, 0), (1, h, h, 0)) + tuple((j, 0, ch, 0) for j in range(2, NJ))
        n_u, n_x = len(units), len(units) + 3
        y_blk = pl.pallas_call(
            functools.partial(mlp_kernel, units),
            out_shape=jax.ShapeDtypeStruct((seq, kd), BF16),
            in_specs=[vmem_spec, any_spec, any_spec],
            out_specs=vmem_spec,
            scratch_shapes=[
                vmem(NX, NJ, ch, width), vmem(width, tiles * 256), vmem(3, 128, width),
                vmem(NX * tiles * 128, kc), vmem(NCH, ch, NX * tiles * 128), vmem(NCH, h, NX * 128), vmem(2 * ch, tiles * 128),
                vmem(ch, 128, dtype=F32), vmem(ch, 128, dtype=F32),
                *reduce_scratch, vmem(2, NJ, ch, kd),
                sems(4, n_x), sems(4, n_x), sems(2, n_u), sems(2, n_u), sems(2, n_u), sems(2, n_u),
                sems(4, NCH, 2), sems(4, NCH, 2), sems(4, NJ), sems(4, NJ), sems(NJ), sems(NJ),
                sems(2 * tiles), sems(NX, 2), sems(NX, 2), sems(NX, 2),
            ],
            compiler_params=pltpu.CompilerParams(collective_id=1, has_side_effects=True, vmem_limit_bytes=VMEM_LIMIT),
            name="mlp_part",
        )(h_blk, w_all, w_down)
        return y_blk[None]

    return jax.shard_map(
        layer,
        mesh=mesh,
        in_specs=(act_spec, col_spec, col_spec, col_spec, row_spec, col_spec, col_spec, row_spec),
        out_specs=act_spec,
        check_vma=False,
    )
```

```python
import functools

import jax
import jax.numpy as jnp
import numpy as np
from jax import lax
from jax.experimental import pallas as pl
from jax.experimental.pallas import tpu as pltpu
from jax.sharding import PartitionSpec as P

HEAD_DIM = 128
EPS = 1e-5
THETA = 10000.0
MESH = pl.DeviceIdType.MESH
F32 = jnp.float32
BF16 = jnp.bfloat16
NX = 4
NJ = 4
NCH = 16
VMEM_LIMIT = 67_043_328
GROUPS = (*(((0, j),) for j in range(NJ)), *(((3, j), (1, j)) for j in range(NJ)), *(((2, j),) for j in range(NJ)))


def rem(a, b):
    return lax.rem(a, jnp.int32(b))


def div(a, b):
    return lax.div(a, jnp.int32(b))


def al(v, m):
    return pl.multiple_of(v, m)


def remote(src, dst, ssem, rsem, dev):
    return pltpu.make_async_remote_copy(src_ref=src, dst_ref=dst, send_sem=ssem, recv_sem=rsem, device_id=dev, device_id_type=MESH)


ATTENTION_STEPS = (
    ("WA", 0), ("S", "b", 0, 0), ("XP", 0), ("O", "b", 1), ("XE", 0), ("O", "b", 0), ("XE", 1), ("WA", 1), ("XP", 2),
    ("ST", 0), ("ST", 1), ("XP", 1), ("S", "b", 1, 0), ("XP", 3), ("XE", 2), ("S", "b", 0, 1), ("S", "b", 1, 1), ("N", 0),
    ("XE", 3), ("N", 1), ("WOP",), ("WP", 1), ("O", "a", 0), ("WP", 0), ("YH", 0), ("YH", 1), ("ST", 2), ("G", 0), ("N", 2),
    ("G", 8), ("ST", 3), ("F", "a", 1), ("G", 4), ("R", 0), ("R", 8), ("A", 8), ("A", 0), ("YH", 2), ("G", 1), ("XE", 4),
    ("N", 3), ("R", 4), ("A", 4), ("P", 8), ("P", 0), ("G", 9), ("G", 2), ("P", 4), ("ST", 4), ("O", "a", 1), ("X", 8),
    ("G", 5), ("YH", 3), ("R", 9), ("X", 0), ("A", 9), ("X", 4), ("M", 0), ("S", "a", 0, 1), ("N", 4), ("G", 10), ("P", 9),
    ("T", 0), ("HF", 0), ("R", 1), ("R", 5), ("A", 5), ("X", 9), ("R", 10), ("HH", 0), ("A", 1), ("YH", 4), ("G", 6),
    ("F", "a", 0), ("P", 5), ("HN", 0), ("A", 10), ("G", 11), ("S", "a", 0, 0), ("R", 2), ("G", 7), ("R", 6), ("P", 10),
    ("A", 6), ("X", 5), ("R", 11), ("S", "a", 1, 0), ("M", 1), ("G", 3), ("A", 11), ("R", 7), ("A", 2), ("X", 10), ("A", 7),
    ("HY", 0), ("R", 3), ("P", 11), ("P", 6), ("F", "b", 0), ("P", 7), ("F", "b", 1), ("X", 11), ("S", "a", 1, 1), ("X", 6),
    ("M", 2), ("A", 3), ("DP", 0), ("P", 1), ("X", 7), ("P", 2), ("M", 3), ("DP", 1), ("P", 3), ("HO", 0), ("X", 1), ("X", 2),
    ("T", 1), ("T", 2), ("X", 3), ("T", 3),
)
MLP_STEPS = (
    ("XF", 0, 1), ("YR", 0), ("WT", 0), ("XF", 0, 0), ("XH", 0, 1), ("XF", 0, 3), ("YRH", 0), ("XF", 2, 0), ("N", 0, 1),
    ("WT", 1), ("WT", 2), ("XH", 0, 3), ("XF", 0, 2), ("WT", 3), ("XF", 1, 0), ("XF", 3, 0), ("N", 0, 3), ("G", 8), ("YH", 1),
    ("XH", 2, 0), ("G", 4), ("P", 8), ("XH", 3, 0), ("XH", 0, 0), ("XH", 0, 2), ("G", 3), ("XH", 1, 0), ("YH", 3), ("G", 7),
    ("N", 2, 0), ("N", 0, 0), ("G", 9), ("N", 0, 2), ("P", 7), ("G", 11), ("P", 4), ("P", 9), ("N", 1, 0), ("N", 3, 0),
    ("G", 5), ("X", 8), ("G", 1), ("X", 4), ("YH", 2), ("P", 11), ("G", 6), ("X", 9), ("X", 7), ("X", 11), ("P", 5), ("M", 0),
    ("G", 10), ("G", 0), ("M", 3), ("X", 5), ("P", 10), ("P", 3), ("M", 1), ("P", 6), ("G", 2), ("P", 1), ("X", 10), ("X", 3),
    ("P", 0), ("X", 6), ("M", 2), ("T", 3), ("P", 2), ("X", 1), ("T", 1), ("X", 0), ("T", 0), ("X", 2), ("T", 2),
)


class Place:
    def __init__(self):
        tx, ty = lax.axis_index("tx"), lax.axis_index("ty")
        self.x, self.c, self.y = div(tx, 2), rem(tx, 2), ty
        x, c, y = self.x, self.c, self.y
        self.xr, self.xl, self.xo = rem(x + 1, NX), rem(x + 3, NX), rem(x + 2, NX)
        self.yu, self.yd, self.yo = rem(y + 1, NX), rem(y + 3, NX), rem(y + 2, NX)
        self.right = {"tx": self.xr * 2 + c, "ty": y}
        self.left = {"tx": self.xl * 2 + c, "ty": y}
        self.up = {"tx": tx, "ty": self.yu}
        self.down = {"tx": tx, "ty": self.yd}
        self.partner = {"tx": x * 2 + 1 - c, "ty": y}
        self.xa, self.xb = x + 1 - 2 * rem(x, 2), rem(x + 3 + 2 * rem(x, 2), NX)
        self.pa, self.pb = {"tx": self.xa * 2 + c, "ty": y}, {"tx": self.xb * 2 + c, "ty": y}

    def barrier(self):
        sem = pltpu.get_barrier_semaphore()
        for dev in (self.right, self.left, self.up, self.down, self.partner):
            pl.semaphore_signal(sem, inc=1, device_id=dev, device_id_type=MESH)
        pl.semaphore_wait(sem, 5)


class Spread:
    def __init__(self, at, src, xg, units, sums, sx, rx, sy, ry, syh, ryh):
        self.sums = sums
        self.at, self.src, self.xg, self.units, self.kc = at, src, xg, units, src.shape[2]
        self.sx, self.rx, self.sy, self.ry, self.syh, self.ryh = sx, rx, sy, ry, syh, ryh
        pairs = [(r, u) for u, unit in enumerate(units) for r in ((0, 3, 1, 2) if unit[3] else (0,))]
        self.index = {pair: i for i, pair in enumerate(pairs)}
        self.seqs = (at.y, at.yu, at.yo, at.yd)

    def cols(self, x):
        return pl.ds(al(x * self.kc, 128), self.kc)

    def keep_own(self):
        for j in {unit[0]: 0 for unit in self.units}:
            self.xg[self.at.y, j, :, self.cols(self.at.x)] = self.src[j]

    def xcopy(self, kind, r, u):
        at, s = self.at, self.seqs[r]
        j, lo, n, _ = self.units[u]
        i = self.index[r, u]
        if kind < 2:
            dst = self.xg.at[s, j, pl.ds(lo, n), self.cols(at.x)]
            src = self.src.at[j, pl.ds(lo, n)] if r == 0 else dst
        elif kind == 2:
            src = dst = self.xg.at[s, j, pl.ds(lo, n // 2), self.cols(at.xl)]
        else:
            src = dst = self.xg.at[s, j, pl.ds(lo + n // 2, n // 2), self.cols(at.xr)]
        return remote(src, dst, self.sx.at[kind, i], self.rx.at[kind, i], at.left if kind % 2 else at.right)

    def xwait(self, kind, r, u):
        at = self.at
        j, lo, n, _ = self.units[u]
        i = self.index[r, u]
        x = (at.xl, at.xr, at.xo, at.xo)[kind]
        rows = (pl.ds(lo, n), pl.ds(lo, n), pl.ds(lo, n // 2), pl.ds(lo + n // 2, n // 2))[kind]
        dst = self.xg.at[self.seqs[r], j, rows, self.cols(x)]
        remote(dst, dst, self.sx.at[kind, i], self.rx.at[kind, i], at.right).wait_recv()

    def yref(self, s, u, lo, n):
        j, _, _, first = self.units[u]
        rows = pl.ds(lo, n)
        return self.xg.at[s, j, rows, self.cols(self.at.x)] if first else self.xg.at[s, j, rows]

    def ycopy(self, d, u):
        j, lo, n, first = self.units[u]
        dst = self.yref(self.at.y, u, lo, n)
        src = self.src.at[j, pl.ds(lo, n)] if first else dst
        return remote(src, dst, self.sy.at[d, u], self.ry.at[d, u], self.at.down if d else self.at.up)

    def ywait(self, d, u):
        _, lo, n, _ = self.units[u]
        dst = self.yref(self.at.yu if d else self.at.yd, u, lo, n)
        remote(dst, dst, self.sy.at[d, u], self.ry.at[d, u], self.at.up).wait_recv()

    def yhalf(self, d, u):
        _, lo, n, _ = self.units[u]
        ref = self.yref(self.at.yu if d else self.at.yd, u, lo + d * (n // 2), n // 2)
        return remote(ref, ref, self.syh.at[d, u], self.ryh.at[d, u], self.at.down if d else self.at.up)

    def yhalf_wait(self, d, u):
        _, lo, n, _ = self.units[u]
        dst = self.yref(self.at.yo, u, lo + d * (n // 2), n // 2)
        remote(dst, dst, self.syh.at[d, u], self.ryh.at[d, u], self.at.up).wait_recv()

    def YR(self, u):
        for d in range(2):
            self.ycopy(d, u).start()

    def YH(self, u):
        for d in range(2):
            self.ywait(d, u)
            self.yhalf(d, u).start()

    YRH = YH

    def XF(self, r, u):
        if r == 2:
            for d in range(2):
                self.yhalf_wait(d, u)
        for kind in range(2):
            self.xcopy(kind, r, u).start()

    def XH(self, r, u):
        for kind in range(2):
            self.xwait(kind, r, u)
            self.xcopy(kind + 2, r, u).start()

    def N(self, r, u):
        j, lo, n, first = self.units[u]
        for kind in (2, 3):
            self.xwait(kind, r, u)
            self.xcopy(kind, r, u).wait_send()
        if r:
            for kind in range(2):
                self.xcopy(kind, r, u).wait_send()
        if r % 2:
            self.yhalf(0 if r == 3 else 1, u).wait_send()
        width, ref = self.xg.shape[-1], self.xg.at[self.seqs[r], j]
        s1, s2 = self.sums
        lane_sums(ref, lo, n, s1, s2)
        mean = jnp.sum(s1[0:n, :], axis=-1, keepdims=True) / width
        var = jnp.sum(s2[0:n, :], axis=-1, keepdims=True) / width - mean * mean
        s1[0:n, :] = jnp.broadcast_to(mean, (n, 128))
        s2[0:n, :] = jnp.broadcast_to(lax.rsqrt(var + EPS), (n, 128))
        scale_rows(ref, lo, n, s1, s2)
        if not first:
            self.YR(u)

    def chunk_wait(self, r, j):
        if r == 2:
            for u, unit in enumerate(self.units):
                if unit[0] == j and not unit[3]:
                    for d in range(2):
                        self.yhalf_wait(d, u)

    def drain(self):
        for u, unit in enumerate(self.units):
            for d in range(2):
                self.xcopy(d, 0, u).wait_send()
                self.ycopy(d, u).wait_send()
                if not unit[3]:
                    self.yhalf(d, u).wait_send()


def rows_of(refs):
    return refs[0][...] if len(refs) == 1 else jnp.concatenate([ref[...] for ref in refs], axis=0)


def product(refs, weight, depth, n_cols, done):
    step = 256

    def columns(i, carry):
        out = jnp.dot(rows_of(refs), weight[0:depth, pl.ds(al(i * step, 128), step)], preferred_element_type=F32)
        done(i * step, step, out)
        return carry

    lax.fori_loop(0, n_cols // step, columns, 0)


def lane_sums(ref, lo, n, s1, s2):
    width, rows, wide = ref.shape[-1], 32, 512

    def some_rows(i, carry):
        def some_columns(k, sums):
            a, b = sums
            v = ref[pl.ds(al(lo + i * rows, 8), rows), pl.ds(al(k * wide, 128), wide)].astype(F32)
            for c in range(0, wide, 128):
                part = v[:, c : c + 128]
                a, b = a + part, b + part * part
            return a, b

        zero = jnp.zeros((rows, 128), F32)
        a, b = lax.fori_loop(0, width // wide, some_columns, (zero, zero))
        s1[pl.ds(al(i * rows, 8), rows), :] = a
        s2[pl.ds(al(i * rows, 8), rows), :] = b
        return carry

    lax.fori_loop(0, n // rows, some_rows, 0)


def scale_rows(ref, lo, n, means, scales):
    width, rows, wide = ref.shape[-1], 32, 512

    def some_rows(i, carry):
        mean, scale = (t[pl.ds(al(i * rows, 8), rows), :] for t in (means, scales))

        def some_columns(k, carry):
            at_rows = pl.ds(al(lo + i * rows, 8), rows)
            for c in range(0, wide, 128):
                cols = pl.ds(al(k * wide + c, 128), 128)
                ref[at_rows, cols] = ((ref[at_rows, cols].astype(F32) - mean) * scale).astype(BF16)
            return carry

        lax.fori_loop(0, width // wide, some_columns, 0)
        return carry

    lax.fori_loop(0, n // rows, some_rows, 0)


class Reduce:
    def __init__(self, at, zb, ya, yb, yfd, yfu, ss, rs):
        self.at, self.zb, self.ya, self.yb, self.yfd, self.yfu, self.ss, self.rs = at, zb, ya, yb, yfd, yfu, ss, rs
        self.ch = zb.shape[2]
        self.h = self.ch // 2

    def copy(self, kind, j):
        at, h, ch = self.at, self.h, self.ch
        src, dst = (
            lambda: (self.zb.at[2, j, pl.ds(0, h)], self.ya.at[j]),
            lambda: (self.zb.at[2, j, pl.ds(h, ch - h)], self.yb.at[j]),
            lambda: (self.zb.at[1, j], self.yfd.at[j]),
            lambda: (self.zb.at[3, j], self.yfu.at[j]),
        )[kind]()
        return remote(src, dst, self.ss.at[kind, j], self.rs.at[kind, j], at.down if kind % 2 else at.up)

    def wait(self, kind, j):
        self.copy(kind, j).wait_recv()

    def halves(self, j):
        self.copy(0, j).start()
        self.copy(1, j).start()

    def middle(self, j):
        h = self.h
        self.wait(0, j)
        self.zb[1, j, 0:h] = (self.zb[1, j, 0:h].astype(F32) + self.ya[j].astype(F32)).astype(BF16)
        self.copy(2, j).start()
        self.wait(1, j)
        self.zb[3, j, h:] = (self.zb[3, j, h:].astype(F32) + self.yb[j].astype(F32)).astype(BF16)
        self.copy(3, j).start()

    def total(self, j):
        self.wait(2, j)
        self.wait(3, j)
        return self.zb[0, j].astype(F32) + self.yfd[j].astype(F32) + self.yfu[j].astype(F32)

    def drain(self):
        for j in range(NJ):
            for kind in range(4):
                self.copy(kind, j).wait_send()


def attention_kernel(
    units, x_ref, turn_ref, base_ref, wq, wk, wv, wo, wg_t, wu_t,
    h_ref, w_all, hg_all,
    xc, xg, hg, cos_all, sin_all, st_own, st_in, s1, s2, wb, wob, part, precv, qb, kvo, kvp, og, zb, ya, yb, yfd, yfu, own, drel_a, drel_b,
    sxe, rxe, sst, rst, sy, ry, syh, ryh, sd, rd, swa, rwa, swo, rwo, swp, rwp, lw, so, ro, spr, rpr, skv, rkv, sog, rog, syr, ryr,
    lg, sds, rds, sdo, rdo, sdf, rdf, sdp, rdp, shx, rhx, shy, rhy, shz, rhz, lh,
):
    at = Place()
    x, c, y = at.x, at.c, at.y
    ch, kc = xc.shape[1], xc.shape[2]
    kd = wq.shape[0]
    hc = qb.shape[2]
    fc, f_a = w_all.shape[1], drel_a.shape[1]
    width = 2 * xg.shape[3]
    kh = div(x, 2)
    ng = rem(div(x + 1, 2), 2)
    gather = Spread(at, xc, xg, units, (s1, s2), None, None, sy, ry, syh, ryh)
    reduce = Reduce(at, zb, ya, yb, yfd, yfu, syr, ryr)
    ahead = Spread(at, h_ref, hg, ((0, 0, ch, 0),), (s1, s2), shx, rhx, shy, rhy, shz, rhz)
    weights = (wq, wk, wv)

    def half_cols(core):
        return pl.ds(al(core * kd, 128), kd)

    def x_rows(j, core):
        return pl.ds(al((2 * j + core) * ch, 8), ch)

    def x_pair(j):
        return remote(x_ref.at[x_rows(j, 1 - c)], xc.at[j, :, half_cols(c)], sd.at[j], rd.at[j], at.partner)

    def pair_cols(xx):
        return pl.ds(al(rem(xx, 2) * kc, 128), kc)

    def xe_copy(u, xx):
        j, lo, n, _ = units[u]
        rows = pl.ds(lo, n)
        return remote(xc.at[j, rows], xg.at[y, j, rows, pair_cols(xx)], sxe.at[u], rxe.at[u], at.pa)

    def st_copy(u):
        j, lo, n, _ = units[u]
        rows = pl.ds(lo // 4, n // 4)
        return remote(st_own.at[j, rows], st_in.at[j, rows], sst.at[u], rst.at[u], at.pb)

    def XP(j):
        x_pair(j).start()

    def XE(u):
        j, lo, n, _ = units[u]
        if lo == 0:
            dst = xc.at[j, :, half_cols(1 - c)]
            remote(dst, dst, sd.at[j], rd.at[j], at.partner).wait_recv()
        xe_copy(u, x).start()
        xg[y, j, lo : lo + n, pair_cols(x)] = xc[j, lo : lo + n]

    def ST(u):
        j, lo, n, _ = units[u]
        xe_copy(u, at.xa).wait_recv()
        quarter = n // 4
        lane = lax.broadcasted_iota(jnp.int32, (quarter, 128), 1)
        lane_sums(xg.at[y, j], lo, n, s1, s2)
        packed = jnp.zeros((quarter, 128), F32)
        for g in range(4):
            rows = pl.ds(g * quarter, quarter)
            total, square = (jnp.sum(t[rows, :], axis=-1, keepdims=True) for t in (s1, s2))
            packed = jnp.where(lane // 32 == g, jnp.where(lane % 32 < 16, total, square), packed)
        st_own[j, lo // 4 : lo // 4 + quarter, :] = packed
        st_copy(u).start()

    def N(u):
        j, lo, n, _ = units[u]
        st_copy(u).wait_recv()
        quarter = n // 4
        at_rows = slice(lo // 4, lo // 4 + quarter)
        moments = (st_own[j, at_rows, :] + st_in[j, at_rows, :]) / width
        for g in range(4):
            mean = moments[:, 32 * g : 32 * g + 1]
            var = moments[:, 32 * g + 16 : 32 * g + 17] - mean * mean
            rows = pl.ds(g * quarter, quarter)
            s1[rows, :] = jnp.broadcast_to(mean, (quarter, 128))
            s2[rows, :] = jnp.broadcast_to(lax.rsqrt(var + EPS), (quarter, 128))
        scale_rows(xg.at[y, j], lo, n, s1, s2)
        gather.YR(u)

    def w_rows(xx, core):
        return pl.ds(al(rem(xx, 2) * kc + core * kd, 128), kd)

    def w_part(group, half, i):
        return weights[i].at[:, pl.ds(al((2 * group + half) * hc, 128), hc)]

    def w_cols(half, i):
        return pl.ds(half * 3 * hc + i * hc, hc)

    def wa_copy(half, i, xx):
        return remote(w_part(1 - ng, half, i), wb.at[w_rows(xx, c), w_cols(half, i)], swa.at[half, i], rwa.at[half, i], at.pa)

    def wo_copy(half, i, core):
        return remote(w_part(ng, half, i), wb.at[w_rows(x, core), w_cols(half, i)], swo.at[half, i], rwo.at[half, i], at.partner)

    def w_local(half, i):
        return pltpu.make_async_copy(w_part(ng, half, i), wb.at[w_rows(x, c), w_cols(half, i)], lw.at[half, i])

    def wp_copy(half, core):
        ref = wb.at[w_rows(at.xa, core), pl.ds(half * 3 * hc, 3 * hc)]
        return remote(ref, ref, swp.at[half], rwp.at[half], at.partner)

    o_local = pltpu.make_async_copy(wo, wob.at[:, half_cols(c)], lw.at[2, 0])
    o_pair = remote(wo, wob.at[:, half_cols(c)], so.at[0], ro.at[0], at.partner)
    pieces = [(half, i) for half in range(2) for i in range(3)]

    def WOP():
        for half, i in pieces:
            wo_copy(half, i, c).start()
        o_pair.start()

    def WA(half):
        for i in range(3):
            wa_copy(half, i, x).start()

    def WP(half):
        for i in range(3):
            wa_copy(half, i, at.xa).wait_recv()
        wp_copy(half, c).start()

    def w_ready():
        for half, i in pieces:
            w_local(half, i).wait()
            wo_copy(half, i, 1 - c).wait_recv()
        for half in range(2):
            wp_copy(half, 1 - c).wait_recv()
        for m in range(2):
            d_in(m).wait()
            d_out(m).start()
            d_pair(m, 3, c).start()

    def o_ready():
        o_local.wait()
        dst = wob.at[:, half_cols(1 - c)]
        remote(dst, dst, so.at[0], ro.at[0], at.partner).wait_recv()

    mlp_weights = (wg_t, wu_t)
    parts = ((0, f_a), (f_a, fc - f_a))

    def d_src(m, xx, p):
        return mlp_weights[m].at[pl.ds(al(xx * fc + parts[p][0], 8), parts[p][1])]

    def d_dst(m, xx, p):
        return w_all.at[m, pl.ds(*parts[p]), pl.ds(al((2 * xx + c) * kd, 128), kd)]

    def s_copy(d, m, p, xx):
        to, dev = ((at.xa, at.pa), (at.xb, at.pb))[d]
        return remote(d_src(m, to, p), d_dst(m, xx, p), sds.at[d, m, p], rds.at[d, m, p], dev)

    def o_copy(d, m):
        return remote(d_src(m, at.xo, d), (drel_a, drel_b)[d].at[m], sdo.at[d, m], rdo.at[d, m], (at.pa, at.pb)[d])

    def f_copy(d, m, xx):
        return remote((drel_a, drel_b)[d].at[m], d_dst(m, xx, d), sdf.at[d, m], rdf.at[d, m], (at.pb, at.pa)[d])

    def d_in(m):
        return pltpu.make_async_copy(mlp_weights[m].at[pl.ds(al(x * fc, 8), fc)], own.at[m], lg.at[0, m])

    def d_all(m, xx, core):
        return w_all.at[m, :, pl.ds(al((2 * xx + core) * kd, 128), kd)]

    def d_out(m):
        return pltpu.make_async_copy(own.at[m], d_all(m, x, c), lg.at[1, m])

    def d_pair(m, k, core):
        dst = d_all(m, (at.xa, at.xb, at.xo, x)[k], core)
        return remote(own.at[m] if k == 3 else dst, dst, sdp.at[m, k], rdp.at[m, k], at.partner)

    def S(link, m, p):
        s_copy("ab".index(link), m, p, x).start()

    def O(link, m):
        o_copy("ab".index(link), m).start()

    def F(link, m):
        d = "ba".index(link)
        o_copy(d, m).wait_recv()
        f_copy(d, m, (at.xa, at.xb)[d]).start()

    def DP(m):
        for d in range(2):
            for p in range(2):
                s_copy(d, m, p, (at.xa, at.xb)[d]).wait_recv()
            f_copy(d, m, at.xo).wait_recv()
        for k in range(3):
            d_pair(m, k, c).start()

    def pr_copy(n):
        src = part.at[n, :, pl.ds(al((1 - kh) * 3 * hc, 128), 3 * hc)]
        return remote(src, precv.at[n], spr.at[n], rpr.at[n], at.pb)

    def G(g):
        for r, j in GROUPS[g]:
            gather.chunk_wait(r, j)

        def done(col, size, out):
            for i, (r, j) in enumerate(GROUPS[g]):
                part[r * NJ + j, :, pl.ds(al(col, 128), size)] = out[i * ch : (i + 1) * ch].astype(BF16)

        product([xg.at[gather.seqs[r], j] for r, j in GROUPS[g]], wb, wb.shape[0], wb.shape[1], done)
        for r, j in GROUPS[g]:
            pr_copy(r * NJ + j).start()

    def kv_copy(r, j):
        s, n = gather.seqs[r], r * NJ + j
        return remote(kvo.at[s, j], kvp.at[s, j], skv.at[n], rkv.at[n], at.partner)

    def rotate(r, j):
        s, n = gather.seqs[r], r * NJ + j
        pr_copy(n).wait_recv()
        cos_t, sin_t = cos_all[j], sin_all[j]

        def total(col, size):
            mine = part[n, :, pl.ds(al(kh * 3 * hc + col, 128), size)]
            return (mine.astype(F32) + precv[n, :, col : col + size].astype(F32)).astype(BF16)

        def turned(col):
            v = total(col, HEAD_DIM).astype(F32)
            return (v * cos_t + pltpu.roll(v, HEAD_DIM // 2, axis=1) * sin_t).astype(BF16)

        for col in range(0, hc, HEAD_DIM):
            qb[n, :, col : col + HEAD_DIM] = turned(col)
            kvo[s, j, :, col : col + HEAD_DIM] = turned(hc + col)
        kvo[s, j, :, hc:] = total(2 * hc, hc)
        kv_copy(r, j).start()

    def R(g):
        for r, j in GROUPS[g]:
            rotate(r, j)

    def o_cols(xx):
        return pl.ds(al((2 * rem(div(xx + 1, 2), 2) + div(xx, 2)) * hc, 128), hc)

    cut = ch // 8

    def og_copy(kind, n):
        if kind < 2:
            ref = og.at[n, :, o_cols(x)]
        elif kind == 2:
            ref = og.at[n, pl.ds(0, cut), o_cols(at.xa)]
        else:
            ref = og.at[n, pl.ds(cut, ch - cut), o_cols(at.xb)]
        return remote(ref, ref, sog.at[kind, n], rog.at[kind, n], at.pa if kind in (0, 3) else at.pb)

    def og_wait(kind, n):
        xx = (at.xa, at.xb, at.xo, at.xo)[kind]
        rows = (pl.ds(0, ch), pl.ds(0, ch), pl.ds(0, cut), pl.ds(cut, ch - cut))[kind]
        dst = og.at[n, rows, o_cols(xx)]
        remote(dst, dst, sog.at[kind, n], rog.at[kind, n], at.pa).wait_recv()

    def attend(r, j, i):
        s, n = gather.seqs[r], r * NJ + j
        keys = (j + 1) * ch
        iq = lax.broadcasted_iota(jnp.int32, (ch, keys), 0) + j * ch
        ik = lax.broadcasted_iota(jnp.int32, (ch, keys), 1)
        own_ok = iq >= ik
        par_ok = ik < (j + c) * ch
        contract = (((1,), (1,)), ((), ()))
        cols = pl.ds(al(i * HEAD_DIM, 128), HEAD_DIM)
        v_cols = pl.ds(al(hc + i * HEAD_DIM, 128), HEAD_DIM)
        q = qb[n, :, cols]
        k_own = kvo[s, 0 : j + 1, :, cols].reshape(keys, HEAD_DIM)
        k_par = kvp[s, 0 : j + 1, :, cols].reshape(keys, HEAD_DIM)
        s_own = lax.dot_general(q, k_own, contract, preferred_element_type=F32) * HEAD_DIM**-0.5
        s_par = lax.dot_general(q, k_par, contract, preferred_element_type=F32) * HEAD_DIM**-0.5
        s_own = jnp.where(own_ok, s_own, -1e30)
        s_par = jnp.where(par_ok, s_par, -1e30)
        top = jnp.maximum(jnp.max(s_own, axis=1, keepdims=True), jnp.max(s_par, axis=1, keepdims=True))
        e_own, e_par = jnp.exp(s_own - top), jnp.exp(s_par - top)
        inv = 1.0 / (jnp.sum(e_own, axis=1, keepdims=True) + jnp.sum(e_par, axis=1, keepdims=True))
        v_own = kvo[s, 0 : j + 1, :, v_cols].reshape(keys, HEAD_DIM)
        v_par = kvp[s, 0 : j + 1, :, v_cols].reshape(keys, HEAD_DIM)
        out = jnp.dot((e_own * inv).astype(BF16), v_own, preferred_element_type=F32)
        out += jnp.dot((e_par * inv).astype(BF16), v_par, preferred_element_type=F32)
        og[n, :, pl.ds(al((2 * ng + kh) * hc + i * HEAD_DIM, 128), HEAD_DIM)] = out.astype(BF16)

    def A(g):
        for r, j in GROUPS[g]:
            kv_copy(r, j).wait_recv()

        def head(i, carry):
            for r, j in GROUPS[g]:
                attend(r, j, i)
            return carry

        lax.fori_loop(0, hc // HEAD_DIM, head, 0)
        for r, j in GROUPS[g]:
            og_copy(0, r * NJ + j).start()
            og_copy(1, r * NJ + j).start()

    def P(g):
        for r, j in GROUPS[g]:
            for kind in range(2):
                og_wait(kind, r * NJ + j)
                og_copy(kind + 2, r * NJ + j).start()

    def X(g):
        for r, j in GROUPS[g]:
            og_wait(2, r * NJ + j)
            og_wait(3, r * NJ + j)

        def done(col, size, out):
            for i, (r, j) in enumerate(GROUPS[g]):
                zb[r, j, :, pl.ds(al(col, 128), size)] = out[i * ch : (i + 1) * ch].astype(BF16)

        product([og.at[r * NJ + j] for r, j in GROUPS[g]], wob, wob.shape[0], kc, done)
        for r, j in GROUPS[g]:
            if r == 2:
                reduce.halves(j)

    def T(j):
        attn = reduce.total(j).astype(BF16)
        h_ref[j] = (xc[j].astype(F32) + attn.astype(F32)).astype(BF16)

    def h_out(r):
        return pltpu.make_async_copy(hg.at[ahead.seqs[r], 0], hg_all.at[ahead.seqs[r]], lh.at[r])

    def HF(u):
        ahead.keep_own()
        ahead.XF(0, u)

    def HY(u):
        ahead.YH(u)
        for r in (0, 1, 3):
            h_out(r).start()

    def HO(u):
        for d in range(2):
            ahead.yhalf_wait(d, u)
        h_out(2).start()

    for half, i in pieces:
        w_local(half, i).start()
    o_local.start()
    for m in range(2):
        d_in(m).start()
    for j in range(NJ):
        xc[j, :, half_cols(c)] = x_ref[x_rows(j, c), :]
    at.barrier()

    def angles():
        lane = lax.broadcasted_iota(jnp.int32, (ch, HEAD_DIM), 1)
        for j in range(NJ):
            base_cos, base_sin = base_ref[0, pl.ds(2 * j + c, 1), :], base_ref[1, pl.ds(2 * j + c, 1), :]
            cos_all[j] = base_cos * turn_ref[0] - base_sin * turn_ref[1]
            sine = base_sin * turn_ref[0] + base_cos * turn_ref[1]
            sin_all[j] = jnp.where(lane < HEAD_DIM // 2, -sine, sine)

    ops = {
        "XP": XP, "WOP": WOP, "XE": XE, "ST": ST, "N": N, "YH": gather.YH, "WA": WA, "WP": WP, "S": S, "O": O, "F": F, "DP": DP,
        "G": G, "R": R, "A": A, "P": P, "X": X, "M": reduce.middle, "T": T,
        "HF": HF, "HH": lambda u: ahead.XH(0, u), "HN": lambda u: ahead.N(0, u), "HY": HY, "HO": HO,
    }
    waits = {"G": w_ready, "X": o_ready, "WP": angles}
    for step in ATTENTION_STEPS:
        if step[0] in waits:
            waits.pop(step[0])()
        ops[step[0]](*step[1:])

    for m in range(2):
        for k in range(4):
            d_pair(m, k, 1 - c).wait_recv()
            d_pair(m, k, c).wait_send()
        d_out(m).wait()
        for d in range(2):
            for p in range(2):
                s_copy(d, m, p, x).wait_send()
            o_copy(d, m).wait_send()
            f_copy(d, m, x).wait_send()
    for j in range(NJ):
        x_pair(j).wait_send()
    for u in range(len(units)):
        xe_copy(u, x).wait_send()
        st_copy(u).wait_send()
        for d in range(2):
            gather.ycopy(d, u).wait_send()
            gather.yhalf(d, u).wait_send()
    reduce.drain()
    ahead.drain()
    for r in range(NX):
        h_out(r).wait()
    o_pair.wait_send()
    for half, i in pieces:
        wa_copy(half, i, x).wait_send()
        wo_copy(half, i, c).wait_send()
    for half in range(2):
        wp_copy(half, c).wait_send()

    def chunk_sent(n, carry):
        pr_copy(n).wait_send()
        remote(kvo.at[0, 0], kvp.at[0, 0], skv.at[n], rkv.at[n], at.partner).wait_send()
        for kind in range(4):
            og_copy(kind, n).wait_send()
        return carry

    lax.fori_loop(0, NCH, chunk_sent, 0)


def mlp_kernel(
    units, h_ref, w_hbm, wdn, hg_hbm, y_ref,
    xg, wt, raw, wd, ag, ar, act, s1, s2, zb, ya, yb, yfd, yfu, yst,
    sx, rx, sy, ry, syh, ryh, sa, ra, syr, ryr, sd, rd, lw, lwd, swd, rwd, lh,
):
    at = Place()
    x, c, y = at.x, at.c, at.y
    ch, kc, h = h_ref.shape[1], h_ref.shape[2], h_ref.shape[1] // 2
    width = xg.shape[-1]
    kd = kc // 2
    fc, tiles = w_hbm.shape[1], wt.shape[1] // 256
    fm = (tiles - 1) * 128
    fr = fc - fm
    blocks, slots = 2 * tiles, raw.shape[0]
    gather = Spread(at, h_ref, xg, units, (s1, s2), sx, rx, sy, ry, syh, ryh)
    reduce = Reduce(at, zb, ya, yb, yfd, yfu, syr, ryr)

    def w_in(q):
        i, m = q // 2, q % 2
        n = min(128, fc - i * 128)
        return pltpu.make_async_copy(w_hbm.at[m, pl.ds(i * 128, n)], raw.at[q % slots, pl.ds(0, n)], lw.at[q])

    def WT(g):
        for q in range(g * blocks // 4, (g + 1) * blocks // 4):
            i, m, slot = q // 2, q % 2, q % slots
            w_in(q).wait()
            if fc < (i + 1) * 128:
                raw[slot, fc - i * 128 :, :] = jnp.zeros(((i + 1) * 128 - fc, width), BF16)

            def turn(k, carry, slot=slot, q=q):
                part = pl.ds(al(k * (width // 4), 128), width // 4)
                wt[part, q * 128 : (q + 1) * 128] = raw[slot, :, part].T
                return carry

            lax.fori_loop(0, 4, turn, 0)
            if q + slots < blocks:
                w_in(q + slots).start()

    def d_refs(q, core):
        cols = pl.ds(al(core * kd, 128), kd)
        main, rest = wdn.at[pl.ds(q * fc, fm)], wdn.at[pl.ds(q * fc + fm, fr)]
        return (main, wd.at[pl.ds(q * fm, fm), cols]), (rest, wd.at[pl.ds(NX * fm + q * 128, fr), cols])

    def d_own(q, k):
        src, dst = d_refs(q, c)[k]
        return pltpu.make_async_copy(src, dst, lwd.at[q, k])

    def d_pair(q, k, core):
        src, dst = d_refs(q, core)[k]
        return remote(src, dst, swd.at[q, k], rwd.at[q, k], at.partner)

    quarters = [(q, k) for q in range(NX) for k in range(2)]
    for q in range(slots):
        w_in(q).start()
    def h_in(s):
        return pltpu.make_async_copy(hg_hbm.at[s], xg.at[s, 0], lh.at[s])

    for s in range(NX):
        h_in(s).start()
    for q, k in quarters:
        d_own(q, k).start()
    for q in range(NX):
        wd[NX * fm + q * 128 + fr : NX * fm + (q + 1) * 128, :] = jnp.zeros((128 - fr, kc), BF16)
    at.barrier()
    for q, k in quarters:
        d_pair(q, k, c).start()

    def a_refs(kind, n, xx):
        main, rest = pl.ds(al(xx * fm, 128), fm), pl.ds(al(xx * 128, 128), 128)
        if kind < 2:
            return ag.at[n, :, main], ar.at[n, :, rest]
        lo = (kind - 2) * h
        return ag.at[n, pl.ds(lo, h), main], ar.at[n, pl.ds(lo // 2, h // 2), rest]

    def a_copies(kind, n):
        refs = a_refs(kind, n, (x, x, at.xl, at.xr)[kind])
        return [remote(v, v, sa.at[kind, n, k], ra.at[kind, n, k], at.left if kind % 2 else at.right) for k, v in enumerate(refs)]

    def a_wait(kind, n):
        for k, v in enumerate(a_refs(kind, n, (at.xl, at.xr, at.xo, at.xo)[kind])):
            remote(v, v, sa.at[kind, n, k], ra.at[kind, n, k], at.right).wait_recv()

    def a_start(kind, n):
        for copy in a_copies(kind, n):
            copy.start()

    def G(g):
        for r, j in GROUPS[g]:
            gather.chunk_wait(r, j)

        def done(col, size, out):
            for k in range(0, size, 256):
                gate, up = out[:, k : k + 128].astype(BF16).astype(F32), out[:, k + 128 : k + 256].astype(BF16).astype(F32)
                value = (gate / (1.0 + jnp.exp(-gate)) * up).astype(BF16)
                act[0 : value.shape[0], pl.ds(al(div(col + k, 2), 128), 128)] = value

        product([xg.at[gather.seqs[r], j] for r, j in GROUPS[g]], wt, width, wt.shape[1], done)
        for i, (r, j) in enumerate(GROUPS[g]):
            n, lo = r * NJ + j, i * ch
            ag[n, :, pl.ds(al(x * fm, 128), fm)] = act[lo : lo + ch, :fm]
            below = pltpu.roll(act[lo + h : lo + ch, fm:].astype(F32), 64, axis=1)
            ar[n, :, pl.ds(al(x * 128, 128), 128)] = (act[lo : lo + h, fm:].astype(F32) + below).astype(BF16)
            for kind in range(2):
                a_start(kind, n)

    def P(g):
        for r, j in GROUPS[g]:
            for kind in range(2):
                a_wait(kind, r * NJ + j)
                a_start(kind + 2, r * NJ + j)

    def X(g):
        for r, j in GROUPS[g]:
            n = r * NJ + j
            for kind in (2, 3):
                a_wait(kind, n)
            for q in range(NX):
                cols = pl.ds(NX * fm + q * 128, 128)
                rest = ar[n, :, q * 128 : (q + 1) * 128]
                ag[n, 0:h, cols] = rest
                ag[n, h:, cols] = pltpu.roll(rest.astype(F32), 64, axis=1).astype(BF16)

        def done(col, size, out):
            for i, (r, j) in enumerate(GROUPS[g]):
                zb[r, j, :, pl.ds(al(col, 128), size)] = out[i * ch : (i + 1) * ch].astype(BF16)

        product([ag.at[r * NJ + j] for r, j in GROUPS[g]], wd, wd.shape[0], kc, done)
        for r, j in GROUPS[g]:
            if r == 2:
                reduce.halves(j)

    def y_rows(j, core):
        return pl.ds(al((2 * j + core) * ch, 8), ch)

    def y_copy(j):
        return remote(yst.at[1 - c, j], y_ref.at[y_rows(j, c)], sd.at[j], rd.at[j], at.partner)

    def y_wait(j):
        dst = y_ref.at[y_rows(j, 1 - c)]
        remote(dst, dst, sd.at[j], rd.at[j], at.partner).wait_recv()

    def T(j):
        mlp = reduce.total(j).astype(BF16)
        out = (h_ref[j].astype(F32) + mlp.astype(F32)).astype(BF16)
        yst[0, j] = out[:, :kd]
        yst[1, j] = out[:, kd:]
        y_copy(j).start()
        y_ref[y_rows(j, c), :] = yst[c, j]

    ops = {"G": G, "P": P, "X": X, "M": reduce.middle, "T": T, "WT": WT}
    for name in ("YR", "YRH", "YH", "XF", "XH", "N"):
        ops[name] = getattr(gather, name)
    waits = {
        "N": gather.keep_own,
        "G": lambda: [h_in(s).wait() for s in range(NX)],
        "X": lambda: [(d_own(q, k).wait(), d_pair(q, k, 1 - c).wait_recv()) for q, k in quarters],
    }
    for step in MLP_STEPS:
        if step[0] in waits:
            waits.pop(step[0])()
        ops[step[0]](*step[1:])

    gather.drain()
    reduce.drain()
    for q, k in quarters:
        d_pair(q, k, c).wait_send()

    def chunk_sent(n, carry):
        for kind in range(4):
            for copy in a_copies(kind, n):
                copy.wait_send()
        return carry

    lax.fori_loop(0, NCH, chunk_sent, 0)
    for j in range(NJ):
        y_copy(j).wait_send()
        y_wait(j)


def vmem(*shape, dtype=BF16):
    return pltpu.VMEM(shape, dtype)


def sems(*shape):
    return pltpu.SemaphoreType.DMA(shape)


def solution(mesh):
    assert mesh.shape["tx"] == 2 * NX and mesh.shape["ty"] == NX
    act_spec = P(("dp", "ty"), None, "tx")
    col_spec = P("tx", "ty")
    row_spec = P("ty", "tx")
    any_spec = pl.BlockSpec(memory_space=pl.ANY)
    vmem_spec = pl.BlockSpec(memory_space=pltpu.VMEM)

    def layer(x_blk, w_q, w_k, w_v, w_o, w_gate, w_up, w_down):
        _, seq, kd = x_blk.shape
        kc, width = 2 * kd, 2 * NX * kd
        ch = seq // (2 * NJ)
        h = ch // 2
        row_heads = w_q.shape[1]
        hc = row_heads // NX
        fc = w_down.shape[0] // NX
        assert hc % HEAD_DIM == 0
        tiles = (fc + 127) // 128
        f_a = (fc // 2 + 15) // 16 * 16

        inv_freq = THETA ** (-2.0 * np.arange(HEAD_DIM // 2) / HEAD_DIM)
        inv_freq = np.concatenate([inv_freq, inv_freq])
        turn = np.arange(ch)[:, None] * inv_freq
        base = np.arange(2 * NJ)[:, None] * ch * inv_freq
        turn = jnp.asarray(np.stack([np.cos(turn), np.sin(turn)]), F32)
        base = jnp.asarray(np.stack([np.cos(base), np.sin(base)]), F32)

        reduce_scratch = [vmem(NX, NJ, ch, kc), vmem(NJ, h, kc), vmem(NJ, ch - h, kc), vmem(NJ, ch, kc), vmem(NJ, ch, kc)]
        units = ((0, 0, h, 0), (0, h, h, 0)) + tuple((j, 0, ch, 0) for j in range(1, NJ))
        n_u = len(units)
        h_blk, w_all, hg_all = pl.pallas_call(
            functools.partial(attention_kernel, units),
            out_shape=(
                jax.ShapeDtypeStruct((NJ, ch, kc), BF16),
                jax.ShapeDtypeStruct((2, fc, width), BF16),
                jax.ShapeDtypeStruct((NX, ch, width), BF16),
            ),
            in_specs=[vmem_spec] * 3 + [any_spec] * 6,
            out_specs=(vmem_spec, any_spec, any_spec),
            scratch_shapes=[
                vmem(NJ, ch, kc), vmem(NX, NJ, ch, 2 * kc), vmem(NX, 1, ch, width), vmem(NJ, ch, HEAD_DIM, dtype=F32), vmem(NJ, ch, HEAD_DIM, dtype=F32),
                vmem(NJ, ch // 4, 128, dtype=F32), vmem(NJ, ch // 4, 128, dtype=F32), vmem(ch, 128, dtype=F32), vmem(ch, 128, dtype=F32),
                vmem(2 * kc, 6 * hc), vmem(row_heads, kc), vmem(NCH, ch, 6 * hc), vmem(NCH, ch, 3 * hc), vmem(NCH, ch, hc),
                vmem(NX, NJ, ch, 2 * hc), vmem(NX, NJ, ch, 2 * hc), vmem(NCH, ch, row_heads), *reduce_scratch,
                vmem(2, fc, kd), vmem(2, f_a, kd), vmem(2, fc - f_a, kd),
                sems(n_u), sems(n_u), sems(n_u), sems(n_u), sems(2, n_u), sems(2, n_u), sems(2, n_u), sems(2, n_u),
                sems(NJ), sems(NJ), sems(2, 3), sems(2, 3), sems(2, 3), sems(2, 3), sems(2), sems(2), sems(3, 3), sems(1), sems(1),
                sems(NCH), sems(NCH), sems(NCH), sems(NCH), sems(4, NCH), sems(4, NCH), sems(4, NJ), sems(4, NJ),
                sems(2, 2), sems(2, 2, 2), sems(2, 2, 2), sems(2, 2), sems(2, 2), sems(2, 2), sems(2, 2), sems(2, 4), sems(2, 4),
                sems(4, 1), sems(4, 1), sems(2, 1), sems(2, 1), sems(2, 1), sems(2, 1), sems(NX),
            ],
            compiler_params=pltpu.CompilerParams(collective_id=0, has_side_effects=True, vmem_limit_bytes=VMEM_LIMIT),
            name="attention_part",
        )(x_blk[0], turn, base, w_q, w_k, w_v, w_o, w_gate.T, w_up.T)

        units = ((1, 0, h, 1), (1, h, h, 0)) + tuple((j, 0, ch, 0) for j in range(2, NJ))
        n_u, n_x = len(units), len(units) + 3
        y_blk = pl.pallas_call(
            functools.partial(mlp_kernel, units),
            out_shape=jax.ShapeDtypeStruct((seq, kd), BF16),
            in_specs=[vmem_spec, any_spec, any_spec, any_spec],
            out_specs=vmem_spec,
            scratch_shapes=[
                vmem(NX, NJ, ch, width), vmem(width, tiles * 256), vmem(3, 128, width),
                vmem(NX * tiles * 128, kc), vmem(NCH, ch, NX * tiles * 128), vmem(NCH, h, NX * 128), vmem(2 * ch, tiles * 128),
                vmem(ch, 128, dtype=F32), vmem(ch, 128, dtype=F32),
                *reduce_scratch, vmem(2, NJ, ch, kd),
                sems(4, n_x), sems(4, n_x), sems(2, n_u), sems(2, n_u), sems(2, n_u), sems(2, n_u),
                sems(4, NCH, 2), sems(4, NCH, 2), sems(4, NJ), sems(4, NJ), sems(NJ), sems(NJ),
                sems(2 * tiles), sems(NX, 2), sems(NX, 2), sems(NX, 2), sems(NX),
            ],
            compiler_params=pltpu.CompilerParams(collective_id=1, has_side_effects=True, vmem_limit_bytes=VMEM_LIMIT),
            name="mlp_part",
        )(h_blk, w_all, w_down, hg_all)
        return y_blk[None]

    return jax.shard_map(
        layer,
        mesh=mesh,
        in_specs=(act_spec, col_spec, col_spec, col_spec, row_spec, col_spec, col_spec, row_spec),
        out_specs=act_spec,
        check_vma=False,
    )
```

```python
import functools

import jax
import jax.numpy as jnp
import numpy as np
from jax import lax
from jax.experimental import pallas as pl
from jax.experimental.pallas import tpu as pltpu
from jax.sharding import PartitionSpec as P

HEAD_DIM = 128
EPS = 1e-5
THETA = 10000.0
MESH = pl.DeviceIdType.MESH
F32 = jnp.float32
BF16 = jnp.bfloat16
NX = 4
NJ = 4
NCH = 16
VMEM_LIMIT = 67_043_328
GROUPS = (*(((0, j),) for j in range(NJ)), *(((3, j), (1, j)) for j in range(NJ)), *(((2, j),) for j in range(NJ)))


def rem(a, b):
    return lax.rem(a, jnp.int32(b))


def div(a, b):
    return lax.div(a, jnp.int32(b))


def al(v, m):
    return pl.multiple_of(v, m)


def remote(src, dst, ssem, rsem, dev):
    return pltpu.make_async_remote_copy(src_ref=src, dst_ref=dst, send_sem=ssem, recv_sem=rsem, device_id=dev, device_id_type=MESH)


ATTENTION_STEPS = (
    ("S", "b", 0, 0), ("WA", 0), ("XP", 3), ("XP", 0), ("WOP",), ("XE", 1), ("XE", 0), ("O", "b", 0), ("XP", 1), ("XE", 2),
    ("XP", 2), ("WA", 1), ("S", "b", 1, 0), ("ST", 1), ("S", "b", 0, 1), ("ST", 0), ("XE", 3), ("O", "b", 1), ("N", 1),
    ("WP", 0), ("ST", 2), ("N", 0), ("S", "b", 1, 1), ("YH", 1), ("YH", 0), ("G", 0), ("N", 2), ("S", "a", 1, 0), ("WP", 1),
    ("G", 8), ("G", 4), ("Q", 8), ("ST", 3), ("Q", 0), ("R", 8), ("A", 8), ("O", "a", 1), ("R", 0), ("YH", 2), ("G", 5),
    ("N", 3), ("R", 4), ("P", 8), ("A", 4), ("G", 9), ("XE", 4), ("A", 0), ("R", 5), ("X", 8), ("P", 4), ("A", 5), ("YH", 3),
    ("G", 1), ("R", 9), ("P", 0), ("ST", 4), ("A", 9), ("F", "a", 1), ("X", 4), ("M", 0), ("G", 2), ("G", 10), ("N", 4),
    ("P", 5), ("X", 0), ("P", 9), ("T", 0), ("R", 2), ("HF", 0), ("G", 3), ("X", 9), ("O", "a", 0), ("X", 5), ("YH", 4),
    ("HH", 0), ("G", 6), ("M", 1), ("S", "a", 1, 1), ("R", 10), ("A", 10), ("F", "a", 0), ("HN", 0), ("G", 11), ("G", 7),
    ("P", 10), ("R", 6), ("R", 11), ("A", 6), ("A", 11), ("S", "a", 0, 0), ("R", 7), ("F", "b", 1), ("X", 10), ("A", 7),
    ("P", 6), ("HY", 0), ("R", 1), ("P", 11), ("R", 3), ("A", 1), ("A", 2), ("P", 7), ("S", "a", 0, 1), ("X", 6),
    ("F", "b", 0), ("DP", 1), ("X", 11), ("A", 3), ("M", 2), ("HO", 0), ("X", 7), ("P", 1), ("P", 2), ("M", 3), ("DP", 0),
    ("P", 3), ("X", 1), ("T", 1), ("X", 2), ("T", 2), ("X", 3), ("T", 3),
)
MLP_STEPS = (
    ("XF", 0, 1), ("YR", 0), ("WT", 0), ("XF", 0, 0), ("XH", 0, 1), ("XF", 0, 3), ("YRH", 0), ("XF", 2, 0), ("N", 0, 1),
    ("WT", 1), ("WT", 2), ("XH", 0, 3), ("XF", 0, 2), ("WT", 3), ("XF", 1, 0), ("XF", 3, 0), ("N", 0, 3), ("G", 8), ("YH", 1),
    ("XH", 2, 0), ("G", 4), ("P", 8), ("XH", 3, 0), ("XH", 0, 0), ("XH", 0, 2), ("G", 3), ("XH", 1, 0), ("YH", 3), ("G", 7),
    ("N", 2, 0), ("N", 0, 0), ("G", 9), ("N", 0, 2), ("P", 7), ("G", 11), ("P", 4), ("P", 9), ("N", 1, 0), ("N", 3, 0),
    ("G", 5), ("X", 8), ("G", 1), ("X", 4), ("YH", 2), ("P", 11), ("G", 6), ("X", 9), ("X", 7), ("X", 11), ("P", 5), ("M", 0),
    ("G", 10), ("G", 0), ("M", 3), ("X", 5), ("P", 10), ("P", 3), ("M", 1), ("P", 6), ("G", 2), ("P", 1), ("X", 10), ("X", 3),
    ("P", 0), ("X", 6), ("M", 2), ("T", 3), ("P", 2), ("X", 1), ("T", 1), ("X", 0), ("T", 0), ("X", 2), ("T", 2),
)


class Place:
    def __init__(self):
        tx, ty = lax.axis_index("tx"), lax.axis_index("ty")
        self.x, self.c, self.y = div(tx, 2), rem(tx, 2), ty
        x, c, y = self.x, self.c, self.y
        self.xr, self.xl, self.xo = rem(x + 1, NX), rem(x + 3, NX), rem(x + 2, NX)
        self.yu, self.yd, self.yo = rem(y + 1, NX), rem(y + 3, NX), rem(y + 2, NX)
        self.right = {"tx": self.xr * 2 + c, "ty": y}
        self.left = {"tx": self.xl * 2 + c, "ty": y}
        self.up = {"tx": tx, "ty": self.yu}
        self.down = {"tx": tx, "ty": self.yd}
        self.partner = {"tx": x * 2 + 1 - c, "ty": y}
        self.xa, self.xb = x + 1 - 2 * rem(x, 2), rem(x + 3 + 2 * rem(x, 2), NX)
        self.pa, self.pb = {"tx": self.xa * 2 + c, "ty": y}, {"tx": self.xb * 2 + c, "ty": y}

    def barrier(self, between):
        sem = pltpu.get_barrier_semaphore()
        for dev in (self.right, self.left, self.up, self.down, self.partner):
            pl.semaphore_signal(sem, inc=1, device_id=dev, device_id_type=MESH)
        between()
        pl.semaphore_wait(sem, 5)


class Spread:
    def __init__(self, at, src, xg, units, sums, sx, rx, sy, ry, syh, ryh):
        self.sums = sums
        self.at, self.src, self.xg, self.units, self.kc = at, src, xg, units, src.shape[2]
        self.sx, self.rx, self.sy, self.ry, self.syh, self.ryh = sx, rx, sy, ry, syh, ryh
        pairs = [(r, u) for u, unit in enumerate(units) for r in ((0, 3, 1, 2) if unit[3] else (0,))]
        self.index = {pair: i for i, pair in enumerate(pairs)}
        self.seqs = (at.y, at.yu, at.yo, at.yd)

    def cols(self, x):
        return pl.ds(al(x * self.kc, 128), self.kc)

    def keep_own(self):
        for j in {unit[0]: 0 for unit in self.units}:
            self.xg[self.at.y, j, :, self.cols(self.at.x)] = self.src[j]

    def xcopy(self, kind, r, u):
        at, s = self.at, self.seqs[r]
        j, lo, n, _ = self.units[u]
        i = self.index[r, u]
        if kind < 2:
            dst = self.xg.at[s, j, pl.ds(lo, n), self.cols(at.x)]
            src = self.src.at[j, pl.ds(lo, n)] if r == 0 else dst
        elif kind == 2:
            src = dst = self.xg.at[s, j, pl.ds(lo, n // 2), self.cols(at.xl)]
        else:
            src = dst = self.xg.at[s, j, pl.ds(lo + n // 2, n // 2), self.cols(at.xr)]
        return remote(src, dst, self.sx.at[kind, i], self.rx.at[kind, i], at.left if kind % 2 else at.right)

    def xwait(self, kind, r, u):
        at = self.at
        j, lo, n, _ = self.units[u]
        i = self.index[r, u]
        x = (at.xl, at.xr, at.xo, at.xo)[kind]
        rows = (pl.ds(lo, n), pl.ds(lo, n), pl.ds(lo, n // 2), pl.ds(lo + n // 2, n // 2))[kind]
        dst = self.xg.at[self.seqs[r], j, rows, self.cols(x)]
        remote(dst, dst, self.sx.at[kind, i], self.rx.at[kind, i], at.right).wait_recv()

    def yref(self, s, u, lo, n):
        j, _, _, first = self.units[u]
        rows = pl.ds(lo, n)
        return self.xg.at[s, j, rows, self.cols(self.at.x)] if first else self.xg.at[s, j, rows]

    def ycopy(self, d, u):
        j, lo, n, first = self.units[u]
        dst = self.yref(self.at.y, u, lo, n)
        src = self.src.at[j, pl.ds(lo, n)] if first else dst
        return remote(src, dst, self.sy.at[d, u], self.ry.at[d, u], self.at.down if d else self.at.up)

    def ywait(self, d, u):
        _, lo, n, _ = self.units[u]
        dst = self.yref(self.at.yu if d else self.at.yd, u, lo, n)
        remote(dst, dst, self.sy.at[d, u], self.ry.at[d, u], self.at.up).wait_recv()

    def yhalf(self, d, u):
        _, lo, n, _ = self.units[u]
        ref = self.yref(self.at.yu if d else self.at.yd, u, lo + d * (n // 2), n // 2)
        return remote(ref, ref, self.syh.at[d, u], self.ryh.at[d, u], self.at.down if d else self.at.up)

    def yhalf_wait(self, d, u):
        _, lo, n, _ = self.units[u]
        dst = self.yref(self.at.yo, u, lo + d * (n // 2), n // 2)
        remote(dst, dst, self.syh.at[d, u], self.ryh.at[d, u], self.at.up).wait_recv()

    def YR(self, u):
        for d in range(2):
            self.ycopy(d, u).start()

    def YH(self, u):
        for d in range(2):
            self.ywait(d, u)
            self.yhalf(d, u).start()

    YRH = YH

    def XF(self, r, u):
        if r == 2:
            for d in range(2):
                self.yhalf_wait(d, u)
        for kind in range(2):
            self.xcopy(kind, r, u).start()

    def XH(self, r, u):
        for kind in range(2):
            self.xwait(kind, r, u)
            self.xcopy(kind + 2, r, u).start()

    def N(self, r, u):
        j, lo, n, first = self.units[u]
        for kind in (2, 3):
            self.xwait(kind, r, u)
            self.xcopy(kind, r, u).wait_send()
        if r:
            for kind in range(2):
                self.xcopy(kind, r, u).wait_send()
        if r % 2:
            self.yhalf(0 if r == 3 else 1, u).wait_send()
        width, ref = self.xg.shape[-1], self.xg.at[self.seqs[r], j]
        s1, s2 = self.sums
        lane_sums(ref, lo, n, s1, s2)
        mean = jnp.sum(s1[0:n, :], axis=-1, keepdims=True) / width
        var = jnp.sum(s2[0:n, :], axis=-1, keepdims=True) / width - mean * mean
        s1[0:n, :] = jnp.broadcast_to(mean, (n, 128))
        s2[0:n, :] = jnp.broadcast_to(lax.rsqrt(var + EPS), (n, 128))
        scale_rows(ref, lo, n, s1, s2)
        if not first:
            self.YR(u)

    def chunk_wait(self, r, j):
        if r == 2:
            for u, unit in enumerate(self.units):
                if unit[0] == j and not unit[3]:
                    for d in range(2):
                        self.yhalf_wait(d, u)

    def drain(self):
        for u, unit in enumerate(self.units):
            for d in range(2):
                self.xcopy(d, 0, u).wait_send()
                self.ycopy(d, u).wait_send()
                if not unit[3]:
                    self.yhalf(d, u).wait_send()


def rows_of(refs):
    return refs[0][...] if len(refs) == 1 else jnp.concatenate([ref[...] for ref in refs], axis=0)


def product(refs, weight, depth, n_cols, done):
    step = 256

    def columns(i, carry):
        out = jnp.dot(rows_of(refs), weight[0:depth, pl.ds(al(i * step, 128), step)], preferred_element_type=F32)
        done(i * step, step, out)
        return carry

    lax.fori_loop(0, n_cols // step, columns, 0)


def lane_sums(ref, lo, n, s1, s2):
    width, rows, wide = ref.shape[-1], 32, 512

    def some_rows(i, carry):
        def some_columns(k, sums):
            a, b = sums
            v = ref[pl.ds(al(lo + i * rows, 8), rows), pl.ds(al(k * wide, 128), wide)].astype(F32)
            for c in range(0, wide, 128):
                part = v[:, c : c + 128]
                a, b = a + part, b + part * part
            return a, b

        zero = jnp.zeros((rows, 128), F32)
        a, b = lax.fori_loop(0, width // wide, some_columns, (zero, zero))
        s1[pl.ds(al(i * rows, 8), rows), :] = a
        s2[pl.ds(al(i * rows, 8), rows), :] = b
        return carry

    lax.fori_loop(0, n // rows, some_rows, 0)


def scale_rows(ref, lo, n, means, scales):
    width, rows, wide = ref.shape[-1], 32, 512

    def some_rows(i, carry):
        mean, scale = (t[pl.ds(al(i * rows, 8), rows), :] for t in (means, scales))

        def some_columns(k, carry):
            at_rows = pl.ds(al(lo + i * rows, 8), rows)
            for c in range(0, wide, 128):
                cols = pl.ds(al(k * wide + c, 128), 128)
                ref[at_rows, cols] = ((ref[at_rows, cols].astype(F32) - mean) * scale).astype(BF16)
            return carry

        lax.fori_loop(0, width // wide, some_columns, 0)
        return carry

    lax.fori_loop(0, n // rows, some_rows, 0)


class Reduce:
    def __init__(self, at, zb, ya, yb, yfd, yfu, ss, rs):
        self.at, self.zb, self.ya, self.yb, self.yfd, self.yfu, self.ss, self.rs = at, zb, ya, yb, yfd, yfu, ss, rs
        self.ch = zb.shape[2]
        self.h = self.ch // 2

    def copy(self, kind, j):
        at, h, ch = self.at, self.h, self.ch
        src, dst = (
            lambda: (self.zb.at[2, j, pl.ds(0, h)], self.ya.at[j]),
            lambda: (self.zb.at[2, j, pl.ds(h, ch - h)], self.yb.at[j]),
            lambda: (self.zb.at[1, j], self.yfd.at[j]),
            lambda: (self.zb.at[3, j], self.yfu.at[j]),
        )[kind]()
        return remote(src, dst, self.ss.at[kind, j], self.rs.at[kind, j], at.down if kind % 2 else at.up)

    def wait(self, kind, j):
        self.copy(kind, j).wait_recv()

    def halves(self, j):
        self.copy(0, j).start()
        self.copy(1, j).start()

    def middle(self, j):
        h = self.h
        self.wait(0, j)
        self.zb[1, j, 0:h] = (self.zb[1, j, 0:h].astype(F32) + self.ya[j].astype(F32)).astype(BF16)
        self.copy(2, j).start()
        self.wait(1, j)
        self.zb[3, j, h:] = (self.zb[3, j, h:].astype(F32) + self.yb[j].astype(F32)).astype(BF16)
        self.copy(3, j).start()

    def total(self, j):
        self.wait(2, j)
        self.wait(3, j)
        return self.zb[0, j].astype(F32) + self.yfd[j].astype(F32) + self.yfu[j].astype(F32)

    def drain(self):
        for j in range(NJ):
            for kind in range(4):
                self.copy(kind, j).wait_send()


def attention_kernel(
    units, x_hbm, turn_ref, base_ref, wq, wk, wv, wo, wg_t, wu_t,
    h_hbm, w_all, hg_all,
    x_ref, h_ref, xc, xg, hg, cos_all, sin_all, st_own, st_in, s1, s2, wb, wob, part, precv, qb, kvo, kvp, og, zb, ya, yb, yfd, yfu, own, drel_a, drel_b,
    sxe, rxe, sst, rst, sy, ry, syh, ryh, sd, rd, swa, rwa, swo, rwo, swp, rwp, lw, so, ro, spr, rpr, skv, rkv, sog, rog, syr, ryr,
    lg, sds, rds, sdo, rdo, sdf, rdf, sdp, rdp, shx, rhx, shy, rhy, shz, rhz, lh, lx,
):
    at = Place()
    x, c, y = at.x, at.c, at.y
    ch, kc = xc.shape[1], xc.shape[2]
    kd = wq.shape[0]
    hc = qb.shape[2]
    fc, f_a = w_all.shape[1], drel_a.shape[1]
    width = 2 * xg.shape[3]
    kh = div(x, 2)
    ng = rem(div(x + 1, 2), 2)
    gather = Spread(at, xc, xg, units, (s1, s2), None, None, sy, ry, syh, ryh)
    reduce = Reduce(at, zb, ya, yb, yfd, yfu, syr, ryr)
    ahead = Spread(at, h_ref, hg, ((0, 0, ch, 0),), (s1, s2), shx, rhx, shy, rhy, shz, rhz)
    weights = (wq, wk, wv)

    def half_cols(core):
        return pl.ds(al(core * kd, 128), kd)

    def x_rows(j, core):
        return pl.ds(al((2 * j + core) * ch, 8), ch)

    def x_pair(j):
        return remote(x_ref.at[x_rows(j, 1 - c)], xc.at[j, :, half_cols(c)], sd.at[j], rd.at[j], at.partner)

    def pair_cols(xx):
        return pl.ds(al(rem(xx, 2) * kc, 128), kc)

    def xe_copy(u, xx):
        j, lo, n, _ = units[u]
        rows = pl.ds(lo, n)
        return remote(xc.at[j, rows], xg.at[y, j, rows, pair_cols(xx)], sxe.at[u], rxe.at[u], at.pa)

    def st_copy(u):
        j, lo, n, _ = units[u]
        rows = pl.ds(lo // 4, n // 4)
        return remote(st_own.at[j, rows], st_in.at[j, rows], sst.at[u], rst.at[u], at.pb)

    def XP(j):
        x_pair(j).start()

    arrived = []

    def XE(u):
        j, lo, n, _ = units[u]
        if j not in arrived:
            arrived.append(j)
            dst = xc.at[j, :, half_cols(1 - c)]
            remote(dst, dst, sd.at[j], rd.at[j], at.partner).wait_recv()
        xe_copy(u, x).start()
        xg[y, j, lo : lo + n, pair_cols(x)] = xc[j, lo : lo + n]

    def ST(u):
        j, lo, n, _ = units[u]
        xe_copy(u, at.xa).wait_recv()
        quarter = n // 4
        lane = lax.broadcasted_iota(jnp.int32, (quarter, 128), 1)
        lane_sums(xg.at[y, j], lo, n, s1, s2)
        packed = jnp.zeros((quarter, 128), F32)
        for g in range(4):
            rows = pl.ds(g * quarter, quarter)
            total, square = (jnp.sum(t[rows, :], axis=-1, keepdims=True) for t in (s1, s2))
            packed = jnp.where(lane // 32 == g, jnp.where(lane % 32 < 16, total, square), packed)
        st_own[j, lo // 4 : lo // 4 + quarter, :] = packed
        st_copy(u).start()

    def N(u):
        j, lo, n, _ = units[u]
        st_copy(u).wait_recv()
        quarter = n // 4
        at_rows = slice(lo // 4, lo // 4 + quarter)
        moments = (st_own[j, at_rows, :] + st_in[j, at_rows, :]) / width
        for g in range(4):
            mean = moments[:, 32 * g : 32 * g + 1]
            var = moments[:, 32 * g + 16 : 32 * g + 17] - mean * mean
            rows = pl.ds(g * quarter, quarter)
            s1[rows, :] = jnp.broadcast_to(mean, (quarter, 128))
            s2[rows, :] = jnp.broadcast_to(lax.rsqrt(var + EPS), (quarter, 128))
        scale_rows(xg.at[y, j], lo, n, s1, s2)
        gather.YR(u)

    def w_rows(xx, core):
        return pl.ds(al(rem(xx, 2) * kc + core * kd, 128), kd)

    def w_part(group, half, i):
        side = kh if half else 1 - kh
        return weights[i].at[:, pl.ds(al((2 * group + side) * hc, 128), hc)]

    def w_cols(half, i):
        return pl.ds(half * 3 * hc + i * hc, hc)

    def wa_copy(half, i, xx):
        return remote(w_part(1 - ng, half, i), wb.at[w_rows(xx, c), w_cols(half, i)], swa.at[half, i], rwa.at[half, i], at.pa)

    def wo_copy(half, i, core):
        return remote(w_part(ng, half, i), wb.at[w_rows(x, core), w_cols(half, i)], swo.at[half, i], rwo.at[half, i], at.partner)

    def w_local(half, i):
        return pltpu.make_async_copy(w_part(ng, half, i), wb.at[w_rows(x, c), w_cols(half, i)], lw.at[half, i])

    def wp_copy(half, core):
        ref = wb.at[w_rows(at.xa, core), pl.ds(half * 3 * hc, 3 * hc)]
        return remote(ref, ref, swp.at[half], rwp.at[half], at.partner)

    o_local = pltpu.make_async_copy(wo, wob.at[:, half_cols(c)], lw.at[2, 0])
    o_pair = remote(wo, wob.at[:, half_cols(c)], so.at[0], ro.at[0], at.partner)
    pieces = [(half, i) for half in range(2) for i in range(3)]

    def WOP():
        for half, i in pieces:
            wo_copy(half, i, c).start()
        o_pair.start()

    def WA(half):
        for i in range(3):
            wa_copy(half, i, x).start()

    def WP(half):
        for i in range(3):
            wa_copy(half, i, at.xa).wait_recv()
        wp_copy(half, c).start()

    w_halves = [0, 1]

    def w_ready(half):
        if half not in w_halves:
            return
        w_halves.remove(half)
        for i in range(3):
            w_local(half, i).wait()
            wo_copy(half, i, 1 - c).wait_recv()
        wp_copy(half, 1 - c).wait_recv()
        if half:
            own_out()

    def own_out():
        for m in range(2):
            d_in(m).wait()
            d_out(m).start()
            d_pair(m, 3, c).start()

    def o_ready():
        o_local.wait()
        dst = wob.at[:, half_cols(1 - c)]
        remote(dst, dst, so.at[0], ro.at[0], at.partner).wait_recv()

    mlp_weights = (wg_t, wu_t)
    parts = ((0, f_a), (f_a, fc - f_a))

    def d_src(m, xx, p):
        return mlp_weights[m].at[pl.ds(al(xx * fc + parts[p][0], 8), parts[p][1])]

    def d_dst(m, xx, p):
        return w_all.at[m, pl.ds(*parts[p]), pl.ds(al((2 * xx + c) * kd, 128), kd)]

    def s_copy(d, m, p, xx):
        to, dev = ((at.xa, at.pa), (at.xb, at.pb))[d]
        return remote(d_src(m, to, p), d_dst(m, xx, p), sds.at[d, m, p], rds.at[d, m, p], dev)

    def o_copy(d, m):
        return remote(d_src(m, at.xo, d), (drel_a, drel_b)[d].at[m], sdo.at[d, m], rdo.at[d, m], (at.pa, at.pb)[d])

    def f_copy(d, m, xx):
        return remote((drel_a, drel_b)[d].at[m], d_dst(m, xx, d), sdf.at[d, m], rdf.at[d, m], (at.pb, at.pa)[d])

    def d_in(m):
        return pltpu.make_async_copy(mlp_weights[m].at[pl.ds(al(x * fc, 8), fc)], own.at[m], lg.at[0, m])

    def d_all(m, xx, core):
        return w_all.at[m, :, pl.ds(al((2 * xx + core) * kd, 128), kd)]

    def d_out(m):
        return pltpu.make_async_copy(own.at[m], d_all(m, x, c), lg.at[1, m])

    def d_pair(m, k, core):
        dst = d_all(m, (at.xa, at.xb, at.xo, x)[k], core)
        return remote(own.at[m] if k == 3 else dst, dst, sdp.at[m, k], rdp.at[m, k], at.partner)

    def S(link, m, p):
        s_copy("ab".index(link), m, p, x).start()

    def O(link, m):
        o_copy("ab".index(link), m).start()

    def F(link, m):
        d = "ba".index(link)
        o_copy(d, m).wait_recv()
        f_copy(d, m, (at.xa, at.xb)[d]).start()

    def DP(m):
        for d in range(2):
            for p in range(2):
                s_copy(d, m, p, (at.xa, at.xb)[d]).wait_recv()
            f_copy(d, m, at.xo).wait_recv()
        for k in range(3):
            d_pair(m, k, c).start()

    def pr_copy(n):
        return remote(part.at[n, :, pl.ds(0, 3 * hc)], precv.at[n], spr.at[n], rpr.at[n], at.pb)

    def project(g, first, size):
        def done(col, step, out):
            for i, (r, j) in enumerate(GROUPS[g]):
                part[r * NJ + j, :, pl.ds(al(first + col, 128), step)] = out[i * ch : (i + 1) * ch].astype(BF16)

        refs = [xg.at[gather.seqs[r], j] for r, j in GROUPS[g]]
        product(refs, wb.at[:, pl.ds(first, size)], wb.shape[0], size, done)

    split = {step[1] for step in ATTENTION_STEPS if step[0] == "Q"}

    def G(g):
        w_ready(0)
        for r, j in GROUPS[g]:
            gather.chunk_wait(r, j)
        if g in split:
            project(g, 0, 3 * hc)
        else:
            w_ready(1)
            project(g, 0, 6 * hc)
        for r, j in GROUPS[g]:
            pr_copy(r * NJ + j).start()

    def Q(g):
        w_ready(1)
        project(g, 3 * hc, 3 * hc)

    def kv_copy(r, j):
        s, n = gather.seqs[r], r * NJ + j
        return remote(kvo.at[s, j], kvp.at[s, j], skv.at[n], rkv.at[n], at.partner)

    def rotate(r, j):
        s, n = gather.seqs[r], r * NJ + j
        pr_copy(n).wait_recv()
        cos_t, sin_t = cos_all[j], sin_all[j]

        def total(col, size):
            mine = part[n, :, 3 * hc + col : 3 * hc + col + size]
            return (mine.astype(F32) + precv[n, :, col : col + size].astype(F32)).astype(BF16)

        def turned(col):
            v = total(col, HEAD_DIM).astype(F32)
            return (v * cos_t + pltpu.roll(v, HEAD_DIM // 2, axis=1) * sin_t).astype(BF16)

        for col in range(0, hc, HEAD_DIM):
            qb[n, :, col : col + HEAD_DIM] = turned(col)
            kvo[s, j, :, col : col + HEAD_DIM] = turned(hc + col)
        kvo[s, j, :, hc:] = total(2 * hc, hc)
        kv_copy(r, j).start()

    def R(g):
        for r, j in GROUPS[g]:
            rotate(r, j)

    def o_cols(xx):
        return pl.ds(al((2 * rem(div(xx + 1, 2), 2) + div(xx, 2)) * hc, 128), hc)

    cut = ch // 8

    def og_copy(kind, n):
        if kind < 2:
            ref = og.at[n, :, o_cols(x)]
        elif kind == 2:
            ref = og.at[n, pl.ds(0, cut), o_cols(at.xa)]
        else:
            ref = og.at[n, pl.ds(cut, ch - cut), o_cols(at.xb)]
        return remote(ref, ref, sog.at[kind, n], rog.at[kind, n], at.pa if kind in (0, 3) else at.pb)

    def og_wait(kind, n):
        xx = (at.xa, at.xb, at.xo, at.xo)[kind]
        rows = (pl.ds(0, ch), pl.ds(0, ch), pl.ds(0, cut), pl.ds(cut, ch - cut))[kind]
        dst = og.at[n, rows, o_cols(xx)]
        remote(dst, dst, sog.at[kind, n], rog.at[kind, n], at.pa).wait_recv()

    def attend(r, j, i):
        s, n = gather.seqs[r], r * NJ + j
        keys = (j + 1) * ch
        iq = lax.broadcasted_iota(jnp.int32, (ch, keys), 0) + j * ch
        ik = lax.broadcasted_iota(jnp.int32, (ch, keys), 1)
        own_ok = iq >= ik
        par_ok = ik < (j + c) * ch
        contract = (((1,), (1,)), ((), ()))
        cols = pl.ds(al(i * HEAD_DIM, 128), HEAD_DIM)
        v_cols = pl.ds(al(hc + i * HEAD_DIM, 128), HEAD_DIM)
        q = qb[n, :, cols]
        k_own = kvo[s, 0 : j + 1, :, cols].reshape(keys, HEAD_DIM)
        k_par = kvp[s, 0 : j + 1, :, cols].reshape(keys, HEAD_DIM)
        s_own = lax.dot_general(q, k_own, contract, preferred_element_type=F32) * HEAD_DIM**-0.5
        s_par = lax.dot_general(q, k_par, contract, preferred_element_type=F32) * HEAD_DIM**-0.5
        s_own = jnp.where(own_ok, s_own, -1e30)
        s_par = jnp.where(par_ok, s_par, -1e30)
        top = jnp.maximum(jnp.max(s_own, axis=1, keepdims=True), jnp.max(s_par, axis=1, keepdims=True))
        e_own, e_par = jnp.exp(s_own - top), jnp.exp(s_par - top)
        inv = 1.0 / (jnp.sum(e_own, axis=1, keepdims=True) + jnp.sum(e_par, axis=1, keepdims=True))
        v_own = kvo[s, 0 : j + 1, :, v_cols].reshape(keys, HEAD_DIM)
        v_par = kvp[s, 0 : j + 1, :, v_cols].reshape(keys, HEAD_DIM)
        out = jnp.dot((e_own * inv).astype(BF16), v_own, preferred_element_type=F32)
        out += jnp.dot((e_par * inv).astype(BF16), v_par, preferred_element_type=F32)
        og[n, :, pl.ds(al((2 * ng + kh) * hc + i * HEAD_DIM, 128), HEAD_DIM)] = out.astype(BF16)

    def A(g):
        for r, j in GROUPS[g]:
            kv_copy(r, j).wait_recv()

        def head(i, carry):
            for r, j in GROUPS[g]:
                attend(r, j, i)
            return carry

        lax.fori_loop(0, hc // HEAD_DIM, head, 0)
        for r, j in GROUPS[g]:
            og_copy(0, r * NJ + j).start()
            og_copy(1, r * NJ + j).start()

    def P(g):
        for r, j in GROUPS[g]:
            for kind in range(2):
                og_wait(kind, r * NJ + j)
                og_copy(kind + 2, r * NJ + j).start()

    def X(g):
        for r, j in GROUPS[g]:
            og_wait(2, r * NJ + j)
            og_wait(3, r * NJ + j)

        def done(col, size, out):
            for i, (r, j) in enumerate(GROUPS[g]):
                zb[r, j, :, pl.ds(al(col, 128), size)] = out[i * ch : (i + 1) * ch].astype(BF16)

        product([og.at[r * NJ + j] for r, j in GROUPS[g]], wob, wob.shape[0], kc, done)
        for r, j in GROUPS[g]:
            if r == 2:
                reduce.halves(j)

    def T(j):
        attn = reduce.total(j).astype(BF16)
        h_ref[j] = (xc[j].astype(F32) + attn.astype(F32)).astype(BF16)
        chunk_out(j).start()

    def chunk_out(j):
        return pltpu.make_async_copy(h_ref.at[j], h_hbm.at[j], lx.at[1 + j])

    def h_out(r):
        return pltpu.make_async_copy(hg.at[ahead.seqs[r], 0], hg_all.at[ahead.seqs[r]], lh.at[r])

    def HF(u):
        ahead.keep_own()
        ahead.XF(0, u)

    def HY(u):
        ahead.YH(u)
        for r in (0, 1, 3):
            h_out(r).start()

    def HO(u):
        for d in range(2):
            ahead.yhalf_wait(d, u)
        h_out(2).start()

    def own_rows():
        for half, i in pieces:
            w_local(half, i).start()
        o_local.start()
        for m in range(2):
            d_in(m).start()
        x_in.wait()
        for j in range(NJ):
            xc[j, :, half_cols(c)] = x_ref[x_rows(j, c), :]

    x_in = pltpu.make_async_copy(x_hbm, x_ref, lx.at[0])
    x_in.start()
    at.barrier(own_rows)

    def angles():
        lane = lax.broadcasted_iota(jnp.int32, (ch, HEAD_DIM), 1)
        for j in range(NJ):
            base_cos, base_sin = base_ref[0, pl.ds(2 * j + c, 1), :], base_ref[1, pl.ds(2 * j + c, 1), :]
            cos_all[j] = base_cos * turn_ref[0] - base_sin * turn_ref[1]
            sine = base_sin * turn_ref[0] + base_cos * turn_ref[1]
            sin_all[j] = jnp.where(lane < HEAD_DIM // 2, -sine, sine)

    ops = {
        "XP": XP, "WOP": WOP, "XE": XE, "ST": ST, "N": N, "YH": gather.YH, "WA": WA, "WP": WP, "S": S, "O": O, "F": F, "DP": DP,
        "G": G, "Q": Q, "R": R, "A": A, "P": P, "X": X, "M": reduce.middle, "T": T,
        "HF": HF, "HH": lambda u: ahead.XH(0, u), "HN": lambda u: ahead.N(0, u), "HY": HY, "HO": HO,
    }
    waits = {"X": o_ready, "WP": angles}
    for step in ATTENTION_STEPS:
        if step[0] in waits:
            waits.pop(step[0])()
        ops[step[0]](*step[1:])

    for m in range(2):
        for k in range(4):
            d_pair(m, k, 1 - c).wait_recv()
            d_pair(m, k, c).wait_send()
        d_out(m).wait()
        for d in range(2):
            for p in range(2):
                s_copy(d, m, p, x).wait_send()
            o_copy(d, m).wait_send()
            f_copy(d, m, x).wait_send()
    for j in range(NJ):
        x_pair(j).wait_send()
    for u in range(len(units)):
        xe_copy(u, x).wait_send()
        st_copy(u).wait_send()
        for d in range(2):
            gather.ycopy(d, u).wait_send()
            gather.yhalf(d, u).wait_send()
    reduce.drain()
    ahead.drain()
    for r in range(NX):
        h_out(r).wait()
    for j in range(NJ):
        chunk_out(j).wait()
    o_pair.wait_send()
    for half, i in pieces:
        wa_copy(half, i, x).wait_send()
        wo_copy(half, i, c).wait_send()
    for half in range(2):
        wp_copy(half, c).wait_send()

    def chunk_sent(n, carry):
        pr_copy(n).wait_send()
        remote(kvo.at[0, 0], kvp.at[0, 0], skv.at[n], rkv.at[n], at.partner).wait_send()
        for kind in range(4):
            og_copy(kind, n).wait_send()
        return carry

    lax.fori_loop(0, NCH, chunk_sent, 0)


def mlp_kernel(
    units, h_hbm, w_hbm, wdn, hg_hbm, y_ref,
    h_ref, xg, wt, raw, wd, ag, ar, act, s1, s2, zb, ya, yb, yfd, yfu, yst,
    sx, rx, sy, ry, syh, ryh, sa, ra, syr, ryr, sd, rd, lw, lwd, swd, rwd, lh, lo,
):
    at = Place()
    x, c, y = at.x, at.c, at.y
    ch, kc, h = h_ref.shape[1], h_ref.shape[2], h_ref.shape[1] // 2
    width = xg.shape[-1]
    kd = kc // 2
    fc, tiles = w_hbm.shape[1], wt.shape[1] // 256
    fm = (tiles - 1) * 128
    fr = fc - fm
    blocks, slots = 2 * tiles, raw.shape[0]
    gather = Spread(at, h_ref, xg, units, (s1, s2), sx, rx, sy, ry, syh, ryh)
    reduce = Reduce(at, zb, ya, yb, yfd, yfu, syr, ryr)

    def w_in(q):
        i, m = q // 2, q % 2
        n = min(128, fc - i * 128)
        return pltpu.make_async_copy(w_hbm.at[m, pl.ds(i * 128, n)], raw.at[q % slots, pl.ds(0, n)], lw.at[q])

    def WT(g):
        for q in range(g * blocks // 4, (g + 1) * blocks // 4):
            i, m, slot = q // 2, q % 2, q % slots
            w_in(q).wait()
            if fc < (i + 1) * 128:
                raw[slot, fc - i * 128 :, :] = jnp.zeros(((i + 1) * 128 - fc, width), BF16)

            def turn(k, carry, slot=slot, q=q):
                part = pl.ds(al(k * (width // 4), 128), width // 4)
                wt[part, q * 128 : (q + 1) * 128] = raw[slot, :, part].T
                return carry

            lax.fori_loop(0, 4, turn, 0)
            if q + slots < blocks:
                w_in(q + slots).start()

    def d_refs(q, core):
        cols = pl.ds(al(core * kd, 128), kd)
        main, rest = wdn.at[pl.ds(q * fc, fm)], wdn.at[pl.ds(q * fc + fm, fr)]
        return (main, wd.at[pl.ds(q * fm, fm), cols]), (rest, wd.at[pl.ds(NX * fm + q * 128, fr), cols])

    def d_own(q, k):
        src, dst = d_refs(q, c)[k]
        return pltpu.make_async_copy(src, dst, lwd.at[q, k])

    def d_pair(q, k, core):
        src, dst = d_refs(q, core)[k]
        return remote(src, dst, swd.at[q, k], rwd.at[q, k], at.partner)

    quarters = [(q, k) for q in range(NX) for k in range(2)]
    h_in_all = pltpu.make_async_copy(h_hbm, h_ref, lo.at[NJ])
    h_in_all.start()
    for q in range(slots):
        w_in(q).start()
    def h_in(s):
        return pltpu.make_async_copy(hg_hbm.at[s], xg.at[s, 0], lh.at[s])

    for s in range(NX):
        h_in(s).start()
    for q, k in quarters:
        d_own(q, k).start()
    for q in range(NX):
        wd[NX * fm + q * 128 + fr : NX * fm + (q + 1) * 128, :] = jnp.zeros((128 - fr, kc), BF16)
    at.barrier(h_in_all.wait)
    for q, k in quarters:
        d_pair(q, k, c).start()

    def a_refs(kind, n, xx):
        main, rest = pl.ds(al(xx * fm, 128), fm), pl.ds(al(xx * 128, 128), 128)
        if kind < 2:
            return ag.at[n, :, main], ar.at[n, :, rest]
        lo = (kind - 2) * h
        return ag.at[n, pl.ds(lo, h), main], ar.at[n, pl.ds(lo // 2, h // 2), rest]

    def a_copies(kind, n):
        refs = a_refs(kind, n, (x, x, at.xl, at.xr)[kind])
        return [remote(v, v, sa.at[kind, n, k], ra.at[kind, n, k], at.left if kind % 2 else at.right) for k, v in enumerate(refs)]

    def a_wait(kind, n):
        for k, v in enumerate(a_refs(kind, n, (at.xl, at.xr, at.xo, at.xo)[kind])):
            remote(v, v, sa.at[kind, n, k], ra.at[kind, n, k], at.right).wait_recv()

    def a_start(kind, n):
        for copy in a_copies(kind, n):
            copy.start()

    def G(g):
        for r, j in GROUPS[g]:
            gather.chunk_wait(r, j)

        def done(col, size, out):
            for k in range(0, size, 256):
                gate, up = out[:, k : k + 128].astype(BF16).astype(F32), out[:, k + 128 : k + 256].astype(BF16).astype(F32)
                value = (gate / (1.0 + jnp.exp(-gate)) * up).astype(BF16)
                act[0 : value.shape[0], pl.ds(al(div(col + k, 2), 128), 128)] = value

        product([xg.at[gather.seqs[r], j] for r, j in GROUPS[g]], wt, width, wt.shape[1], done)
        for i, (r, j) in enumerate(GROUPS[g]):
            n, lo = r * NJ + j, i * ch
            ag[n, :, pl.ds(al(x * fm, 128), fm)] = act[lo : lo + ch, :fm]
            below = pltpu.roll(act[lo + h : lo + ch, fm:].astype(F32), 64, axis=1)
            ar[n, :, pl.ds(al(x * 128, 128), 128)] = (act[lo : lo + h, fm:].astype(F32) + below).astype(BF16)
            for kind in range(2):
                a_start(kind, n)

    def P(g):
        for r, j in GROUPS[g]:
            for kind in range(2):
                a_wait(kind, r * NJ + j)
                a_start(kind + 2, r * NJ + j)

    def X(g):
        for r, j in GROUPS[g]:
            n = r * NJ + j
            for kind in (2, 3):
                a_wait(kind, n)
            for q in range(NX):
                cols = pl.ds(NX * fm + q * 128, 128)
                rest = ar[n, :, q * 128 : (q + 1) * 128]
                ag[n, 0:h, cols] = rest
                ag[n, h:, cols] = pltpu.roll(rest.astype(F32), 64, axis=1).astype(BF16)

        def done(col, size, out):
            for i, (r, j) in enumerate(GROUPS[g]):
                zb[r, j, :, pl.ds(al(col, 128), size)] = out[i * ch : (i + 1) * ch].astype(BF16)

        product([ag.at[r * NJ + j] for r, j in GROUPS[g]], wd, wd.shape[0], kc, done)
        for r, j in GROUPS[g]:
            if r == 2:
                reduce.halves(j)

    def y_rows(j, core):
        return pl.ds(al((2 * j + core) * ch, 8), ch)

    def y_copy(j):
        return remote(yst.at[1 - c, j], y_ref.at[y_rows(j, c)], sd.at[j], rd.at[j], at.partner)

    def y_own(j):
        return pltpu.make_async_copy(yst.at[c, j], y_ref.at[y_rows(j, c)], lo.at[j])

    def y_wait(j):
        dst = y_ref.at[y_rows(j, 1 - c)]
        remote(dst, dst, sd.at[j], rd.at[j], at.partner).wait_recv()

    def T(j):
        mlp = reduce.total(j).astype(BF16)
        out = (h_ref[j].astype(F32) + mlp.astype(F32)).astype(BF16)
        yst[0, j] = out[:, :kd]
        yst[1, j] = out[:, kd:]
        y_copy(j).start()
        y_own(j).start()

    ops = {"G": G, "P": P, "X": X, "M": reduce.middle, "T": T, "WT": WT}
    for name in ("YR", "YRH", "YH", "XF", "XH", "N"):
        ops[name] = getattr(gather, name)
    waits = {
        "N": gather.keep_own,
        "G": lambda: [h_in(s).wait() for s in range(NX)],
        "X": lambda: [(d_own(q, k).wait(), d_pair(q, k, 1 - c).wait_recv()) for q, k in quarters],
    }
    for step in MLP_STEPS:
        if step[0] in waits:
            waits.pop(step[0])()
        ops[step[0]](*step[1:])

    gather.drain()
    reduce.drain()
    for q, k in quarters:
        d_pair(q, k, c).wait_send()

    def chunk_sent(n, carry):
        for kind in range(4):
            for copy in a_copies(kind, n):
                copy.wait_send()
        return carry

    lax.fori_loop(0, NCH, chunk_sent, 0)
    for j in range(NJ):
        y_copy(j).wait_send()
        y_own(j).wait()
        y_wait(j)


def vmem(*shape, dtype=BF16):
    return pltpu.VMEM(shape, dtype)


def sems(*shape):
    return pltpu.SemaphoreType.DMA(shape)


def solution(mesh):
    assert mesh.shape["tx"] == 2 * NX and mesh.shape["ty"] == NX
    act_spec = P(("dp", "ty"), None, "tx")
    col_spec = P("tx", "ty")
    row_spec = P("ty", "tx")
    any_spec = pl.BlockSpec(memory_space=pl.ANY)
    vmem_spec = pl.BlockSpec(memory_space=pltpu.VMEM)

    def layer(x_blk, w_q, w_k, w_v, w_o, w_gate, w_up, w_down):
        _, seq, kd = x_blk.shape
        kc, width = 2 * kd, 2 * NX * kd
        ch = seq // (2 * NJ)
        h = ch // 2
        row_heads = w_q.shape[1]
        hc = row_heads // NX
        fc = w_down.shape[0] // NX
        assert hc % HEAD_DIM == 0
        tiles = (fc + 127) // 128
        f_a = (fc // 2 + 15) // 16 * 16

        inv_freq = THETA ** (-2.0 * np.arange(HEAD_DIM // 2) / HEAD_DIM)
        inv_freq = np.concatenate([inv_freq, inv_freq])
        turn = np.arange(ch)[:, None] * inv_freq
        base = np.arange(2 * NJ)[:, None] * ch * inv_freq
        turn = jnp.asarray(np.stack([np.cos(turn), np.sin(turn)]), F32)
        base = jnp.asarray(np.stack([np.cos(base), np.sin(base)]), F32)

        reduce_scratch = [vmem(NX, NJ, ch, kc), vmem(NJ, h, kc), vmem(NJ, ch - h, kc), vmem(NJ, ch, kc), vmem(NJ, ch, kc)]
        units = ((0, 0, h, 0), (0, h, h, 0)) + tuple((j, 0, ch, 0) for j in range(1, NJ))
        n_u = len(units)
        h_blk, w_all, hg_all = pl.pallas_call(
            functools.partial(attention_kernel, units),
            out_shape=(
                jax.ShapeDtypeStruct((NJ, ch, kc), BF16),
                jax.ShapeDtypeStruct((2, fc, width), BF16),
                jax.ShapeDtypeStruct((NX, ch, width), BF16),
            ),
            in_specs=[any_spec] + [vmem_spec] * 2 + [any_spec] * 6,
            out_specs=(any_spec, any_spec, any_spec),
            scratch_shapes=[
                vmem(seq, kd), vmem(NJ, ch, kc), vmem(NJ, ch, kc), vmem(NX, NJ, ch, 2 * kc), vmem(NX, 1, ch, width), vmem(NJ, ch, HEAD_DIM, dtype=F32), vmem(NJ, ch, HEAD_DIM, dtype=F32),
                vmem(NJ, ch // 4, 128, dtype=F32), vmem(NJ, ch // 4, 128, dtype=F32), vmem(ch, 128, dtype=F32), vmem(ch, 128, dtype=F32),
                vmem(2 * kc, 6 * hc), vmem(row_heads, kc), vmem(NCH, ch, 6 * hc), vmem(NCH, ch, 3 * hc), vmem(NCH, ch, hc),
                vmem(NX, NJ, ch, 2 * hc), vmem(NX, NJ, ch, 2 * hc), vmem(NCH, ch, row_heads), *reduce_scratch,
                vmem(2, fc, kd), vmem(2, f_a, kd), vmem(2, fc - f_a, kd),
                sems(n_u), sems(n_u), sems(n_u), sems(n_u), sems(2, n_u), sems(2, n_u), sems(2, n_u), sems(2, n_u),
                sems(NJ), sems(NJ), sems(2, 3), sems(2, 3), sems(2, 3), sems(2, 3), sems(2), sems(2), sems(3, 3), sems(1), sems(1),
                sems(NCH), sems(NCH), sems(NCH), sems(NCH), sems(4, NCH), sems(4, NCH), sems(4, NJ), sems(4, NJ),
                sems(2, 2), sems(2, 2, 2), sems(2, 2, 2), sems(2, 2), sems(2, 2), sems(2, 2), sems(2, 2), sems(2, 4), sems(2, 4),
                sems(4, 1), sems(4, 1), sems(2, 1), sems(2, 1), sems(2, 1), sems(2, 1), sems(NX), sems(1 + NJ),
            ],
            compiler_params=pltpu.CompilerParams(collective_id=0, has_side_effects=True, vmem_limit_bytes=VMEM_LIMIT),
            name="attention_part",
        )(x_blk[0], turn, base, w_q, w_k, w_v, w_o, w_gate.T, w_up.T)

        units = ((1, 0, h, 1), (1, h, h, 0)) + tuple((j, 0, ch, 0) for j in range(2, NJ))
        n_u, n_x = len(units), len(units) + 3
        y_blk = pl.pallas_call(
            functools.partial(mlp_kernel, units),
            out_shape=jax.ShapeDtypeStruct((seq, kd), BF16),
            in_specs=[any_spec] * 4,
            out_specs=any_spec,
            scratch_shapes=[
                vmem(NJ, ch, kc),
                vmem(NX, NJ, ch, width), vmem(width, tiles * 256), vmem(3, 128, width),
                vmem(NX * tiles * 128, kc), vmem(NCH, ch, NX * tiles * 128), vmem(NCH, h, NX * 128), vmem(2 * ch, tiles * 128),
                vmem(ch, 128, dtype=F32), vmem(ch, 128, dtype=F32),
                *reduce_scratch, vmem(2, NJ, ch, kd),
                sems(4, n_x), sems(4, n_x), sems(2, n_u), sems(2, n_u), sems(2, n_u), sems(2, n_u),
                sems(4, NCH, 2), sems(4, NCH, 2), sems(4, NJ), sems(4, NJ), sems(NJ), sems(NJ),
                sems(2 * tiles), sems(NX, 2), sems(NX, 2), sems(NX, 2), sems(NX), sems(NJ + 1),
            ],
            compiler_params=pltpu.CompilerParams(collective_id=1, has_side_effects=True, vmem_limit_bytes=VMEM_LIMIT),
            name="mlp_part",
        )(h_blk, w_all, w_down, hg_all)
        return y_blk[None]

    return jax.shard_map(
        layer,
        mesh=mesh,
        in_specs=(act_spec, col_spec, col_spec, col_spec, row_spec, col_spec, col_spec, row_spec),
        out_specs=act_spec,
        check_vma=False,
    )
```

```python
import functools

import jax
import jax.numpy as jnp
import numpy as np
from jax import lax
from jax.experimental import pallas as pl
from jax.experimental.pallas import tpu as pltpu
from jax.sharding import PartitionSpec as P

HEAD_DIM = 128
EPS = 1e-5
THETA = 10000.0
MESH = pl.DeviceIdType.MESH
F32 = jnp.float32
BF16 = jnp.bfloat16
NX = 4
NJ = 4
NCH = 16
VMEM_LIMIT = 67_043_328
GROUPS = (*(((0, j),) for j in range(NJ)), *(((3, j), (1, j)) for j in range(NJ)), *(((2, j),) for j in range(NJ)))


def rem(a, b):
    return lax.rem(a, jnp.int32(b))


def div(a, b):
    return lax.div(a, jnp.int32(b))


def al(v, m):
    return pl.multiple_of(v, m)


def remote(src, dst, ssem, rsem, dev):
    return pltpu.make_async_remote_copy(src_ref=src, dst_ref=dst, send_sem=ssem, recv_sem=rsem, device_id=dev, device_id_type=MESH)


ATTENTION_STEPS = (
    ("WA", 0), ("XP", 1), ("S", "b", 0, 1), ("XP", 0), ("XE", 1), ("XE", 0), ("XE", 2), ("XP", 2), ("S", "b", 0, 0), ("XP", 3),
    ("S", "b", 1, 0), ("ST", 1), ("WP", 0), ("WA", 1), ("O", "b", 1), ("ST", 0), ("N", 1), ("O", "b", 0), ("ST", 2),
    ("S", "b", 1, 1), ("WOP",), ("N", 0), ("G", 0), ("XE", 3), ("YH", 1), ("YH", 0), ("S", "a", 0, 1), ("N", 2), ("WP", 1),
    ("G", 8), ("G", 4), ("ST", 3), ("Q", 8), ("Q", 0), ("R", 8), ("XE", 4), ("A", 8), ("F", "a", 1), ("YH", 2), ("G", 5),
    ("R", 4), ("ST", 4), ("N", 3), ("P", 8), ("G", 9), ("A", 4), ("R", 0), ("S", "a", 1, 1), ("X", 8), ("G", 1), ("N", 4),
    ("R", 5), ("A", 0), ("R", 9), ("P", 4), ("A", 9), ("A", 5), ("G", 2), ("P", 0), ("X", 4), ("M", 0), ("P", 9),
    ("S", "a", 1, 0), ("YH", 3), ("G", 6), ("P", 5), ("X", 0), ("T", 0), ("HF", 1), ("HF", 0), ("R", 2), ("X", 9), ("R", 1),
    ("A", 1), ("YH", 4), ("X", 5), ("M", 1), ("HH", 1), ("O", "a", 0), ("G", 10), ("R", 6), ("HH", 0), ("G", 7), ("O", "a", 1),
    ("HN", 1), ("R", 10), ("G", 11), ("A", 10), ("A", 6), ("HN", 0), ("R", 7), ("A", 2), ("HY", 1), ("A", 7), ("R", 11),
    ("P", 10), ("A", 11), ("P", 6), ("G", 3), ("P", 7), ("P", 11), ("F", "b", 1), ("F", "a", 0), ("X", 10), ("HY", 0),
    ("S", "a", 0, 0), ("F", "b", 0), ("R", 3), ("X", 11), ("A", 3), ("X", 6), ("HO", 1), ("X", 7), ("P", 1), ("P", 2),
    ("M", 2), ("M", 3), ("DP", 1), ("DP", 0), ("P", 3), ("HO", 0), ("X", 1), ("T", 1), ("X", 2), ("T", 2), ("X", 3), ("T", 3),
)
MLP_STEPS = (
    ("XF", 0, 1), ("YR", 0), ("WT", 0), ("XF", 0, 0), ("XH", 0, 1), ("XF", 0, 3), ("YRH", 0), ("XF", 2, 0), ("N", 0, 1),
    ("WT", 1), ("WT", 2), ("XH", 0, 3), ("XF", 0, 2), ("WT", 3), ("XF", 1, 0), ("XF", 3, 0), ("N", 0, 3), ("G", 8), ("YH", 1),
    ("XH", 2, 0), ("G", 4), ("P", 8), ("XH", 3, 0), ("XH", 0, 0), ("XH", 0, 2), ("G", 3), ("XH", 1, 0), ("YH", 3), ("G", 7),
    ("N", 2, 0), ("N", 0, 0), ("G", 9), ("N", 0, 2), ("P", 7), ("G", 11), ("P", 4), ("P", 9), ("N", 1, 0), ("N", 3, 0),
    ("G", 5), ("X", 8), ("G", 1), ("X", 4), ("YH", 2), ("P", 11), ("G", 6), ("X", 9), ("X", 7), ("X", 11), ("P", 5), ("M", 0),
    ("G", 10), ("G", 0), ("M", 3), ("X", 5), ("P", 10), ("P", 3), ("M", 1), ("P", 6), ("G", 2), ("P", 1), ("X", 10), ("X", 3),
    ("P", 0), ("X", 6), ("M", 2), ("T", 3), ("P", 2), ("X", 1), ("T", 1), ("X", 0), ("T", 0), ("X", 2), ("T", 2),
)


class Place:
    def __init__(self):
        tx, ty = lax.axis_index("tx"), lax.axis_index("ty")
        self.x, self.c, self.y = div(tx, 2), rem(tx, 2), ty
        x, c, y = self.x, self.c, self.y
        self.xr, self.xl, self.xo = rem(x + 1, NX), rem(x + 3, NX), rem(x + 2, NX)
        self.yu, self.yd, self.yo = rem(y + 1, NX), rem(y + 3, NX), rem(y + 2, NX)
        self.right = {"tx": self.xr * 2 + c, "ty": y}
        self.left = {"tx": self.xl * 2 + c, "ty": y}
        self.up = {"tx": tx, "ty": self.yu}
        self.down = {"tx": tx, "ty": self.yd}
        self.partner = {"tx": x * 2 + 1 - c, "ty": y}
        self.xa, self.xb = x + 1 - 2 * rem(x, 2), rem(x + 3 + 2 * rem(x, 2), NX)
        self.pa, self.pb = {"tx": self.xa * 2 + c, "ty": y}, {"tx": self.xb * 2 + c, "ty": y}

    def barrier(self, between):
        sem = pltpu.get_barrier_semaphore()
        for dev in (self.right, self.left, self.up, self.down, self.partner):
            pl.semaphore_signal(sem, inc=1, device_id=dev, device_id_type=MESH)
        between()
        pl.semaphore_wait(sem, 5)


class Spread:
    def __init__(self, at, src, xg, units, sums, sx, rx, sy, ry, syh, ryh):
        self.sums = sums
        self.at, self.src, self.xg, self.units, self.kc = at, src, xg, units, src.shape[2]
        self.sx, self.rx, self.sy, self.ry, self.syh, self.ryh = sx, rx, sy, ry, syh, ryh
        pairs = [(r, u) for u, unit in enumerate(units) for r in ((0, 3, 1, 2) if unit[3] else (0,))]
        self.index = {pair: i for i, pair in enumerate(pairs)}
        self.seqs = (at.y, at.yu, at.yo, at.yd)

    def cols(self, x):
        return pl.ds(al(x * self.kc, 128), self.kc)

    def keep_own(self):
        for j in {unit[0]: 0 for unit in self.units}:
            self.xg[self.at.y, j, :, self.cols(self.at.x)] = self.src[j]

    def xcopy(self, kind, r, u):
        at, s = self.at, self.seqs[r]
        j, lo, n, _ = self.units[u]
        i = self.index[r, u]
        if kind < 2:
            dst = self.xg.at[s, j, pl.ds(lo, n), self.cols(at.x)]
            src = self.src.at[j, pl.ds(lo, n)] if r == 0 else dst
        elif kind == 2:
            src = dst = self.xg.at[s, j, pl.ds(lo, n // 2), self.cols(at.xl)]
        else:
            src = dst = self.xg.at[s, j, pl.ds(lo + n // 2, n // 2), self.cols(at.xr)]
        return remote(src, dst, self.sx.at[kind, i], self.rx.at[kind, i], at.left if kind % 2 else at.right)

    def xwait(self, kind, r, u):
        at = self.at
        j, lo, n, _ = self.units[u]
        i = self.index[r, u]
        x = (at.xl, at.xr, at.xo, at.xo)[kind]
        rows = (pl.ds(lo, n), pl.ds(lo, n), pl.ds(lo, n // 2), pl.ds(lo + n // 2, n // 2))[kind]
        dst = self.xg.at[self.seqs[r], j, rows, self.cols(x)]
        remote(dst, dst, self.sx.at[kind, i], self.rx.at[kind, i], at.right).wait_recv()

    def yref(self, s, u, lo, n):
        j, _, _, first = self.units[u]
        rows = pl.ds(lo, n)
        return self.xg.at[s, j, rows, self.cols(self.at.x)] if first else self.xg.at[s, j, rows]

    def ycopy(self, d, u):
        j, lo, n, first = self.units[u]
        dst = self.yref(self.at.y, u, lo, n)
        src = self.src.at[j, pl.ds(lo, n)] if first else dst
        return remote(src, dst, self.sy.at[d, u], self.ry.at[d, u], self.at.down if d else self.at.up)

    def ywait(self, d, u):
        _, lo, n, _ = self.units[u]
        dst = self.yref(self.at.yu if d else self.at.yd, u, lo, n)
        remote(dst, dst, self.sy.at[d, u], self.ry.at[d, u], self.at.up).wait_recv()

    def yhalf(self, d, u):
        _, lo, n, _ = self.units[u]
        ref = self.yref(self.at.yu if d else self.at.yd, u, lo + d * (n // 2), n // 2)
        return remote(ref, ref, self.syh.at[d, u], self.ryh.at[d, u], self.at.down if d else self.at.up)

    def yhalf_wait(self, d, u):
        _, lo, n, _ = self.units[u]
        dst = self.yref(self.at.yo, u, lo + d * (n // 2), n // 2)
        remote(dst, dst, self.syh.at[d, u], self.ryh.at[d, u], self.at.up).wait_recv()

    def YR(self, u):
        for d in range(2):
            self.ycopy(d, u).start()

    def YH(self, u):
        for d in range(2):
            self.ywait(d, u)
            self.yhalf(d, u).start()

    YRH = YH

    def XF(self, r, u):
        if r == 2:
            for d in range(2):
                self.yhalf_wait(d, u)
        for kind in range(2):
            self.xcopy(kind, r, u).start()

    def XH(self, r, u):
        for kind in range(2):
            self.xwait(kind, r, u)
            self.xcopy(kind + 2, r, u).start()

    def N(self, r, u):
        j, lo, n, first = self.units[u]
        for kind in (2, 3):
            self.xwait(kind, r, u)
            self.xcopy(kind, r, u).wait_send()
        if r:
            for kind in range(2):
                self.xcopy(kind, r, u).wait_send()
        if r % 2:
            self.yhalf(0 if r == 3 else 1, u).wait_send()
        width, ref = self.xg.shape[-1], self.xg.at[self.seqs[r], j]
        s1, s2 = self.sums
        lane_sums(ref, lo, n, s1, s2)
        mean = jnp.sum(s1[0:n, :], axis=-1, keepdims=True) / width
        var = jnp.sum(s2[0:n, :], axis=-1, keepdims=True) / width - mean * mean
        s1[0:n, :] = jnp.broadcast_to(mean, (n, 128))
        s2[0:n, :] = jnp.broadcast_to(lax.rsqrt(var + EPS), (n, 128))
        scale_rows(ref, lo, n, s1, s2)
        if not first:
            self.YR(u)

    def chunk_wait(self, r, j):
        if r == 2:
            for u, unit in enumerate(self.units):
                if unit[0] == j and not unit[3]:
                    for d in range(2):
                        self.yhalf_wait(d, u)

    def drain(self):
        for u, unit in enumerate(self.units):
            for d in range(2):
                self.xcopy(d, 0, u).wait_send()
                self.ycopy(d, u).wait_send()
                if not unit[3]:
                    self.yhalf(d, u).wait_send()


def rows_of(refs):
    return refs[0][...] if len(refs) == 1 else jnp.concatenate([ref[...] for ref in refs], axis=0)


def product(refs, weight, depth, n_cols, done):
    step = 256

    def columns(i, carry):
        out = jnp.dot(rows_of(refs), weight[0:depth, pl.ds(al(i * step, 128), step)], preferred_element_type=F32)
        done(i * step, step, out)
        return carry

    lax.fori_loop(0, n_cols // step, columns, 0)


def lane_sums(ref, lo, n, s1, s2):
    width, rows, wide = ref.shape[-1], 32, 512

    def some_rows(i, carry):
        def some_columns(k, sums):
            a, b = sums
            v = ref[pl.ds(al(lo + i * rows, 8), rows), pl.ds(al(k * wide, 128), wide)].astype(F32)
            for c in range(0, wide, 128):
                part = v[:, c : c + 128]
                a, b = a + part, b + part * part
            return a, b

        zero = jnp.zeros((rows, 128), F32)
        a, b = lax.fori_loop(0, width // wide, some_columns, (zero, zero))
        s1[pl.ds(al(i * rows, 8), rows), :] = a
        s2[pl.ds(al(i * rows, 8), rows), :] = b
        return carry

    lax.fori_loop(0, n // rows, some_rows, 0)


def scale_rows(ref, lo, n, means, scales):
    width, rows, wide = ref.shape[-1], 32, 512

    def some_rows(i, carry):
        mean, scale = (t[pl.ds(al(i * rows, 8), rows), :] for t in (means, scales))

        def some_columns(k, carry):
            at_rows = pl.ds(al(lo + i * rows, 8), rows)
            for c in range(0, wide, 128):
                cols = pl.ds(al(k * wide + c, 128), 128)
                ref[at_rows, cols] = ((ref[at_rows, cols].astype(F32) - mean) * scale).astype(BF16)
            return carry

        lax.fori_loop(0, width // wide, some_columns, 0)
        return carry

    lax.fori_loop(0, n // rows, some_rows, 0)


class Reduce:
    def __init__(self, at, zb, ya, yb, yfd, yfu, ss, rs):
        self.at, self.zb, self.ya, self.yb, self.yfd, self.yfu, self.ss, self.rs = at, zb, ya, yb, yfd, yfu, ss, rs
        self.ch = zb.shape[2]
        self.h = self.ch // 2

    def copy(self, kind, j):
        at, h, ch = self.at, self.h, self.ch
        src, dst = (
            lambda: (self.zb.at[2, j, pl.ds(0, h)], self.ya.at[j]),
            lambda: (self.zb.at[2, j, pl.ds(h, ch - h)], self.yb.at[j]),
            lambda: (self.zb.at[1, j], self.yfd.at[j]),
            lambda: (self.zb.at[3, j], self.yfu.at[j]),
        )[kind]()
        return remote(src, dst, self.ss.at[kind, j], self.rs.at[kind, j], at.down if kind % 2 else at.up)

    def wait(self, kind, j):
        self.copy(kind, j).wait_recv()

    def halves(self, j):
        self.copy(0, j).start()
        self.copy(1, j).start()

    def middle(self, j):
        h = self.h
        self.wait(0, j)
        self.zb[1, j, 0:h] = (self.zb[1, j, 0:h].astype(F32) + self.ya[j].astype(F32)).astype(BF16)
        self.copy(2, j).start()
        self.wait(1, j)
        self.zb[3, j, h:] = (self.zb[3, j, h:].astype(F32) + self.yb[j].astype(F32)).astype(BF16)
        self.copy(3, j).start()

    def total(self, j):
        self.wait(2, j)
        self.wait(3, j)
        return self.zb[0, j].astype(F32) + self.yfd[j].astype(F32) + self.yfu[j].astype(F32)

    def drain(self):
        for j in range(NJ):
            for kind in range(4):
                self.copy(kind, j).wait_send()


def attention_kernel(
    units, x_hbm, turn_ref, base_ref, wq, wk, wv, wo, wg_t, wu_t,
    h_hbm, w_all, hg_all,
    x_ref, h_ref, xc, xg, hg, cos_all, sin_all, st_own, st_in, s1, s2, wb, wob, part, precv, qb, kvo, kvp, og, zb, ya, yb, yfd, yfu, own, drel_a, drel_b,
    sxe, rxe, sst, rst, sy, ry, syh, ryh, sd, rd, swa, rwa, swo, rwo, swp, rwp, lw, so, ro, spr, rpr, skv, rkv, sog, rog, syr, ryr,
    lg, sds, rds, sdo, rdo, sdf, rdf, sdp, rdp, shx, rhx, shy, rhy, shz, rhz, lh, lx,
):
    at = Place()
    x, c, y = at.x, at.c, at.y
    ch, kc = xc.shape[1], xc.shape[2]
    kd = wq.shape[0]
    hc = qb.shape[2]
    fc, f_a = w_all.shape[1], drel_a.shape[1]
    width = 2 * xg.shape[3]
    kh = div(x, 2)
    ng = rem(div(x + 1, 2), 2)
    gather = Spread(at, xc, xg, units, (s1, s2), None, None, sy, ry, syh, ryh)
    reduce = Reduce(at, zb, ya, yb, yfd, yfu, syr, ryr)
    ahead = Spread(at, h_ref, hg, ((0, 0, ch // 2, 0), (0, ch // 2, ch // 2, 0)), (s1, s2), shx, rhx, shy, rhy, shz, rhz)
    weights = (wq, wk, wv)

    def half_cols(core):
        return pl.ds(al(core * kd, 128), kd)

    def x_rows(j, core):
        return pl.ds(al((2 * j + core) * ch, 8), ch)

    def x_pair(j):
        return remote(x_ref.at[x_rows(j, 1 - c)], xc.at[j, :, half_cols(c)], sd.at[j], rd.at[j], at.partner)

    def pair_cols(xx):
        return pl.ds(al(rem(xx, 2) * kc, 128), kc)

    def xe_copy(u, xx):
        j, lo, n, _ = units[u]
        rows = pl.ds(lo, n)
        return remote(xc.at[j, rows], xg.at[y, j, rows, pair_cols(xx)], sxe.at[u], rxe.at[u], at.pa)

    def st_copy(u):
        j, lo, n, _ = units[u]
        rows = pl.ds(lo // 4, n // 4)
        return remote(st_own.at[j, rows], st_in.at[j, rows], sst.at[u], rst.at[u], at.pb)

    def XP(j):
        x_pair(j).start()

    arrived = []

    def XE(u):
        j, lo, n, _ = units[u]
        if j not in arrived:
            arrived.append(j)
            dst = xc.at[j, :, half_cols(1 - c)]
            remote(dst, dst, sd.at[j], rd.at[j], at.partner).wait_recv()
        xe_copy(u, x).start()
        xg[y, j, lo : lo + n, pair_cols(x)] = xc[j, lo : lo + n]

    def ST(u):
        j, lo, n, _ = units[u]
        xe_copy(u, at.xa).wait_recv()
        quarter = n // 4
        lane = lax.broadcasted_iota(jnp.int32, (quarter, 128), 1)
        lane_sums(xg.at[y, j], lo, n, s1, s2)
        packed = jnp.zeros((quarter, 128), F32)
        for g in range(4):
            rows = pl.ds(g * quarter, quarter)
            total, square = (jnp.sum(t[rows, :], axis=-1, keepdims=True) for t in (s1, s2))
            packed = jnp.where(lane // 32 == g, jnp.where(lane % 32 < 16, total, square), packed)
        st_own[j, lo // 4 : lo // 4 + quarter, :] = packed
        st_copy(u).start()

    def N(u):
        j, lo, n, _ = units[u]
        st_copy(u).wait_recv()
        quarter = n // 4
        at_rows = slice(lo // 4, lo // 4 + quarter)
        moments = (st_own[j, at_rows, :] + st_in[j, at_rows, :]) / width
        for g in range(4):
            mean = moments[:, 32 * g : 32 * g + 1]
            var = moments[:, 32 * g + 16 : 32 * g + 17] - mean * mean
            rows = pl.ds(g * quarter, quarter)
            s1[rows, :] = jnp.broadcast_to(mean, (quarter, 128))
            s2[rows, :] = jnp.broadcast_to(lax.rsqrt(var + EPS), (quarter, 128))
        scale_rows(xg.at[y, j], lo, n, s1, s2)
        gather.YR(u)

    def w_rows(xx, core):
        return pl.ds(al(rem(xx, 2) * kc + core * kd, 128), kd)

    def w_part(group, half, i):
        side = kh if half else 1 - kh
        return weights[i].at[:, pl.ds(al((2 * group + side) * hc, 128), hc)]

    def w_cols(half, i):
        return pl.ds(half * 3 * hc + i * hc, hc)

    def wa_copy(half, i, xx):
        return remote(w_part(1 - ng, half, i), wb.at[w_rows(xx, c), w_cols(half, i)], swa.at[half, i], rwa.at[half, i], at.pa)

    def wo_copy(half, i, core):
        return remote(w_part(ng, half, i), wb.at[w_rows(x, core), w_cols(half, i)], swo.at[half, i], rwo.at[half, i], at.partner)

    def w_local(half, i):
        return pltpu.make_async_copy(w_part(ng, half, i), wb.at[w_rows(x, c), w_cols(half, i)], lw.at[half, i])

    def wp_copy(half, core):
        ref = wb.at[w_rows(at.xa, core), pl.ds(half * 3 * hc, 3 * hc)]
        return remote(ref, ref, swp.at[half], rwp.at[half], at.partner)

    o_local = pltpu.make_async_copy(wo, wob.at[:, half_cols(c)], lw.at[2, 0])
    o_pair = remote(wo, wob.at[:, half_cols(c)], so.at[0], ro.at[0], at.partner)
    pieces = [(half, i) for half in range(2) for i in range(3)]

    def WOP():
        for half, i in pieces:
            wo_copy(half, i, c).start()
        o_pair.start()

    def WA(half):
        for i in range(3):
            wa_copy(half, i, x).start()

    def WP(half):
        for i in range(3):
            wa_copy(half, i, at.xa).wait_recv()
        wp_copy(half, c).start()

    w_halves = [0, 1]

    def w_ready(half):
        if half not in w_halves:
            return
        w_halves.remove(half)
        for i in range(3):
            w_local(half, i).wait()
            wo_copy(half, i, 1 - c).wait_recv()
        wp_copy(half, 1 - c).wait_recv()
        if half:
            own_out()

    def own_out():
        for m in range(2):
            d_in(m).wait()
            d_out(m).start()
            d_pair(m, 3, c).start()

    def o_ready():
        o_local.wait()
        dst = wob.at[:, half_cols(1 - c)]
        remote(dst, dst, so.at[0], ro.at[0], at.partner).wait_recv()

    mlp_weights = (wg_t, wu_t)
    parts = ((0, f_a), (f_a, fc - f_a))

    def d_src(m, xx, p):
        return mlp_weights[m].at[pl.ds(al(xx * fc + parts[p][0], 8), parts[p][1])]

    def d_dst(m, xx, p):
        return w_all.at[m, pl.ds(*parts[p]), pl.ds(al((2 * xx + c) * kd, 128), kd)]

    def s_copy(d, m, p, xx):
        to, dev = ((at.xa, at.pa), (at.xb, at.pb))[d]
        return remote(d_src(m, to, p), d_dst(m, xx, p), sds.at[d, m, p], rds.at[d, m, p], dev)

    def o_copy(d, m):
        return remote(d_src(m, at.xo, d), (drel_a, drel_b)[d].at[m], sdo.at[d, m], rdo.at[d, m], (at.pa, at.pb)[d])

    def f_copy(d, m, xx):
        return remote((drel_a, drel_b)[d].at[m], d_dst(m, xx, d), sdf.at[d, m], rdf.at[d, m], (at.pb, at.pa)[d])

    def d_in(m):
        return pltpu.make_async_copy(mlp_weights[m].at[pl.ds(al(x * fc, 8), fc)], own.at[m], lg.at[0, m])

    def d_all(m, xx, core):
        return w_all.at[m, :, pl.ds(al((2 * xx + core) * kd, 128), kd)]

    def d_out(m):
        return pltpu.make_async_copy(own.at[m], d_all(m, x, c), lg.at[1, m])

    def d_pair(m, k, core):
        dst = d_all(m, (at.xa, at.xb, at.xo, x)[k], core)
        return remote(own.at[m] if k == 3 else dst, dst, sdp.at[m, k], rdp.at[m, k], at.partner)

    def S(link, m, p):
        s_copy("ab".index(link), m, p, x).start()

    def O(link, m):
        o_copy("ab".index(link), m).start()

    def F(link, m):
        d = "ba".index(link)
        o_copy(d, m).wait_recv()
        f_copy(d, m, (at.xa, at.xb)[d]).start()

    def DP(m):
        for d in range(2):
            for p in range(2):
                s_copy(d, m, p, (at.xa, at.xb)[d]).wait_recv()
            f_copy(d, m, at.xo).wait_recv()
        for k in range(3):
            d_pair(m, k, c).start()

    def pr_copy(n):
        return remote(part.at[n, :, pl.ds(0, 3 * hc)], precv.at[n], spr.at[n], rpr.at[n], at.pb)

    def project(g, first, size):
        def done(col, step, out):
            for i, (r, j) in enumerate(GROUPS[g]):
                part[r * NJ + j, :, pl.ds(al(first + col, 128), step)] = out[i * ch : (i + 1) * ch].astype(BF16)

        refs = [xg.at[gather.seqs[r], j] for r, j in GROUPS[g]]
        product(refs, wb.at[:, pl.ds(first, size)], wb.shape[0], size, done)

    split = {step[1] for step in ATTENTION_STEPS if step[0] == "Q"}

    def G(g):
        w_ready(0)
        for r, j in GROUPS[g]:
            gather.chunk_wait(r, j)
        if g in split:
            project(g, 0, 3 * hc)
        else:
            w_ready(1)
            project(g, 0, 6 * hc)
        for r, j in GROUPS[g]:
            pr_copy(r * NJ + j).start()

    def Q(g):
        w_ready(1)
        project(g, 3 * hc, 3 * hc)

    def kv_copy(r, j):
        s, n = gather.seqs[r], r * NJ + j
        return remote(kvo.at[s, j], kvp.at[s, j], skv.at[n], rkv.at[n], at.partner)

    def rotate(r, j):
        s, n = gather.seqs[r], r * NJ + j
        pr_copy(n).wait_recv()
        cos_t, sin_t = cos_all[j], sin_all[j]

        def total(col, size):
            mine = part[n, :, 3 * hc + col : 3 * hc + col + size]
            return (mine.astype(F32) + precv[n, :, col : col + size].astype(F32)).astype(BF16)

        def turned(col):
            v = total(col, HEAD_DIM).astype(F32)
            return (v * cos_t + pltpu.roll(v, HEAD_DIM // 2, axis=1) * sin_t).astype(BF16)

        for col in range(0, hc, HEAD_DIM):
            qb[n, :, col : col + HEAD_DIM] = turned(col)
            kvo[s, j, :, col : col + HEAD_DIM] = turned(hc + col)
        kvo[s, j, :, hc:] = total(2 * hc, hc)
        kv_copy(r, j).start()

    def R(g):
        for r, j in GROUPS[g]:
            rotate(r, j)

    def o_cols(xx):
        return pl.ds(al((2 * rem(div(xx + 1, 2), 2) + div(xx, 2)) * hc, 128), hc)

    cut = ch // 8

    def og_copy(kind, n):
        if kind < 2:
            ref = og.at[n, :, o_cols(x)]
        elif kind == 2:
            ref = og.at[n, pl.ds(0, cut), o_cols(at.xa)]
        else:
            ref = og.at[n, pl.ds(cut, ch - cut), o_cols(at.xb)]
        return remote(ref, ref, sog.at[kind, n], rog.at[kind, n], at.pa if kind in (0, 3) else at.pb)

    def og_wait(kind, n):
        xx = (at.xa, at.xb, at.xo, at.xo)[kind]
        rows = (pl.ds(0, ch), pl.ds(0, ch), pl.ds(0, cut), pl.ds(cut, ch - cut))[kind]
        dst = og.at[n, rows, o_cols(xx)]
        remote(dst, dst, sog.at[kind, n], rog.at[kind, n], at.pa).wait_recv()

    def attend(r, j, i):
        s, n = gather.seqs[r], r * NJ + j
        keys = (j + 1) * ch
        iq = lax.broadcasted_iota(jnp.int32, (ch, keys), 0) + j * ch
        ik = lax.broadcasted_iota(jnp.int32, (ch, keys), 1)
        own_ok = iq >= ik
        par_ok = ik < (j + c) * ch
        contract = (((1,), (1,)), ((), ()))
        cols = pl.ds(al(i * HEAD_DIM, 128), HEAD_DIM)
        v_cols = pl.ds(al(hc + i * HEAD_DIM, 128), HEAD_DIM)
        q = qb[n, :, cols]
        k_own = kvo[s, 0 : j + 1, :, cols].reshape(keys, HEAD_DIM)
        k_par = kvp[s, 0 : j + 1, :, cols].reshape(keys, HEAD_DIM)
        s_own = lax.dot_general(q, k_own, contract, preferred_element_type=F32) * HEAD_DIM**-0.5
        s_par = lax.dot_general(q, k_par, contract, preferred_element_type=F32) * HEAD_DIM**-0.5
        s_own = jnp.where(own_ok, s_own, -1e30)
        s_par = jnp.where(par_ok, s_par, -1e30)
        top = jnp.maximum(jnp.max(s_own, axis=1, keepdims=True), jnp.max(s_par, axis=1, keepdims=True))
        e_own, e_par = jnp.exp(s_own - top), jnp.exp(s_par - top)
        inv = 1.0 / (jnp.sum(e_own, axis=1, keepdims=True) + jnp.sum(e_par, axis=1, keepdims=True))
        v_own = kvo[s, 0 : j + 1, :, v_cols].reshape(keys, HEAD_DIM)
        v_par = kvp[s, 0 : j + 1, :, v_cols].reshape(keys, HEAD_DIM)
        out = jnp.dot((e_own * inv).astype(BF16), v_own, preferred_element_type=F32)
        out += jnp.dot((e_par * inv).astype(BF16), v_par, preferred_element_type=F32)
        og[n, :, pl.ds(al((2 * ng + kh) * hc + i * HEAD_DIM, 128), HEAD_DIM)] = out.astype(BF16)

    def A(g):
        for r, j in GROUPS[g]:
            kv_copy(r, j).wait_recv()

        def head(i, carry):
            for r, j in GROUPS[g]:
                attend(r, j, i)
            return carry

        lax.fori_loop(0, hc // HEAD_DIM, head, 0)
        for r, j in GROUPS[g]:
            og_copy(0, r * NJ + j).start()
            og_copy(1, r * NJ + j).start()

    def P(g):
        for r, j in GROUPS[g]:
            for kind in range(2):
                og_wait(kind, r * NJ + j)
                og_copy(kind + 2, r * NJ + j).start()

    def X(g):
        for r, j in GROUPS[g]:
            og_wait(2, r * NJ + j)
            og_wait(3, r * NJ + j)

        def done(col, size, out):
            for i, (r, j) in enumerate(GROUPS[g]):
                zb[r, j, :, pl.ds(al(col, 128), size)] = out[i * ch : (i + 1) * ch].astype(BF16)

        product([og.at[r * NJ + j] for r, j in GROUPS[g]], wob, wob.shape[0], kc, done)
        for r, j in GROUPS[g]:
            if r == 2:
                reduce.halves(j)

    def T(j):
        attn = reduce.total(j).astype(BF16)
        h_ref[j] = (xc[j].astype(F32) + attn.astype(F32)).astype(BF16)
        chunk_out(j).start()

    def chunk_out(j):
        return pltpu.make_async_copy(h_ref.at[j], h_hbm.at[j], lx.at[1 + j])

    def h_out(r, u):
        rows = pl.ds(u * (ch // 2), ch // 2)
        return pltpu.make_async_copy(hg.at[ahead.seqs[r], 0, rows], hg_all.at[ahead.seqs[r], rows], lh.at[r, u])

    kept = []

    def HF(u):
        if not kept:
            kept.append(u)
            ahead.keep_own()
        ahead.XF(0, u)

    def HY(u):
        ahead.YH(u)
        for r in (0, 1, 3):
            h_out(r, u).start()

    def HO(u):
        for d in range(2):
            ahead.yhalf_wait(d, u)
        h_out(2, u).start()

    def own_rows():
        for half, i in pieces:
            w_local(half, i).start()
        o_local.start()
        for m in range(2):
            d_in(m).start()
        x_in.wait()
        for j in range(NJ):
            xc[j, :, half_cols(c)] = x_ref[x_rows(j, c), :]

    x_in = pltpu.make_async_copy(x_hbm, x_ref, lx.at[0])
    x_in.start()
    at.barrier(own_rows)

    def angles():
        lane = lax.broadcasted_iota(jnp.int32, (ch, HEAD_DIM), 1)
        for j in range(NJ):
            base_cos, base_sin = base_ref[0, pl.ds(2 * j + c, 1), :], base_ref[1, pl.ds(2 * j + c, 1), :]
            cos_all[j] = base_cos * turn_ref[0] - base_sin * turn_ref[1]
            sine = base_sin * turn_ref[0] + base_cos * turn_ref[1]
            sin_all[j] = jnp.where(lane < HEAD_DIM // 2, -sine, sine)

    ops = {
        "XP": XP, "WOP": WOP, "XE": XE, "ST": ST, "N": N, "YH": gather.YH, "WA": WA, "WP": WP, "S": S, "O": O, "F": F, "DP": DP,
        "G": G, "Q": Q, "R": R, "A": A, "P": P, "X": X, "M": reduce.middle, "T": T,
        "HF": HF, "HH": lambda u: ahead.XH(0, u), "HN": lambda u: ahead.N(0, u), "HY": HY, "HO": HO,
    }
    def sent():
        for m in range(2):
            for k in range(4):
                d_pair(m, k, 1 - c).wait_recv()
                d_pair(m, k, c).wait_send()
            d_out(m).wait()
            for d in range(2):
                for p in range(2):
                    s_copy(d, m, p, x).wait_send()
                o_copy(d, m).wait_send()
                f_copy(d, m, x).wait_send()
        for j in range(NJ):
            x_pair(j).wait_send()
        for u in range(len(units)):
            xe_copy(u, x).wait_send()
            st_copy(u).wait_send()
            for d in range(2):
                gather.ycopy(d, u).wait_send()
                gather.yhalf(d, u).wait_send()
        reduce.drain()
        ahead.drain()
        for r in range(NX):
            for u in range(2):
                h_out(r, u).wait()
        o_pair.wait_send()
        for half, i in pieces:
            wa_copy(half, i, x).wait_send()
            wo_copy(half, i, c).wait_send()
        for half in range(2):
            wp_copy(half, c).wait_send()

        def chunk_sent(n, carry):
            pr_copy(n).wait_send()
            remote(kvo.at[0, 0], kvp.at[0, 0], skv.at[n], rkv.at[n], at.partner).wait_send()
            for kind in range(4):
                og_copy(kind, n).wait_send()
            return carry

        lax.fori_loop(0, NCH, chunk_sent, 0)

    waits = {"X": o_ready, "WP": angles}
    last = max(i for i, step in enumerate(ATTENTION_STEPS) if step[0] == "X")
    for i, step in enumerate(ATTENTION_STEPS):
        if step[0] in waits:
            waits.pop(step[0])()
        if i == last:
            sent()
        ops[step[0]](*step[1:])
    for j in range(NJ):
        chunk_out(j).wait()


def mlp_kernel(
    units, h_hbm, w_hbm, wdn, hg_hbm, y_ref,
    h_ref, xg, wt, raw, wd, ag, ar, act, s1, s2, zb, ya, yb, yfd, yfu, yst,
    sx, rx, sy, ry, syh, ryh, sa, ra, syr, ryr, sd, rd, lw, lwd, swd, rwd, lh, lo,
):
    at = Place()
    x, c, y = at.x, at.c, at.y
    ch, kc, h = h_ref.shape[1], h_ref.shape[2], h_ref.shape[1] // 2
    width = xg.shape[-1]
    kd = kc // 2
    fc, tiles = w_hbm.shape[1], wt.shape[1] // 256
    fm = (tiles - 1) * 128
    fr = fc - fm
    blocks, slots = 2 * tiles, raw.shape[0]
    gather = Spread(at, h_ref, xg, units, (s1, s2), sx, rx, sy, ry, syh, ryh)
    reduce = Reduce(at, zb, ya, yb, yfd, yfu, syr, ryr)

    def w_in(q):
        i, m = q // 2, q % 2
        n = min(128, fc - i * 128)
        return pltpu.make_async_copy(w_hbm.at[m, pl.ds(i * 128, n)], raw.at[q % slots, pl.ds(0, n)], lw.at[q])

    def WT(g):
        for q in range(g * blocks // 4, (g + 1) * blocks // 4):
            i, m, slot = q // 2, q % 2, q % slots
            w_in(q).wait()
            if fc < (i + 1) * 128:
                raw[slot, fc - i * 128 :, :] = jnp.zeros(((i + 1) * 128 - fc, width), BF16)

            def turn(k, carry, slot=slot, q=q):
                part = pl.ds(al(k * (width // 4), 128), width // 4)
                wt[part, q * 128 : (q + 1) * 128] = raw[slot, :, part].T
                return carry

            lax.fori_loop(0, 4, turn, 0)
            if q + slots < blocks:
                w_in(q + slots).start()

    def d_refs(q, core):
        cols = pl.ds(al(core * kd, 128), kd)
        main, rest = wdn.at[pl.ds(q * fc, fm)], wdn.at[pl.ds(q * fc + fm, fr)]
        return (main, wd.at[pl.ds(q * fm, fm), cols]), (rest, wd.at[pl.ds(NX * fm + q * 128, fr), cols])

    def d_own(q, k):
        src, dst = d_refs(q, c)[k]
        return pltpu.make_async_copy(src, dst, lwd.at[q, k])

    def d_pair(q, k, core):
        src, dst = d_refs(q, core)[k]
        return remote(src, dst, swd.at[q, k], rwd.at[q, k], at.partner)

    quarters = [(q, k) for q in range(NX) for k in range(2)]
    h_in_all = pltpu.make_async_copy(h_hbm, h_ref, lo.at[NJ])
    h_in_all.start()
    for q in range(slots):
        w_in(q).start()
    def h_in(s):
        return pltpu.make_async_copy(hg_hbm.at[s], xg.at[s, 0], lh.at[s])

    for s in range(NX):
        h_in(s).start()
    for q, k in quarters:
        d_own(q, k).start()
    for q in range(NX):
        wd[NX * fm + q * 128 + fr : NX * fm + (q + 1) * 128, :] = jnp.zeros((128 - fr, kc), BF16)
    at.barrier(h_in_all.wait)
    for q, k in quarters:
        d_pair(q, k, c).start()

    def a_refs(kind, n, xx):
        main, rest = pl.ds(al(xx * fm, 128), fm), pl.ds(al(xx * 128, 128), 128)
        if kind < 2:
            return ag.at[n, :, main], ar.at[n, :, rest]
        lo = (kind - 2) * h
        return ag.at[n, pl.ds(lo, h), main], ar.at[n, pl.ds(lo // 2, h // 2), rest]

    def a_copies(kind, n):
        refs = a_refs(kind, n, (x, x, at.xl, at.xr)[kind])
        return [remote(v, v, sa.at[kind, n, k], ra.at[kind, n, k], at.left if kind % 2 else at.right) for k, v in enumerate(refs)]

    def a_wait(kind, n):
        for k, v in enumerate(a_refs(kind, n, (at.xl, at.xr, at.xo, at.xo)[kind])):
            remote(v, v, sa.at[kind, n, k], ra.at[kind, n, k], at.right).wait_recv()

    def a_start(kind, n):
        for copy in a_copies(kind, n):
            copy.start()

    def G(g):
        for r, j in GROUPS[g]:
            gather.chunk_wait(r, j)

        def done(col, size, out):
            for k in range(0, size, 256):
                gate, up = out[:, k : k + 128].astype(BF16).astype(F32), out[:, k + 128 : k + 256].astype(BF16).astype(F32)
                value = (gate / (1.0 + jnp.exp(-gate)) * up).astype(BF16)
                act[0 : value.shape[0], pl.ds(al(div(col + k, 2), 128), 128)] = value

        product([xg.at[gather.seqs[r], j] for r, j in GROUPS[g]], wt, width, wt.shape[1], done)
        for i, (r, j) in enumerate(GROUPS[g]):
            n, lo = r * NJ + j, i * ch
            ag[n, :, pl.ds(al(x * fm, 128), fm)] = act[lo : lo + ch, :fm]
            below = pltpu.roll(act[lo + h : lo + ch, fm:].astype(F32), 64, axis=1)
            ar[n, :, pl.ds(al(x * 128, 128), 128)] = (act[lo : lo + h, fm:].astype(F32) + below).astype(BF16)
            for kind in range(2):
                a_start(kind, n)

    def P(g):
        for r, j in GROUPS[g]:
            for kind in range(2):
                a_wait(kind, r * NJ + j)
                a_start(kind + 2, r * NJ + j)

    def X(g):
        for r, j in GROUPS[g]:
            n = r * NJ + j
            for kind in (2, 3):
                a_wait(kind, n)
            for q in range(NX):
                cols = pl.ds(NX * fm + q * 128, 128)
                rest = ar[n, :, q * 128 : (q + 1) * 128]
                ag[n, 0:h, cols] = rest
                ag[n, h:, cols] = pltpu.roll(rest.astype(F32), 64, axis=1).astype(BF16)

        def done(col, size, out):
            for i, (r, j) in enumerate(GROUPS[g]):
                zb[r, j, :, pl.ds(al(col, 128), size)] = out[i * ch : (i + 1) * ch].astype(BF16)

        product([ag.at[r * NJ + j] for r, j in GROUPS[g]], wd, wd.shape[0], kc, done)
        for r, j in GROUPS[g]:
            if r == 2:
                reduce.halves(j)

    def y_rows(j, core):
        return pl.ds(al((2 * j + core) * ch, 8), ch)

    def y_copy(j):
        return remote(yst.at[1 - c, j], y_ref.at[y_rows(j, c)], sd.at[j], rd.at[j], at.partner)

    def y_own(j):
        return pltpu.make_async_copy(yst.at[c, j], y_ref.at[y_rows(j, c)], lo.at[j])

    def y_wait(j):
        dst = y_ref.at[y_rows(j, 1 - c)]
        remote(dst, dst, sd.at[j], rd.at[j], at.partner).wait_recv()

    def T(j):
        mlp = reduce.total(j).astype(BF16)
        out = (h_ref[j].astype(F32) + mlp.astype(F32)).astype(BF16)
        yst[0, j] = out[:, :kd]
        yst[1, j] = out[:, kd:]
        y_copy(j).start()
        y_own(j).start()

    ops = {"G": G, "P": P, "X": X, "M": reduce.middle, "T": T, "WT": WT}
    for name in ("YR", "YRH", "YH", "XF", "XH", "N"):
        ops[name] = getattr(gather, name)
    waits = {
        "N": gather.keep_own,
        "G": lambda: [h_in(s).wait() for s in range(NX)],
        "X": lambda: [(d_own(q, k).wait(), d_pair(q, k, 1 - c).wait_recv()) for q, k in quarters],
    }
    def sent():
        gather.drain()
        reduce.drain()
        for q, k in quarters:
            d_pair(q, k, c).wait_send()

        def chunk_sent(n, carry):
            for kind in range(4):
                for copy in a_copies(kind, n):
                    copy.wait_send()
            return carry

        lax.fori_loop(0, NCH, chunk_sent, 0)

    last = max(i for i, step in enumerate(MLP_STEPS) if step[0] == "X")
    for i, step in enumerate(MLP_STEPS):
        if step[0] in waits:
            waits.pop(step[0])()
        if i == last:
            sent()
        ops[step[0]](*step[1:])
    for j in range(NJ):
        y_copy(j).wait_send()
        y_own(j).wait()
        y_wait(j)


def vmem(*shape, dtype=BF16):
    return pltpu.VMEM(shape, dtype)


def sems(*shape):
    return pltpu.SemaphoreType.DMA(shape)


def solution(mesh):
    assert mesh.shape["tx"] == 2 * NX and mesh.shape["ty"] == NX
    act_spec = P(("dp", "ty"), None, "tx")
    col_spec = P("tx", "ty")
    row_spec = P("ty", "tx")
    any_spec = pl.BlockSpec(memory_space=pl.ANY)
    vmem_spec = pl.BlockSpec(memory_space=pltpu.VMEM)

    def layer(x_blk, w_q, w_k, w_v, w_o, w_gate, w_up, w_down):
        _, seq, kd = x_blk.shape
        kc, width = 2 * kd, 2 * NX * kd
        ch = seq // (2 * NJ)
        h = ch // 2
        row_heads = w_q.shape[1]
        hc = row_heads // NX
        fc = w_down.shape[0] // NX
        assert hc % HEAD_DIM == 0
        tiles = (fc + 127) // 128
        f_a = (fc // 2 + 15) // 16 * 16

        inv_freq = THETA ** (-2.0 * np.arange(HEAD_DIM // 2) / HEAD_DIM)
        inv_freq = np.concatenate([inv_freq, inv_freq])
        turn = np.arange(ch)[:, None] * inv_freq
        base = np.arange(2 * NJ)[:, None] * ch * inv_freq
        turn = jnp.asarray(np.stack([np.cos(turn), np.sin(turn)]), F32)
        base = jnp.asarray(np.stack([np.cos(base), np.sin(base)]), F32)

        reduce_scratch = [vmem(NX, NJ, ch, kc), vmem(NJ, h, kc), vmem(NJ, ch - h, kc), vmem(NJ, ch, kc), vmem(NJ, ch, kc)]
        units = ((0, 0, h, 0), (0, h, h, 0)) + tuple((j, 0, ch, 0) for j in range(1, NJ))
        n_u = len(units)
        h_blk, w_all, hg_all = pl.pallas_call(
            functools.partial(attention_kernel, units),
            out_shape=(
                jax.ShapeDtypeStruct((NJ, ch, kc), BF16),
                jax.ShapeDtypeStruct((2, fc, width), BF16),
                jax.ShapeDtypeStruct((NX, ch, width), BF16),
            ),
            in_specs=[any_spec] + [vmem_spec] * 2 + [any_spec] * 6,
            out_specs=(any_spec, any_spec, any_spec),
            scratch_shapes=[
                vmem(seq, kd), vmem(NJ, ch, kc), vmem(NJ, ch, kc), vmem(NX, NJ, ch, 2 * kc), vmem(NX, 1, ch, width), vmem(NJ, ch, HEAD_DIM, dtype=F32), vmem(NJ, ch, HEAD_DIM, dtype=F32),
                vmem(NJ, ch // 4, 128, dtype=F32), vmem(NJ, ch // 4, 128, dtype=F32), vmem(ch, 128, dtype=F32), vmem(ch, 128, dtype=F32),
                vmem(2 * kc, 6 * hc), vmem(row_heads, kc), vmem(NCH, ch, 6 * hc), vmem(NCH, ch, 3 * hc), vmem(NCH, ch, hc),
                vmem(NX, NJ, ch, 2 * hc), vmem(NX, NJ, ch, 2 * hc), vmem(NCH, ch, row_heads), *reduce_scratch,
                vmem(2, fc, kd), vmem(2, f_a, kd), vmem(2, fc - f_a, kd),
                sems(n_u), sems(n_u), sems(n_u), sems(n_u), sems(2, n_u), sems(2, n_u), sems(2, n_u), sems(2, n_u),
                sems(NJ), sems(NJ), sems(2, 3), sems(2, 3), sems(2, 3), sems(2, 3), sems(2), sems(2), sems(3, 3), sems(1), sems(1),
                sems(NCH), sems(NCH), sems(NCH), sems(NCH), sems(4, NCH), sems(4, NCH), sems(4, NJ), sems(4, NJ),
                sems(2, 2), sems(2, 2, 2), sems(2, 2, 2), sems(2, 2), sems(2, 2), sems(2, 2), sems(2, 2), sems(2, 4), sems(2, 4),
                sems(4, 2), sems(4, 2), sems(2, 2), sems(2, 2), sems(2, 2), sems(2, 2), sems(NX, 2), sems(1 + NJ),
            ],
            compiler_params=pltpu.CompilerParams(collective_id=0, has_side_effects=True, vmem_limit_bytes=VMEM_LIMIT),
            name="attention_part",
        )(x_blk[0], turn, base, w_q, w_k, w_v, w_o, w_gate.T, w_up.T)

        units = ((1, 0, h, 1), (1, h, h, 0)) + tuple((j, 0, ch, 0) for j in range(2, NJ))
        n_u, n_x = len(units), len(units) + 3
        y_blk = pl.pallas_call(
            functools.partial(mlp_kernel, units),
            out_shape=jax.ShapeDtypeStruct((seq, kd), BF16),
            in_specs=[any_spec] * 4,
            out_specs=any_spec,
            scratch_shapes=[
                vmem(NJ, ch, kc),
                vmem(NX, NJ, ch, width), vmem(width, tiles * 256), vmem(3, 128, width),
                vmem(NX * tiles * 128, kc), vmem(NCH, ch, NX * tiles * 128), vmem(NCH, h, NX * 128), vmem(2 * ch, tiles * 128),
                vmem(ch, 128, dtype=F32), vmem(ch, 128, dtype=F32),
                *reduce_scratch, vmem(2, NJ, ch, kd),
                sems(4, n_x), sems(4, n_x), sems(2, n_u), sems(2, n_u), sems(2, n_u), sems(2, n_u),
                sems(4, NCH, 2), sems(4, NCH, 2), sems(4, NJ), sems(4, NJ), sems(NJ), sems(NJ),
                sems(2 * tiles), sems(NX, 2), sems(NX, 2), sems(NX, 2), sems(NX), sems(NJ + 1),
            ],
            compiler_params=pltpu.CompilerParams(collective_id=1, has_side_effects=True, vmem_limit_bytes=VMEM_LIMIT),
            name="mlp_part",
        )(h_blk, w_all, w_down, hg_all)
        return y_blk[None]

    return jax.shard_map(
        layer,
        mesh=mesh,
        in_specs=(act_spec, col_spec, col_spec, col_spec, row_spec, col_spec, col_spec, row_spec),
        out_specs=act_spec,
        check_vma=False,
    )
```

```python
import functools

import jax
import jax.numpy as jnp
import numpy as np
from jax import lax
from jax.experimental import pallas as pl
from jax.experimental.pallas import tpu as pltpu
from jax.sharding import PartitionSpec as P

HEAD_DIM = 128
EPS = 1e-5
THETA = 10000.0
MESH = pl.DeviceIdType.MESH
F32 = jnp.float32
BF16 = jnp.bfloat16
NX = 4
NJ = 4
NCH = 16
VMEM_LIMIT = 67_043_328
GROUPS = (*(((0, j),) for j in range(NJ)), *(((3, j), (1, j)) for j in range(NJ)), *(((2, j),) for j in range(NJ)))


def rem(a, b):
    return lax.rem(a, jnp.int32(b))


def div(a, b):
    return lax.div(a, jnp.int32(b))


def al(v, m):
    return pl.multiple_of(v, m)


def remote(src, dst, ssem, rsem, dev):
    return pltpu.make_async_remote_copy(src_ref=src, dst_ref=dst, send_sem=ssem, recv_sem=rsem, device_id=dev, device_id_type=MESH)


ATTENTION_STEPS = (
    ("WA", 0), ("XP", 1), ("S", "b", 0, 1), ("XP", 0), ("XE", 1), ("XE", 0), ("XE", 2), ("XP", 2), ("S", "b", 0, 0), ("XP", 3),
    ("S", "b", 1, 0), ("ST", 1), ("WP", 0), ("WA", 1), ("O", "b", 1), ("ST", 0), ("N", 1), ("O", "b", 0), ("ST", 2),
    ("S", "b", 1, 1), ("WOP",), ("N", 0), ("G", 0), ("XE", 3), ("YH", 1), ("YH", 0), ("S", "a", 0, 1), ("N", 2), ("WP", 1),
    ("G", 8), ("G", 4), ("ST", 3), ("Q", 8), ("Q", 0), ("R", 8), ("XE", 4), ("A", 8), ("F", "a", 1), ("YH", 2), ("G", 5),
    ("R", 4), ("ST", 4), ("N", 3), ("P", 8), ("G", 9), ("A", 4), ("R", 0), ("S", "a", 1, 1), ("X", 8), ("G", 1), ("N", 4),
    ("R", 5), ("A", 0), ("R", 9), ("P", 4), ("A", 9), ("A", 5), ("G", 2), ("P", 0), ("X", 4), ("M", 0), ("P", 9),
    ("S", "a", 1, 0), ("YH", 3), ("G", 6), ("P", 5), ("X", 0), ("T", 0), ("HF", 1), ("HF", 0), ("R", 2), ("X", 9), ("R", 1),
    ("A", 1), ("YH", 4), ("X", 5), ("M", 1), ("HH", 1), ("O", "a", 0), ("G", 10), ("R", 6), ("HH", 0), ("G", 7), ("O", "a", 1),
    ("HN", 1), ("R", 10), ("G", 11), ("A", 10), ("A", 6), ("HN", 0), ("R", 7), ("A", 2), ("HY", 1), ("A", 7), ("R", 11),
    ("P", 10), ("A", 11), ("P", 6), ("G", 3), ("P", 7), ("P", 11), ("F", "b", 1), ("F", "a", 0), ("X", 10), ("HY", 0),
    ("S", "a", 0, 0), ("F", "b", 0), ("R", 3), ("X", 11), ("A", 3), ("X", 6), ("HO", 1), ("X", 7), ("P", 1), ("P", 2),
    ("M", 2), ("M", 3), ("DP", 1), ("DP", 0), ("P", 3), ("HO", 0), ("X", 1), ("T", 1), ("X", 2), ("T", 2), ("X", 3), ("T", 3),
)
MLP_STEPS = (
    ("XF", 0, 1), ("YR", 0), ("WT", 0), ("XF", 0, 0), ("XH", 0, 1), ("XF", 0, 3), ("YRH", 0), ("XF", 2, 0), ("N", 0, 1),
    ("WT", 1), ("WT", 2), ("XH", 0, 3), ("XF", 0, 2), ("WT", 3), ("XF", 1, 0), ("XF", 3, 0), ("N", 0, 3), ("G", 8), ("YH", 1),
    ("XH", 2, 0), ("G", 4), ("P", 8), ("XH", 3, 0), ("XH", 0, 0), ("XH", 0, 2), ("G", 3), ("XH", 1, 0), ("YH", 3), ("G", 7),
    ("N", 2, 0), ("N", 0, 0), ("G", 9), ("N", 0, 2), ("P", 7), ("G", 11), ("P", 4), ("P", 9), ("N", 1, 0), ("N", 3, 0),
    ("G", 5), ("X", 8), ("G", 1), ("X", 4), ("YH", 2), ("P", 11), ("G", 6), ("X", 9), ("X", 7), ("X", 11), ("P", 5), ("M", 0),
    ("G", 10), ("G", 0), ("M", 3), ("X", 5), ("P", 10), ("P", 3), ("M", 1), ("P", 6), ("G", 2), ("P", 1), ("X", 10), ("X", 3),
    ("P", 0), ("X", 6), ("M", 2), ("T", 3), ("P", 2), ("X", 1), ("T", 1), ("X", 0), ("T", 0), ("X", 2), ("T", 2),
)


class Place:
    def __init__(self):
        tx, ty = lax.axis_index("tx"), lax.axis_index("ty")
        self.x, self.c, self.y = div(tx, 2), rem(tx, 2), ty
        x, c, y = self.x, self.c, self.y
        self.xr, self.xl, self.xo = rem(x + 1, NX), rem(x + 3, NX), rem(x + 2, NX)
        self.yu, self.yd, self.yo = rem(y + 1, NX), rem(y + 3, NX), rem(y + 2, NX)
        self.right = {"tx": self.xr * 2 + c, "ty": y}
        self.left = {"tx": self.xl * 2 + c, "ty": y}
        self.up = {"tx": tx, "ty": self.yu}
        self.down = {"tx": tx, "ty": self.yd}
        self.partner = {"tx": x * 2 + 1 - c, "ty": y}
        self.xa, self.xb = x + 1 - 2 * rem(x, 2), rem(x + 3 + 2 * rem(x, 2), NX)
        self.pa, self.pb = {"tx": self.xa * 2 + c, "ty": y}, {"tx": self.xb * 2 + c, "ty": y}

    def barrier(self, between):
        sem = pltpu.get_barrier_semaphore()
        for dev in (self.right, self.left, self.up, self.down, self.partner):
            pl.semaphore_signal(sem, inc=1, device_id=dev, device_id_type=MESH)
        between()
        pl.semaphore_wait(sem, 5)


class Spread:
    def __init__(self, at, src, xg, units, sums, sx, rx, sy, ry, syh, ryh):
        self.sums = sums
        self.at, self.src, self.xg, self.units, self.kc = at, src, xg, units, src.shape[2]
        self.sx, self.rx, self.sy, self.ry, self.syh, self.ryh = sx, rx, sy, ry, syh, ryh
        pairs = [(r, u) for u, unit in enumerate(units) for r in ((0, 3, 1, 2) if unit[3] else (0,))]
        self.index = {pair: i for i, pair in enumerate(pairs)}
        self.seqs = (at.y, at.yu, at.yo, at.yd)

    def cols(self, x):
        return pl.ds(al(x * self.kc, 128), self.kc)

    def keep_own(self):
        for j in {unit[0]: 0 for unit in self.units}:
            self.xg[self.at.y, j, :, self.cols(self.at.x)] = self.src[j]

    def xcopy(self, kind, r, u):
        at, s = self.at, self.seqs[r]
        j, lo, n, _ = self.units[u]
        i = self.index[r, u]
        if kind < 2:
            dst = self.xg.at[s, j, pl.ds(lo, n), self.cols(at.x)]
            src = self.src.at[j, pl.ds(lo, n)] if r == 0 else dst
        elif kind == 2:
            src = dst = self.xg.at[s, j, pl.ds(lo, n // 2), self.cols(at.xl)]
        else:
            src = dst = self.xg.at[s, j, pl.ds(lo + n // 2, n // 2), self.cols(at.xr)]
        return remote(src, dst, self.sx.at[kind, i], self.rx.at[kind, i], at.left if kind % 2 else at.right)

    def xwait(self, kind, r, u):
        at = self.at
        j, lo, n, _ = self.units[u]
        i = self.index[r, u]
        x = (at.xl, at.xr, at.xo, at.xo)[kind]
        rows = (pl.ds(lo, n), pl.ds(lo, n), pl.ds(lo, n // 2), pl.ds(lo + n // 2, n // 2))[kind]
        dst = self.xg.at[self.seqs[r], j, rows, self.cols(x)]
        remote(dst, dst, self.sx.at[kind, i], self.rx.at[kind, i], at.right).wait_recv()

    def yref(self, s, u, lo, n):
        j, _, _, first = self.units[u]
        rows = pl.ds(lo, n)
        return self.xg.at[s, j, rows, self.cols(self.at.x)] if first else self.xg.at[s, j, rows]

    def ycopy(self, d, u):
        j, lo, n, first = self.units[u]
        dst = self.yref(self.at.y, u, lo, n)
        src = self.src.at[j, pl.ds(lo, n)] if first else dst
        return remote(src, dst, self.sy.at[d, u], self.ry.at[d, u], self.at.down if d else self.at.up)

    def ywait(self, d, u):
        _, lo, n, _ = self.units[u]
        dst = self.yref(self.at.yu if d else self.at.yd, u, lo, n)
        remote(dst, dst, self.sy.at[d, u], self.ry.at[d, u], self.at.up).wait_recv()

    def yhalf(self, d, u):
        _, lo, n, _ = self.units[u]
        ref = self.yref(self.at.yu if d else self.at.yd, u, lo + d * (n // 2), n // 2)
        return remote(ref, ref, self.syh.at[d, u], self.ryh.at[d, u], self.at.down if d else self.at.up)

    def yhalf_wait(self, d, u):
        _, lo, n, _ = self.units[u]
        dst = self.yref(self.at.yo, u, lo + d * (n // 2), n // 2)
        remote(dst, dst, self.syh.at[d, u], self.ryh.at[d, u], self.at.up).wait_recv()

    def YR(self, u):
        for d in range(2):
            self.ycopy(d, u).start()

    def YH(self, u):
        for d in range(2):
            self.ywait(d, u)
            self.yhalf(d, u).start()

    YRH = YH

    def XF(self, r, u):
        if r == 2:
            for d in range(2):
                self.yhalf_wait(d, u)
        for kind in range(2):
            self.xcopy(kind, r, u).start()

    def XH(self, r, u):
        for kind in range(2):
            self.xwait(kind, r, u)
            self.xcopy(kind + 2, r, u).start()

    def N(self, r, u):
        j, lo, n, first = self.units[u]
        for kind in (2, 3):
            self.xwait(kind, r, u)
            self.xcopy(kind, r, u).wait_send()
        if r:
            for kind in range(2):
                self.xcopy(kind, r, u).wait_send()
        if r % 2:
            self.yhalf(0 if r == 3 else 1, u).wait_send()
        width, ref = self.xg.shape[-1], self.xg.at[self.seqs[r], j]
        s1, s2 = self.sums
        lane_sums(ref, lo, n, s1, s2)
        mean = jnp.sum(s1[0:n, :], axis=-1, keepdims=True) / width
        var = jnp.sum(s2[0:n, :], axis=-1, keepdims=True) / width - mean * mean
        s1[0:n, :] = jnp.broadcast_to(mean, (n, 128))
        s2[0:n, :] = jnp.broadcast_to(lax.rsqrt(var + EPS), (n, 128))
        scale_rows(ref, lo, n, s1, s2)
        if not first:
            self.YR(u)

    def chunk_wait(self, r, j):
        if r == 2:
            for u, unit in enumerate(self.units):
                if unit[0] == j and not unit[3]:
                    for d in range(2):
                        self.yhalf_wait(d, u)

    def drain(self):
        for u, unit in enumerate(self.units):
            for d in range(2):
                self.xcopy(d, 0, u).wait_send()
                self.ycopy(d, u).wait_send()
                if not unit[3]:
                    self.yhalf(d, u).wait_send()


def rows_of(refs):
    return refs[0][...] if len(refs) == 1 else jnp.concatenate([ref[...] for ref in refs], axis=0)


def product(refs, weight, depth, n_cols, done):
    step = 256

    def columns(i, carry):
        out = jnp.dot(rows_of(refs), weight[0:depth, pl.ds(al(i * step, 128), step)], preferred_element_type=F32)
        done(i * step, step, out)
        return carry

    lax.fori_loop(0, n_cols // step, columns, 0)


def lane_sums(ref, lo, n, s1, s2):
    width, rows, wide = ref.shape[-1], 32, 512

    def some_rows(i, carry):
        def some_columns(k, sums):
            a, b = sums
            v = ref[pl.ds(al(lo + i * rows, 8), rows), pl.ds(al(k * wide, 128), wide)].astype(F32)
            for c in range(0, wide, 128):
                part = v[:, c : c + 128]
                a, b = a + part, b + part * part
            return a, b

        zero = jnp.zeros((rows, 128), F32)
        a, b = lax.fori_loop(0, width // wide, some_columns, (zero, zero))
        s1[pl.ds(al(i * rows, 8), rows), :] = a
        s2[pl.ds(al(i * rows, 8), rows), :] = b
        return carry

    lax.fori_loop(0, n // rows, some_rows, 0)


def scale_rows(ref, lo, n, means, scales):
    width, rows, wide = ref.shape[-1], 32, 512

    def some_rows(i, carry):
        mean, scale = (t[pl.ds(al(i * rows, 8), rows), :] for t in (means, scales))

        def some_columns(k, carry):
            at_rows = pl.ds(al(lo + i * rows, 8), rows)
            for c in range(0, wide, 128):
                cols = pl.ds(al(k * wide + c, 128), 128)
                ref[at_rows, cols] = ((ref[at_rows, cols].astype(F32) - mean) * scale).astype(BF16)
            return carry

        lax.fori_loop(0, width // wide, some_columns, 0)
        return carry

    lax.fori_loop(0, n // rows, some_rows, 0)


class Reduce:
    def __init__(self, at, zb, ya, yb, yfd, yfu, ss, rs):
        self.at, self.zb, self.ya, self.yb, self.yfd, self.yfu, self.ss, self.rs = at, zb, ya, yb, yfd, yfu, ss, rs
        self.ch = zb.shape[2]
        self.h = self.ch // 2

    def copy(self, kind, j):
        at, h, ch = self.at, self.h, self.ch
        src, dst = (
            lambda: (self.zb.at[2, j, pl.ds(0, h)], self.ya.at[j]),
            lambda: (self.zb.at[2, j, pl.ds(h, ch - h)], self.yb.at[j]),
            lambda: (self.zb.at[1, j], self.yfd.at[j]),
            lambda: (self.zb.at[3, j], self.yfu.at[j]),
        )[kind]()
        return remote(src, dst, self.ss.at[kind, j], self.rs.at[kind, j], at.down if kind % 2 else at.up)

    def wait(self, kind, j):
        self.copy(kind, j).wait_recv()

    def halves(self, j):
        self.copy(0, j).start()
        self.copy(1, j).start()

    def middle(self, j):
        h = self.h
        self.wait(0, j)
        self.zb[1, j, 0:h] = (self.zb[1, j, 0:h].astype(F32) + self.ya[j].astype(F32)).astype(BF16)
        self.copy(2, j).start()
        self.wait(1, j)
        self.zb[3, j, h:] = (self.zb[3, j, h:].astype(F32) + self.yb[j].astype(F32)).astype(BF16)
        self.copy(3, j).start()

    def total(self, j):
        self.wait(2, j)
        self.wait(3, j)
        return self.zb[0, j].astype(F32) + self.yfd[j].astype(F32) + self.yfu[j].astype(F32)

    def drain(self):
        for j in range(NJ):
            for kind in range(4):
                self.copy(kind, j).wait_send()


def attention_kernel(
    units, x_hbm, turn_hbm, base_hbm, wq, wk, wv, wo, wg_t, wu_t,
    h_hbm, w_all, hg_all,
    x_ref, turn_ref, base_ref, h_ref, xc, xg, hg, cos_all, sin_all, st_own, st_in, s1, s2, wb, wob, part, precv, qb, kvo, kvp, og, zb, ya, yb, yfd, yfu, own, drel_a, drel_b,
    sxe, rxe, sst, rst, sy, ry, syh, ryh, sd, rd, swa, rwa, swo, rwo, swp, rwp, lw, so, ro, spr, rpr, skv, rkv, sog, rog, syr, ryr,
    lg, sds, rds, sdo, rdo, sdf, rdf, sdp, rdp, shx, rhx, shy, rhy, shz, rhz, lh, lx,
):
    at = Place()
    x, c, y = at.x, at.c, at.y
    ch, kc = xc.shape[1], xc.shape[2]
    kd = wq.shape[0]
    hc = qb.shape[2]
    fc, f_a = w_all.shape[1], drel_a.shape[1]
    width = 2 * xg.shape[3]
    kh = div(x, 2)
    ng = rem(div(x + 1, 2), 2)
    gather = Spread(at, xc, xg, units, (s1, s2), None, None, sy, ry, syh, ryh)
    reduce = Reduce(at, zb, ya, yb, yfd, yfu, syr, ryr)
    ahead = Spread(at, h_ref, hg, ((0, 0, ch // 2, 0), (0, ch // 2, ch // 2, 0)), (s1, s2), shx, rhx, shy, rhy, shz, rhz)
    weights = (wq, wk, wv)

    def half_cols(core):
        return pl.ds(al(core * kd, 128), kd)

    def x_rows(j, core):
        return pl.ds(al((2 * j + core) * ch, 8), ch)

    def x_pair(j):
        return remote(x_ref.at[x_rows(j, 1 - c)], xc.at[j, :, half_cols(c)], sd.at[j], rd.at[j], at.partner)

    def pair_cols(xx):
        return pl.ds(al(rem(xx, 2) * kc, 128), kc)

    def xe_copy(u, xx):
        j, lo, n, _ = units[u]
        rows = pl.ds(lo, n)
        return remote(xc.at[j, rows], xg.at[y, j, rows, pair_cols(xx)], sxe.at[u], rxe.at[u], at.pa)

    def st_copy(u):
        j, lo, n, _ = units[u]
        rows = pl.ds(lo // 4, n // 4)
        return remote(st_own.at[j, rows], st_in.at[j, rows], sst.at[u], rst.at[u], at.pb)

    def XP(j):
        x_pair(j).start()

    arrived = []

    def XE(u):
        j, lo, n, _ = units[u]
        if j not in arrived:
            arrived.append(j)
            dst = xc.at[j, :, half_cols(1 - c)]
            remote(dst, dst, sd.at[j], rd.at[j], at.partner).wait_recv()
        xe_copy(u, x).start()
        xg[y, j, lo : lo + n, pair_cols(x)] = xc[j, lo : lo + n]

    def ST(u):
        j, lo, n, _ = units[u]
        xe_copy(u, at.xa).wait_recv()
        quarter = n // 4
        lane = lax.broadcasted_iota(jnp.int32, (quarter, 128), 1)
        lane_sums(xg.at[y, j], lo, n, s1, s2)
        packed = jnp.zeros((quarter, 128), F32)
        for g in range(4):
            rows = pl.ds(g * quarter, quarter)
            total, square = (jnp.sum(t[rows, :], axis=-1, keepdims=True) for t in (s1, s2))
            packed = jnp.where(lane // 32 == g, jnp.where(lane % 32 < 16, total, square), packed)
        st_own[j, lo // 4 : lo // 4 + quarter, :] = packed
        st_copy(u).start()

    def N(u):
        j, lo, n, _ = units[u]
        st_copy(u).wait_recv()
        quarter = n // 4
        at_rows = slice(lo // 4, lo // 4 + quarter)
        moments = (st_own[j, at_rows, :] + st_in[j, at_rows, :]) / width
        for g in range(4):
            mean = moments[:, 32 * g : 32 * g + 1]
            var = moments[:, 32 * g + 16 : 32 * g + 17] - mean * mean
            rows = pl.ds(g * quarter, quarter)
            s1[rows, :] = jnp.broadcast_to(mean, (quarter, 128))
            s2[rows, :] = jnp.broadcast_to(lax.rsqrt(var + EPS), (quarter, 128))
        scale_rows(xg.at[y, j], lo, n, s1, s2)
        gather.YR(u)

    def w_rows(xx, core):
        return pl.ds(al(rem(xx, 2) * kc + core * kd, 128), kd)

    def w_part(group, half, i):
        side = kh if half else 1 - kh
        return weights[i].at[:, pl.ds(al((2 * group + side) * hc, 128), hc)]

    def w_cols(half, i):
        return pl.ds(half * 3 * hc + i * hc, hc)

    def wa_copy(half, i, xx):
        return remote(w_part(1 - ng, half, i), wb.at[w_rows(xx, c), w_cols(half, i)], swa.at[half, i], rwa.at[half, i], at.pa)

    def wo_copy(half, i, core):
        return remote(w_part(ng, half, i), wb.at[w_rows(x, core), w_cols(half, i)], swo.at[half, i], rwo.at[half, i], at.partner)

    def w_local(half, i):
        return pltpu.make_async_copy(w_part(ng, half, i), wb.at[w_rows(x, c), w_cols(half, i)], lw.at[half, i])

    def wp_copy(half, core):
        ref = wb.at[w_rows(at.xa, core), pl.ds(half * 3 * hc, 3 * hc)]
        return remote(ref, ref, swp.at[half], rwp.at[half], at.partner)

    o_local = pltpu.make_async_copy(wo, wob.at[:, half_cols(c)], lw.at[2, 0])
    o_pair = remote(wo, wob.at[:, half_cols(c)], so.at[0], ro.at[0], at.partner)
    pieces = [(half, i) for half in range(2) for i in range(3)]

    def WOP():
        for half, i in pieces:
            wo_copy(half, i, c).start()
        o_pair.start()

    def WA(half):
        for i in range(3):
            wa_copy(half, i, x).start()

    def WP(half):
        for i in range(3):
            wa_copy(half, i, at.xa).wait_recv()
        wp_copy(half, c).start()

    w_halves = [0, 1]

    def w_ready(half):
        if half not in w_halves:
            return
        w_halves.remove(half)
        for i in range(3):
            w_local(half, i).wait()
            wo_copy(half, i, 1 - c).wait_recv()
        wp_copy(half, 1 - c).wait_recv()
        if half:
            own_out()

    def own_out():
        for m in range(2):
            d_in(m).wait()
            d_out(m).start()
            d_pair(m, 3, c).start()

    def o_ready():
        o_local.wait()
        dst = wob.at[:, half_cols(1 - c)]
        remote(dst, dst, so.at[0], ro.at[0], at.partner).wait_recv()

    mlp_weights = (wg_t, wu_t)
    parts = ((0, f_a), (f_a, fc - f_a))

    def d_src(m, xx, p):
        return mlp_weights[m].at[pl.ds(al(xx * fc + parts[p][0], 8), parts[p][1])]

    def d_dst(m, xx, p):
        return w_all.at[m, pl.ds(*parts[p]), pl.ds(al((2 * xx + c) * kd, 128), kd)]

    def s_copy(d, m, p, xx):
        to, dev = ((at.xa, at.pa), (at.xb, at.pb))[d]
        return remote(d_src(m, to, p), d_dst(m, xx, p), sds.at[d, m, p], rds.at[d, m, p], dev)

    def o_copy(d, m):
        return remote(d_src(m, at.xo, d), (drel_a, drel_b)[d].at[m], sdo.at[d, m], rdo.at[d, m], (at.pa, at.pb)[d])

    def f_copy(d, m, xx):
        return remote((drel_a, drel_b)[d].at[m], d_dst(m, xx, d), sdf.at[d, m], rdf.at[d, m], (at.pb, at.pa)[d])

    def d_in(m):
        return pltpu.make_async_copy(mlp_weights[m].at[pl.ds(al(x * fc, 8), fc)], own.at[m], lg.at[0, m])

    def d_all(m, xx, core):
        return w_all.at[m, :, pl.ds(al((2 * xx + core) * kd, 128), kd)]

    def d_out(m):
        return pltpu.make_async_copy(own.at[m], d_all(m, x, c), lg.at[1, m])

    def d_pair(m, k, core):
        dst = d_all(m, (at.xa, at.xb, at.xo, x)[k], core)
        return remote(own.at[m] if k == 3 else dst, dst, sdp.at[m, k], rdp.at[m, k], at.partner)

    def S(link, m, p):
        s_copy("ab".index(link), m, p, x).start()

    def O(link, m):
        o_copy("ab".index(link), m).start()

    def F(link, m):
        d = "ba".index(link)
        o_copy(d, m).wait_recv()
        f_copy(d, m, (at.xa, at.xb)[d]).start()

    def DP(m):
        for d in range(2):
            for p in range(2):
                s_copy(d, m, p, (at.xa, at.xb)[d]).wait_recv()
            f_copy(d, m, at.xo).wait_recv()
        for k in range(3):
            d_pair(m, k, c).start()

    def pr_copy(n):
        return remote(part.at[n, :, pl.ds(0, 3 * hc)], precv.at[n], spr.at[0], rpr.at[n], at.pb)

    def project(g, first, size):
        def done(col, step, out):
            for i, (r, j) in enumerate(GROUPS[g]):
                part[r * NJ + j, :, pl.ds(al(first + col, 128), step)] = out[i * ch : (i + 1) * ch].astype(BF16)

        refs = [xg.at[gather.seqs[r], j] for r, j in GROUPS[g]]
        product(refs, wb.at[:, pl.ds(first, size)], wb.shape[0], size, done)

    split = {step[1] for step in ATTENTION_STEPS if step[0] == "Q"}

    def G(g):
        w_ready(0)
        for r, j in GROUPS[g]:
            gather.chunk_wait(r, j)
        if g in split:
            project(g, 0, 3 * hc)
        else:
            w_ready(1)
            project(g, 0, 6 * hc)
        for r, j in GROUPS[g]:
            pr_copy(r * NJ + j).start()

    def Q(g):
        w_ready(1)
        project(g, 3 * hc, 3 * hc)

    def kv_copy(r, j):
        s, n = gather.seqs[r], r * NJ + j
        return remote(kvo.at[s, j], kvp.at[s, j], skv.at[0], rkv.at[n], at.partner)

    def rotate(r, j):
        s, n = gather.seqs[r], r * NJ + j
        pr_copy(n).wait_recv()
        cos_t, sin_t = cos_all[j], sin_all[j]

        def total(col, size):
            mine = part[n, :, 3 * hc + col : 3 * hc + col + size]
            return (mine.astype(F32) + precv[n, :, col : col + size].astype(F32)).astype(BF16)

        def turned(col):
            v = total(col, HEAD_DIM).astype(F32)
            return (v * cos_t + pltpu.roll(v, HEAD_DIM // 2, axis=1) * sin_t).astype(BF16)

        for col in range(0, hc, HEAD_DIM):
            qb[n, :, col : col + HEAD_DIM] = turned(col)
            kvo[s, j, :, col : col + HEAD_DIM] = turned(hc + col)
        kvo[s, j, :, hc:] = total(2 * hc, hc)
        kv_copy(r, j).start()

    def R(g):
        for r, j in GROUPS[g]:
            rotate(r, j)

    def o_cols(xx):
        return pl.ds(al((2 * rem(div(xx + 1, 2), 2) + div(xx, 2)) * hc, 128), hc)

    cut = ch // 8

    def og_copy(kind, n):
        if kind < 2:
            ref = og.at[n, :, o_cols(x)]
        elif kind == 2:
            ref = og.at[n, pl.ds(0, cut), o_cols(at.xa)]
        else:
            ref = og.at[n, pl.ds(cut, ch - cut), o_cols(at.xb)]
        return remote(ref, ref, sog.at[kind], rog.at[kind, n], at.pa if kind in (0, 3) else at.pb)

    def og_wait(kind, n):
        xx = (at.xa, at.xb, at.xo, at.xo)[kind]
        rows = (pl.ds(0, ch), pl.ds(0, ch), pl.ds(0, cut), pl.ds(cut, ch - cut))[kind]
        dst = og.at[n, rows, o_cols(xx)]
        remote(dst, dst, sog.at[kind], rog.at[kind, n], at.pa).wait_recv()

    def attend(r, j, i):
        s, n = gather.seqs[r], r * NJ + j
        keys = (j + 1) * ch
        iq = lax.broadcasted_iota(jnp.int32, (ch, keys), 0) + j * ch
        ik = lax.broadcasted_iota(jnp.int32, (ch, keys), 1)
        own_ok = iq >= ik
        par_ok = ik < (j + c) * ch
        contract = (((1,), (1,)), ((), ()))
        cols = pl.ds(al(i * HEAD_DIM, 128), HEAD_DIM)
        v_cols = pl.ds(al(hc + i * HEAD_DIM, 128), HEAD_DIM)
        q = qb[n, :, cols]
        k_own = kvo[s, 0 : j + 1, :, cols].reshape(keys, HEAD_DIM)
        k_par = kvp[s, 0 : j + 1, :, cols].reshape(keys, HEAD_DIM)
        s_own = lax.dot_general(q, k_own, contract, preferred_element_type=F32) * HEAD_DIM**-0.5
        s_par = lax.dot_general(q, k_par, contract, preferred_element_type=F32) * HEAD_DIM**-0.5
        s_own = jnp.where(own_ok, s_own, -1e30)
        s_par = jnp.where(par_ok, s_par, -1e30)
        top = jnp.maximum(jnp.max(s_own, axis=1, keepdims=True), jnp.max(s_par, axis=1, keepdims=True))
        e_own, e_par = jnp.exp(s_own - top), jnp.exp(s_par - top)
        inv = 1.0 / (jnp.sum(e_own, axis=1, keepdims=True) + jnp.sum(e_par, axis=1, keepdims=True))
        v_own = kvo[s, 0 : j + 1, :, v_cols].reshape(keys, HEAD_DIM)
        v_par = kvp[s, 0 : j + 1, :, v_cols].reshape(keys, HEAD_DIM)
        out = jnp.dot((e_own * inv).astype(BF16), v_own, preferred_element_type=F32)
        out += jnp.dot((e_par * inv).astype(BF16), v_par, preferred_element_type=F32)
        og[n, :, pl.ds(al((2 * ng + kh) * hc + i * HEAD_DIM, 128), HEAD_DIM)] = out.astype(BF16)

    def A(g):
        for r, j in GROUPS[g]:
            kv_copy(r, j).wait_recv()

        def head(i, carry):
            for r, j in GROUPS[g]:
                attend(r, j, i)
            return carry

        lax.fori_loop(0, hc // HEAD_DIM, head, 0)
        for r, j in GROUPS[g]:
            og_copy(0, r * NJ + j).start()
            og_copy(1, r * NJ + j).start()

    def P(g):
        for r, j in GROUPS[g]:
            for kind in range(2):
                og_wait(kind, r * NJ + j)
                og_copy(kind + 2, r * NJ + j).start()

    def X(g):
        for r, j in GROUPS[g]:
            og_wait(2, r * NJ + j)
            og_wait(3, r * NJ + j)

        def done(col, size, out):
            for i, (r, j) in enumerate(GROUPS[g]):
                zb[r, j, :, pl.ds(al(col, 128), size)] = out[i * ch : (i + 1) * ch].astype(BF16)

        product([og.at[r * NJ + j] for r, j in GROUPS[g]], wob, wob.shape[0], kc, done)
        for r, j in GROUPS[g]:
            if r == 2:
                reduce.halves(j)

    def T(j):
        attn = reduce.total(j).astype(BF16)
        h_ref[j] = (xc[j].astype(F32) + attn.astype(F32)).astype(BF16)
        chunk_out(j).start()

    def chunk_out(j):
        return pltpu.make_async_copy(h_ref.at[j], h_hbm.at[j], lx.at[1 + j])

    def h_out(r, u):
        rows = pl.ds(u * (ch // 2), ch // 2)
        return pltpu.make_async_copy(hg.at[ahead.seqs[r], 0, rows], hg_all.at[ahead.seqs[r], rows], lh.at[r, u])

    kept = []

    def HF(u):
        if not kept:
            kept.append(u)
            ahead.keep_own()
        ahead.XF(0, u)

    def HY(u):
        ahead.YH(u)
        for r in (0, 1, 3):
            h_out(r, u).start()

    def HO(u):
        for d in range(2):
            ahead.yhalf_wait(d, u)
        h_out(2, u).start()

    def own_rows():
        for half, i in pieces:
            w_local(half, i).start()
        o_local.start()
        for m in range(2):
            d_in(m).start()
        x_in.wait()
        for j in range(NJ):
            xc[j, :, half_cols(c)] = x_ref[x_rows(j, c), :]

    x_in = pltpu.make_async_copy(x_hbm, x_ref, lx.at[0])
    x_in.start()
    tables = [pltpu.make_async_copy(src, dst, lx.at[1 + NJ + i]) for i, (src, dst) in enumerate(((turn_hbm, turn_ref), (base_hbm, base_ref)))]
    for copy in tables:
        copy.start()
    at.barrier(own_rows)

    def angles():
        for copy in tables:
            copy.wait()
        lane = lax.broadcasted_iota(jnp.int32, (ch, HEAD_DIM), 1)
        for j in range(NJ):
            base_cos, base_sin = base_ref[0, pl.ds(2 * j + c, 1), :], base_ref[1, pl.ds(2 * j + c, 1), :]
            cos_all[j] = base_cos * turn_ref[0] - base_sin * turn_ref[1]
            sine = base_sin * turn_ref[0] + base_cos * turn_ref[1]
            sin_all[j] = jnp.where(lane < HEAD_DIM // 2, -sine, sine)

    ops = {
        "XP": XP, "WOP": WOP, "XE": XE, "ST": ST, "N": N, "YH": gather.YH, "WA": WA, "WP": WP, "S": S, "O": O, "F": F, "DP": DP,
        "G": G, "Q": Q, "R": R, "A": A, "P": P, "X": X, "M": reduce.middle, "T": T,
        "HF": HF, "HH": lambda u: ahead.XH(0, u), "HN": lambda u: ahead.N(0, u), "HY": HY, "HO": HO,
    }
    def sent():
        for m in range(2):
            for k in range(4):
                d_pair(m, k, 1 - c).wait_recv()
                d_pair(m, k, c).wait_send()
            d_out(m).wait()
            for d in range(2):
                for p in range(2):
                    s_copy(d, m, p, x).wait_send()
                o_copy(d, m).wait_send()
                f_copy(d, m, x).wait_send()
        for j in range(NJ):
            x_pair(j).wait_send()
        for u in range(len(units)):
            xe_copy(u, x).wait_send()
            st_copy(u).wait_send()
            for d in range(2):
                gather.ycopy(d, u).wait_send()
                gather.yhalf(d, u).wait_send()
        reduce.drain()
        ahead.drain()
        for r in range(NX):
            for u in range(2):
                h_out(r, u).wait()
        o_pair.wait_send()
        for half, i in pieces:
            wa_copy(half, i, x).wait_send()
            wo_copy(half, i, c).wait_send()
        for half in range(2):
            wp_copy(half, c).wait_send()

        every = part.at[:, :, pl.ds(0, 3 * hc)]
        remote(every, precv, spr.at[0], rpr.at[0], at.pb).wait_send()
        remote(kvo, kvp, skv.at[0], rkv.at[0], at.partner).wait_send()
        for kind, (lo, n) in enumerate(((0, ch), (0, ch), (0, cut), (cut, ch - cut))):
            every = og.at[:, pl.ds(lo, n), o_cols(x)]
            remote(every, every, sog.at[kind], rog.at[kind, 0], at.pa).wait_send()

    waits = {"X": o_ready, "WP": angles}
    last = max(i for i, step in enumerate(ATTENTION_STEPS) if step[0] == "X")
    for i, step in enumerate(ATTENTION_STEPS):
        if step[0] in waits:
            waits.pop(step[0])()
        if i == last:
            sent()
        ops[step[0]](*step[1:])
    for j in range(NJ):
        chunk_out(j).wait()


def mlp_kernel(
    units, h_hbm, w_hbm, wdn, hg_hbm, y_ref,
    h_ref, xg, wt, raw, wd, ag, ar, act, s1, s2, zb, ya, yb, yfd, yfu, yst,
    sx, rx, sy, ry, syh, ryh, sa, ra, syr, ryr, sd, rd, lw, lwd, swd, rwd, lh, lo,
):
    at = Place()
    x, c, y = at.x, at.c, at.y
    ch, kc, h = h_ref.shape[1], h_ref.shape[2], h_ref.shape[1] // 2
    width = xg.shape[-1]
    kd = kc // 2
    fc, tiles = w_hbm.shape[1], wt.shape[1] // 256
    fm = (tiles - 1) * 128
    fr = fc - fm
    blocks, slots = 2 * tiles, raw.shape[0]
    gather = Spread(at, h_ref, xg, units, (s1, s2), sx, rx, sy, ry, syh, ryh)
    reduce = Reduce(at, zb, ya, yb, yfd, yfu, syr, ryr)

    def w_in(q):
        i, m = q // 2, q % 2
        n = min(128, fc - i * 128)
        return pltpu.make_async_copy(w_hbm.at[m, pl.ds(i * 128, n)], raw.at[q % slots, pl.ds(0, n)], lw.at[q])

    def WT(g):
        for q in range(g * blocks // 4, (g + 1) * blocks // 4):
            i, m, slot = q // 2, q % 2, q % slots
            w_in(q).wait()
            if fc < (i + 1) * 128:
                raw[slot, fc - i * 128 :, :] = jnp.zeros(((i + 1) * 128 - fc, width), BF16)

            def turn(k, carry, slot=slot, q=q):
                part = pl.ds(al(k * (width // 4), 128), width // 4)
                wt[part, q * 128 : (q + 1) * 128] = raw[slot, :, part].T
                return carry

            lax.fori_loop(0, 4, turn, 0)
            if q + slots < blocks:
                w_in(q + slots).start()

    def d_refs(q, core):
        cols = pl.ds(al(core * kd, 128), kd)
        main, rest = wdn.at[pl.ds(q * fc, fm)], wdn.at[pl.ds(q * fc + fm, fr)]
        return (main, wd.at[pl.ds(q * fm, fm), cols]), (rest, wd.at[pl.ds(NX * fm + q * 128, fr), cols])

    def d_own(q, k):
        src, dst = d_refs(q, c)[k]
        return pltpu.make_async_copy(src, dst, lwd.at[q, k])

    def d_pair(q, k, core):
        src, dst = d_refs(q, core)[k]
        return remote(src, dst, swd.at[q, k], rwd.at[q, k], at.partner)

    quarters = [(q, k) for q in range(NX) for k in range(2)]
    h_in_all = pltpu.make_async_copy(h_hbm, h_ref, lo.at[NJ])
    h_in_all.start()
    for q in range(slots):
        w_in(q).start()
    def h_in(s):
        return pltpu.make_async_copy(hg_hbm.at[s], xg.at[s, 0], lh.at[s])

    for s in range(NX):
        h_in(s).start()
    for q, k in quarters:
        d_own(q, k).start()
    for q in range(NX):
        wd[NX * fm + q * 128 + fr : NX * fm + (q + 1) * 128, :] = jnp.zeros((128 - fr, kc), BF16)
    at.barrier(h_in_all.wait)
    for q, k in quarters:
        d_pair(q, k, c).start()

    def a_refs(kind, n, xx):
        main, rest = pl.ds(al(xx * fm, 128), fm), pl.ds(al(xx * 128, 128), 128)
        if kind < 2:
            return ag.at[n, :, main], ar.at[n, :, rest]
        lo = (kind - 2) * h
        return ag.at[n, pl.ds(lo, h), main], ar.at[n, pl.ds(lo // 2, h // 2), rest]

    def a_copies(kind, n):
        refs = a_refs(kind, n, (x, x, at.xl, at.xr)[kind])
        return [remote(v, v, sa.at[kind, k], ra.at[kind, n, k], at.left if kind % 2 else at.right) for k, v in enumerate(refs)]

    def a_wait(kind, n):
        for k, v in enumerate(a_refs(kind, n, (at.xl, at.xr, at.xo, at.xo)[kind])):
            remote(v, v, sa.at[kind, k], ra.at[kind, n, k], at.right).wait_recv()

    def a_start(kind, n):
        for copy in a_copies(kind, n):
            copy.start()

    def G(g):
        for r, j in GROUPS[g]:
            gather.chunk_wait(r, j)

        def done(col, size, out):
            for k in range(0, size, 256):
                gate, up = out[:, k : k + 128].astype(BF16).astype(F32), out[:, k + 128 : k + 256].astype(BF16).astype(F32)
                value = (gate / (1.0 + jnp.exp(-gate)) * up).astype(BF16)
                act[0 : value.shape[0], pl.ds(al(div(col + k, 2), 128), 128)] = value

        product([xg.at[gather.seqs[r], j] for r, j in GROUPS[g]], wt, width, wt.shape[1], done)
        for i, (r, j) in enumerate(GROUPS[g]):
            n, lo = r * NJ + j, i * ch
            ag[n, :, pl.ds(al(x * fm, 128), fm)] = act[lo : lo + ch, :fm]
            below = pltpu.roll(act[lo + h : lo + ch, fm:].astype(F32), 64, axis=1)
            ar[n, :, pl.ds(al(x * 128, 128), 128)] = (act[lo : lo + h, fm:].astype(F32) + below).astype(BF16)
            for kind in range(2):
                a_start(kind, n)

    def P(g):
        for r, j in GROUPS[g]:
            for kind in range(2):
                a_wait(kind, r * NJ + j)
                a_start(kind + 2, r * NJ + j)

    def X(g):
        for r, j in GROUPS[g]:
            n = r * NJ + j
            for kind in (2, 3):
                a_wait(kind, n)
            for q in range(NX):
                cols = pl.ds(NX * fm + q * 128, 128)
                rest = ar[n, :, q * 128 : (q + 1) * 128]
                ag[n, 0:h, cols] = rest
                ag[n, h:, cols] = pltpu.roll(rest.astype(F32), 64, axis=1).astype(BF16)

        def done(col, size, out):
            for i, (r, j) in enumerate(GROUPS[g]):
                zb[r, j, :, pl.ds(al(col, 128), size)] = out[i * ch : (i + 1) * ch].astype(BF16)

        product([ag.at[r * NJ + j] for r, j in GROUPS[g]], wd, wd.shape[0], kc, done)
        for r, j in GROUPS[g]:
            if r == 2:
                reduce.halves(j)

    def y_rows(j, core):
        return pl.ds(al((2 * j + core) * ch, 8), ch)

    def y_copy(j):
        return remote(yst.at[1 - c, j], y_ref.at[y_rows(j, c)], sd.at[j], rd.at[j], at.partner)

    def y_own(j):
        return pltpu.make_async_copy(yst.at[c, j], y_ref.at[y_rows(j, c)], lo.at[j])

    def y_wait(j):
        dst = y_ref.at[y_rows(j, 1 - c)]
        remote(dst, dst, sd.at[j], rd.at[j], at.partner).wait_recv()

    def T(j):
        mlp = reduce.total(j).astype(BF16)
        out = (h_ref[j].astype(F32) + mlp.astype(F32)).astype(BF16)
        yst[0, j] = out[:, :kd]
        yst[1, j] = out[:, kd:]
        y_copy(j).start()
        y_own(j).start()

    ops = {"G": G, "P": P, "X": X, "M": reduce.middle, "T": T, "WT": WT}
    for name in ("YR", "YRH", "YH", "XF", "XH", "N"):
        ops[name] = getattr(gather, name)
    waits = {
        "N": gather.keep_own,
        "G": lambda: [h_in(s).wait() for s in range(NX)],
        "X": lambda: [(d_own(q, k).wait(), d_pair(q, k, 1 - c).wait_recv()) for q, k in quarters],
    }
    def sent():
        gather.drain()
        reduce.drain()
        for q, k in quarters:
            d_pair(q, k, c).wait_send()

        for kind in range(4):
            for k, every in enumerate(a_refs(kind, slice(None), x)):
                remote(every, every, sa.at[kind, k], ra.at[kind, 0, k], at.right).wait_send()

    for step in MLP_STEPS:
        if step[0] in waits:
            waits.pop(step[0])()
        ops[step[0]](*step[1:])
    sent()
    for j in range(NJ):
        y_copy(j).wait_send()
        y_own(j).wait()
        y_wait(j)


def vmem(*shape, dtype=BF16):
    return pltpu.VMEM(shape, dtype)


def sems(*shape):
    return pltpu.SemaphoreType.DMA(shape)


def solution(mesh):
    assert mesh.shape["tx"] == 2 * NX and mesh.shape["ty"] == NX
    act_spec = P(("dp", "ty"), None, "tx")
    col_spec = P("tx", "ty")
    row_spec = P("ty", "tx")
    any_spec = pl.BlockSpec(memory_space=pl.ANY)
    vmem_spec = pl.BlockSpec(memory_space=pltpu.VMEM)

    def layer(x_blk, w_q, w_k, w_v, w_o, w_gate, w_up, w_down):
        _, seq, kd = x_blk.shape
        kc, width = 2 * kd, 2 * NX * kd
        ch = seq // (2 * NJ)
        h = ch // 2
        row_heads = w_q.shape[1]
        hc = row_heads // NX
        fc = w_down.shape[0] // NX
        assert hc % HEAD_DIM == 0
        tiles = (fc + 127) // 128
        f_a = (fc // 2 + 15) // 16 * 16

        inv_freq = THETA ** (-2.0 * np.arange(HEAD_DIM // 2) / HEAD_DIM)
        inv_freq = np.concatenate([inv_freq, inv_freq])
        turn = np.arange(ch)[:, None] * inv_freq
        base = np.arange(2 * NJ)[:, None] * ch * inv_freq
        turn = jnp.asarray(np.stack([np.cos(turn), np.sin(turn)]), F32)
        base = jnp.asarray(np.stack([np.cos(base), np.sin(base)]), F32)

        reduce_scratch = [vmem(NX, NJ, ch, kc), vmem(NJ, h, kc), vmem(NJ, ch - h, kc), vmem(NJ, ch, kc), vmem(NJ, ch, kc)]
        units = ((0, 0, h, 0), (0, h, h, 0)) + tuple((j, 0, ch, 0) for j in range(1, NJ))
        n_u = len(units)
        h_blk, w_all, hg_all = pl.pallas_call(
            functools.partial(attention_kernel, units),
            out_shape=(
                jax.ShapeDtypeStruct((NJ, ch, kc), BF16),
                jax.ShapeDtypeStruct((2, fc, width), BF16),
                jax.ShapeDtypeStruct((NX, ch, width), BF16),
            ),
            in_specs=[any_spec] * 9,
            out_specs=(any_spec, any_spec, any_spec),
            scratch_shapes=[
                vmem(seq, kd), vmem(2, ch, HEAD_DIM, dtype=F32), vmem(2, 2 * NJ, HEAD_DIM, dtype=F32),
                vmem(NJ, ch, kc), vmem(NJ, ch, kc), vmem(NX, NJ, ch, 2 * kc), vmem(NX, 1, ch, width), vmem(NJ, ch, HEAD_DIM, dtype=F32), vmem(NJ, ch, HEAD_DIM, dtype=F32),
                vmem(NJ, ch // 4, 128, dtype=F32), vmem(NJ, ch // 4, 128, dtype=F32), vmem(ch, 128, dtype=F32), vmem(ch, 128, dtype=F32),
                vmem(2 * kc, 6 * hc), vmem(row_heads, kc), vmem(NCH, ch, 6 * hc), vmem(NCH, ch, 3 * hc), vmem(NCH, ch, hc),
                vmem(NX, NJ, ch, 2 * hc), vmem(NX, NJ, ch, 2 * hc), vmem(NCH, ch, row_heads), *reduce_scratch,
                vmem(2, fc, kd), vmem(2, f_a, kd), vmem(2, fc - f_a, kd),
                sems(n_u), sems(n_u), sems(n_u), sems(n_u), sems(2, n_u), sems(2, n_u), sems(2, n_u), sems(2, n_u),
                sems(NJ), sems(NJ), sems(2, 3), sems(2, 3), sems(2, 3), sems(2, 3), sems(2), sems(2), sems(3, 3), sems(1), sems(1),
                sems(1), sems(NCH), sems(1), sems(NCH), sems(4), sems(4, NCH), sems(4, NJ), sems(4, NJ),
                sems(2, 2), sems(2, 2, 2), sems(2, 2, 2), sems(2, 2), sems(2, 2), sems(2, 2), sems(2, 2), sems(2, 4), sems(2, 4),
                sems(4, 2), sems(4, 2), sems(2, 2), sems(2, 2), sems(2, 2), sems(2, 2), sems(NX, 2), sems(3 + NJ),
            ],
            compiler_params=pltpu.CompilerParams(collective_id=0, has_side_effects=True, vmem_limit_bytes=VMEM_LIMIT),
            name="attention_part",
        )(x_blk[0], turn, base, w_q, w_k, w_v, w_o, w_gate.T, w_up.T)

        units = ((1, 0, h, 1), (1, h, h, 0)) + tuple((j, 0, ch, 0) for j in range(2, NJ))
        n_u, n_x = len(units), len(units) + 3
        y_blk = pl.pallas_call(
            functools.partial(mlp_kernel, units),
            out_shape=jax.ShapeDtypeStruct((seq, kd), BF16),
            in_specs=[any_spec] * 4,
            out_specs=any_spec,
            scratch_shapes=[
                vmem(NJ, ch, kc),
                vmem(NX, NJ, ch, width), vmem(width, tiles * 256), vmem(3, 128, width),
                vmem(NX * tiles * 128, kc), vmem(NCH, ch, NX * tiles * 128), vmem(NCH, h, NX * 128), vmem(2 * ch, tiles * 128),
                vmem(ch, 128, dtype=F32), vmem(ch, 128, dtype=F32),
                *reduce_scratch, vmem(2, NJ, ch, kd),
                sems(4, n_x), sems(4, n_x), sems(2, n_u), sems(2, n_u), sems(2, n_u), sems(2, n_u),
                sems(4, 2), sems(4, NCH, 2), sems(4, NJ), sems(4, NJ), sems(NJ), sems(NJ),
                sems(2 * tiles), sems(NX, 2), sems(NX, 2), sems(NX, 2), sems(NX), sems(NJ + 1),
            ],
            compiler_params=pltpu.CompilerParams(collective_id=1, has_side_effects=True, vmem_limit_bytes=VMEM_LIMIT),
            name="mlp_part",
        )(h_blk, w_all, w_down, hg_all)
        return y_blk[None]

    return jax.shard_map(
        layer,
        mesh=mesh,
        in_specs=(act_spec, col_spec, col_spec, col_spec, row_spec, col_spec, col_spec, row_spec),
        out_specs=act_spec,
        check_vma=False,
    )
```

```python
import functools

import jax
import jax.numpy as jnp
import numpy as np
from jax import lax
from jax.experimental import pallas as pl
from jax.experimental.pallas import tpu as pltpu
from jax.sharding import PartitionSpec as P

HEAD_DIM = 128
EPS = 1e-5
THETA = 10000.0
MESH = pl.DeviceIdType.MESH
F32 = jnp.float32
BF16 = jnp.bfloat16
NX = 4
NJ = 4
NCH = 16
VMEM_LIMIT = 67_043_328
GROUPS = (*(((0, j),) for j in range(NJ)), *(((3, j), (1, j)) for j in range(NJ)), *(((2, j),) for j in range(NJ)))


def rem(a, b):
    return lax.rem(a, jnp.int32(b))


def div(a, b):
    return lax.div(a, jnp.int32(b))


def al(v, m):
    return pl.multiple_of(v, m)


def remote(src, dst, ssem, rsem, dev):
    return pltpu.make_async_remote_copy(src_ref=src, dst_ref=dst, send_sem=ssem, recv_sem=rsem, device_id=dev, device_id_type=MESH)


ATTENTION_STEPS = (
    ("WA", 0), ("XP", 1), ("S", "b", 0, 1), ("XP", 0), ("XE", 1), ("XE", 0), ("XE", 2), ("XP", 2), ("S", "b", 0, 0), ("XP", 3),
    ("S", "b", 1, 0), ("ST", 1), ("WP", 0), ("WA", 1), ("O", "b", 1), ("ST", 0), ("N", 1), ("O", "b", 0), ("ST", 2),
    ("S", "b", 1, 1), ("WOP",), ("N", 0), ("G", 0), ("XE", 3), ("YH", 1), ("YH", 0), ("S", "a", 0, 1), ("N", 2), ("WP", 1),
    ("G", 8), ("G", 4), ("ST", 3), ("Q", 8), ("Q", 0), ("R", 8), ("XE", 4), ("A", 8), ("F", "a", 1), ("YH", 2), ("G", 5),
    ("R", 4), ("ST", 4), ("N", 3), ("P", 8), ("G", 9), ("A", 4), ("R", 0), ("S", "a", 1, 1), ("X", 8), ("G", 1), ("N", 4),
    ("R", 5), ("A", 0), ("R", 9), ("P", 4), ("A", 9), ("A", 5), ("G", 2), ("P", 0), ("X", 4), ("M", 0), ("P", 9),
    ("S", "a", 1, 0), ("YH", 3), ("G", 6), ("P", 5), ("X", 0), ("T", 0), ("HF", 1), ("HF", 0), ("R", 2), ("X", 9), ("R", 1),
    ("A", 1), ("YH", 4), ("X", 5), ("M", 1), ("HH", 1), ("O", "a", 0), ("G", 10), ("R", 6), ("HH", 0), ("G", 7), ("O", "a", 1),
    ("HN", 1), ("R", 10), ("G", 11), ("A", 10), ("A", 6), ("HN", 0), ("R", 7), ("A", 2), ("HY", 1), ("A", 7), ("R", 11),
    ("P", 10), ("A", 11), ("P", 6), ("G", 3), ("P", 7), ("P", 11), ("F", "b", 1), ("F", "a", 0), ("X", 10), ("HY", 0),
    ("S", "a", 0, 0), ("F", "b", 0), ("R", 3), ("X", 11), ("A", 3), ("X", 6), ("HO", 1), ("X", 7), ("P", 1), ("P", 2),
    ("M", 2), ("M", 3), ("DP", 1), ("DP", 0), ("P", 3), ("HO", 0), ("X", 1), ("T", 1), ("X", 2), ("T", 2), ("X", 3), ("T", 3),
)
MLP_STEPS = (
    ("XF", 0, 1), ("YR", 0), ("WT", 0), ("XF", 0, 0), ("XH", 0, 1), ("XF", 0, 3), ("YRH", 0), ("XF", 2, 0), ("N", 0, 1),
    ("WT", 1), ("WT", 2), ("XH", 0, 3), ("XF", 0, 2), ("WT", 3), ("XF", 1, 0), ("XF", 3, 0), ("N", 0, 3), ("G", 8), ("YH", 1),
    ("XH", 2, 0), ("G", 4), ("P", 8), ("XH", 3, 0), ("XH", 0, 0), ("XH", 0, 2), ("G", 3), ("XH", 1, 0), ("YH", 3), ("G", 7),
    ("N", 2, 0), ("N", 0, 0), ("G", 9), ("N", 0, 2), ("P", 7), ("G", 11), ("P", 4), ("P", 9), ("N", 1, 0), ("N", 3, 0),
    ("G", 5), ("X", 8), ("G", 1), ("X", 4), ("YH", 2), ("P", 11), ("G", 6), ("X", 9), ("X", 7), ("X", 11), ("P", 5), ("M", 0),
    ("G", 10), ("G", 0), ("M", 3), ("X", 5), ("P", 10), ("P", 3), ("M", 1), ("P", 6), ("G", 2), ("P", 1), ("X", 10), ("X", 3),
    ("P", 0), ("X", 6), ("M", 2), ("T", 3), ("P", 2), ("X", 1), ("T", 1), ("X", 0), ("T", 0), ("X", 2), ("T", 2),
)


class Place:
    def __init__(self):
        tx, ty = lax.axis_index("tx"), lax.axis_index("ty")
        self.x, self.c, self.y = div(tx, 2), rem(tx, 2), ty
        x, c, y = self.x, self.c, self.y
        self.xr, self.xl, self.xo = rem(x + 1, NX), rem(x + 3, NX), rem(x + 2, NX)
        self.yu, self.yd, self.yo = rem(y + 1, NX), rem(y + 3, NX), rem(y + 2, NX)
        self.right = {"tx": self.xr * 2 + c, "ty": y}
        self.left = {"tx": self.xl * 2 + c, "ty": y}
        self.up = {"tx": tx, "ty": self.yu}
        self.down = {"tx": tx, "ty": self.yd}
        self.partner = {"tx": x * 2 + 1 - c, "ty": y}
        self.xa, self.xb = x + 1 - 2 * rem(x, 2), rem(x + 3 + 2 * rem(x, 2), NX)
        self.pa, self.pb = {"tx": self.xa * 2 + c, "ty": y}, {"tx": self.xb * 2 + c, "ty": y}

    def barrier(self, between):
        sem = pltpu.get_barrier_semaphore()
        for dev in (self.right, self.left, self.up, self.down, self.partner):
            pl.semaphore_signal(sem, inc=1, device_id=dev, device_id_type=MESH)
        between()
        pl.semaphore_wait(sem, 5)


class Spread:
    def __init__(self, at, src, xg, units, sums, sx, rx, sy, ry, syh, ryh):
        self.sums = sums
        self.at, self.src, self.xg, self.units, self.kc = at, src, xg, units, src.shape[2]
        self.sx, self.rx, self.sy, self.ry, self.syh, self.ryh = sx, rx, sy, ry, syh, ryh
        pairs = [(r, u) for u, unit in enumerate(units) for r in ((0, 3, 1, 2) if unit[3] else (0,))]
        self.index = {pair: i for i, pair in enumerate(pairs)}
        self.seqs = (at.y, at.yu, at.yo, at.yd)

    def cols(self, x):
        return pl.ds(al(x * self.kc, 128), self.kc)

    def keep_own(self):
        for j in {unit[0]: 0 for unit in self.units}:
            self.xg[self.at.y, j, :, self.cols(self.at.x)] = self.src[j]

    def xcopy(self, kind, r, u):
        at, s = self.at, self.seqs[r]
        j, lo, n, _ = self.units[u]
        i = self.index[r, u]
        if kind < 2:
            dst = self.xg.at[s, j, pl.ds(lo, n), self.cols(at.x)]
            src = self.src.at[j, pl.ds(lo, n)] if r == 0 else dst
        elif kind == 2:
            src = dst = self.xg.at[s, j, pl.ds(lo, n // 2), self.cols(at.xl)]
        else:
            src = dst = self.xg.at[s, j, pl.ds(lo + n // 2, n // 2), self.cols(at.xr)]
        return remote(src, dst, self.sx.at[kind, i], self.rx.at[kind, i], at.left if kind % 2 else at.right)

    def xwait(self, kind, r, u):
        at = self.at
        j, lo, n, _ = self.units[u]
        i = self.index[r, u]
        x = (at.xl, at.xr, at.xo, at.xo)[kind]
        rows = (pl.ds(lo, n), pl.ds(lo, n), pl.ds(lo, n // 2), pl.ds(lo + n // 2, n // 2))[kind]
        dst = self.xg.at[self.seqs[r], j, rows, self.cols(x)]
        remote(dst, dst, self.sx.at[kind, i], self.rx.at[kind, i], at.right).wait_recv()

    def yref(self, s, u, lo, n):
        j, _, _, first = self.units[u]
        rows = pl.ds(lo, n)
        return self.xg.at[s, j, rows, self.cols(self.at.x)] if first else self.xg.at[s, j, rows]

    def ycopy(self, d, u):
        j, lo, n, first = self.units[u]
        dst = self.yref(self.at.y, u, lo, n)
        src = self.src.at[j, pl.ds(lo, n)] if first else dst
        return remote(src, dst, self.sy.at[d, u], self.ry.at[d, u], self.at.down if d else self.at.up)

    def ywait(self, d, u):
        _, lo, n, _ = self.units[u]
        dst = self.yref(self.at.yu if d else self.at.yd, u, lo, n)
        remote(dst, dst, self.sy.at[d, u], self.ry.at[d, u], self.at.up).wait_recv()

    def yhalf(self, d, u):
        _, lo, n, _ = self.units[u]
        ref = self.yref(self.at.yu if d else self.at.yd, u, lo + d * (n // 2), n // 2)
        return remote(ref, ref, self.syh.at[d, u], self.ryh.at[d, u], self.at.down if d else self.at.up)

    def yhalf_wait(self, d, u):
        _, lo, n, _ = self.units[u]
        dst = self.yref(self.at.yo, u, lo + d * (n // 2), n // 2)
        remote(dst, dst, self.syh.at[d, u], self.ryh.at[d, u], self.at.up).wait_recv()

    def YR(self, u):
        for d in range(2):
            self.ycopy(d, u).start()

    def YH(self, u):
        for d in range(2):
            self.ywait(d, u)
            self.yhalf(d, u).start()

    YRH = YH

    def XF(self, r, u):
        if r == 2:
            for d in range(2):
                self.yhalf_wait(d, u)
        for kind in range(2):
            self.xcopy(kind, r, u).start()

    def XH(self, r, u):
        for kind in range(2):
            self.xwait(kind, r, u)
            self.xcopy(kind + 2, r, u).start()

    def N(self, r, u):
        j, lo, n, first = self.units[u]
        for kind in (2, 3):
            self.xwait(kind, r, u)
            self.xcopy(kind, r, u).wait_send()
        if r:
            for kind in range(2):
                self.xcopy(kind, r, u).wait_send()
        if r % 2:
            self.yhalf(0 if r == 3 else 1, u).wait_send()
        width, ref = self.xg.shape[-1], self.xg.at[self.seqs[r], j]
        s1, s2 = self.sums
        lane_sums(ref, lo, n, s1, s2)
        mean = jnp.sum(s1[0:n, :], axis=-1, keepdims=True) / width
        var = jnp.sum(s2[0:n, :], axis=-1, keepdims=True) / width - mean * mean
        s1[0:n, :] = jnp.broadcast_to(mean, (n, 128))
        s2[0:n, :] = jnp.broadcast_to(lax.rsqrt(var + EPS), (n, 128))
        scale_rows(ref, lo, n, s1, s2)
        if not first:
            self.YR(u)

    def chunk_wait(self, r, j):
        if r == 2:
            for u, unit in enumerate(self.units):
                if unit[0] == j and not unit[3]:
                    for d in range(2):
                        self.yhalf_wait(d, u)

    def drain(self):
        for u, unit in enumerate(self.units):
            for d in range(2):
                self.xcopy(d, 0, u).wait_send()
                self.ycopy(d, u).wait_send()
                if not unit[3]:
                    self.yhalf(d, u).wait_send()


def rows_of(refs):
    return refs[0][...] if len(refs) == 1 else jnp.concatenate([ref[...] for ref in refs], axis=0)


def product(refs, weight, depth, n_cols, done):
    step = 256

    def columns(i, carry):
        out = jnp.dot(rows_of(refs), weight[0:depth, pl.ds(al(i * step, 128), step)], preferred_element_type=F32)
        done(i * step, step, out)
        return carry

    lax.fori_loop(0, n_cols // step, columns, 0)


def lane_sums(ref, lo, n, s1, s2):
    width, rows, wide = ref.shape[-1], 32, 512

    def some_rows(i, carry):
        def some_columns(k, sums):
            a, b = sums
            v = ref[pl.ds(al(lo + i * rows, 8), rows), pl.ds(al(k * wide, 128), wide)].astype(F32)
            for c in range(0, wide, 128):
                part = v[:, c : c + 128]
                a, b = a + part, b + part * part
            return a, b

        zero = jnp.zeros((rows, 128), F32)
        a, b = lax.fori_loop(0, width // wide, some_columns, (zero, zero))
        s1[pl.ds(al(i * rows, 8), rows), :] = a
        s2[pl.ds(al(i * rows, 8), rows), :] = b
        return carry

    lax.fori_loop(0, n // rows, some_rows, 0)


def scale_rows(ref, lo, n, means, scales):
    width, rows, wide = ref.shape[-1], 32, 512

    def some_rows(i, carry):
        mean, scale = (t[pl.ds(al(i * rows, 8), rows), :] for t in (means, scales))

        def some_columns(k, carry):
            at_rows = pl.ds(al(lo + i * rows, 8), rows)
            for c in range(0, wide, 128):
                cols = pl.ds(al(k * wide + c, 128), 128)
                ref[at_rows, cols] = ((ref[at_rows, cols].astype(F32) - mean) * scale).astype(BF16)
            return carry

        lax.fori_loop(0, width // wide, some_columns, 0)
        return carry

    lax.fori_loop(0, n // rows, some_rows, 0)


class Reduce:
    def __init__(self, at, zb, ya, yb, yfd, yfu, ss, rs):
        self.at, self.zb, self.ya, self.yb, self.yfd, self.yfu, self.ss, self.rs = at, zb, ya, yb, yfd, yfu, ss, rs
        self.ch = zb.shape[2]
        self.h = self.ch // 2

    def copy(self, kind, j):
        at, h, ch = self.at, self.h, self.ch
        src, dst = (
            lambda: (self.zb.at[2, j, pl.ds(0, h)], self.ya.at[j]),
            lambda: (self.zb.at[2, j, pl.ds(h, ch - h)], self.yb.at[j]),
            lambda: (self.zb.at[1, j], self.yfd.at[j]),
            lambda: (self.zb.at[3, j], self.yfu.at[j]),
        )[kind]()
        return remote(src, dst, self.ss.at[kind], self.rs.at[kind, j], at.down if kind % 2 else at.up)

    def wait(self, kind, j):
        self.copy(kind, j).wait_recv()

    def halves(self, j):
        self.copy(0, j).start()
        self.copy(1, j).start()

    def middle(self, j):
        h = self.h
        self.wait(0, j)
        self.zb[1, j, 0:h] = (self.zb[1, j, 0:h].astype(F32) + self.ya[j].astype(F32)).astype(BF16)
        self.copy(2, j).start()
        self.wait(1, j)
        self.zb[3, j, h:] = (self.zb[3, j, h:].astype(F32) + self.yb[j].astype(F32)).astype(BF16)
        self.copy(3, j).start()

    def total(self, j):
        self.wait(2, j)
        self.wait(3, j)
        return self.zb[0, j].astype(F32) + self.yfd[j].astype(F32) + self.yfu[j].astype(F32)

    def drain(self):
        h = self.h
        for kind, every in enumerate((self.zb.at[2, :, 0:h], self.zb.at[2, :, h:], self.zb.at[1], self.zb.at[3])):
            remote(every, every, self.ss.at[kind], self.rs.at[kind, 0], self.at.up).wait_send()


def attention_kernel(
    units, x_hbm, turn_hbm, base_hbm, wq, wk, wv, wo, wg_t, wu_t,
    h_hbm, w_all, hg_all,
    x_ref, turn_ref, base_ref, h_ref, xc, xg, hg, cos_all, sin_all, st_own, st_in, s1, s2, wb, wob, part, precv, qb, kvo, kvp, og, zb, ya, yb, yfd, yfu, own, drel_a, drel_b,
    sxe, rxe, sst, rst, sy, ry, syh, ryh, sd, rd, swa, rwa, swo, rwo, swp, rwp, lw, so, ro, spr, rpr, skv, rkv, sog, rog, syr, ryr,
    lg, sds, rds, sdo, rdo, sdf, rdf, sdp, rdp, shx, rhx, shy, rhy, shz, rhz, lh, lx,
):
    at = Place()
    x, c, y = at.x, at.c, at.y
    ch, kc = xc.shape[1], xc.shape[2]
    kd = wq.shape[0]
    hc = qb.shape[2]
    fc, f_a = w_all.shape[1], drel_a.shape[1]
    width = 2 * xg.shape[3]
    kh = div(x, 2)
    ng = rem(div(x + 1, 2), 2)
    gather = Spread(at, xc, xg, units, (s1, s2), None, None, sy, ry, syh, ryh)
    reduce = Reduce(at, zb, ya, yb, yfd, yfu, syr, ryr)
    ahead = Spread(at, h_ref, hg, ((0, 0, ch // 2, 0), (0, ch // 2, ch // 2, 0)), (s1, s2), shx, rhx, shy, rhy, shz, rhz)
    weights = (wq, wk, wv)

    def half_cols(core):
        return pl.ds(al(core * kd, 128), kd)

    def x_rows(j, core):
        return pl.ds(al((2 * j + core) * ch, 8), ch)

    def x_pair(j):
        return remote(x_ref.at[x_rows(j, 1 - c)], xc.at[j, :, half_cols(c)], sd.at[0], rd.at[j], at.partner)

    def pair_cols(xx):
        return pl.ds(al(rem(xx, 2) * kc, 128), kc)

    def xe_copy(u, xx):
        j, lo, n, _ = units[u]
        rows = pl.ds(lo, n)
        return remote(xc.at[j, rows], xg.at[y, j, rows, pair_cols(xx)], sxe.at[0], rxe.at[u], at.pa)

    def st_copy(u):
        j, lo, n, _ = units[u]
        rows = pl.ds(lo // 4, n // 4)
        return remote(st_own.at[j, rows], st_in.at[j, rows], sst.at[0], rst.at[u], at.pb)

    def XP(j):
        x_pair(j).start()

    arrived = []

    def XE(u):
        j, lo, n, _ = units[u]
        if j not in arrived:
            arrived.append(j)
            dst = xc.at[j, :, half_cols(1 - c)]
            remote(dst, dst, sd.at[0], rd.at[j], at.partner).wait_recv()
        xe_copy(u, x).start()
        xg[y, j, lo : lo + n, pair_cols(x)] = xc[j, lo : lo + n]

    def ST(u):
        j, lo, n, _ = units[u]
        xe_copy(u, at.xa).wait_recv()
        quarter = n // 4
        lane = lax.broadcasted_iota(jnp.int32, (quarter, 128), 1)
        lane_sums(xg.at[y, j], lo, n, s1, s2)
        packed = jnp.zeros((quarter, 128), F32)
        for g in range(4):
            rows = pl.ds(g * quarter, quarter)
            total, square = (jnp.sum(t[rows, :], axis=-1, keepdims=True) for t in (s1, s2))
            packed = jnp.where(lane // 32 == g, jnp.where(lane % 32 < 16, total, square), packed)
        st_own[j, lo // 4 : lo // 4 + quarter, :] = packed
        st_copy(u).start()

    def N(u):
        j, lo, n, _ = units[u]
        st_copy(u).wait_recv()
        quarter = n // 4
        at_rows = slice(lo // 4, lo // 4 + quarter)
        moments = (st_own[j, at_rows, :] + st_in[j, at_rows, :]) / width
        for g in range(4):
            mean = moments[:, 32 * g : 32 * g + 1]
            var = moments[:, 32 * g + 16 : 32 * g + 17] - mean * mean
            rows = pl.ds(g * quarter, quarter)
            s1[rows, :] = jnp.broadcast_to(mean, (quarter, 128))
            s2[rows, :] = jnp.broadcast_to(lax.rsqrt(var + EPS), (quarter, 128))
        scale_rows(xg.at[y, j], lo, n, s1, s2)
        gather.YR(u)

    def w_rows(xx, core):
        return pl.ds(al(rem(xx, 2) * kc + core * kd, 128), kd)

    def w_part(group, half, i):
        side = kh if half else 1 - kh
        return weights[i].at[:, pl.ds(al((2 * group + side) * hc, 128), hc)]

    def w_cols(half, i):
        return pl.ds(half * 3 * hc + i * hc, hc)

    def wa_copy(half, i, xx):
        return remote(w_part(1 - ng, half, i), wb.at[w_rows(xx, c), w_cols(half, i)], swa.at[0], rwa.at[half, i], at.pa)

    def wo_copy(half, i, core):
        return remote(w_part(ng, half, i), wb.at[w_rows(x, core), w_cols(half, i)], swo.at[0], rwo.at[half, i], at.partner)

    def w_local(half, i):
        return pltpu.make_async_copy(w_part(ng, half, i), wb.at[w_rows(x, c), w_cols(half, i)], lw.at[half, i])

    def wp_copy(half, core):
        ref = wb.at[w_rows(at.xa, core), pl.ds(half * 3 * hc, 3 * hc)]
        return remote(ref, ref, swp.at[0], rwp.at[half], at.partner)

    o_local = pltpu.make_async_copy(wo, wob.at[:, half_cols(c)], lw.at[2, 0])
    o_pair = remote(wo, wob.at[:, half_cols(c)], so.at[0], ro.at[0], at.partner)
    pieces = [(half, i) for half in range(2) for i in range(3)]

    def WOP():
        for half, i in pieces:
            wo_copy(half, i, c).start()
        o_pair.start()

    def WA(half):
        for i in range(3):
            wa_copy(half, i, x).start()

    def WP(half):
        for i in range(3):
            wa_copy(half, i, at.xa).wait_recv()
        wp_copy(half, c).start()

    w_halves = [0, 1]

    def w_ready(half):
        if half not in w_halves:
            return
        w_halves.remove(half)
        for i in range(3):
            w_local(half, i).wait()
            wo_copy(half, i, 1 - c).wait_recv()
        wp_copy(half, 1 - c).wait_recv()
        if half:
            own_out()

    def own_out():
        for m in range(2):
            d_in(m).wait()
            d_out(m).start()
            d_pair(m, 3, c).start()

    def o_ready():
        o_local.wait()
        dst = wob.at[:, half_cols(1 - c)]
        remote(dst, dst, so.at[0], ro.at[0], at.partner).wait_recv()

    mlp_weights = (wg_t, wu_t)
    parts = ((0, f_a), (f_a, fc - f_a))

    def d_src(m, xx, p):
        return mlp_weights[m].at[pl.ds(al(xx * fc + parts[p][0], 8), parts[p][1])]

    def d_dst(m, xx, p):
        return w_all.at[m, pl.ds(*parts[p]), pl.ds(al((2 * xx + c) * kd, 128), kd)]

    def s_copy(d, m, p, xx):
        to, dev = ((at.xa, at.pa), (at.xb, at.pb))[d]
        return remote(d_src(m, to, p), d_dst(m, xx, p), sds.at[d], rds.at[d, m, p], dev)

    def o_copy(d, m):
        return remote(d_src(m, at.xo, d), (drel_a, drel_b)[d].at[m], sdo.at[d], rdo.at[d, m], (at.pa, at.pb)[d])

    def f_copy(d, m, xx):
        return remote((drel_a, drel_b)[d].at[m], d_dst(m, xx, d), sdf.at[d], rdf.at[d, m], (at.pb, at.pa)[d])

    def d_in(m):
        return pltpu.make_async_copy(mlp_weights[m].at[pl.ds(al(x * fc, 8), fc)], own.at[m], lg.at[0, m])

    def d_all(m, xx, core):
        return w_all.at[m, :, pl.ds(al((2 * xx + core) * kd, 128), kd)]

    def d_out(m):
        return pltpu.make_async_copy(own.at[m], d_all(m, x, c), lg.at[1, m])

    def d_pair(m, k, core):
        dst = d_all(m, (at.xa, at.xb, at.xo, x)[k], core)
        return remote(own.at[m] if k == 3 else dst, dst, sdp.at[0], rdp.at[m, k], at.partner)

    def S(link, m, p):
        s_copy("ab".index(link), m, p, x).start()

    def O(link, m):
        o_copy("ab".index(link), m).start()

    def F(link, m):
        d = "ba".index(link)
        o_copy(d, m).wait_recv()
        f_copy(d, m, (at.xa, at.xb)[d]).start()

    def DP(m):
        for d in range(2):
            for p in range(2):
                s_copy(d, m, p, (at.xa, at.xb)[d]).wait_recv()
            f_copy(d, m, at.xo).wait_recv()
        for k in range(3):
            d_pair(m, k, c).start()

    def pr_copy(n):
        return remote(part.at[n, :, pl.ds(0, 3 * hc)], precv.at[n], spr.at[0], rpr.at[n], at.pb)

    def project(g, first, size):
        def done(col, step, out):
            for i, (r, j) in enumerate(GROUPS[g]):
                part[r * NJ + j, :, pl.ds(al(first + col, 128), step)] = out[i * ch : (i + 1) * ch].astype(BF16)

        refs = [xg.at[gather.seqs[r], j] for r, j in GROUPS[g]]
        product(refs, wb.at[:, pl.ds(first, size)], wb.shape[0], size, done)

    split = {step[1] for step in ATTENTION_STEPS if step[0] == "Q"}

    def G(g):
        w_ready(0)
        for r, j in GROUPS[g]:
            gather.chunk_wait(r, j)
        if g in split:
            project(g, 0, 3 * hc)
        else:
            w_ready(1)
            project(g, 0, 6 * hc)
        for r, j in GROUPS[g]:
            pr_copy(r * NJ + j).start()

    def Q(g):
        w_ready(1)
        project(g, 3 * hc, 3 * hc)

    def kv_copy(r, j):
        s, n = gather.seqs[r], r * NJ + j
        return remote(kvo.at[s, j], kvp.at[s, j], skv.at[0], rkv.at[n], at.partner)

    def rotate(r, j):
        s, n = gather.seqs[r], r * NJ + j
        pr_copy(n).wait_recv()
        cos_t, sin_t = cos_all[j], sin_all[j]

        def total(col, size):
            mine = part[n, :, 3 * hc + col : 3 * hc + col + size]
            return (mine.astype(F32) + precv[n, :, col : col + size].astype(F32)).astype(BF16)

        def turned(col):
            v = total(col, HEAD_DIM).astype(F32)
            return (v * cos_t + pltpu.roll(v, HEAD_DIM // 2, axis=1) * sin_t).astype(BF16)

        for col in range(0, hc, HEAD_DIM):
            qb[n, :, col : col + HEAD_DIM] = turned(col)
            kvo[s, j, :, col : col + HEAD_DIM] = turned(hc + col)
        kvo[s, j, :, hc:] = total(2 * hc, hc)
        kv_copy(r, j).start()

    def R(g):
        for r, j in GROUPS[g]:
            rotate(r, j)

    def o_cols(xx):
        return pl.ds(al((2 * rem(div(xx + 1, 2), 2) + div(xx, 2)) * hc, 128), hc)

    cut = ch // 8

    def og_copy(kind, n):
        if kind < 2:
            ref = og.at[n, :, o_cols(x)]
        elif kind == 2:
            ref = og.at[n, pl.ds(0, cut), o_cols(at.xa)]
        else:
            ref = og.at[n, pl.ds(cut, ch - cut), o_cols(at.xb)]
        return remote(ref, ref, sog.at[kind], rog.at[kind, n], at.pa if kind in (0, 3) else at.pb)

    def og_wait(kind, n):
        xx = (at.xa, at.xb, at.xo, at.xo)[kind]
        rows = (pl.ds(0, ch), pl.ds(0, ch), pl.ds(0, cut), pl.ds(cut, ch - cut))[kind]
        dst = og.at[n, rows, o_cols(xx)]
        remote(dst, dst, sog.at[kind], rog.at[kind, n], at.pa).wait_recv()

    def attend(r, j, i):
        s, n = gather.seqs[r], r * NJ + j
        keys = (j + 1) * ch
        iq = lax.broadcasted_iota(jnp.int32, (ch, keys), 0) + j * ch
        ik = lax.broadcasted_iota(jnp.int32, (ch, keys), 1)
        own_ok = iq >= ik
        par_ok = ik < (j + c) * ch
        contract = (((1,), (1,)), ((), ()))
        cols = pl.ds(al(i * HEAD_DIM, 128), HEAD_DIM)
        v_cols = pl.ds(al(hc + i * HEAD_DIM, 128), HEAD_DIM)
        q = qb[n, :, cols]
        k_own = kvo[s, 0 : j + 1, :, cols].reshape(keys, HEAD_DIM)
        k_par = kvp[s, 0 : j + 1, :, cols].reshape(keys, HEAD_DIM)
        s_own = lax.dot_general(q, k_own, contract, preferred_element_type=F32) * HEAD_DIM**-0.5
        s_par = lax.dot_general(q, k_par, contract, preferred_element_type=F32) * HEAD_DIM**-0.5
        s_own = jnp.where(own_ok, s_own, -1e30)
        s_par = jnp.where(par_ok, s_par, -1e30)
        top = jnp.maximum(jnp.max(s_own, axis=1, keepdims=True), jnp.max(s_par, axis=1, keepdims=True))
        e_own, e_par = jnp.exp(s_own - top), jnp.exp(s_par - top)
        inv = 1.0 / (jnp.sum(e_own, axis=1, keepdims=True) + jnp.sum(e_par, axis=1, keepdims=True))
        v_own = kvo[s, 0 : j + 1, :, v_cols].reshape(keys, HEAD_DIM)
        v_par = kvp[s, 0 : j + 1, :, v_cols].reshape(keys, HEAD_DIM)
        out = jnp.dot((e_own * inv).astype(BF16), v_own, preferred_element_type=F32)
        out += jnp.dot((e_par * inv).astype(BF16), v_par, preferred_element_type=F32)
        og[n, :, pl.ds(al((2 * ng + kh) * hc + i * HEAD_DIM, 128), HEAD_DIM)] = out.astype(BF16)

    def A(g):
        for r, j in GROUPS[g]:
            kv_copy(r, j).wait_recv()

        def head(i, carry):
            for r, j in GROUPS[g]:
                attend(r, j, i)
            return carry

        lax.fori_loop(0, hc // HEAD_DIM, head, 0)
        for r, j in GROUPS[g]:
            og_copy(0, r * NJ + j).start()
            og_copy(1, r * NJ + j).start()

    def P(g):
        for r, j in GROUPS[g]:
            for kind in range(2):
                og_wait(kind, r * NJ + j)
                og_copy(kind + 2, r * NJ + j).start()

    def X(g):
        for r, j in GROUPS[g]:
            og_wait(2, r * NJ + j)
            og_wait(3, r * NJ + j)

        def done(col, size, out):
            for i, (r, j) in enumerate(GROUPS[g]):
                zb[r, j, :, pl.ds(al(col, 128), size)] = out[i * ch : (i + 1) * ch].astype(BF16)

        product([og.at[r * NJ + j] for r, j in GROUPS[g]], wob, wob.shape[0], kc, done)
        for r, j in GROUPS[g]:
            if r == 2:
                reduce.halves(j)

    def T(j):
        attn = reduce.total(j).astype(BF16)
        h_ref[j] = (xc[j].astype(F32) + attn.astype(F32)).astype(BF16)
        chunk_out(j).start()

    def chunk_out(j):
        return pltpu.make_async_copy(h_ref.at[j], h_hbm.at[j], lx.at[1 + j])

    def h_out(r, u):
        rows = pl.ds(u * (ch // 2), ch // 2)
        return pltpu.make_async_copy(hg.at[ahead.seqs[r], 0, rows], hg_all.at[ahead.seqs[r], rows], lh.at[r, u])

    kept = []

    def HF(u):
        if not kept:
            kept.append(u)
            ahead.keep_own()
        ahead.XF(0, u)

    def HY(u):
        ahead.YH(u)
        for r in (0, 1, 3):
            h_out(r, u).start()

    def HO(u):
        for d in range(2):
            ahead.yhalf_wait(d, u)
        h_out(2, u).start()

    def own_rows():
        for half, i in pieces:
            w_local(half, i).start()
        o_local.start()
        for m in range(2):
            d_in(m).start()
        x_in.wait()
        for j in range(NJ):
            xc[j, :, half_cols(c)] = x_ref[x_rows(j, c), :]

    x_in = pltpu.make_async_copy(x_hbm, x_ref, lx.at[0])
    x_in.start()
    tables = [pltpu.make_async_copy(src, dst, lx.at[1 + NJ + i]) for i, (src, dst) in enumerate(((turn_hbm, turn_ref), (base_hbm, base_ref)))]
    for copy in tables:
        copy.start()
    at.barrier(own_rows)

    def angles():
        for copy in tables:
            copy.wait()
        lane = lax.broadcasted_iota(jnp.int32, (ch, HEAD_DIM), 1)
        for j in range(NJ):
            base_cos, base_sin = base_ref[0, pl.ds(2 * j + c, 1), :], base_ref[1, pl.ds(2 * j + c, 1), :]
            cos_all[j] = base_cos * turn_ref[0] - base_sin * turn_ref[1]
            sine = base_sin * turn_ref[0] + base_cos * turn_ref[1]
            sin_all[j] = jnp.where(lane < HEAD_DIM // 2, -sine, sine)

    ops = {
        "XP": XP, "WOP": WOP, "XE": XE, "ST": ST, "N": N, "YH": gather.YH, "WA": WA, "WP": WP, "S": S, "O": O, "F": F, "DP": DP,
        "G": G, "Q": Q, "R": R, "A": A, "P": P, "X": X, "M": reduce.middle, "T": T,
        "HF": HF, "HH": lambda u: ahead.XH(0, u), "HN": lambda u: ahead.N(0, u), "HY": HY, "HO": HO,
    }
    def all_sent(ref, sem):
        remote(ref, ref, sem, ro.at[0], at.partner).wait_send()

    def sent():
        for m in range(2):
            for k in range(4):
                d_pair(m, k, 1 - c).wait_recv()
            d_out(m).wait()
        all_sent(w_all.at[:, :, pl.ds(0, 4 * kd)], sdp.at[0])
        for d in range(2):
            all_sent(w_all.at[:, :, pl.ds(0, kd)], sds.at[d])
            all_sent((drel_a, drel_b)[d], sdo.at[d])
            all_sent((drel_a, drel_b)[d], sdf.at[d])
            for u in range(len(units)):
                gather.ycopy(d, u).wait_send()
                gather.yhalf(d, u).wait_send()
        all_sent(x_ref.at[pl.ds(0, NJ * ch)], sd.at[0])
        all_sent(xc, sxe.at[0])
        all_sent(st_own, sst.at[0])
        reduce.drain()
        ahead.drain()
        for r in range(NX):
            for u in range(2):
                h_out(r, u).wait()
        o_pair.wait_send()
        for sem in (swa, swo, swp):
            all_sent(wb.at[pl.ds(0, kd)], sem.at[0])
        all_sent(part.at[:, :, pl.ds(0, 3 * hc)], spr.at[0])
        all_sent(kvo, skv.at[0])
        for kind, (lo, n) in enumerate(((0, ch), (0, ch), (0, cut), (cut, ch - cut))):
            all_sent(og.at[:, pl.ds(lo, n), o_cols(x)], sog.at[kind])

    waits = {"X": o_ready, "WP": angles}
    last = max(i for i, step in enumerate(ATTENTION_STEPS) if step[0] == "X")
    for i, step in enumerate(ATTENTION_STEPS):
        if step[0] in waits:
            waits.pop(step[0])()
        if i == last:
            sent()
        ops[step[0]](*step[1:])
    for j in range(NJ):
        chunk_out(j).wait()


def mlp_kernel(
    units, h_hbm, w_hbm, wdn, hg_hbm, y_ref,
    h_ref, xg, wt, raw, wd, ag, ar, act, s1, s2, zb, ya, yb, yfd, yfu, yst,
    sx, rx, sy, ry, syh, ryh, sa, ra, syr, ryr, sd, rd, lw, lwd, swd, rwd, lh, lo,
):
    at = Place()
    x, c, y = at.x, at.c, at.y
    ch, kc, h = h_ref.shape[1], h_ref.shape[2], h_ref.shape[1] // 2
    width = xg.shape[-1]
    kd = kc // 2
    fc, tiles = w_hbm.shape[1], wt.shape[1] // 256
    fm = (tiles - 1) * 128
    fr = fc - fm
    blocks, slots = 2 * tiles, raw.shape[0]
    gather = Spread(at, h_ref, xg, units, (s1, s2), sx, rx, sy, ry, syh, ryh)
    reduce = Reduce(at, zb, ya, yb, yfd, yfu, syr, ryr)

    def w_in(q):
        i, m = q // 2, q % 2
        n = min(128, fc - i * 128)
        return pltpu.make_async_copy(w_hbm.at[m, pl.ds(i * 128, n)], raw.at[q % slots, pl.ds(0, n)], lw.at[q])

    def WT(g):
        for q in range(g * blocks // 4, (g + 1) * blocks // 4):
            i, m, slot = q // 2, q % 2, q % slots
            w_in(q).wait()
            if fc < (i + 1) * 128:
                raw[slot, fc - i * 128 :, :] = jnp.zeros(((i + 1) * 128 - fc, width), BF16)

            def turn(k, carry, slot=slot, q=q):
                part = pl.ds(al(k * (width // 4), 128), width // 4)
                wt[part, q * 128 : (q + 1) * 128] = raw[slot, :, part].T
                return carry

            lax.fori_loop(0, 4, turn, 0)
            if q + slots < blocks:
                w_in(q + slots).start()

    def d_refs(q, core):
        cols = pl.ds(al(core * kd, 128), kd)
        main, rest = wdn.at[pl.ds(q * fc, fm)], wdn.at[pl.ds(q * fc + fm, fr)]
        return (main, wd.at[pl.ds(q * fm, fm), cols]), (rest, wd.at[pl.ds(NX * fm + q * 128, fr), cols])

    def d_own(q, k):
        src, dst = d_refs(q, c)[k]
        return pltpu.make_async_copy(src, dst, lwd.at[q, k])

    def d_pair(q, k, core):
        src, dst = d_refs(q, core)[k]
        return remote(src, dst, swd.at[q, k], rwd.at[q, k], at.partner)

    quarters = [(q, k) for q in range(NX) for k in range(2)]
    h_in_all = pltpu.make_async_copy(h_hbm, h_ref, lo.at[NJ])
    h_in_all.start()
    for q in range(slots):
        w_in(q).start()
    def h_in(s):
        return pltpu.make_async_copy(hg_hbm.at[s], xg.at[s, 0], lh.at[s])

    for s in range(NX):
        h_in(s).start()
    for q, k in quarters:
        d_own(q, k).start()
    for q in range(NX):
        wd[NX * fm + q * 128 + fr : NX * fm + (q + 1) * 128, :] = jnp.zeros((128 - fr, kc), BF16)
    at.barrier(h_in_all.wait)
    for q, k in quarters:
        d_pair(q, k, c).start()

    def a_refs(kind, n, xx):
        main, rest = pl.ds(al(xx * fm, 128), fm), pl.ds(al(xx * 128, 128), 128)
        if kind < 2:
            return ag.at[n, :, main], ar.at[n, :, rest]
        lo = (kind - 2) * h
        return ag.at[n, pl.ds(lo, h), main], ar.at[n, pl.ds(lo // 2, h // 2), rest]

    def a_copies(kind, n):
        refs = a_refs(kind, n, (x, x, at.xl, at.xr)[kind])
        return [remote(v, v, sa.at[kind, k], ra.at[kind, n, k], at.left if kind % 2 else at.right) for k, v in enumerate(refs)]

    def a_wait(kind, n):
        for k, v in enumerate(a_refs(kind, n, (at.xl, at.xr, at.xo, at.xo)[kind])):
            remote(v, v, sa.at[kind, k], ra.at[kind, n, k], at.right).wait_recv()

    def a_start(kind, n):
        for copy in a_copies(kind, n):
            copy.start()

    def G(g):
        for r, j in GROUPS[g]:
            gather.chunk_wait(r, j)

        def done(col, size, out):
            for k in range(0, size, 256):
                gate, up = out[:, k : k + 128].astype(BF16).astype(F32), out[:, k + 128 : k + 256].astype(BF16).astype(F32)
                value = (gate / (1.0 + jnp.exp(-gate)) * up).astype(BF16)
                act[0 : value.shape[0], pl.ds(al(div(col + k, 2), 128), 128)] = value

        product([xg.at[gather.seqs[r], j] for r, j in GROUPS[g]], wt, width, wt.shape[1], done)
        for i, (r, j) in enumerate(GROUPS[g]):
            n, lo = r * NJ + j, i * ch
            ag[n, :, pl.ds(al(x * fm, 128), fm)] = act[lo : lo + ch, :fm]
            below = pltpu.roll(act[lo + h : lo + ch, fm:].astype(F32), 64, axis=1)
            ar[n, :, pl.ds(al(x * 128, 128), 128)] = (act[lo : lo + h, fm:].astype(F32) + below).astype(BF16)
            for kind in range(2):
                a_start(kind, n)

    def P(g):
        for r, j in GROUPS[g]:
            for kind in range(2):
                a_wait(kind, r * NJ + j)
                a_start(kind + 2, r * NJ + j)

    def X(g):
        for r, j in GROUPS[g]:
            n = r * NJ + j
            for kind in (2, 3):
                a_wait(kind, n)
            lane = lax.broadcasted_iota(jnp.int32, (h, 128), 1)
            for q in range(NX):
                cols = pl.ds(NX * fm + q * 128, 128)
                rest = ar[n, :, q * 128 : (q + 1) * 128].astype(F32)
                ag[n, 0:h, cols] = jnp.where(lane < 64, rest, 0.0).astype(BF16)
                ag[n, h:, cols] = jnp.where(lane < 64, pltpu.roll(rest, 64, axis=1), 0.0).astype(BF16)

        def done(col, size, out):
            for i, (r, j) in enumerate(GROUPS[g]):
                zb[r, j, :, pl.ds(al(col, 128), size)] = out[i * ch : (i + 1) * ch].astype(BF16)

        product([ag.at[r * NJ + j] for r, j in GROUPS[g]], wd, wd.shape[0], kc, done)
        for r, j in GROUPS[g]:
            if r == 2:
                reduce.halves(j)

    def y_rows(j, core):
        return pl.ds(al((2 * j + core) * ch, 8), ch)

    def y_copy(j):
        return remote(yst.at[1 - c, j], y_ref.at[y_rows(j, c)], sd.at[j], rd.at[j], at.partner)

    def y_own(j):
        return pltpu.make_async_copy(yst.at[c, j], y_ref.at[y_rows(j, c)], lo.at[j])

    def y_wait(j):
        dst = y_ref.at[y_rows(j, 1 - c)]
        remote(dst, dst, sd.at[j], rd.at[j], at.partner).wait_recv()

    def T(j):
        mlp = reduce.total(j).astype(BF16)
        out = (h_ref[j].astype(F32) + mlp.astype(F32)).astype(BF16)
        yst[0, j] = out[:, :kd]
        yst[1, j] = out[:, kd:]
        y_copy(j).start()
        y_own(j).start()

    ops = {"G": G, "P": P, "X": X, "M": reduce.middle, "T": T, "WT": WT}
    for name in ("YR", "YRH", "YH", "XF", "XH", "N"):
        ops[name] = getattr(gather, name)
    waits = {
        "N": gather.keep_own,
        "G": lambda: [h_in(s).wait() for s in range(NX)],
        "X": lambda: [(d_own(q, k).wait(), d_pair(q, k, 1 - c).wait_recv()) for q, k in quarters],
    }
    def sent():
        gather.drain()
        reduce.drain()
        for q, k in quarters:
            d_pair(q, k, c).wait_send()

        for kind in range(4):
            for k, every in enumerate(a_refs(kind, slice(None), x)):
                remote(every, every, sa.at[kind, k], ra.at[kind, 0, k], at.right).wait_send()

    for step in MLP_STEPS:
        if step[0] in waits:
            waits.pop(step[0])()
        ops[step[0]](*step[1:])
    sent()
    for j in range(NJ):
        y_copy(j).wait_send()
        y_own(j).wait()
        y_wait(j)


def vmem(*shape, dtype=BF16):
    return pltpu.VMEM(shape, dtype)


def sems(*shape):
    return pltpu.SemaphoreType.DMA(shape)


def solution(mesh):
    assert mesh.shape["tx"] == 2 * NX and mesh.shape["ty"] == NX
    act_spec = P(("dp", "ty"), None, "tx")
    col_spec = P("tx", "ty")
    row_spec = P("ty", "tx")
    any_spec = pl.BlockSpec(memory_space=pl.ANY)
    vmem_spec = pl.BlockSpec(memory_space=pltpu.VMEM)

    def layer(x_blk, w_q, w_k, w_v, w_o, w_gate, w_up, w_down):
        _, seq, kd = x_blk.shape
        kc, width = 2 * kd, 2 * NX * kd
        ch = seq // (2 * NJ)
        h = ch // 2
        row_heads = w_q.shape[1]
        hc = row_heads // NX
        fc = w_down.shape[0] // NX
        assert hc % HEAD_DIM == 0
        tiles = (fc + 127) // 128
        f_a = (fc // 2 + 15) // 16 * 16

        inv_freq = THETA ** (-2.0 * np.arange(HEAD_DIM // 2) / HEAD_DIM)
        inv_freq = np.concatenate([inv_freq, inv_freq])
        turn = np.arange(ch)[:, None] * inv_freq
        base = np.arange(2 * NJ)[:, None] * ch * inv_freq
        turn = jnp.asarray(np.stack([np.cos(turn), np.sin(turn)]), F32)
        base = jnp.asarray(np.stack([np.cos(base), np.sin(base)]), F32)

        reduce_scratch = [vmem(NX, NJ, ch, kc), vmem(NJ, h, kc), vmem(NJ, ch - h, kc), vmem(NJ, ch, kc), vmem(NJ, ch, kc)]
        units = ((0, 0, h, 0), (0, h, h, 0)) + tuple((j, 0, ch, 0) for j in range(1, NJ))
        n_u = len(units)
        h_blk, w_all, hg_all = pl.pallas_call(
            functools.partial(attention_kernel, units),
            out_shape=(
                jax.ShapeDtypeStruct((NJ, ch, kc), BF16),
                jax.ShapeDtypeStruct((2, fc, width), BF16),
                jax.ShapeDtypeStruct((NX, ch, width), BF16),
            ),
            in_specs=[any_spec] * 9,
            out_specs=(any_spec, any_spec, any_spec),
            scratch_shapes=[
                vmem(seq, kd), vmem(2, ch, HEAD_DIM, dtype=F32), vmem(2, 2 * NJ, HEAD_DIM, dtype=F32),
                vmem(NJ, ch, kc), vmem(NJ, ch, kc), vmem(NX, NJ, ch, 2 * kc), vmem(NX, 1, ch, width), vmem(NJ, ch, HEAD_DIM, dtype=F32), vmem(NJ, ch, HEAD_DIM, dtype=F32),
                vmem(NJ, ch // 4, 128, dtype=F32), vmem(NJ, ch // 4, 128, dtype=F32), vmem(ch, 128, dtype=F32), vmem(ch, 128, dtype=F32),
                vmem(2 * kc, 6 * hc), vmem(row_heads, kc), vmem(NCH, ch, 6 * hc), vmem(NCH, ch, 3 * hc), vmem(NCH, ch, hc),
                vmem(NX, NJ, ch, 2 * hc), vmem(NX, NJ, ch, 2 * hc), vmem(NCH, ch, row_heads), *reduce_scratch,
                vmem(2, fc, kd), vmem(2, f_a, kd), vmem(2, fc - f_a, kd),
                sems(1), sems(n_u), sems(1), sems(n_u), sems(2, n_u), sems(2, n_u), sems(2, n_u), sems(2, n_u),
                sems(1), sems(NJ), sems(1), sems(2, 3), sems(1), sems(2, 3), sems(1), sems(2), sems(3, 3), sems(1), sems(1),
                sems(1), sems(NCH), sems(1), sems(NCH), sems(4), sems(4, NCH), sems(4), sems(4, NJ),
                sems(2, 2), sems(2), sems(2, 2, 2), sems(2), sems(2, 2), sems(2), sems(2, 2), sems(1), sems(2, 4),
                sems(4, 2), sems(4, 2), sems(2, 2), sems(2, 2), sems(2, 2), sems(2, 2), sems(NX, 2), sems(3 + NJ),
            ],
            compiler_params=pltpu.CompilerParams(collective_id=0, has_side_effects=True, vmem_limit_bytes=VMEM_LIMIT),
            name="attention_part",
        )(x_blk[0], turn, base, w_q, w_k, w_v, w_o, w_gate.T, w_up.T)

        units = ((1, 0, h, 1), (1, h, h, 0)) + tuple((j, 0, ch, 0) for j in range(2, NJ))
        n_u, n_x = len(units), len(units) + 3
        y_blk = pl.pallas_call(
            functools.partial(mlp_kernel, units),
            out_shape=jax.ShapeDtypeStruct((seq, kd), BF16),
            in_specs=[any_spec] * 4,
            out_specs=any_spec,
            scratch_shapes=[
                vmem(NJ, ch, kc),
                vmem(NX, NJ, ch, width), vmem(width, tiles * 256), vmem(3, 128, width),
                vmem(NX * tiles * 128, kc), vmem(NCH, ch, NX * tiles * 128), vmem(NCH, h, NX * 128), vmem(2 * ch, tiles * 128),
                vmem(ch, 128, dtype=F32), vmem(ch, 128, dtype=F32),
                *reduce_scratch, vmem(2, NJ, ch, kd),
                sems(4, n_x), sems(4, n_x), sems(2, n_u), sems(2, n_u), sems(2, n_u), sems(2, n_u),
                sems(4, 2), sems(4, NCH, 2), sems(4), sems(4, NJ), sems(NJ), sems(NJ),
                sems(2 * tiles), sems(NX, 2), sems(NX, 2), sems(NX, 2), sems(NX), sems(NJ + 1),
            ],
            compiler_params=pltpu.CompilerParams(collective_id=1, has_side_effects=True, vmem_limit_bytes=VMEM_LIMIT),
            name="mlp_part",
        )(h_blk, w_all, w_down, hg_all)
        return y_blk[None]

    return jax.shard_map(
        layer,
        mesh=mesh,
        in_specs=(act_spec, col_spec, col_spec, col_spec, row_spec, col_spec, col_spec, row_spec),
        out_specs=act_spec,
        check_vma=False,
    )
```

```python
import functools

import jax
import jax.numpy as jnp
import numpy as np
from jax import lax
from jax.experimental import pallas as pl
from jax.experimental.pallas import tpu as pltpu
from jax.sharding import PartitionSpec as P

HEAD_DIM = 128
EPS = 1e-5
THETA = 10000.0
MESH = pl.DeviceIdType.MESH
F32 = jnp.float32
BF16 = jnp.bfloat16
NX = 4
NJ = 4
NCH = 16
VMEM_LIMIT = 67_043_328
GROUPS = (*(((0, j),) for j in range(NJ)), *(((3, j), (1, j)) for j in range(NJ)), *(((2, j),) for j in range(NJ)))


def rem(a, b):
    return lax.rem(a, jnp.int32(b))


def div(a, b):
    return lax.div(a, jnp.int32(b))


def al(v, m):
    return pl.multiple_of(v, m)


def remote(src, dst, ssem, rsem, dev):
    return pltpu.make_async_remote_copy(src_ref=src, dst_ref=dst, send_sem=ssem, recv_sem=rsem, device_id=dev, device_id_type=MESH)


ATTENTION_STEPS = (
    ("WA", 0), ("XP", 1), ("S", "b", 0, 1), ("XP", 0), ("XE", 1), ("XE", 0), ("XE", 2), ("XP", 2), ("S", "b", 0, 0), ("XP", 3),
    ("S", "b", 1, 0), ("ST", 1), ("WP", 0), ("WA", 1), ("O", "b", 1), ("ST", 0), ("N", 1), ("O", "b", 0), ("ST", 2),
    ("S", "b", 1, 1), ("WOP",), ("N", 0), ("G", 0), ("XE", 3), ("YH", 1), ("YH", 0), ("S", "a", 0, 1), ("N", 2), ("WP", 1),
    ("G", 8), ("G", 4), ("ST", 3), ("Q", 8), ("Q", 0), ("R", 8), ("XE", 4), ("A", 8), ("F", "a", 1), ("YH", 2), ("G", 5),
    ("R", 4), ("ST", 4), ("N", 3), ("P", 8), ("G", 9), ("A", 4), ("R", 0), ("S", "a", 1, 1), ("X", 8), ("G", 1), ("N", 4),
    ("R", 5), ("A", 0), ("R", 9), ("P", 4), ("A", 9), ("A", 5), ("G", 2), ("P", 0), ("X", 4), ("M", 0), ("P", 9),
    ("S", "a", 1, 0), ("YH", 3), ("G", 6), ("P", 5), ("X", 0), ("T", 0), ("HF", 1), ("HF", 0), ("R", 2), ("X", 9), ("R", 1),
    ("A", 1), ("YH", 4), ("X", 5), ("M", 1), ("HH", 1), ("O", "a", 0), ("G", 10), ("R", 6), ("HH", 0), ("G", 7), ("O", "a", 1),
    ("HN", 1), ("R", 10), ("G", 11), ("A", 10), ("A", 6), ("HN", 0), ("R", 7), ("A", 2), ("HY", 1), ("A", 7), ("R", 11),
    ("P", 10), ("A", 11), ("P", 6), ("G", 3), ("P", 7), ("P", 11), ("F", "b", 1), ("F", "a", 0), ("X", 10), ("HY", 0),
    ("S", "a", 0, 0), ("F", "b", 0), ("R", 3), ("X", 11), ("A", 3), ("X", 6), ("HO", 1), ("X", 7), ("P", 1), ("P", 2),
    ("M", 2), ("M", 3), ("DP", 1), ("DP", 0), ("P", 3), ("HO", 0), ("X", 1), ("T", 1), ("X", 2), ("T", 2), ("X", 3), ("T", 3),
)
MLP_STEPS = (
    ("XF", 0, 1), ("XF", 0, 0), ("WT", 0), ("YR", 0), ("WT", 1), ("XH", 0, 1), ("XF", 0, 3), ("YRH", 0), ("XF", 3, 0),
    ("N", 0, 1), ("XH", 0, 3), ("XF", 1, 0), ("XF", 2, 0), ("WT", 2), ("WT", 3), ("N", 0, 3), ("XF", 0, 2), ("G", 4),
    ("YH", 1), ("G", 0), ("XH", 2, 0), ("G", 8), ("XH", 1, 0), ("XH", 0, 0), ("XH", 3, 0), ("XH", 0, 2), ("G", 3), ("YH", 3),
    ("G", 7), ("N", 3, 0), ("N", 0, 2), ("N", 1, 0), ("P", 8), ("N", 2, 0), ("G", 9), ("G", 11), ("P", 4), ("G", 5), ("P", 11),
    ("X", 8), ("P", 7), ("P", 9), ("X", 4), ("YH", 2), ("G", 6), ("X", 11), ("X", 7), ("P", 5), ("X", 9), ("N", 0, 0),
    ("M", 0), ("G", 10), ("G", 1), ("M", 3), ("X", 5), ("M", 1), ("P", 10), ("P", 6), ("P", 0), ("G", 2), ("X", 10), ("P", 3),
    ("P", 1), ("X", 6), ("M", 2), ("P", 2), ("X", 0), ("T", 0), ("X", 3), ("T", 3), ("X", 1), ("T", 1), ("X", 2), ("T", 2),
)


class Place:
    def __init__(self):
        tx, ty = lax.axis_index("tx"), lax.axis_index("ty")
        self.x, self.c, self.y = div(tx, 2), rem(tx, 2), ty
        x, c, y = self.x, self.c, self.y
        self.xr, self.xl, self.xo = rem(x + 1, NX), rem(x + 3, NX), rem(x + 2, NX)
        self.yu, self.yd, self.yo = rem(y + 1, NX), rem(y + 3, NX), rem(y + 2, NX)
        self.right = {"tx": self.xr * 2 + c, "ty": y}
        self.left = {"tx": self.xl * 2 + c, "ty": y}
        self.up = {"tx": tx, "ty": self.yu}
        self.down = {"tx": tx, "ty": self.yd}
        self.partner = {"tx": x * 2 + 1 - c, "ty": y}
        self.xa, self.xb = x + 1 - 2 * rem(x, 2), rem(x + 3 + 2 * rem(x, 2), NX)
        self.pa, self.pb = {"tx": self.xa * 2 + c, "ty": y}, {"tx": self.xb * 2 + c, "ty": y}

    def barrier(self, between):
        sem = pltpu.get_barrier_semaphore()
        for dev in (self.right, self.left, self.up, self.down, self.partner):
            pl.semaphore_signal(sem, inc=1, device_id=dev, device_id_type=MESH)
        between()
        pl.semaphore_wait(sem, 5)


class Spread:
    def __init__(self, at, src, xg, units, sums, sx, rx, sy, ry, syh, ryh):
        self.sums = sums
        self.at, self.src, self.xg, self.units, self.kc = at, src, xg, units, src.shape[2]
        self.sx, self.rx, self.sy, self.ry, self.syh, self.ryh = sx, rx, sy, ry, syh, ryh
        pairs = [(r, u) for u, unit in enumerate(units) for r in ((0, 3, 1, 2) if unit[3] else (0,))]
        self.index = {pair: i for i, pair in enumerate(pairs)}
        self.seqs = (at.y, at.yu, at.yo, at.yd)

    def cols(self, x):
        return pl.ds(al(x * self.kc, 128), self.kc)

    def keep_own(self):
        for j in {unit[0]: 0 for unit in self.units}:
            self.xg[self.at.y, j, :, self.cols(self.at.x)] = self.src[j]

    def xcopy(self, kind, r, u):
        at, s = self.at, self.seqs[r]
        j, lo, n, _ = self.units[u]
        i = self.index[r, u]
        if kind < 2:
            dst = self.xg.at[s, j, pl.ds(lo, n), self.cols(at.x)]
            src = self.src.at[j, pl.ds(lo, n)] if r == 0 else dst
        elif kind == 2:
            src = dst = self.xg.at[s, j, pl.ds(lo, n // 2), self.cols(at.xl)]
        else:
            src = dst = self.xg.at[s, j, pl.ds(lo + n // 2, n // 2), self.cols(at.xr)]
        return remote(src, dst, self.sx.at[kind, i], self.rx.at[kind, i], at.left if kind % 2 else at.right)

    def xwait(self, kind, r, u):
        at = self.at
        j, lo, n, _ = self.units[u]
        i = self.index[r, u]
        x = (at.xl, at.xr, at.xo, at.xo)[kind]
        rows = (pl.ds(lo, n), pl.ds(lo, n), pl.ds(lo, n // 2), pl.ds(lo + n // 2, n // 2))[kind]
        dst = self.xg.at[self.seqs[r], j, rows, self.cols(x)]
        remote(dst, dst, self.sx.at[kind, i], self.rx.at[kind, i], at.right).wait_recv()

    def yref(self, s, u, lo, n):
        j, _, _, first = self.units[u]
        rows = pl.ds(lo, n)
        return self.xg.at[s, j, rows, self.cols(self.at.x)] if first else self.xg.at[s, j, rows]

    def ycopy(self, d, u):
        j, lo, n, first = self.units[u]
        dst = self.yref(self.at.y, u, lo, n)
        src = self.src.at[j, pl.ds(lo, n)] if first else dst
        return remote(src, dst, self.sy.at[d, u], self.ry.at[d, u], self.at.down if d else self.at.up)

    def ywait(self, d, u):
        _, lo, n, _ = self.units[u]
        dst = self.yref(self.at.yu if d else self.at.yd, u, lo, n)
        remote(dst, dst, self.sy.at[d, u], self.ry.at[d, u], self.at.up).wait_recv()

    def yhalf(self, d, u):
        _, lo, n, _ = self.units[u]
        ref = self.yref(self.at.yu if d else self.at.yd, u, lo + d * (n // 2), n // 2)
        return remote(ref, ref, self.syh.at[d, u], self.ryh.at[d, u], self.at.down if d else self.at.up)

    def yhalf_wait(self, d, u):
        _, lo, n, _ = self.units[u]
        dst = self.yref(self.at.yo, u, lo + d * (n // 2), n // 2)
        remote(dst, dst, self.syh.at[d, u], self.ryh.at[d, u], self.at.up).wait_recv()

    def YR(self, u):
        for d in range(2):
            self.ycopy(d, u).start()

    def YH(self, u):
        for d in range(2):
            self.ywait(d, u)
            self.yhalf(d, u).start()

    YRH = YH

    def XF(self, r, u):
        if r == 2:
            for d in range(2):
                self.yhalf_wait(d, u)
        for kind in range(2):
            self.xcopy(kind, r, u).start()

    def XH(self, r, u):
        for kind in range(2):
            self.xwait(kind, r, u)
            self.xcopy(kind + 2, r, u).start()

    def N(self, r, u):
        j, lo, n, first = self.units[u]
        for kind in (2, 3):
            self.xwait(kind, r, u)
            self.xcopy(kind, r, u).wait_send()
        if r:
            for kind in range(2):
                self.xcopy(kind, r, u).wait_send()
        if r % 2:
            self.yhalf(0 if r == 3 else 1, u).wait_send()
        width, ref = self.xg.shape[-1], self.xg.at[self.seqs[r], j]
        s1, s2 = self.sums
        lane_sums(ref, lo, n, s1, s2)
        mean = jnp.sum(s1[0:n, :], axis=-1, keepdims=True) / width
        var = jnp.sum(s2[0:n, :], axis=-1, keepdims=True) / width - mean * mean
        s1[0:n, :] = jnp.broadcast_to(mean, (n, 128))
        s2[0:n, :] = jnp.broadcast_to(lax.rsqrt(var + EPS), (n, 128))
        scale_rows(ref, lo, n, s1, s2)
        if not first:
            self.YR(u)

    def chunk_wait(self, r, j):
        if r == 2:
            for u, unit in enumerate(self.units):
                if unit[0] == j and not unit[3]:
                    for d in range(2):
                        self.yhalf_wait(d, u)

    def drain(self):
        for u, unit in enumerate(self.units):
            for d in range(2):
                self.xcopy(d, 0, u).wait_send()
                self.ycopy(d, u).wait_send()
                if not unit[3]:
                    self.yhalf(d, u).wait_send()


def rows_of(refs):
    return refs[0][...] if len(refs) == 1 else jnp.concatenate([ref[...] for ref in refs], axis=0)


def product(refs, weight, depth, n_cols, done, step=256):
    def columns(i, carry):
        out = jnp.dot(rows_of(refs), weight[0:depth, pl.ds(al(i * step, 128), step)], preferred_element_type=F32)
        done(i * step, step, out)
        return carry

    lax.fori_loop(0, n_cols // step, columns, 0)


def lane_sums(ref, lo, n, s1, s2):
    width, rows, wide = ref.shape[-1], 32, 512

    def some_rows(i, carry):
        def some_columns(k, sums):
            a, b = sums
            v = ref[pl.ds(al(lo + i * rows, 8), rows), pl.ds(al(k * wide, 128), wide)].astype(F32)
            for c in range(0, wide, 128):
                part = v[:, c : c + 128]
                a, b = a + part, b + part * part
            return a, b

        zero = jnp.zeros((rows, 128), F32)
        a, b = lax.fori_loop(0, width // wide, some_columns, (zero, zero))
        s1[pl.ds(al(i * rows, 8), rows), :] = a
        s2[pl.ds(al(i * rows, 8), rows), :] = b
        return carry

    lax.fori_loop(0, n // rows, some_rows, 0)


def scale_rows(ref, lo, n, means, scales):
    width, rows, wide = ref.shape[-1], 32, 512

    def some_rows(i, carry):
        mean, scale = (t[pl.ds(al(i * rows, 8), rows), :] for t in (means, scales))

        def some_columns(k, carry):
            at_rows = pl.ds(al(lo + i * rows, 8), rows)
            for c in range(0, wide, 128):
                cols = pl.ds(al(k * wide + c, 128), 128)
                ref[at_rows, cols] = ((ref[at_rows, cols].astype(F32) - mean) * scale).astype(BF16)
            return carry

        lax.fori_loop(0, width // wide, some_columns, 0)
        return carry

    lax.fori_loop(0, n // rows, some_rows, 0)


class Reduce:
    def __init__(self, at, zb, ya, yb, yfd, yfu, ss, rs):
        self.at, self.zb, self.ya, self.yb, self.yfd, self.yfu, self.ss, self.rs = at, zb, ya, yb, yfd, yfu, ss, rs
        self.ch = zb.shape[2]
        self.h = self.ch // 2

    def copy(self, kind, j):
        at, h, ch = self.at, self.h, self.ch
        src, dst = (
            lambda: (self.zb.at[2, j, pl.ds(0, h)], self.ya.at[j]),
            lambda: (self.zb.at[2, j, pl.ds(h, ch - h)], self.yb.at[j]),
            lambda: (self.zb.at[1, j], self.yfd.at[j]),
            lambda: (self.zb.at[3, j], self.yfu.at[j]),
        )[kind]()
        return remote(src, dst, self.ss.at[kind], self.rs.at[kind, j], at.down if kind % 2 else at.up)

    def wait(self, kind, j):
        self.copy(kind, j).wait_recv()

    def halves(self, j):
        self.copy(0, j).start()
        self.copy(1, j).start()

    def middle(self, j):
        h = self.h

        def add(r, lo, part):
            def some_rows(i, carry):
                rows, src = pl.ds(al(lo + i * 32, 8), 32), pl.ds(al(i * 32, 8), 32)
                self.zb[r, j, rows, :] = (self.zb[r, j, rows, :].astype(F32) + part[j, src, :].astype(F32)).astype(BF16)
                return carry

            lax.fori_loop(0, h // 32, some_rows, 0)

        self.wait(0, j)
        add(1, 0, self.ya)
        self.copy(2, j).start()
        self.wait(1, j)
        add(3, h, self.yb)
        self.copy(3, j).start()

    def total(self, j, done):
        self.wait(2, j)
        self.wait(3, j)

        def some_rows(i, carry):
            rows = pl.ds(al(i * 32, 8), 32)
            out = self.zb[0, j, rows, :].astype(F32) + self.yfd[j, rows, :].astype(F32) + self.yfu[j, rows, :].astype(F32)
            done(rows, out)
            return carry

        lax.fori_loop(0, self.ch // 32, some_rows, 0)

    def drain(self):
        h = self.h
        for kind, every in enumerate((self.zb.at[2, :, 0:h], self.zb.at[2, :, h:], self.zb.at[1], self.zb.at[3])):
            remote(every, every, self.ss.at[kind], self.rs.at[kind, 0], self.at.up).wait_send()


def attention_kernel(
    units, x_hbm, turn_hbm, base_hbm, wq, wk, wv, wo, wg_t, wu_t,
    h_hbm, w_all, hg_all,
    x_ref, turn_ref, base_ref, h_ref, xc, xg, hg, cos_all, sin_all, st_own, st_in, s1, s2, wb, wob, part, precv, qb, kvo, kvp, og, zb, ya, yb, yfd, yfu, own, drel_a, drel_b,
    sxe, rxe, sst, rst, sy, ry, syh, ryh, sd, rd, swa, rwa, swo, rwo, swp, rwp, lw, so, ro, spr, rpr, skv, rkv, sog, rog, syr, ryr,
    lg, sds, rds, sdo, rdo, sdf, rdf, sdp, rdp, shx, rhx, shy, rhy, shz, rhz, lh, lx,
):
    at = Place()
    x, c, y = at.x, at.c, at.y
    ch, kc = xc.shape[1], xc.shape[2]
    kd = wq.shape[0]
    hc = qb.shape[2]
    fc, f_a = w_all.shape[1], drel_a.shape[1]
    width = 2 * xg.shape[3]
    kh = div(x, 2)
    ng = rem(div(x + 1, 2), 2)
    gather = Spread(at, xc, xg, units, (s1, s2), None, None, sy, ry, syh, ryh)
    reduce = Reduce(at, zb, ya, yb, yfd, yfu, syr, ryr)
    ahead = Spread(at, h_ref, hg, ((0, 0, ch // 2, 0), (0, ch // 2, ch // 2, 0)), (s1, s2), shx, rhx, shy, rhy, shz, rhz)
    weights = (wq, wk, wv)

    def half_cols(core):
        return pl.ds(al(core * kd, 128), kd)

    def x_rows(j, core):
        return pl.ds(al((2 * j + core) * ch, 8), ch)

    def x_pair(j):
        return remote(x_ref.at[x_rows(j, 1 - c)], xc.at[j, :, half_cols(c)], sd.at[0], rd.at[j], at.partner)

    def pair_cols(xx):
        return pl.ds(al(rem(xx, 2) * kc, 128), kc)

    def xe_copy(u, xx):
        j, lo, n, _ = units[u]
        rows = pl.ds(lo, n)
        return remote(xc.at[j, rows], xg.at[y, j, rows, pair_cols(xx)], sxe.at[0], rxe.at[u], at.pa)

    def st_copy(u):
        j, lo, n, _ = units[u]
        rows = pl.ds(lo // 4, n // 4)
        return remote(st_own.at[j, rows], st_in.at[j, rows], sst.at[0], rst.at[u], at.pb)

    def XP(j):
        x_pair(j).start()

    arrived = []

    def XE(u):
        j, lo, n, _ = units[u]
        if j not in arrived:
            arrived.append(j)
            dst = xc.at[j, :, half_cols(1 - c)]
            remote(dst, dst, sd.at[0], rd.at[j], at.partner).wait_recv()
        xe_copy(u, x).start()
        xg[y, j, lo : lo + n, pair_cols(x)] = xc[j, lo : lo + n]

    def ST(u):
        j, lo, n, _ = units[u]
        xe_copy(u, at.xa).wait_recv()
        quarter = n // 4
        lane = lax.broadcasted_iota(jnp.int32, (quarter, 128), 1)
        lane_sums(xg.at[y, j], lo, n, s1, s2)
        packed = jnp.zeros((quarter, 128), F32)
        for g in range(4):
            rows = pl.ds(g * quarter, quarter)
            total, square = (jnp.sum(t[rows, :], axis=-1, keepdims=True) for t in (s1, s2))
            packed = jnp.where(lane // 32 == g, jnp.where(lane % 32 < 16, total, square), packed)
        st_own[j, lo // 4 : lo // 4 + quarter, :] = packed
        st_copy(u).start()

    def N(u):
        j, lo, n, _ = units[u]
        st_copy(u).wait_recv()
        quarter = n // 4
        at_rows = slice(lo // 4, lo // 4 + quarter)
        moments = (st_own[j, at_rows, :] + st_in[j, at_rows, :]) / width
        for g in range(4):
            mean = moments[:, 32 * g : 32 * g + 1]
            var = moments[:, 32 * g + 16 : 32 * g + 17] - mean * mean
            rows = pl.ds(g * quarter, quarter)
            s1[rows, :] = jnp.broadcast_to(mean, (quarter, 128))
            s2[rows, :] = jnp.broadcast_to(lax.rsqrt(var + EPS), (quarter, 128))
        scale_rows(xg.at[y, j], lo, n, s1, s2)
        gather.YR(u)

    def w_rows(xx, core):
        return pl.ds(al(rem(xx, 2) * kc + core * kd, 128), kd)

    def w_part(group, half, i):
        side = kh if half else 1 - kh
        return weights[i].at[:, pl.ds(al((2 * group + side) * hc, 128), hc)]

    def w_cols(half, i):
        return pl.ds(half * 3 * hc + i * hc, hc)

    def wa_copy(half, i, xx):
        return remote(w_part(1 - ng, half, i), wb.at[w_rows(xx, c), w_cols(half, i)], swa.at[0], rwa.at[half, i], at.pa)

    def wo_copy(half, i, core):
        return remote(w_part(ng, half, i), wb.at[w_rows(x, core), w_cols(half, i)], swo.at[0], rwo.at[half, i], at.partner)

    def w_local(half, i):
        return pltpu.make_async_copy(w_part(ng, half, i), wb.at[w_rows(x, c), w_cols(half, i)], lw.at[half, i])

    def wp_copy(half, core):
        ref = wb.at[w_rows(at.xa, core), pl.ds(half * 3 * hc, 3 * hc)]
        return remote(ref, ref, swp.at[0], rwp.at[half], at.partner)

    o_local = pltpu.make_async_copy(wo, wob.at[:, half_cols(c)], lw.at[2, 0])
    o_pair = remote(wo, wob.at[:, half_cols(c)], so.at[0], ro.at[0], at.partner)
    pieces = [(half, i) for half in range(2) for i in range(3)]

    def WOP():
        for half, i in pieces:
            wo_copy(half, i, c).start()
        o_pair.start()

    def WA(half):
        for i in range(3):
            wa_copy(half, i, x).start()

    def WP(half):
        for i in range(3):
            wa_copy(half, i, at.xa).wait_recv()
        wp_copy(half, c).start()

    w_halves = [0, 1]

    def w_ready(half):
        if half not in w_halves:
            return
        w_halves.remove(half)
        for i in range(3):
            w_local(half, i).wait()
            wo_copy(half, i, 1 - c).wait_recv()
        wp_copy(half, 1 - c).wait_recv()
        if half:
            own_out()

    def own_out():
        for m in range(2):
            d_in(m).wait()
            d_out(m).start()
            d_pair(m, 3, c).start()

    def o_ready():
        o_local.wait()
        dst = wob.at[:, half_cols(1 - c)]
        remote(dst, dst, so.at[0], ro.at[0], at.partner).wait_recv()

    mlp_weights = (wg_t, wu_t)
    parts = ((0, f_a), (f_a, fc - f_a))

    def d_src(m, xx, p):
        return mlp_weights[m].at[pl.ds(al(xx * fc + parts[p][0], 8), parts[p][1])]

    def d_dst(m, xx, p):
        return w_all.at[m, pl.ds(*parts[p]), pl.ds(al((2 * xx + c) * kd, 128), kd)]

    def s_copy(d, m, p, xx):
        to, dev = ((at.xa, at.pa), (at.xb, at.pb))[d]
        return remote(d_src(m, to, p), d_dst(m, xx, p), sds.at[d], rds.at[d, m, p], dev)

    def o_copy(d, m):
        return remote(d_src(m, at.xo, d), (drel_a, drel_b)[d].at[m], sdo.at[d], rdo.at[d, m], (at.pa, at.pb)[d])

    def f_copy(d, m, xx):
        return remote((drel_a, drel_b)[d].at[m], d_dst(m, xx, d), sdf.at[d], rdf.at[d, m], (at.pb, at.pa)[d])

    def d_in(m):
        return pltpu.make_async_copy(mlp_weights[m].at[pl.ds(al(x * fc, 8), fc)], own.at[m], lg.at[0, m])

    def d_all(m, xx, core):
        return w_all.at[m, :, pl.ds(al((2 * xx + core) * kd, 128), kd)]

    def d_out(m):
        return pltpu.make_async_copy(own.at[m], d_all(m, x, c), lg.at[1, m])

    def d_pair(m, k, core):
        dst = d_all(m, (at.xa, at.xb, at.xo, x)[k], core)
        return remote(own.at[m] if k == 3 else dst, dst, sdp.at[0], rdp.at[m, k], at.partner)

    def S(link, m, p):
        s_copy("ab".index(link), m, p, x).start()

    def O(link, m):
        o_copy("ab".index(link), m).start()

    def F(link, m):
        d = "ba".index(link)
        o_copy(d, m).wait_recv()
        f_copy(d, m, (at.xa, at.xb)[d]).start()

    def DP(m):
        for d in range(2):
            for p in range(2):
                s_copy(d, m, p, (at.xa, at.xb)[d]).wait_recv()
            f_copy(d, m, at.xo).wait_recv()
        for k in range(3):
            d_pair(m, k, c).start()

    def pr_copy(n):
        return remote(part.at[n, :, pl.ds(0, 3 * hc)], precv.at[n], spr.at[0], rpr.at[n], at.pb)

    def project(g, first, size):
        def done(col, step, out):
            for i, (r, j) in enumerate(GROUPS[g]):
                part[r * NJ + j, :, pl.ds(al(first + col, 128), step)] = out[i * ch : (i + 1) * ch].astype(BF16)

        refs = [xg.at[gather.seqs[r], j] for r, j in GROUPS[g]]
        product(refs, wb.at[:, pl.ds(first, size)], wb.shape[0], size, done)

    split = {step[1] for step in ATTENTION_STEPS if step[0] == "Q"}

    def G(g):
        w_ready(0)
        for r, j in GROUPS[g]:
            gather.chunk_wait(r, j)
        if g in split:
            project(g, 0, 3 * hc)
        else:
            w_ready(1)
            project(g, 0, 6 * hc)
        for r, j in GROUPS[g]:
            pr_copy(r * NJ + j).start()

    def Q(g):
        w_ready(1)
        project(g, 3 * hc, 3 * hc)

    def kv_copy(r, j):
        s, n = gather.seqs[r], r * NJ + j
        return remote(kvo.at[s, j], kvp.at[s, j], skv.at[0], rkv.at[n], at.partner)

    def rotate(r, j):
        s, n = gather.seqs[r], r * NJ + j
        pr_copy(n).wait_recv()
        cos_t, sin_t = cos_all[j], sin_all[j]

        def total(col, size):
            mine = part[n, :, 3 * hc + col : 3 * hc + col + size]
            return (mine.astype(F32) + precv[n, :, col : col + size].astype(F32)).astype(BF16)

        def turned(col):
            v = total(col, HEAD_DIM).astype(F32)
            return (v * cos_t + pltpu.roll(v, HEAD_DIM // 2, axis=1) * sin_t).astype(BF16)

        for col in range(0, hc, HEAD_DIM):
            qb[n, :, col : col + HEAD_DIM] = turned(col)
            kvo[s, j, :, col : col + HEAD_DIM] = turned(hc + col)
        kvo[s, j, :, hc:] = total(2 * hc, hc)
        kv_copy(r, j).start()

    def R(g):
        for r, j in GROUPS[g]:
            rotate(r, j)

    def o_cols(xx):
        return pl.ds(al((2 * rem(div(xx + 1, 2), 2) + div(xx, 2)) * hc, 128), hc)

    cut = ch // 8

    def og_copy(kind, n):
        if kind < 2:
            ref = og.at[n, :, o_cols(x)]
        elif kind == 2:
            ref = og.at[n, pl.ds(0, cut), o_cols(at.xa)]
        else:
            ref = og.at[n, pl.ds(cut, ch - cut), o_cols(at.xb)]
        return remote(ref, ref, sog.at[kind], rog.at[kind, n], at.pa if kind in (0, 3) else at.pb)

    def og_wait(kind, n):
        xx = (at.xa, at.xb, at.xo, at.xo)[kind]
        rows = (pl.ds(0, ch), pl.ds(0, ch), pl.ds(0, cut), pl.ds(cut, ch - cut))[kind]
        dst = og.at[n, rows, o_cols(xx)]
        remote(dst, dst, sog.at[kind], rog.at[kind, n], at.pa).wait_recv()

    def attend(r, j, i):
        s, n = gather.seqs[r], r * NJ + j
        keys = (j + 1) * ch
        iq = lax.broadcasted_iota(jnp.int32, (ch, keys), 0) + j * ch
        ik = lax.broadcasted_iota(jnp.int32, (ch, keys), 1)
        own_ok = iq >= ik
        par_ok = ik < (j + c) * ch
        contract = (((1,), (1,)), ((), ()))
        cols = pl.ds(al(i * HEAD_DIM, 128), HEAD_DIM)
        v_cols = pl.ds(al(hc + i * HEAD_DIM, 128), HEAD_DIM)
        q = qb[n, :, cols]
        k_own = kvo[s, 0 : j + 1, :, cols].reshape(keys, HEAD_DIM)
        k_par = kvp[s, 0 : j + 1, :, cols].reshape(keys, HEAD_DIM)
        s_own = lax.dot_general(q, k_own, contract, preferred_element_type=F32) * HEAD_DIM**-0.5
        s_par = lax.dot_general(q, k_par, contract, preferred_element_type=F32) * HEAD_DIM**-0.5
        s_own = jnp.where(own_ok, s_own, -1e30)
        s_par = jnp.where(par_ok, s_par, -1e30)
        top = jnp.maximum(jnp.max(s_own, axis=1, keepdims=True), jnp.max(s_par, axis=1, keepdims=True))
        e_own, e_par = jnp.exp(s_own - top), jnp.exp(s_par - top)
        inv = 1.0 / (jnp.sum(e_own, axis=1, keepdims=True) + jnp.sum(e_par, axis=1, keepdims=True))
        v_own = kvo[s, 0 : j + 1, :, v_cols].reshape(keys, HEAD_DIM)
        v_par = kvp[s, 0 : j + 1, :, v_cols].reshape(keys, HEAD_DIM)
        out = jnp.dot((e_own * inv).astype(BF16), v_own, preferred_element_type=F32)
        out += jnp.dot((e_par * inv).astype(BF16), v_par, preferred_element_type=F32)
        og[n, :, pl.ds(al((2 * ng + kh) * hc + i * HEAD_DIM, 128), HEAD_DIM)] = out.astype(BF16)

    def A(g):
        for r, j in GROUPS[g]:
            kv_copy(r, j).wait_recv()

        def head(i, carry):
            for r, j in GROUPS[g]:
                attend(r, j, i)
            return carry

        lax.fori_loop(0, hc // HEAD_DIM, head, 0)
        for r, j in GROUPS[g]:
            og_copy(0, r * NJ + j).start()
            og_copy(1, r * NJ + j).start()

    def P(g):
        for r, j in GROUPS[g]:
            for kind in range(2):
                og_wait(kind, r * NJ + j)
                og_copy(kind + 2, r * NJ + j).start()

    def X(g):
        for r, j in GROUPS[g]:
            og_wait(2, r * NJ + j)
            og_wait(3, r * NJ + j)

        def done(col, size, out):
            for i, (r, j) in enumerate(GROUPS[g]):
                zb[r, j, :, pl.ds(al(col, 128), size)] = out[i * ch : (i + 1) * ch].astype(BF16)

        product([og.at[r * NJ + j] for r, j in GROUPS[g]], wob, wob.shape[0], kc, done)
        for r, j in GROUPS[g]:
            if r == 2:
                reduce.halves(j)

    def T(j):
        def done(rows, attn):
            h_ref[j, rows, :] = (xc[j, rows, :].astype(F32) + attn.astype(BF16).astype(F32)).astype(BF16)

        reduce.total(j, done)
        chunk_out(j).start()

    def chunk_out(j):
        return pltpu.make_async_copy(h_ref.at[j], h_hbm.at[j], lx.at[1 + j])

    def h_out(r, u):
        rows = pl.ds(u * (ch // 2), ch // 2)
        return pltpu.make_async_copy(hg.at[ahead.seqs[r], 0, rows], hg_all.at[ahead.seqs[r], rows], lh.at[r, u])

    kept = []

    def HF(u):
        if not kept:
            kept.append(u)
            ahead.keep_own()
        ahead.XF(0, u)

    def HY(u):
        ahead.YH(u)
        for r in (0, 1, 3):
            h_out(r, u).start()

    def HO(u):
        for d in range(2):
            ahead.yhalf_wait(d, u)
        h_out(2, u).start()

    def own_rows():
        for half, i in pieces:
            w_local(half, i).start()
        o_local.start()
        for m in range(2):
            d_in(m).start()
        x_in.wait()
        for j in range(NJ):
            xc[j, :, half_cols(c)] = x_ref[x_rows(j, c), :]

    x_in = pltpu.make_async_copy(x_hbm, x_ref, lx.at[0])
    x_in.start()
    tables = [pltpu.make_async_copy(src, dst, lx.at[1 + NJ + i]) for i, (src, dst) in enumerate(((turn_hbm, turn_ref), (base_hbm, base_ref)))]
    for copy in tables:
        copy.start()
    at.barrier(own_rows)

    def angles():
        for copy in tables:
            copy.wait()
        lane = lax.broadcasted_iota(jnp.int32, (ch, HEAD_DIM), 1)
        for j in range(NJ):
            base_cos, base_sin = base_ref[0, pl.ds(2 * j + c, 1), :], base_ref[1, pl.ds(2 * j + c, 1), :]
            cos_all[j] = base_cos * turn_ref[0] - base_sin * turn_ref[1]
            sine = base_sin * turn_ref[0] + base_cos * turn_ref[1]
            sin_all[j] = jnp.where(lane < HEAD_DIM // 2, -sine, sine)

    ops = {
        "XP": XP, "WOP": WOP, "XE": XE, "ST": ST, "N": N, "YH": gather.YH, "WA": WA, "WP": WP, "S": S, "O": O, "F": F, "DP": DP,
        "G": G, "Q": Q, "R": R, "A": A, "P": P, "X": X, "M": reduce.middle, "T": T,
        "HF": HF, "HH": lambda u: ahead.XH(0, u), "HN": lambda u: ahead.N(0, u), "HY": HY, "HO": HO,
    }
    def all_sent(ref, sem):
        remote(ref, ref, sem, ro.at[0], at.partner).wait_send()

    def sent():
        for m in range(2):
            for k in range(4):
                d_pair(m, k, 1 - c).wait_recv()
            d_out(m).wait()
        all_sent(w_all.at[:, :, pl.ds(0, 4 * kd)], sdp.at[0])
        for d in range(2):
            all_sent(w_all.at[:, :, pl.ds(0, kd)], sds.at[d])
            all_sent((drel_a, drel_b)[d], sdo.at[d])
            all_sent((drel_a, drel_b)[d], sdf.at[d])
            for u in range(len(units)):
                gather.ycopy(d, u).wait_send()
                gather.yhalf(d, u).wait_send()
        all_sent(x_ref.at[pl.ds(0, NJ * ch)], sd.at[0])
        all_sent(xc, sxe.at[0])
        all_sent(st_own, sst.at[0])
        reduce.drain()
        ahead.drain()
        for r in range(NX):
            for u in range(2):
                h_out(r, u).wait()
        o_pair.wait_send()
        for sem in (swa, swo, swp):
            all_sent(wb.at[pl.ds(0, kd)], sem.at[0])
        all_sent(part.at[:, :, pl.ds(0, 3 * hc)], spr.at[0])
        all_sent(kvo, skv.at[0])
        for kind, (lo, n) in enumerate(((0, ch), (0, ch), (0, cut), (cut, ch - cut))):
            all_sent(og.at[:, pl.ds(lo, n), o_cols(x)], sog.at[kind])

    waits = {"X": o_ready, "WP": angles}
    last = max(i for i, step in enumerate(ATTENTION_STEPS) if step[0] == "X")
    for i, step in enumerate(ATTENTION_STEPS):
        if step[0] in waits:
            waits.pop(step[0])()
        if i == last:
            sent()
        ops[step[0]](*step[1:])
    for j in range(NJ):
        chunk_out(j).wait()


def mlp_kernel(
    units, h_hbm, w_hbm, wdn, hg_hbm, y_ref,
    h_ref, xg, wt, raw, wd, ag, ar, act, s1, s2, zb, ya, yb, yfd, yfu, yst,
    sx, rx, sy, ry, syh, ryh, sa, ra, syr, ryr, sd, rd, lw, lwd, swd, rwd, lh, lo,
):
    at = Place()
    x, c, y = at.x, at.c, at.y
    ch, kc, h = h_ref.shape[1], h_ref.shape[2], h_ref.shape[1] // 2
    width = xg.shape[-1]
    kd = kc // 2
    fc, tiles = w_hbm.shape[1], wt.shape[1] // 256
    fm = (tiles - 1) * 128
    fr = fc - fm
    blocks, slots = 2 * tiles, raw.shape[0]
    gather = Spread(at, h_ref, xg, units, (s1, s2), sx, rx, sy, ry, syh, ryh)
    reduce = Reduce(at, zb, ya, yb, yfd, yfu, syr, ryr)

    def w_in(q):
        i, m = q // 2, q % 2
        n = min(128, fc - i * 128)
        return pltpu.make_async_copy(w_hbm.at[m, pl.ds(i * 128, n)], raw.at[q % slots, pl.ds(0, n)], lw.at[q])

    def WT(g):
        for q in range(g * blocks // 4, (g + 1) * blocks // 4):
            i, m, slot = q // 2, q % 2, q % slots
            w_in(q).wait()
            if fc < (i + 1) * 128:
                raw[slot, fc - i * 128 :, :] = jnp.zeros(((i + 1) * 128 - fc, width), BF16)

            def turn(k, carry, slot=slot, q=q):
                part = pl.ds(al(k * (width // 4), 128), width // 4)
                wt[part, q * 128 : (q + 1) * 128] = raw[slot, :, part].T
                return carry

            lax.fori_loop(0, 4, turn, 0)
            if q + slots < blocks:
                w_in(q + slots).start()

    def d_refs(q, core):
        cols = pl.ds(al(core * kd, 128), kd)
        main, rest = wdn.at[pl.ds(q * fc, fm)], wdn.at[pl.ds(q * fc + fm, fr)]
        return (main, wd.at[pl.ds(q * fm, fm), cols]), (rest, wd.at[pl.ds(NX * fm + q * 128, fr), cols])

    def d_own(q, k):
        src, dst = d_refs(q, c)[k]
        return pltpu.make_async_copy(src, dst, lwd.at[q, k])

    def d_pair(q, k, core):
        src, dst = d_refs(q, core)[k]
        return remote(src, dst, swd.at[q, k], rwd.at[q, k], at.partner)

    quarters = [(q, k) for q in range(NX) for k in range(2)]
    h_in_all = pltpu.make_async_copy(h_hbm, h_ref, lo.at[NJ])
    h_in_all.start()
    for q in range(slots):
        w_in(q).start()
    def h_in(s):
        return pltpu.make_async_copy(hg_hbm.at[s], xg.at[s, 0], lh.at[s])

    for s in range(NX):
        h_in(s).start()
    for q, k in quarters:
        d_own(q, k).start()
    for q in range(NX):
        wd[NX * fm + q * 128 + fr : NX * fm + (q + 1) * 128, :] = jnp.zeros((128 - fr, kc), BF16)
    at.barrier(h_in_all.wait)
    for q, k in quarters:
        d_pair(q, k, c).start()

    def a_refs(kind, n, xx):
        main, rest = pl.ds(al(xx * fm, 128), fm), pl.ds(al(xx * 128, 128), 128)
        if kind < 2:
            return ag.at[n, :, main], ar.at[n, :, rest]
        lo = (kind - 2) * h
        return ag.at[n, pl.ds(lo, h), main], ar.at[n, pl.ds(lo // 2, h // 2), rest]

    def a_copies(kind, n):
        refs = a_refs(kind, n, (x, x, at.xl, at.xr)[kind])
        return [remote(v, v, sa.at[kind, k], ra.at[kind, n, k], at.left if kind % 2 else at.right) for k, v in enumerate(refs)]

    def a_wait(kind, n):
        for k, v in enumerate(a_refs(kind, n, (at.xl, at.xr, at.xo, at.xo)[kind])):
            remote(v, v, sa.at[kind, k], ra.at[kind, n, k], at.right).wait_recv()

    def a_start(kind, n):
        for copy in a_copies(kind, n):
            copy.start()

    def G(g):
        for r, j in GROUPS[g]:
            gather.chunk_wait(r, j)

        def done(col, size, out):
            for k in range(0, size, 256):
                gate, up = out[:, k : k + 128].astype(BF16).astype(F32), out[:, k + 128 : k + 256].astype(BF16).astype(F32)
                value = (gate / (1.0 + jnp.exp(-gate)) * up).astype(BF16)
                act[0 : value.shape[0], pl.ds(al(div(col + k, 2), 128), 128)] = value

        product([xg.at[gather.seqs[r], j] for r, j in GROUPS[g]], wt, width, wt.shape[1], done)
        for i, (r, j) in enumerate(GROUPS[g]):
            n, lo = r * NJ + j, i * ch
            ag[n, :, pl.ds(al(x * fm, 128), fm)] = act[lo : lo + ch, :fm]
            below = pltpu.roll(act[lo + h : lo + ch, fm:].astype(F32), 64, axis=1)
            ar[n, :, pl.ds(al(x * 128, 128), 128)] = (act[lo : lo + h, fm:].astype(F32) + below).astype(BF16)
            for kind in range(2):
                a_start(kind, n)

    def P(g):
        for r, j in GROUPS[g]:
            for kind in range(2):
                a_wait(kind, r * NJ + j)
                a_start(kind + 2, r * NJ + j)

    def X(g):
        for r, j in GROUPS[g]:
            n = r * NJ + j
            for kind in (2, 3):
                a_wait(kind, n)
            lane = lax.broadcasted_iota(jnp.int32, (h, 128), 1)
            for q in range(NX):
                cols = pl.ds(NX * fm + q * 128, 128)
                rest = ar[n, :, q * 128 : (q + 1) * 128].astype(F32)
                ag[n, 0:h, cols] = jnp.where(lane < 64, rest, 0.0).astype(BF16)
                ag[n, h:, cols] = jnp.where(lane < 64, pltpu.roll(rest, 64, axis=1), 0.0).astype(BF16)

        def done(col, size, out):
            for i, (r, j) in enumerate(GROUPS[g]):
                zb[r, j, :, pl.ds(al(col, 128), size)] = out[i * ch : (i + 1) * ch].astype(BF16)

        product([ag.at[r * NJ + j] for r, j in GROUPS[g]], wd, wd.shape[0], kc, done, 512 if len(GROUPS[g]) == 1 else 256)
        for r, j in GROUPS[g]:
            if r == 2:
                reduce.halves(j)

    def y_rows(j, core):
        return pl.ds(al((2 * j + core) * ch, 8), ch)

    def y_copy(j):
        return remote(yst.at[1 - c, j], y_ref.at[y_rows(j, c)], sd.at[j], rd.at[j], at.partner)

    def y_own(j):
        return pltpu.make_async_copy(yst.at[c, j], y_ref.at[y_rows(j, c)], lo.at[j])

    def y_wait(j):
        dst = y_ref.at[y_rows(j, 1 - c)]
        remote(dst, dst, sd.at[j], rd.at[j], at.partner).wait_recv()

    def T(j):
        def done(rows, mlp):
            out = (h_ref[j, rows, :].astype(F32) + mlp.astype(BF16).astype(F32)).astype(BF16)
            yst[0, j, rows, :] = out[:, :kd]
            yst[1, j, rows, :] = out[:, kd:]

        reduce.total(j, done)
        y_copy(j).start()
        y_own(j).start()

    ops = {"G": G, "P": P, "X": X, "M": reduce.middle, "T": T, "WT": WT}
    for name in ("YR", "YRH", "YH", "XF", "XH", "N"):
        ops[name] = getattr(gather, name)
    waits = {
        "N": gather.keep_own,
        "G": lambda: [h_in(s).wait() for s in range(NX)],
        "X": lambda: [(d_own(q, k).wait(), d_pair(q, k, 1 - c).wait_recv()) for q, k in quarters],
    }
    def sent():
        gather.drain()
        reduce.drain()
        for q, k in quarters:
            d_pair(q, k, c).wait_send()

        for kind in range(4):
            for k, every in enumerate(a_refs(kind, slice(None), x)):
                remote(every, every, sa.at[kind, k], ra.at[kind, 0, k], at.right).wait_send()

    for step in MLP_STEPS:
        if step[0] in waits:
            waits.pop(step[0])()
        ops[step[0]](*step[1:])
    sent()
    for j in range(NJ):
        y_copy(j).wait_send()
        y_own(j).wait()
        y_wait(j)


def vmem(*shape, dtype=BF16):
    return pltpu.VMEM(shape, dtype)


def sems(*shape):
    return pltpu.SemaphoreType.DMA(shape)


def solution(mesh):
    assert mesh.shape["tx"] == 2 * NX and mesh.shape["ty"] == NX
    act_spec = P(("dp", "ty"), None, "tx")
    col_spec = P("tx", "ty")
    row_spec = P("ty", "tx")
    any_spec = pl.BlockSpec(memory_space=pl.ANY)
    vmem_spec = pl.BlockSpec(memory_space=pltpu.VMEM)

    def layer(x_blk, w_q, w_k, w_v, w_o, w_gate, w_up, w_down):
        _, seq, kd = x_blk.shape
        kc, width = 2 * kd, 2 * NX * kd
        ch = seq // (2 * NJ)
        h = ch // 2
        row_heads = w_q.shape[1]
        hc = row_heads // NX
        fc = w_down.shape[0] // NX
        assert hc % HEAD_DIM == 0
        tiles = (fc + 127) // 128
        f_a = (fc // 2 + 15) // 16 * 16

        inv_freq = THETA ** (-2.0 * np.arange(HEAD_DIM // 2) / HEAD_DIM)
        inv_freq = np.concatenate([inv_freq, inv_freq])
        turn = np.arange(ch)[:, None] * inv_freq
        base = np.arange(2 * NJ)[:, None] * ch * inv_freq
        turn = jnp.asarray(np.stack([np.cos(turn), np.sin(turn)]), F32)
        base = jnp.asarray(np.stack([np.cos(base), np.sin(base)]), F32)

        reduce_scratch = [vmem(NX, NJ, ch, kc), vmem(NJ, h, kc), vmem(NJ, ch - h, kc), vmem(NJ, ch, kc), vmem(NJ, ch, kc)]
        units = ((0, 0, h, 0), (0, h, h, 0)) + tuple((j, 0, ch, 0) for j in range(1, NJ))
        n_u = len(units)
        h_blk, w_all, hg_all = pl.pallas_call(
            functools.partial(attention_kernel, units),
            out_shape=(
                jax.ShapeDtypeStruct((NJ, ch, kc), BF16),
                jax.ShapeDtypeStruct((2, fc, width), BF16),
                jax.ShapeDtypeStruct((NX, ch, width), BF16),
            ),
            in_specs=[any_spec] * 9,
            out_specs=(any_spec, any_spec, any_spec),
            scratch_shapes=[
                vmem(seq, kd), vmem(2, ch, HEAD_DIM, dtype=F32), vmem(2, 2 * NJ, HEAD_DIM, dtype=F32),
                vmem(NJ, ch, kc), vmem(NJ, ch, kc), vmem(NX, NJ, ch, 2 * kc), vmem(NX, 1, ch, width), vmem(NJ, ch, HEAD_DIM, dtype=F32), vmem(NJ, ch, HEAD_DIM, dtype=F32),
                vmem(NJ, ch // 4, 128, dtype=F32), vmem(NJ, ch // 4, 128, dtype=F32), vmem(ch, 128, dtype=F32), vmem(ch, 128, dtype=F32),
                vmem(2 * kc, 6 * hc), vmem(row_heads, kc), vmem(NCH, ch, 6 * hc), vmem(NCH, ch, 3 * hc), vmem(NCH, ch, hc),
                vmem(NX, NJ, ch, 2 * hc), vmem(NX, NJ, ch, 2 * hc), vmem(NCH, ch, row_heads), *reduce_scratch,
                vmem(2, fc, kd), vmem(2, f_a, kd), vmem(2, fc - f_a, kd),
                sems(1), sems(n_u), sems(1), sems(n_u), sems(2, n_u), sems(2, n_u), sems(2, n_u), sems(2, n_u),
                sems(1), sems(NJ), sems(1), sems(2, 3), sems(1), sems(2, 3), sems(1), sems(2), sems(3, 3), sems(1), sems(1),
                sems(1), sems(NCH), sems(1), sems(NCH), sems(4), sems(4, NCH), sems(4), sems(4, NJ),
                sems(2, 2), sems(2), sems(2, 2, 2), sems(2), sems(2, 2), sems(2), sems(2, 2), sems(1), sems(2, 4),
                sems(4, 2), sems(4, 2), sems(2, 2), sems(2, 2), sems(2, 2), sems(2, 2), sems(NX, 2), sems(3 + NJ),
            ],
            compiler_params=pltpu.CompilerParams(collective_id=0, has_side_effects=True, vmem_limit_bytes=VMEM_LIMIT),
            name="attention_part",
        )(x_blk[0], turn, base, w_q, w_k, w_v, w_o, w_gate.T, w_up.T)

        units = ((1, 0, h, 1), (1, h, h, 0)) + tuple((j, 0, ch, 0) for j in range(2, NJ))
        n_u, n_x = len(units), len(units) + 3
        y_blk = pl.pallas_call(
            functools.partial(mlp_kernel, units),
            out_shape=jax.ShapeDtypeStruct((seq, kd), BF16),
            in_specs=[any_spec] * 4,
            out_specs=any_spec,
            scratch_shapes=[
                vmem(NJ, ch, kc),
                vmem(NX, NJ, ch, width), vmem(width, tiles * 256), vmem(3, 128, width),
                vmem(NX * tiles * 128, kc), vmem(NCH, ch, NX * tiles * 128), vmem(NCH, h, NX * 128), vmem(2 * ch, tiles * 128),
                vmem(ch, 128, dtype=F32), vmem(ch, 128, dtype=F32),
                *reduce_scratch, vmem(2, NJ, ch, kd),
                sems(4, n_x), sems(4, n_x), sems(2, n_u), sems(2, n_u), sems(2, n_u), sems(2, n_u),
                sems(4, 2), sems(4, NCH, 2), sems(4), sems(4, NJ), sems(NJ), sems(NJ),
                sems(2 * tiles), sems(NX, 2), sems(NX, 2), sems(NX, 2), sems(NX), sems(NJ + 1),
            ],
            compiler_params=pltpu.CompilerParams(collective_id=1, has_side_effects=True, vmem_limit_bytes=VMEM_LIMIT),
            name="mlp_part",
        )(h_blk, w_all, w_down, hg_all)
        return y_blk[None]

    return jax.shard_map(
        layer,
        mesh=mesh,
        in_specs=(act_spec, col_spec, col_spec, col_spec, row_spec, col_spec, col_spec, row_spec),
        out_specs=act_spec,
        check_vma=False,
    )
```

```python
import functools

import jax
import jax.numpy as jnp
import numpy as np
from jax import lax
from jax.experimental import pallas as pl
from jax.experimental.pallas import tpu as pltpu
from jax.sharding import PartitionSpec as P

HEAD_DIM = 128
EPS = 1e-5
THETA = 10000.0
MESH = pl.DeviceIdType.MESH
F32 = jnp.float32
BF16 = jnp.bfloat16
NX = 4
NJ = 4
NCH = 16
VMEM_LIMIT = 67_043_328
GROUPS = (*(((0, j),) for j in range(NJ)), *(((3, j), (1, j)) for j in range(NJ)), *(((2, j),) for j in range(NJ)))


def rem(a, b):
    return lax.rem(a, jnp.int32(b))


def div(a, b):
    return lax.div(a, jnp.int32(b))


def al(v, m):
    return pl.multiple_of(v, m)


def remote(src, dst, ssem, rsem, dev):
    return pltpu.make_async_remote_copy(src_ref=src, dst_ref=dst, send_sem=ssem, recv_sem=rsem, device_id=dev, device_id_type=MESH)


ATTENTION_STEPS = (
    ("WA", 0), ("XP", 1), ("S", "b", 0, 1), ("XP", 0), ("XE", 1), ("XE", 0), ("XE", 2), ("XP", 2), ("S", "b", 0, 0), ("XP", 3),
    ("S", "b", 1, 0), ("ST", 1), ("WP", 0), ("WA", 1), ("O", "b", 1), ("ST", 0), ("N", 1), ("O", "b", 0), ("ST", 2),
    ("S", "b", 1, 1), ("WOP",), ("N", 0), ("G", 0), ("XE", 3), ("YH", 1), ("YH", 0), ("S", "a", 0, 1), ("N", 2), ("WP", 1),
    ("G", 8), ("G", 4), ("ST", 3), ("Q", 8), ("Q", 0), ("R", 8), ("XE", 4), ("A", 8), ("F", "a", 1), ("YH", 2), ("G", 5),
    ("R", 4), ("ST", 4), ("N", 3), ("P", 8), ("G", 9), ("A", 4), ("R", 0), ("S", "a", 1, 1), ("X", 8), ("G", 1), ("N", 4),
    ("R", 5), ("A", 0), ("R", 9), ("P", 4), ("A", 9), ("A", 5), ("G", 2), ("P", 0), ("X", 4), ("M", 0), ("P", 9),
    ("S", "a", 1, 0), ("YH", 3), ("G", 6), ("P", 5), ("X", 0), ("T", 0), ("HF", 1), ("HF", 0), ("R", 2), ("X", 9), ("R", 1),
    ("A", 1), ("YH", 4), ("X", 5), ("M", 1), ("HH", 1), ("O", "a", 0), ("G", 10), ("R", 6), ("HH", 0), ("G", 7), ("O", "a", 1),
    ("HN", 1), ("R", 10), ("G", 11), ("A", 10), ("A", 6), ("HN", 0), ("R", 7), ("A", 2), ("HY", 1), ("A", 7), ("R", 11),
    ("P", 10), ("A", 11), ("P", 6), ("G", 3), ("P", 7), ("P", 11), ("F", "b", 1), ("F", "a", 0), ("X", 10), ("HY", 0),
    ("S", "a", 0, 0), ("F", "b", 0), ("R", 3), ("X", 11), ("A", 3), ("X", 6), ("HO", 1), ("X", 7), ("P", 1), ("P", 2),
    ("M", 2), ("M", 3), ("DP", 1), ("DP", 0), ("P", 3), ("HO", 0), ("X", 1), ("T", 1), ("X", 2), ("T", 2), ("X", 3), ("T", 3),
)
MLP_STEPS = (
    ("XF", 0, 1), ("XF", 0, 0), ("WT", 0), ("YR", 0), ("WT", 1), ("XH", 0, 1), ("XF", 0, 3), ("YRH", 0), ("XF", 3, 0),
    ("N", 0, 1), ("XH", 0, 3), ("XF", 1, 0), ("XF", 2, 0), ("WT", 2), ("WT", 3), ("N", 0, 3), ("XF", 0, 2), ("G", 4),
    ("YH", 1), ("G", 0), ("XH", 2, 0), ("G", 8), ("XH", 1, 0), ("XH", 0, 0), ("XH", 3, 0), ("XH", 0, 2), ("G", 3), ("YH", 3),
    ("G", 7), ("N", 3, 0), ("N", 0, 2), ("N", 1, 0), ("P", 8), ("N", 2, 0), ("G", 9), ("G", 11), ("P", 4), ("G", 5), ("P", 11),
    ("X", 8), ("P", 7), ("P", 9), ("X", 4), ("YH", 2), ("G", 6), ("X", 11), ("X", 7), ("P", 5), ("X", 9), ("N", 0, 0),
    ("M", 0), ("G", 10), ("G", 1), ("M", 3), ("X", 5), ("M", 1), ("P", 10), ("P", 6), ("P", 0), ("G", 2), ("X", 10), ("P", 3),
    ("P", 1), ("X", 6), ("M", 2), ("P", 2), ("X", 0), ("T", 0), ("X", 3), ("T", 3), ("X", 1), ("T", 1), ("X", 2), ("T", 2),
)


class Place:
    def __init__(self):
        tx, ty = lax.axis_index("tx"), lax.axis_index("ty")
        self.x, self.c, self.y = div(tx, 2), rem(tx, 2), ty
        x, c, y = self.x, self.c, self.y
        self.xr, self.xl, self.xo = rem(x + 1, NX), rem(x + 3, NX), rem(x + 2, NX)
        self.yu, self.yd, self.yo = rem(y + 1, NX), rem(y + 3, NX), rem(y + 2, NX)
        self.right = {"tx": self.xr * 2 + c, "ty": y}
        self.left = {"tx": self.xl * 2 + c, "ty": y}
        self.up = {"tx": tx, "ty": self.yu}
        self.down = {"tx": tx, "ty": self.yd}
        self.partner = {"tx": x * 2 + 1 - c, "ty": y}
        self.xa, self.xb = x + 1 - 2 * rem(x, 2), rem(x + 3 + 2 * rem(x, 2), NX)
        self.pa, self.pb = {"tx": self.xa * 2 + c, "ty": y}, {"tx": self.xb * 2 + c, "ty": y}

    def barrier(self, between):
        sem = pltpu.get_barrier_semaphore()
        for dev in (self.right, self.left, self.up, self.down, self.partner):
            pl.semaphore_signal(sem, inc=1, device_id=dev, device_id_type=MESH)
        between()
        pl.semaphore_wait(sem, 5)


class Spread:
    def __init__(self, at, src, xg, units, sums, sx, rx, sy, ry, syh, ryh):
        self.sums = sums
        self.at, self.src, self.xg, self.units, self.kc = at, src, xg, units, src.shape[2]
        self.sx, self.rx, self.sy, self.ry, self.syh, self.ryh = sx, rx, sy, ry, syh, ryh
        pairs = [(r, u) for u, unit in enumerate(units) for r in ((0, 3, 1, 2) if unit[3] else (0,))]
        self.index = {pair: i for i, pair in enumerate(pairs)}
        self.seqs = (at.y, at.yu, at.yo, at.yd)

    def cols(self, x):
        return pl.ds(al(x * self.kc, 128), self.kc)

    def keep_own(self):
        for j in {unit[0]: 0 for unit in self.units}:
            self.xg[self.at.y, j, :, self.cols(self.at.x)] = self.src[j]

    def xcopy(self, kind, r, u):
        at, s = self.at, self.seqs[r]
        j, lo, n, _ = self.units[u]
        i = self.index[r, u]
        if kind < 2:
            dst = self.xg.at[s, j, pl.ds(lo, n), self.cols(at.x)]
            src = self.src.at[j, pl.ds(lo, n)] if r == 0 else dst
        elif kind == 2:
            src = dst = self.xg.at[s, j, pl.ds(lo, n // 2), self.cols(at.xl)]
        else:
            src = dst = self.xg.at[s, j, pl.ds(lo + n // 2, n // 2), self.cols(at.xr)]
        return remote(src, dst, self.sx.at[kind, i], self.rx.at[kind, i], at.left if kind % 2 else at.right)

    def xwait(self, kind, r, u):
        at = self.at
        j, lo, n, _ = self.units[u]
        i = self.index[r, u]
        x = (at.xl, at.xr, at.xo, at.xo)[kind]
        rows = (pl.ds(lo, n), pl.ds(lo, n), pl.ds(lo, n // 2), pl.ds(lo + n // 2, n // 2))[kind]
        dst = self.xg.at[self.seqs[r], j, rows, self.cols(x)]
        remote(dst, dst, self.sx.at[kind, i], self.rx.at[kind, i], at.right).wait_recv()

    def yref(self, s, u, lo, n):
        j, _, _, first = self.units[u]
        rows = pl.ds(lo, n)
        return self.xg.at[s, j, rows, self.cols(self.at.x)] if first else self.xg.at[s, j, rows]

    def ycopy(self, d, u):
        j, lo, n, first = self.units[u]
        dst = self.yref(self.at.y, u, lo, n)
        src = self.src.at[j, pl.ds(lo, n)] if first else dst
        return remote(src, dst, self.sy.at[d, u], self.ry.at[d, u], self.at.down if d else self.at.up)

    def ywait(self, d, u):
        _, lo, n, _ = self.units[u]
        dst = self.yref(self.at.yu if d else self.at.yd, u, lo, n)
        remote(dst, dst, self.sy.at[d, u], self.ry.at[d, u], self.at.up).wait_recv()

    def yhalf(self, d, u):
        _, lo, n, _ = self.units[u]
        ref = self.yref(self.at.yu if d else self.at.yd, u, lo + d * (n // 2), n // 2)
        return remote(ref, ref, self.syh.at[d, u], self.ryh.at[d, u], self.at.down if d else self.at.up)

    def yhalf_wait(self, d, u):
        _, lo, n, _ = self.units[u]
        dst = self.yref(self.at.yo, u, lo + d * (n // 2), n // 2)
        remote(dst, dst, self.syh.at[d, u], self.ryh.at[d, u], self.at.up).wait_recv()

    def YR(self, u):
        for d in range(2):
            self.ycopy(d, u).start()

    def YH(self, u):
        for d in range(2):
            self.ywait(d, u)
            self.yhalf(d, u).start()

    YRH = YH

    def XF(self, r, u):
        if r == 2:
            for d in range(2):
                self.yhalf_wait(d, u)
        for kind in range(2):
            self.xcopy(kind, r, u).start()

    def XH(self, r, u):
        for kind in range(2):
            self.xwait(kind, r, u)
            self.xcopy(kind + 2, r, u).start()

    def N(self, r, u):
        j, lo, n, first = self.units[u]
        for kind in (2, 3):
            self.xwait(kind, r, u)
            self.xcopy(kind, r, u).wait_send()
        if r:
            for kind in range(2):
                self.xcopy(kind, r, u).wait_send()
        if r % 2:
            self.yhalf(0 if r == 3 else 1, u).wait_send()
        width, ref = self.xg.shape[-1], self.xg.at[self.seqs[r], j]
        s1, s2 = self.sums
        lane_sums(ref, lo, n, s1, s2)
        mean = jnp.sum(s1[0:n, :], axis=-1, keepdims=True) / width
        var = jnp.sum(s2[0:n, :], axis=-1, keepdims=True) / width - mean * mean
        s1[0:n, :] = jnp.broadcast_to(mean, (n, 128))
        s2[0:n, :] = jnp.broadcast_to(lax.rsqrt(var + EPS), (n, 128))
        scale_rows(ref, lo, n, s1, s2)
        if not first:
            self.YR(u)

    def chunk_wait(self, r, j):
        if r == 2:
            for u, unit in enumerate(self.units):
                if unit[0] == j and not unit[3]:
                    for d in range(2):
                        self.yhalf_wait(d, u)

    def drain(self):
        for u, unit in enumerate(self.units):
            for d in range(2):
                self.xcopy(d, 0, u).wait_send()
                self.ycopy(d, u).wait_send()
                if not unit[3]:
                    self.yhalf(d, u).wait_send()


def rows_of(refs):
    return refs[0][...] if len(refs) == 1 else jnp.concatenate([ref[...] for ref in refs], axis=0)


def product(refs, weight, depth, n_cols, done, step=256):
    step = 256 if n_cols % step else step

    def columns(i, carry):
        out = jnp.dot(rows_of(refs), weight[0:depth, pl.ds(al(i * step, 128), step)], preferred_element_type=F32)
        done(i * step, step, out)
        return carry

    lax.fori_loop(0, n_cols // step, columns, 0)


def lane_sums(ref, lo, n, s1, s2):
    width, rows, wide = ref.shape[-1], 32, 512

    def some_rows(i, carry):
        def some_columns(k, sums):
            a, b = sums
            v = ref[pl.ds(al(lo + i * rows, 8), rows), pl.ds(al(k * wide, 128), wide)].astype(F32)
            for c in range(0, wide, 128):
                part = v[:, c : c + 128]
                a, b = a + part, b + part * part
            return a, b

        zero = jnp.zeros((rows, 128), F32)
        a, b = lax.fori_loop(0, width // wide, some_columns, (zero, zero))
        s1[pl.ds(al(i * rows, 8), rows), :] = a
        s2[pl.ds(al(i * rows, 8), rows), :] = b
        return carry

    lax.fori_loop(0, n // rows, some_rows, 0)


def scale_rows(ref, lo, n, means, scales):
    width, rows, wide = ref.shape[-1], 32, 512

    def some_rows(i, carry):
        mean, scale = (t[pl.ds(al(i * rows, 8), rows), :] for t in (means, scales))

        def some_columns(k, carry):
            at_rows = pl.ds(al(lo + i * rows, 8), rows)
            for c in range(0, wide, 128):
                cols = pl.ds(al(k * wide + c, 128), 128)
                ref[at_rows, cols] = ((ref[at_rows, cols].astype(F32) - mean) * scale).astype(BF16)
            return carry

        lax.fori_loop(0, width // wide, some_columns, 0)
        return carry

    lax.fori_loop(0, n // rows, some_rows, 0)


class Reduce:
    def __init__(self, at, zb, ya, yb, yfd, yfu, ss, rs):
        self.at, self.zb, self.ya, self.yb, self.yfd, self.yfu, self.ss, self.rs = at, zb, ya, yb, yfd, yfu, ss, rs
        self.ch = zb.shape[2]
        self.h = self.ch // 2

    def copy(self, kind, j):
        at, h, ch = self.at, self.h, self.ch
        src, dst = (
            lambda: (self.zb.at[2, j, pl.ds(0, h)], self.ya.at[j]),
            lambda: (self.zb.at[2, j, pl.ds(h, ch - h)], self.yb.at[j]),
            lambda: (self.zb.at[1, j], self.yfd.at[j]),
            lambda: (self.zb.at[3, j], self.yfu.at[j]),
        )[kind]()
        return remote(src, dst, self.ss.at[kind], self.rs.at[kind, j], at.down if kind % 2 else at.up)

    def wait(self, kind, j):
        self.copy(kind, j).wait_recv()

    def halves(self, j):
        self.copy(0, j).start()
        self.copy(1, j).start()

    def middle(self, j):
        h = self.h

        def add(r, lo, part):
            def some_rows(i, carry):
                rows, src = pl.ds(al(lo + i * 32, 8), 32), pl.ds(al(i * 32, 8), 32)
                self.zb[r, j, rows, :] = (self.zb[r, j, rows, :].astype(F32) + part[j, src, :].astype(F32)).astype(BF16)
                return carry

            lax.fori_loop(0, h // 32, some_rows, 0)

        self.wait(0, j)
        add(1, 0, self.ya)
        self.copy(2, j).start()
        self.wait(1, j)
        add(3, h, self.yb)
        self.copy(3, j).start()

    def total(self, j, done):
        self.wait(2, j)
        self.wait(3, j)

        def some_rows(i, carry):
            rows = pl.ds(al(i * 32, 8), 32)
            out = self.zb[0, j, rows, :].astype(F32) + self.yfd[j, rows, :].astype(F32) + self.yfu[j, rows, :].astype(F32)
            done(rows, out)
            return carry

        lax.fori_loop(0, self.ch // 32, some_rows, 0)

    def drain(self):
        h = self.h
        for kind, every in enumerate((self.zb.at[2, :, 0:h], self.zb.at[2, :, h:], self.zb.at[1], self.zb.at[3])):
            remote(every, every, self.ss.at[kind], self.rs.at[kind, 0], self.at.up).wait_send()


def attention_kernel(
    units, x_hbm, turn_hbm, base_hbm, wq, wk, wv, wo, wg_t, wu_t,
    h_hbm, w_all, hg_all,
    x_ref, turn_ref, base_ref, h_ref, xc, xg, hg, cos_all, sin_all, st_own, st_in, s1, s2, wb, wob, part, precv, qb, kvo, kvp, og, zb, ya, yb, yfd, yfu, own, drel_a, drel_b,
    sxe, rxe, sst, rst, sy, ry, syh, ryh, sd, rd, swa, rwa, swo, rwo, swp, rwp, lw, so, ro, spr, rpr, skv, rkv, sog, rog, syr, ryr,
    lg, sds, rds, sdo, rdo, sdf, rdf, sdp, rdp, shx, rhx, shy, rhy, shz, rhz, lh, lx,
):
    at = Place()
    x, c, y = at.x, at.c, at.y
    ch, kc = xc.shape[1], xc.shape[2]
    kd = wq.shape[0]
    hc = qb.shape[2]
    fc, f_a = w_all.shape[1], drel_a.shape[1]
    width = 2 * xg.shape[3]
    kh = div(x, 2)
    ng = rem(div(x + 1, 2), 2)
    gather = Spread(at, xc, xg, units, (s1, s2), None, None, sy, ry, syh, ryh)
    reduce = Reduce(at, zb, ya, yb, yfd, yfu, syr, ryr)
    ahead = Spread(at, h_ref, hg, ((0, 0, ch // 2, 0), (0, ch // 2, ch // 2, 0)), (s1, s2), shx, rhx, shy, rhy, shz, rhz)
    weights = (wq, wk, wv)

    def half_cols(core):
        return pl.ds(al(core * kd, 128), kd)

    def x_rows(j, core):
        return pl.ds(al((2 * j + core) * ch, 8), ch)

    def x_pair(j):
        return remote(x_ref.at[x_rows(j, 1 - c)], xc.at[j, :, half_cols(c)], sd.at[0], rd.at[j], at.partner)

    def pair_cols(xx):
        return pl.ds(al(rem(xx, 2) * kc, 128), kc)

    def xe_copy(u, xx):
        j, lo, n, _ = units[u]
        rows = pl.ds(lo, n)
        return remote(xc.at[j, rows], xg.at[y, j, rows, pair_cols(xx)], sxe.at[0], rxe.at[u], at.pa)

    def st_copy(u):
        j, lo, n, _ = units[u]
        rows = pl.ds(lo // 4, n // 4)
        return remote(st_own.at[j, rows], st_in.at[j, rows], sst.at[0], rst.at[u], at.pb)

    def XP(j):
        x_pair(j).start()

    arrived = []

    def XE(u):
        j, lo, n, _ = units[u]
        if j not in arrived:
            arrived.append(j)
            dst = xc.at[j, :, half_cols(1 - c)]
            remote(dst, dst, sd.at[0], rd.at[j], at.partner).wait_recv()
        xe_copy(u, x).start()
        xg[y, j, lo : lo + n, pair_cols(x)] = xc[j, lo : lo + n]

    def ST(u):
        j, lo, n, _ = units[u]
        xe_copy(u, at.xa).wait_recv()
        quarter = n // 4
        lane = lax.broadcasted_iota(jnp.int32, (quarter, 128), 1)
        lane_sums(xg.at[y, j], lo, n, s1, s2)
        packed = jnp.zeros((quarter, 128), F32)
        for g in range(4):
            rows = pl.ds(g * quarter, quarter)
            total, square = (jnp.sum(t[rows, :], axis=-1, keepdims=True) for t in (s1, s2))
            packed = jnp.where(lane // 32 == g, jnp.where(lane % 32 < 16, total, square), packed)
        st_own[j, lo // 4 : lo // 4 + quarter, :] = packed
        st_copy(u).start()

    def N(u):
        j, lo, n, _ = units[u]
        st_copy(u).wait_recv()
        quarter = n // 4
        at_rows = slice(lo // 4, lo // 4 + quarter)
        moments = (st_own[j, at_rows, :] + st_in[j, at_rows, :]) / width
        for g in range(4):
            mean = moments[:, 32 * g : 32 * g + 1]
            var = moments[:, 32 * g + 16 : 32 * g + 17] - mean * mean
            rows = pl.ds(g * quarter, quarter)
            s1[rows, :] = jnp.broadcast_to(mean, (quarter, 128))
            s2[rows, :] = jnp.broadcast_to(lax.rsqrt(var + EPS), (quarter, 128))
        scale_rows(xg.at[y, j], lo, n, s1, s2)
        gather.YR(u)

    def w_rows(xx, core):
        return pl.ds(al(rem(xx, 2) * kc + core * kd, 128), kd)

    def w_part(group, half, i):
        side = kh if half else 1 - kh
        return weights[i].at[:, pl.ds(al((2 * group + side) * hc, 128), hc)]

    def w_cols(half, i):
        return pl.ds(half * 3 * hc + i * hc, hc)

    def wa_copy(half, i, xx):
        return remote(w_part(1 - ng, half, i), wb.at[w_rows(xx, c), w_cols(half, i)], swa.at[0], rwa.at[half, i], at.pa)

    def wo_copy(half, i, core):
        return remote(w_part(ng, half, i), wb.at[w_rows(x, core), w_cols(half, i)], swo.at[0], rwo.at[half, i], at.partner)

    def w_local(half, i):
        return pltpu.make_async_copy(w_part(ng, half, i), wb.at[w_rows(x, c), w_cols(half, i)], lw.at[half, i])

    def wp_copy(half, core):
        ref = wb.at[w_rows(at.xa, core), pl.ds(half * 3 * hc, 3 * hc)]
        return remote(ref, ref, swp.at[0], rwp.at[half], at.partner)

    o_local = pltpu.make_async_copy(wo, wob.at[:, half_cols(c)], lw.at[2, 0])
    o_pair = remote(wo, wob.at[:, half_cols(c)], so.at[0], ro.at[0], at.partner)
    pieces = [(half, i) for half in range(2) for i in range(3)]

    def WOP():
        for half, i in pieces:
            wo_copy(half, i, c).start()
        o_pair.start()

    def WA(half):
        for i in range(3):
            wa_copy(half, i, x).start()

    def WP(half):
        for i in range(3):
            wa_copy(half, i, at.xa).wait_recv()
        wp_copy(half, c).start()

    w_halves = [0, 1]

    def w_ready(half):
        if half not in w_halves:
            return
        w_halves.remove(half)
        for i in range(3):
            w_local(half, i).wait()
            wo_copy(half, i, 1 - c).wait_recv()
        wp_copy(half, 1 - c).wait_recv()
        if half:
            own_out()

    def own_out():
        for m in range(2):
            d_in(m).wait()
            d_out(m).start()
            d_pair(m, 3, c).start()

    def o_ready():
        o_local.wait()
        dst = wob.at[:, half_cols(1 - c)]
        remote(dst, dst, so.at[0], ro.at[0], at.partner).wait_recv()

    mlp_weights = (wg_t, wu_t)
    parts = ((0, f_a), (f_a, fc - f_a))

    def d_src(m, xx, p):
        return mlp_weights[m].at[pl.ds(al(xx * fc + parts[p][0], 8), parts[p][1])]

    def d_dst(m, xx, p):
        return w_all.at[m, pl.ds(*parts[p]), pl.ds(al((2 * xx + c) * kd, 128), kd)]

    def s_copy(d, m, p, xx):
        to, dev = ((at.xa, at.pa), (at.xb, at.pb))[d]
        return remote(d_src(m, to, p), d_dst(m, xx, p), sds.at[d], rds.at[d, m, p], dev)

    def o_copy(d, m):
        return remote(d_src(m, at.xo, d), (drel_a, drel_b)[d].at[m], sdo.at[d], rdo.at[d, m], (at.pa, at.pb)[d])

    def f_copy(d, m, xx):
        return remote((drel_a, drel_b)[d].at[m], d_dst(m, xx, d), sdf.at[d], rdf.at[d, m], (at.pb, at.pa)[d])

    def d_in(m):
        return pltpu.make_async_copy(mlp_weights[m].at[pl.ds(al(x * fc, 8), fc)], own.at[m], lg.at[0, m])

    def d_all(m, xx, core):
        return w_all.at[m, :, pl.ds(al((2 * xx + core) * kd, 128), kd)]

    def d_out(m):
        return pltpu.make_async_copy(own.at[m], d_all(m, x, c), lg.at[1, m])

    def d_pair(m, k, core):
        dst = d_all(m, (at.xa, at.xb, at.xo, x)[k], core)
        return remote(own.at[m] if k == 3 else dst, dst, sdp.at[0], rdp.at[m, k], at.partner)

    def S(link, m, p):
        s_copy("ab".index(link), m, p, x).start()

    def O(link, m):
        o_copy("ab".index(link), m).start()

    def F(link, m):
        d = "ba".index(link)
        o_copy(d, m).wait_recv()
        f_copy(d, m, (at.xa, at.xb)[d]).start()

    def DP(m):
        for d in range(2):
            for p in range(2):
                s_copy(d, m, p, (at.xa, at.xb)[d]).wait_recv()
            f_copy(d, m, at.xo).wait_recv()
        for k in range(3):
            d_pair(m, k, c).start()

    def pr_copy(n):
        return remote(part.at[n, :, pl.ds(0, 3 * hc)], precv.at[n], spr.at[0], rpr.at[n], at.pb)

    def project(g, first, size):
        def done(col, step, out):
            for i, (r, j) in enumerate(GROUPS[g]):
                part[r * NJ + j, :, pl.ds(al(first + col, 128), step)] = out[i * ch : (i + 1) * ch].astype(BF16)

        refs = [xg.at[gather.seqs[r], j] for r, j in GROUPS[g]]
        product(refs, wb.at[:, pl.ds(first, size)], wb.shape[0], size, done)

    split = {step[1] for step in ATTENTION_STEPS if step[0] == "Q"}

    def G(g):
        w_ready(0)
        for r, j in GROUPS[g]:
            gather.chunk_wait(r, j)
        if g in split:
            project(g, 0, 3 * hc)
        else:
            w_ready(1)
            project(g, 0, 6 * hc)
        for r, j in GROUPS[g]:
            pr_copy(r * NJ + j).start()

    def Q(g):
        w_ready(1)
        project(g, 3 * hc, 3 * hc)

    def kv_copy(r, j):
        s, n = gather.seqs[r], r * NJ + j
        return remote(kvo.at[s, j], kvp.at[s, j], skv.at[0], rkv.at[n], at.partner)

    def rotate(r, j):
        s, n = gather.seqs[r], r * NJ + j
        pr_copy(n).wait_recv()
        cos_t, sin_t = cos_all[j], sin_all[j]

        def total(col, size):
            mine = part[n, :, 3 * hc + col : 3 * hc + col + size]
            return (mine.astype(F32) + precv[n, :, col : col + size].astype(F32)).astype(BF16)

        def turned(col):
            v = total(col, HEAD_DIM).astype(F32)
            return (v * cos_t + pltpu.roll(v, HEAD_DIM // 2, axis=1) * sin_t).astype(BF16)

        for col in range(0, hc, HEAD_DIM):
            qb[n, :, col : col + HEAD_DIM] = turned(col)
            kvo[s, j, :, col : col + HEAD_DIM] = turned(hc + col)
        kvo[s, j, :, hc:] = total(2 * hc, hc)
        kv_copy(r, j).start()

    def R(g):
        for r, j in GROUPS[g]:
            rotate(r, j)

    def o_cols(xx):
        return pl.ds(al((2 * rem(div(xx + 1, 2), 2) + div(xx, 2)) * hc, 128), hc)

    cut = ch // 8

    def og_copy(kind, n):
        if kind < 2:
            ref = og.at[n, :, o_cols(x)]
        elif kind == 2:
            ref = og.at[n, pl.ds(0, cut), o_cols(at.xa)]
        else:
            ref = og.at[n, pl.ds(cut, ch - cut), o_cols(at.xb)]
        return remote(ref, ref, sog.at[kind], rog.at[kind, n], at.pa if kind in (0, 3) else at.pb)

    def og_wait(kind, n):
        xx = (at.xa, at.xb, at.xo, at.xo)[kind]
        rows = (pl.ds(0, ch), pl.ds(0, ch), pl.ds(0, cut), pl.ds(cut, ch - cut))[kind]
        dst = og.at[n, rows, o_cols(xx)]
        remote(dst, dst, sog.at[kind], rog.at[kind, n], at.pa).wait_recv()

    def attend(r, j, i):
        s, n = gather.seqs[r], r * NJ + j
        keys = (j + 1) * ch
        iq = lax.broadcasted_iota(jnp.int32, (ch, keys), 0) + j * ch
        ik = lax.broadcasted_iota(jnp.int32, (ch, keys), 1)
        own_ok = iq >= ik
        par_ok = ik < (j + c) * ch
        contract = (((1,), (1,)), ((), ()))
        cols = pl.ds(al(i * HEAD_DIM, 128), HEAD_DIM)
        v_cols = pl.ds(al(hc + i * HEAD_DIM, 128), HEAD_DIM)
        q = qb[n, :, cols]
        k_own = kvo[s, 0 : j + 1, :, cols].reshape(keys, HEAD_DIM)
        k_par = kvp[s, 0 : j + 1, :, cols].reshape(keys, HEAD_DIM)
        s_own = lax.dot_general(q, k_own, contract, preferred_element_type=F32) * HEAD_DIM**-0.5
        s_par = lax.dot_general(q, k_par, contract, preferred_element_type=F32) * HEAD_DIM**-0.5
        s_own = jnp.where(own_ok, s_own, -1e30)
        s_par = jnp.where(par_ok, s_par, -1e30)
        top = jnp.maximum(jnp.max(s_own, axis=1, keepdims=True), jnp.max(s_par, axis=1, keepdims=True))
        e_own, e_par = jnp.exp(s_own - top), jnp.exp(s_par - top)
        inv = 1.0 / (jnp.sum(e_own, axis=1, keepdims=True) + jnp.sum(e_par, axis=1, keepdims=True))
        v_own = kvo[s, 0 : j + 1, :, v_cols].reshape(keys, HEAD_DIM)
        v_par = kvp[s, 0 : j + 1, :, v_cols].reshape(keys, HEAD_DIM)
        out = jnp.dot((e_own * inv).astype(BF16), v_own, preferred_element_type=F32)
        out += jnp.dot((e_par * inv).astype(BF16), v_par, preferred_element_type=F32)
        og[n, :, pl.ds(al((2 * ng + kh) * hc + i * HEAD_DIM, 128), HEAD_DIM)] = out.astype(BF16)

    def A(g):
        for r, j in GROUPS[g]:
            kv_copy(r, j).wait_recv()

        def head(i, carry):
            for r, j in GROUPS[g]:
                attend(r, j, i)
            return carry

        lax.fori_loop(0, hc // HEAD_DIM, head, 0)
        for r, j in GROUPS[g]:
            og_copy(0, r * NJ + j).start()
            og_copy(1, r * NJ + j).start()

    def P(g):
        for r, j in GROUPS[g]:
            for kind in range(2):
                og_wait(kind, r * NJ + j)
                og_copy(kind + 2, r * NJ + j).start()

    def X(g):
        for r, j in GROUPS[g]:
            og_wait(2, r * NJ + j)
            og_wait(3, r * NJ + j)

        def done(col, size, out):
            for i, (r, j) in enumerate(GROUPS[g]):
                zb[r, j, :, pl.ds(al(col, 128), size)] = out[i * ch : (i + 1) * ch].astype(BF16)

        product([og.at[r * NJ + j] for r, j in GROUPS[g]], wob, wob.shape[0], kc, done)
        for r, j in GROUPS[g]:
            if r == 2:
                reduce.halves(j)

    def T(j):
        def done(rows, attn):
            h_ref[j, rows, :] = (xc[j, rows, :].astype(F32) + attn.astype(BF16).astype(F32)).astype(BF16)

        reduce.total(j, done)
        chunk_out(j).start()

    def chunk_out(j):
        return pltpu.make_async_copy(h_ref.at[j], h_hbm.at[j], lx.at[1 + j])

    def h_out(r, u):
        rows = pl.ds(u * (ch // 2), ch // 2)
        return pltpu.make_async_copy(hg.at[ahead.seqs[r], 0, rows], hg_all.at[ahead.seqs[r], rows], lh.at[r, u])

    kept = []

    def HF(u):
        if not kept:
            kept.append(u)
            ahead.keep_own()
        ahead.XF(0, u)

    def HY(u):
        ahead.YH(u)
        for r in (0, 1, 3):
            h_out(r, u).start()

    def HO(u):
        for d in range(2):
            ahead.yhalf_wait(d, u)
        h_out(2, u).start()

    def own_rows():
        for half, i in pieces:
            w_local(half, i).start()
        o_local.start()
        for m in range(2):
            d_in(m).start()
        x_in.wait()
        for j in range(NJ):
            xc[j, :, half_cols(c)] = x_ref[x_rows(j, c), :]

    x_in = pltpu.make_async_copy(x_hbm, x_ref, lx.at[0])
    x_in.start()
    tables = [pltpu.make_async_copy(src, dst, lx.at[1 + NJ + i]) for i, (src, dst) in enumerate(((turn_hbm, turn_ref), (base_hbm, base_ref)))]
    for copy in tables:
        copy.start()
    at.barrier(own_rows)

    def angles():
        for copy in tables:
            copy.wait()
        lane = lax.broadcasted_iota(jnp.int32, (ch, HEAD_DIM), 1)
        for j in range(NJ):
            base_cos, base_sin = base_ref[0, pl.ds(2 * j + c, 1), :], base_ref[1, pl.ds(2 * j + c, 1), :]
            cos_all[j] = base_cos * turn_ref[0] - base_sin * turn_ref[1]
            sine = base_sin * turn_ref[0] + base_cos * turn_ref[1]
            sin_all[j] = jnp.where(lane < HEAD_DIM // 2, -sine, sine)

    ops = {
        "XP": XP, "WOP": WOP, "XE": XE, "ST": ST, "N": N, "YH": gather.YH, "WA": WA, "WP": WP, "S": S, "O": O, "F": F, "DP": DP,
        "G": G, "Q": Q, "R": R, "A": A, "P": P, "X": X, "M": reduce.middle, "T": T,
        "HF": HF, "HH": lambda u: ahead.XH(0, u), "HN": lambda u: ahead.N(0, u), "HY": HY, "HO": HO,
    }
    def all_sent(ref, sem):
        remote(ref, ref, sem, ro.at[0], at.partner).wait_send()

    def sent():
        for m in range(2):
            for k in range(4):
                d_pair(m, k, 1 - c).wait_recv()
            d_out(m).wait()
        all_sent(w_all.at[:, :, pl.ds(0, 4 * kd)], sdp.at[0])
        for d in range(2):
            all_sent(w_all.at[:, :, pl.ds(0, kd)], sds.at[d])
            all_sent((drel_a, drel_b)[d], sdo.at[d])
            all_sent((drel_a, drel_b)[d], sdf.at[d])
            for u in range(len(units)):
                gather.ycopy(d, u).wait_send()
                gather.yhalf(d, u).wait_send()
        all_sent(x_ref.at[pl.ds(0, NJ * ch)], sd.at[0])
        all_sent(xc, sxe.at[0])
        all_sent(st_own, sst.at[0])
        reduce.drain()
        ahead.drain()
        for r in range(NX):
            for u in range(2):
                h_out(r, u).wait()
        o_pair.wait_send()
        for sem in (swa, swo, swp):
            all_sent(wb.at[pl.ds(0, kd)], sem.at[0])
        all_sent(part.at[:, :, pl.ds(0, 3 * hc)], spr.at[0])
        all_sent(kvo, skv.at[0])
        for kind, (lo, n) in enumerate(((0, ch), (0, ch), (0, cut), (cut, ch - cut))):
            all_sent(og.at[:, pl.ds(lo, n), o_cols(x)], sog.at[kind])

    waits = {"X": o_ready, "WP": angles}
    last = max(i for i, step in enumerate(ATTENTION_STEPS) if step[0] == "X")
    for i, step in enumerate(ATTENTION_STEPS):
        if step[0] in waits:
            waits.pop(step[0])()
        if i == last:
            sent()
        ops[step[0]](*step[1:])
    for j in range(NJ):
        chunk_out(j).wait()


def mlp_kernel(
    units, h_hbm, w_hbm, wdn, hg_hbm, y_ref,
    h_ref, xg, wt, raw, wd, ag, ar, act, s1, s2, zb, ya, yb, yfd, yfu, yst,
    sx, rx, sy, ry, syh, ryh, sa, ra, syr, ryr, sd, rd, lw, lwd, swd, rwd, lh, lo,
):
    at = Place()
    x, c, y = at.x, at.c, at.y
    ch, kc, h = h_ref.shape[1], h_ref.shape[2], h_ref.shape[1] // 2
    width = xg.shape[-1]
    kd = kc // 2
    fc, tiles = w_hbm.shape[1], wt.shape[1] // 256
    fm = (tiles - 1) * 128
    fr = fc - fm
    blocks, slots = 2 * tiles, raw.shape[0]
    gather = Spread(at, h_ref, xg, units, (s1, s2), sx, rx, sy, ry, syh, ryh)
    reduce = Reduce(at, zb, ya, yb, yfd, yfu, syr, ryr)

    def w_in(q):
        i, m = q // 2, q % 2
        n = min(128, fc - i * 128)
        return pltpu.make_async_copy(w_hbm.at[m, pl.ds(i * 128, n)], raw.at[q % slots, pl.ds(0, n)], lw.at[q])

    def WT(g):
        for q in range(g * blocks // 4, (g + 1) * blocks // 4):
            i, m, slot = q // 2, q % 2, q % slots
            w_in(q).wait()
            if fc < (i + 1) * 128:
                raw[slot, fc - i * 128 :, :] = jnp.zeros(((i + 1) * 128 - fc, width), BF16)

            def turn(k, carry, slot=slot, q=q):
                part = pl.ds(al(k * (width // 4), 128), width // 4)
                wt[part, q * 128 : (q + 1) * 128] = raw[slot, :, part].T
                return carry

            lax.fori_loop(0, 4, turn, 0)
            if q + slots < blocks:
                w_in(q + slots).start()

    def d_refs(q, core):
        cols = pl.ds(al(core * kd, 128), kd)
        main, rest = wdn.at[pl.ds(q * fc, fm)], wdn.at[pl.ds(q * fc + fm, fr)]
        return (main, wd.at[pl.ds(q * fm, fm), cols]), (rest, wd.at[pl.ds(NX * fm + q * 128, fr), cols])

    def d_own(q, k):
        src, dst = d_refs(q, c)[k]
        return pltpu.make_async_copy(src, dst, lwd.at[q, k])

    def d_pair(q, k, core):
        src, dst = d_refs(q, core)[k]
        return remote(src, dst, swd.at[q, k], rwd.at[q, k], at.partner)

    quarters = [(q, k) for q in range(NX) for k in range(2)]
    h_in_all = pltpu.make_async_copy(h_hbm, h_ref, lo.at[NJ])
    h_in_all.start()
    for q in range(slots):
        w_in(q).start()
    def h_in(s):
        return pltpu.make_async_copy(hg_hbm.at[s], xg.at[s, 0], lh.at[s])

    for s in range(NX):
        h_in(s).start()
    for q, k in quarters:
        d_own(q, k).start()
    for q in range(NX):
        wd[NX * fm + q * 128 + fr : NX * fm + (q + 1) * 128, :] = jnp.zeros((128 - fr, kc), BF16)
    at.barrier(h_in_all.wait)
    for q, k in quarters:
        d_pair(q, k, c).start()

    def a_refs(kind, n, xx):
        main, rest = pl.ds(al(xx * fm, 128), fm), pl.ds(al(xx * 128, 128), 128)
        if kind < 2:
            return ag.at[n, :, main], ar.at[n, :, rest]
        lo = (kind - 2) * h
        return ag.at[n, pl.ds(lo, h), main], ar.at[n, pl.ds(lo // 2, h // 2), rest]

    def a_copies(kind, n):
        refs = a_refs(kind, n, (x, x, at.xl, at.xr)[kind])
        return [remote(v, v, sa.at[kind, k], ra.at[kind, n, k], at.left if kind % 2 else at.right) for k, v in enumerate(refs)]

    def a_wait(kind, n):
        for k, v in enumerate(a_refs(kind, n, (at.xl, at.xr, at.xo, at.xo)[kind])):
            remote(v, v, sa.at[kind, k], ra.at[kind, n, k], at.right).wait_recv()

    def a_start(kind, n):
        for copy in a_copies(kind, n):
            copy.start()

    def G(g):
        for r, j in GROUPS[g]:
            gather.chunk_wait(r, j)

        def done(col, size, out):
            for k in range(0, size, 256):
                gate, up = out[:, k : k + 128].astype(BF16).astype(F32), out[:, k + 128 : k + 256].astype(BF16).astype(F32)
                value = (gate / (1.0 + jnp.exp(-gate)) * up).astype(BF16)
                act[0 : value.shape[0], pl.ds(al(div(col + k, 2), 128), 128)] = value

        product([xg.at[gather.seqs[r], j] for r, j in GROUPS[g]], wt, width, wt.shape[1], done)
        for i, (r, j) in enumerate(GROUPS[g]):
            n, lo = r * NJ + j, i * ch
            ag[n, :, pl.ds(al(x * fm, 128), fm)] = act[lo : lo + ch, :fm]
            below = pltpu.roll(act[lo + h : lo + ch, fm:].astype(F32), 64, axis=1)
            ar[n, :, pl.ds(al(x * 128, 128), 128)] = (act[lo : lo + h, fm:].astype(F32) + below).astype(BF16)
            for kind in range(2):
                a_start(kind, n)

    def P(g):
        for r, j in GROUPS[g]:
            for kind in range(2):
                a_wait(kind, r * NJ + j)
                a_start(kind + 2, r * NJ + j)

    def unpack(g):
        for r, j in GROUPS[g]:
            n = r * NJ + j
            for kind in (2, 3):
                a_wait(kind, n)
            lane = lax.broadcasted_iota(jnp.int32, (h, 128), 1)
            for q in range(NX):
                cols = pl.ds(NX * fm + q * 128, 128)
                rest = ar[n, :, q * 128 : (q + 1) * 128].astype(F32)
                ag[n, 0:h, cols] = jnp.where(lane < 64, rest, 0.0).astype(BF16)
                ag[n, h:, cols] = jnp.where(lane < 64, pltpu.roll(rest, 64, axis=1), 0.0).astype(BF16)

    def X(g):
        unpack(g)

        def done(col, size, out):
            for i, (r, j) in enumerate(GROUPS[g]):
                zb[r, j, :, pl.ds(al(col, 128), size)] = out[i * ch : (i + 1) * ch].astype(BF16)

        product([ag.at[r * NJ + j] for r, j in GROUPS[g]], wd, wd.shape[0], kc, done, 512 if len(GROUPS[g]) == 1 else 256)
        for r, j in GROUPS[g]:
            if r == 2:
                reduce.halves(j)

    def half_cols(core):
        return pl.ds(al(core * kd, 128), kd)

    def y_rows(j, core):
        return pl.ds(al((2 * j + core) * ch, 8), ch)

    def y_copy(j):
        return remote(yst.at[1 - c, j], y_ref.at[y_rows(j, c)], sd.at[j], rd.at[j], at.partner)

    def y_own(j):
        return pltpu.make_async_copy(yst.at[c, j], y_ref.at[y_rows(j, c)], lo.at[j])

    def y_wait(j):
        dst = y_ref.at[y_rows(j, 1 - c)]
        remote(dst, dst, sd.at[j], rd.at[j], at.partner).wait_recv()

    def T(j):
        def done(rows, mlp):
            out = (h_ref[j, rows, :].astype(F32) + mlp.astype(BF16).astype(F32)).astype(BF16)
            yst[0, j, rows, :] = out[:, :kd]
            yst[1, j, rows, :] = out[:, kd:]

        reduce.total(j, done)
        y_copy(j).start()
        y_own(j).start()

    def XT(g):
        ((_, j),) = GROUPS[g]
        unpack(g)
        reduce.wait(2, j)
        reduce.wait(3, j)

        def half(i, carry):
            core = 1 - c + i * (2 * c - 1)
            cols = half_cols(core)
            out = jnp.dot(ag[j], wd[:, cols], preferred_element_type=F32).astype(BF16).astype(F32)
            mlp = out + yfd[j, :, cols].astype(F32) + yfu[j, :, cols].astype(F32)
            yst[core, j] = (h_ref[j, :, cols].astype(F32) + mlp.astype(BF16).astype(F32)).astype(BF16)
            pl.when(i == 0)(lambda: y_copy(j).start())
            return carry

        lax.fori_loop(0, 2, half, 0)
        y_own(j).start()

    ops = {"G": G, "P": P, "X": X, "M": reduce.middle, "T": T, "XT": XT, "WT": WT}
    for name in ("YR", "YRH", "YH", "XF", "XH", "N"):
        ops[name] = getattr(gather, name)
    waits = {
        "N": gather.keep_own,
        "G": lambda: [h_in(s).wait() for s in range(NX)],
        "X": lambda: [(d_own(q, k).wait(), d_pair(q, k, 1 - c).wait_recv()) for q, k in quarters],
    }
    def sent():
        gather.drain()
        reduce.drain()
        for q, k in quarters:
            d_pair(q, k, c).wait_send()

        for kind in range(4):
            for k, every in enumerate(a_refs(kind, slice(None), x)):
                remote(every, every, sa.at[kind, k], ra.at[kind, 0, k], at.right).wait_send()

    (_, g), (_, j) = MLP_STEPS[-2:]
    assert MLP_STEPS[-2:] == (("X", g), ("T", j)) and GROUPS[g] == ((0, j),)
    for step in (*MLP_STEPS[:-2], ("XT", g)):
        if step[0] in waits:
            waits.pop(step[0])()
        ops[step[0]](*step[1:])
    sent()
    for j in range(NJ):
        y_copy(j).wait_send()
        y_own(j).wait()
        y_wait(j)


def vmem(*shape, dtype=BF16):
    return pltpu.VMEM(shape, dtype)


def sems(*shape):
    return pltpu.SemaphoreType.DMA(shape)


def solution(mesh):
    assert mesh.shape["tx"] == 2 * NX and mesh.shape["ty"] == NX
    act_spec = P(("dp", "ty"), None, "tx")
    col_spec = P("tx", "ty")
    row_spec = P("ty", "tx")
    any_spec = pl.BlockSpec(memory_space=pl.ANY)
    vmem_spec = pl.BlockSpec(memory_space=pltpu.VMEM)

    def layer(x_blk, w_q, w_k, w_v, w_o, w_gate, w_up, w_down):
        _, seq, kd = x_blk.shape
        kc, width = 2 * kd, 2 * NX * kd
        ch = seq // (2 * NJ)
        h = ch // 2
        row_heads = w_q.shape[1]
        hc = row_heads // NX
        fc = w_down.shape[0] // NX
        assert hc % HEAD_DIM == 0
        tiles = (fc + 127) // 128
        f_a = (fc // 2 + 15) // 16 * 16

        inv_freq = THETA ** (-2.0 * np.arange(HEAD_DIM // 2) / HEAD_DIM)
        inv_freq = np.concatenate([inv_freq, inv_freq])
        turn = np.arange(ch)[:, None] * inv_freq
        base = np.arange(2 * NJ)[:, None] * ch * inv_freq
        turn = jnp.asarray(np.stack([np.cos(turn), np.sin(turn)]), F32)
        base = jnp.asarray(np.stack([np.cos(base), np.sin(base)]), F32)

        reduce_scratch = [vmem(NX, NJ, ch, kc), vmem(NJ, h, kc), vmem(NJ, ch - h, kc), vmem(NJ, ch, kc), vmem(NJ, ch, kc)]
        units = ((0, 0, h, 0), (0, h, h, 0)) + tuple((j, 0, ch, 0) for j in range(1, NJ))
        n_u = len(units)
        h_blk, w_all, hg_all = pl.pallas_call(
            functools.partial(attention_kernel, units),
            out_shape=(
                jax.ShapeDtypeStruct((NJ, ch, kc), BF16),
                jax.ShapeDtypeStruct((2, fc, width), BF16),
                jax.ShapeDtypeStruct((NX, ch, width), BF16),
            ),
            in_specs=[any_spec] * 9,
            out_specs=(any_spec, any_spec, any_spec),
            scratch_shapes=[
                vmem(seq, kd), vmem(2, ch, HEAD_DIM, dtype=F32), vmem(2, 2 * NJ, HEAD_DIM, dtype=F32),
                vmem(NJ, ch, kc), vmem(NJ, ch, kc), vmem(NX, NJ, ch, 2 * kc), vmem(NX, 1, ch, width), vmem(NJ, ch, HEAD_DIM, dtype=F32), vmem(NJ, ch, HEAD_DIM, dtype=F32),
                vmem(NJ, ch // 4, 128, dtype=F32), vmem(NJ, ch // 4, 128, dtype=F32), vmem(ch, 128, dtype=F32), vmem(ch, 128, dtype=F32),
                vmem(2 * kc, 6 * hc), vmem(row_heads, kc), vmem(NCH, ch, 6 * hc), vmem(NCH, ch, 3 * hc), vmem(NCH, ch, hc),
                vmem(NX, NJ, ch, 2 * hc), vmem(NX, NJ, ch, 2 * hc), vmem(NCH, ch, row_heads), *reduce_scratch,
                vmem(2, fc, kd), vmem(2, f_a, kd), vmem(2, fc - f_a, kd),
                sems(1), sems(n_u), sems(1), sems(n_u), sems(2, n_u), sems(2, n_u), sems(2, n_u), sems(2, n_u),
                sems(1), sems(NJ), sems(1), sems(2, 3), sems(1), sems(2, 3), sems(1), sems(2), sems(3, 3), sems(1), sems(1),
                sems(1), sems(NCH), sems(1), sems(NCH), sems(4), sems(4, NCH), sems(4), sems(4, NJ),
                sems(2, 2), sems(2), sems(2, 2, 2), sems(2), sems(2, 2), sems(2), sems(2, 2), sems(1), sems(2, 4),
                sems(4, 2), sems(4, 2), sems(2, 2), sems(2, 2), sems(2, 2), sems(2, 2), sems(NX, 2), sems(3 + NJ),
            ],
            compiler_params=pltpu.CompilerParams(collective_id=0, has_side_effects=True, vmem_limit_bytes=VMEM_LIMIT),
            name="attention_part",
        )(x_blk[0], turn, base, w_q, w_k, w_v, w_o, w_gate.T, w_up.T)

        units = ((1, 0, h, 1), (1, h, h, 0)) + tuple((j, 0, ch, 0) for j in range(2, NJ))
        n_u, n_x = len(units), len(units) + 3
        y_blk = pl.pallas_call(
            functools.partial(mlp_kernel, units),
            out_shape=jax.ShapeDtypeStruct((seq, kd), BF16),
            in_specs=[any_spec] * 4,
            out_specs=any_spec,
            scratch_shapes=[
                vmem(NJ, ch, kc),
                vmem(NX, NJ, ch, width), vmem(width, tiles * 256), vmem(3, 128, width),
                vmem(NX * tiles * 128, kc), vmem(NCH, ch, NX * tiles * 128), vmem(NCH, h, NX * 128), vmem(2 * ch, tiles * 128),
                vmem(ch, 128, dtype=F32), vmem(ch, 128, dtype=F32),
                *reduce_scratch, vmem(2, NJ, ch, kd),
                sems(4, n_x), sems(4, n_x), sems(2, n_u), sems(2, n_u), sems(2, n_u), sems(2, n_u),
                sems(4, 2), sems(4, NCH, 2), sems(4), sems(4, NJ), sems(NJ), sems(NJ),
                sems(2 * tiles), sems(NX, 2), sems(NX, 2), sems(NX, 2), sems(NX), sems(NJ + 1),
            ],
            compiler_params=pltpu.CompilerParams(collective_id=1, has_side_effects=True, vmem_limit_bytes=VMEM_LIMIT),
            name="mlp_part",
        )(h_blk, w_all, w_down, hg_all)
        return y_blk[None]

    return jax.shard_map(
        layer,
        mesh=mesh,
        in_specs=(act_spec, col_spec, col_spec, col_spec, row_spec, col_spec, col_spec, row_spec),
        out_specs=act_spec,
        check_vma=False,
    )
```

```python
import functools

import jax
import jax.numpy as jnp
import numpy as np
from jax import lax
from jax.experimental import pallas as pl
from jax.experimental.pallas import tpu as pltpu
from jax.sharding import PartitionSpec as P

HEAD_DIM = 128
EPS = 1e-5
THETA = 10000.0
MESH = pl.DeviceIdType.MESH
F32 = jnp.float32
BF16 = jnp.bfloat16
NX = 4
NJ = 4
NCH = 16
VMEM_LIMIT = 67_043_328
GROUPS = (*(((0, j),) for j in range(NJ)), *(((3, j), (1, j)) for j in range(NJ)), *(((2, j),) for j in range(NJ)))


def rem(a, b):
    return lax.rem(a, jnp.int32(b))


def div(a, b):
    return lax.div(a, jnp.int32(b))


def al(v, m):
    return pl.multiple_of(v, m)


def remote(src, dst, ssem, rsem, dev):
    return pltpu.make_async_remote_copy(src_ref=src, dst_ref=dst, send_sem=ssem, recv_sem=rsem, device_id=dev, device_id_type=MESH)


ATTENTION_STEPS = (
    ("WA", 0), ("XP", 1), ("S", "b", 0, 1), ("XP", 0), ("XE", 1), ("XE", 0), ("XE", 2), ("XP", 2), ("S", "b", 0, 0), ("XP", 3),
    ("S", "b", 1, 0), ("ST", 1), ("WP", 0), ("WA", 1), ("O", "b", 1), ("ST", 0), ("N", 1), ("O", "b", 0), ("ST", 2),
    ("S", "b", 1, 1), ("WOP",), ("N", 0), ("G", 0), ("XE", 3), ("YH", 1), ("YH", 0), ("S", "a", 0, 1), ("N", 2), ("WP", 1),
    ("G", 8), ("G", 4), ("ST", 3), ("Q", 8), ("Q", 0), ("R", 8), ("XE", 4), ("A", 8), ("F", "a", 1), ("YH", 2), ("G", 5),
    ("R", 4), ("ST", 4), ("N", 3), ("P", 8), ("G", 9), ("A", 4), ("R", 0), ("S", "a", 1, 1), ("X", 8), ("G", 1), ("N", 4),
    ("R", 5), ("A", 0), ("R", 9), ("P", 4), ("A", 9), ("A", 5), ("G", 2), ("P", 0), ("X", 4), ("M", 0), ("P", 9),
    ("S", "a", 1, 0), ("YH", 3), ("G", 6), ("P", 5), ("X", 0), ("T", 0), ("HF", 1), ("HF", 0), ("R", 2), ("X", 9), ("R", 1),
    ("A", 1), ("YH", 4), ("X", 5), ("M", 1), ("HH", 1), ("O", "a", 0), ("G", 10), ("R", 6), ("HH", 0), ("G", 7), ("O", "a", 1),
    ("HN", 1), ("R", 10), ("G", 11), ("A", 10), ("A", 6), ("HN", 0), ("R", 7), ("A", 2), ("HY", 1), ("A", 7), ("R", 11),
    ("P", 10), ("A", 11), ("P", 6), ("G", 3), ("P", 7), ("P", 11), ("F", "b", 1), ("F", "a", 0), ("X", 10), ("HY", 0),
    ("S", "a", 0, 0), ("F", "b", 0), ("R", 3), ("X", 11), ("A", 3), ("X", 6), ("HO", 1), ("X", 7), ("P", 1), ("P", 2),
    ("M", 2), ("M", 3), ("DP", 1), ("DP", 0), ("P", 3), ("HO", 0), ("X", 1), ("T", 1), ("X", 2), ("T", 2), ("X", 3), ("T", 3),
)
MLP_STEPS = (
    ("XF", 0, 1), ("XF", 0, 0), ("WT", 0), ("YR", 0), ("WT", 1), ("XH", 0, 1), ("XF", 0, 3), ("YRH", 0), ("XF", 3, 0),
    ("N", 0, 1), ("XH", 0, 3), ("XF", 1, 0), ("XF", 2, 0), ("WT", 2), ("WT", 3), ("N", 0, 3), ("XF", 0, 2), ("G", 4),
    ("YH", 1), ("G", 0), ("XH", 2, 0), ("G", 8), ("XH", 1, 0), ("XH", 0, 0), ("XH", 3, 0), ("XH", 0, 2), ("G", 3), ("YH", 3),
    ("G", 7), ("N", 3, 0), ("N", 0, 2), ("N", 1, 0), ("P", 8), ("N", 2, 0), ("G", 9), ("G", 11), ("P", 4), ("G", 5), ("P", 11),
    ("X", 8), ("P", 7), ("P", 9), ("X", 4), ("YH", 2), ("G", 6), ("X", 11), ("X", 7), ("P", 5), ("X", 9), ("N", 0, 0),
    ("M", 0), ("G", 10), ("G", 1), ("M", 3), ("X", 5), ("M", 1), ("P", 10), ("P", 6), ("P", 0), ("G", 2), ("X", 10), ("P", 3),
    ("P", 1), ("X", 6), ("M", 2), ("P", 2), ("X", 0), ("T", 0), ("X", 3), ("T", 3), ("X", 1), ("T", 1), ("X", 2), ("T", 2),
)


class Place:
    def __init__(self):
        tx, ty = lax.axis_index("tx"), lax.axis_index("ty")
        self.x, self.c, self.y = div(tx, 2), rem(tx, 2), ty
        x, c, y = self.x, self.c, self.y
        self.xr, self.xl, self.xo = rem(x + 1, NX), rem(x + 3, NX), rem(x + 2, NX)
        self.yu, self.yd, self.yo = rem(y + 1, NX), rem(y + 3, NX), rem(y + 2, NX)
        self.right = {"tx": self.xr * 2 + c, "ty": y}
        self.left = {"tx": self.xl * 2 + c, "ty": y}
        self.up = {"tx": tx, "ty": self.yu}
        self.down = {"tx": tx, "ty": self.yd}
        self.partner = {"tx": x * 2 + 1 - c, "ty": y}
        self.xa, self.xb = x + 1 - 2 * rem(x, 2), rem(x + 3 + 2 * rem(x, 2), NX)
        self.pa, self.pb = {"tx": self.xa * 2 + c, "ty": y}, {"tx": self.xb * 2 + c, "ty": y}

    def barrier(self, between):
        sem = pltpu.get_barrier_semaphore()
        for dev in (self.right, self.left, self.up, self.down, self.partner):
            pl.semaphore_signal(sem, inc=1, device_id=dev, device_id_type=MESH)
        between()
        pl.semaphore_wait(sem, 5)


class Spread:
    def __init__(self, at, src, xg, units, sums, sx, rx, sy, ry, syh, ryh):
        self.sums = sums
        self.at, self.src, self.xg, self.units, self.kc = at, src, xg, units, src.shape[2]
        self.sx, self.rx, self.sy, self.ry, self.syh, self.ryh = sx, rx, sy, ry, syh, ryh
        pairs = [(r, u) for u, unit in enumerate(units) for r in ((0, 3, 1, 2) if unit[3] else (0,))]
        self.index = {pair: i for i, pair in enumerate(pairs)}
        self.seqs = (at.y, at.yu, at.yo, at.yd)

    def cols(self, x):
        return pl.ds(al(x * self.kc, 128), self.kc)

    def keep_own(self):
        for j in {unit[0]: 0 for unit in self.units}:
            self.xg[self.at.y, j, :, self.cols(self.at.x)] = self.src[j]

    def xcopy(self, kind, r, u):
        at, s = self.at, self.seqs[r]
        j, lo, n, _ = self.units[u]
        i = self.index[r, u]
        if kind < 2:
            dst = self.xg.at[s, j, pl.ds(lo, n), self.cols(at.x)]
            src = self.src.at[j, pl.ds(lo, n)] if r == 0 else dst
        elif kind == 2:
            src = dst = self.xg.at[s, j, pl.ds(lo, n // 2), self.cols(at.xl)]
        else:
            src = dst = self.xg.at[s, j, pl.ds(lo + n // 2, n // 2), self.cols(at.xr)]
        return remote(src, dst, self.sx.at[kind, i], self.rx.at[kind, i], at.left if kind % 2 else at.right)

    def xwait(self, kind, r, u):
        at = self.at
        j, lo, n, _ = self.units[u]
        i = self.index[r, u]
        x = (at.xl, at.xr, at.xo, at.xo)[kind]
        rows = (pl.ds(lo, n), pl.ds(lo, n), pl.ds(lo, n // 2), pl.ds(lo + n // 2, n // 2))[kind]
        dst = self.xg.at[self.seqs[r], j, rows, self.cols(x)]
        remote(dst, dst, self.sx.at[kind, i], self.rx.at[kind, i], at.right).wait_recv()

    def yref(self, s, u, lo, n):
        j, _, _, first = self.units[u]
        rows = pl.ds(lo, n)
        return self.xg.at[s, j, rows, self.cols(self.at.x)] if first else self.xg.at[s, j, rows]

    def ycopy(self, d, u):
        j, lo, n, first = self.units[u]
        dst = self.yref(self.at.y, u, lo, n)
        src = self.src.at[j, pl.ds(lo, n)] if first else dst
        return remote(src, dst, self.sy.at[d, u], self.ry.at[d, u], self.at.down if d else self.at.up)

    def ywait(self, d, u):
        _, lo, n, _ = self.units[u]
        dst = self.yref(self.at.yu if d else self.at.yd, u, lo, n)
        remote(dst, dst, self.sy.at[d, u], self.ry.at[d, u], self.at.up).wait_recv()

    def yhalf(self, d, u):
        _, lo, n, _ = self.units[u]
        ref = self.yref(self.at.yu if d else self.at.yd, u, lo + d * (n // 2), n // 2)
        return remote(ref, ref, self.syh.at[d, u], self.ryh.at[d, u], self.at.down if d else self.at.up)

    def yhalf_wait(self, d, u):
        _, lo, n, _ = self.units[u]
        dst = self.yref(self.at.yo, u, lo + d * (n // 2), n // 2)
        remote(dst, dst, self.syh.at[d, u], self.ryh.at[d, u], self.at.up).wait_recv()

    def YR(self, u):
        for d in range(2):
            self.ycopy(d, u).start()

    def YH(self, u):
        for d in range(2):
            self.ywait(d, u)
            self.yhalf(d, u).start()

    YRH = YH

    def XF(self, r, u):
        if r == 2:
            for d in range(2):
                self.yhalf_wait(d, u)
        for kind in range(2):
            self.xcopy(kind, r, u).start()

    def XH(self, r, u):
        for kind in range(2):
            self.xwait(kind, r, u)
            self.xcopy(kind + 2, r, u).start()

    def N(self, r, u):
        j, lo, n, first = self.units[u]
        for kind in (2, 3):
            self.xwait(kind, r, u)
            self.xcopy(kind, r, u).wait_send()
        if r:
            for kind in range(2):
                self.xcopy(kind, r, u).wait_send()
        if r % 2:
            self.yhalf(0 if r == 3 else 1, u).wait_send()
        width, ref = self.xg.shape[-1], self.xg.at[self.seqs[r], j]
        s1, s2 = self.sums
        lane_sums(ref, lo, n, s1, s2)
        mean = jnp.sum(s1[0:n, :], axis=-1, keepdims=True) / width
        var = jnp.sum(s2[0:n, :], axis=-1, keepdims=True) / width - mean * mean
        s1[0:n, :] = jnp.broadcast_to(mean, (n, 128))
        s2[0:n, :] = jnp.broadcast_to(lax.rsqrt(var + EPS), (n, 128))
        scale_rows(ref, lo, n, s1, s2)
        if not first:
            self.YR(u)

    def chunk_wait(self, r, j):
        if r == 2:
            for u, unit in enumerate(self.units):
                if unit[0] == j and not unit[3]:
                    for d in range(2):
                        self.yhalf_wait(d, u)

    def drain(self):
        for u, unit in enumerate(self.units):
            for d in range(2):
                self.xcopy(d, 0, u).wait_send()
                self.ycopy(d, u).wait_send()
                if not unit[3]:
                    self.yhalf(d, u).wait_send()


def rows_of(refs):
    return refs[0][...] if len(refs) == 1 else jnp.concatenate([ref[...] for ref in refs], axis=0)


def product(refs, weight, depth, n_cols, done, step=256):
    step = 256 if n_cols % step else step

    def columns(i, carry):
        out = jnp.dot(rows_of(refs), weight[0:depth, pl.ds(al(i * step, 128), step)], preferred_element_type=F32)
        done(i * step, step, out)
        return carry

    lax.fori_loop(0, n_cols // step, columns, 0)


def lane_sums(ref, lo, n, s1, s2):
    width, rows, wide = ref.shape[-1], 32, 512

    def some_rows(i, carry):
        def some_columns(k, sums):
            a, b = sums
            v = ref[pl.ds(al(lo + i * rows, 8), rows), pl.ds(al(k * wide, 128), wide)].astype(F32)
            for c in range(0, wide, 128):
                part = v[:, c : c + 128]
                a, b = a + part, b + part * part
            return a, b

        zero = jnp.zeros((rows, 128), F32)
        a, b = lax.fori_loop(0, width // wide, some_columns, (zero, zero))
        s1[pl.ds(al(i * rows, 8), rows), :] = a
        s2[pl.ds(al(i * rows, 8), rows), :] = b
        return carry

    lax.fori_loop(0, n // rows, some_rows, 0)


def scale_rows(ref, lo, n, means, scales):
    width, rows, wide = ref.shape[-1], 32, 512

    def some_rows(i, carry):
        mean, scale = (t[pl.ds(al(i * rows, 8), rows), :] for t in (means, scales))

        def some_columns(k, carry):
            at_rows = pl.ds(al(lo + i * rows, 8), rows)
            for c in range(0, wide, 128):
                cols = pl.ds(al(k * wide + c, 128), 128)
                ref[at_rows, cols] = ((ref[at_rows, cols].astype(F32) - mean) * scale).astype(BF16)
            return carry

        lax.fori_loop(0, width // wide, some_columns, 0)
        return carry

    lax.fori_loop(0, n // rows, some_rows, 0)


class Reduce:
    def __init__(self, at, zb, ya, yb, yfd, yfu, ss, rs):
        self.at, self.zb, self.ya, self.yb, self.yfd, self.yfu, self.ss, self.rs = at, zb, ya, yb, yfd, yfu, ss, rs
        self.ch = zb.shape[2]
        self.h = self.ch // 2

    def copy(self, kind, j):
        at, h, ch = self.at, self.h, self.ch
        src, dst = (
            lambda: (self.zb.at[2, j, pl.ds(0, h)], self.ya.at[j]),
            lambda: (self.zb.at[2, j, pl.ds(h, ch - h)], self.yb.at[j]),
            lambda: (self.zb.at[1, j], self.yfd.at[j]),
            lambda: (self.zb.at[3, j], self.yfu.at[j]),
        )[kind]()
        return remote(src, dst, self.ss.at[kind], self.rs.at[kind, j], at.down if kind % 2 else at.up)

    def wait(self, kind, j):
        self.copy(kind, j).wait_recv()

    def halves(self, j):
        self.copy(0, j).start()
        self.copy(1, j).start()

    def middle(self, j):
        h = self.h

        def add(r, lo, part):
            def some_rows(i, carry):
                rows, src = pl.ds(al(lo + i * 32, 8), 32), pl.ds(al(i * 32, 8), 32)
                self.zb[r, j, rows, :] = (self.zb[r, j, rows, :].astype(F32) + part[j, src, :].astype(F32)).astype(BF16)
                return carry

            lax.fori_loop(0, h // 32, some_rows, 0)

        self.wait(0, j)
        add(1, 0, self.ya)
        self.copy(2, j).start()
        self.wait(1, j)
        add(3, h, self.yb)
        self.copy(3, j).start()

    def total(self, j, done):
        self.wait(2, j)
        self.wait(3, j)

        def some_rows(i, carry):
            rows = pl.ds(al(i * 32, 8), 32)
            out = self.zb[0, j, rows, :].astype(F32) + self.yfd[j, rows, :].astype(F32) + self.yfu[j, rows, :].astype(F32)
            done(rows, out)
            return carry

        lax.fori_loop(0, self.ch // 32, some_rows, 0)

    def drain(self):
        h = self.h
        for kind, every in enumerate((self.zb.at[2, :, 0:h], self.zb.at[2, :, h:], self.zb.at[1], self.zb.at[3])):
            remote(every, every, self.ss.at[kind], self.rs.at[kind, 0], self.at.up).wait_send()


def attention_kernel(
    units, x_hbm, turn_hbm, base_hbm, wq, wk, wv, wo, wg_t, wu_t,
    h_hbm, w_all, hg_all,
    x_ref, turn_ref, base_ref, h_ref, xc, xg, hg, cos_all, sin_all, st_own, st_in, s1, s2, wb, wob, part, precv, qb, kvo, kvp, og, zb, ya, yb, yfd, yfu, own, drel_a, drel_b,
    sxe, rxe, sst, rst, sy, ry, syh, ryh, sd, rd, swa, rwa, swo, rwo, swp, rwp, lw, so, ro, spr, rpr, skv, rkv, sog, rog, syr, ryr,
    lg, sds, rds, sdo, rdo, sdf, rdf, sdp, rdp, shx, rhx, shy, rhy, shz, rhz, lh, lx,
):
    at = Place()
    x, c, y = at.x, at.c, at.y
    ch, kc = xc.shape[1], xc.shape[2]
    kd = wq.shape[0]
    hc = qb.shape[2]
    fc, f_a = w_all.shape[1], drel_a.shape[1]
    width = 2 * xg.shape[3]
    kh = div(x, 2)
    ng = rem(div(x + 1, 2), 2)
    gather = Spread(at, xc, xg, units, (s1, s2), None, None, sy, ry, syh, ryh)
    reduce = Reduce(at, zb, ya, yb, yfd, yfu, syr, ryr)
    ahead = Spread(at, h_ref, hg, ((0, 0, ch // 2, 0), (0, ch // 2, ch // 2, 0)), (s1, s2), shx, rhx, shy, rhy, shz, rhz)
    weights = (wq, wk, wv)

    def half_cols(core):
        return pl.ds(al(core * kd, 128), kd)

    def x_rows(j, core):
        return pl.ds(al((2 * j + core) * ch, 8), ch)

    def x_pair(j):
        return remote(x_ref.at[x_rows(j, 1 - c)], xc.at[j, :, half_cols(c)], sd.at[0], rd.at[j], at.partner)

    def pair_cols(xx):
        return pl.ds(al(rem(xx, 2) * kc, 128), kc)

    def xe_copy(u, xx):
        j, lo, n, _ = units[u]
        rows = pl.ds(lo, n)
        return remote(xc.at[j, rows], xg.at[y, j, rows, pair_cols(xx)], sxe.at[0], rxe.at[u], at.pa)

    def st_copy(u):
        j, lo, n, _ = units[u]
        rows = pl.ds(lo // 4, n // 4)
        return remote(st_own.at[j, rows], st_in.at[j, rows], sst.at[0], rst.at[u], at.pb)

    def XP(j):
        x_pair(j).start()

    arrived = []

    def XE(u):
        j, lo, n, _ = units[u]
        if j not in arrived:
            arrived.append(j)
            dst = xc.at[j, :, half_cols(1 - c)]
            remote(dst, dst, sd.at[0], rd.at[j], at.partner).wait_recv()
        xe_copy(u, x).start()
        xg[y, j, lo : lo + n, pair_cols(x)] = xc[j, lo : lo + n]

    def ST(u):
        j, lo, n, _ = units[u]
        xe_copy(u, at.xa).wait_recv()
        quarter = n // 4
        lane = lax.broadcasted_iota(jnp.int32, (quarter, 128), 1)
        lane_sums(xg.at[y, j], lo, n, s1, s2)
        packed = jnp.zeros((quarter, 128), F32)
        for g in range(4):
            rows = pl.ds(g * quarter, quarter)
            total, square = (jnp.sum(t[rows, :], axis=-1, keepdims=True) for t in (s1, s2))
            packed = jnp.where(lane // 32 == g, jnp.where(lane % 32 < 16, total, square), packed)
        st_own[j, lo // 4 : lo // 4 + quarter, :] = packed
        st_copy(u).start()

    def N(u):
        j, lo, n, _ = units[u]
        st_copy(u).wait_recv()
        quarter = n // 4
        at_rows = slice(lo // 4, lo // 4 + quarter)
        moments = (st_own[j, at_rows, :] + st_in[j, at_rows, :]) / width
        for g in range(4):
            mean = moments[:, 32 * g : 32 * g + 1]
            var = moments[:, 32 * g + 16 : 32 * g + 17] - mean * mean
            rows = pl.ds(g * quarter, quarter)
            s1[rows, :] = jnp.broadcast_to(mean, (quarter, 128))
            s2[rows, :] = jnp.broadcast_to(lax.rsqrt(var + EPS), (quarter, 128))
        scale_rows(xg.at[y, j], lo, n, s1, s2)
        gather.YR(u)

    def w_rows(xx, core):
        return pl.ds(al(rem(xx, 2) * kc + core * kd, 128), kd)

    def w_part(group, half, i):
        side = kh if half else 1 - kh
        return weights[i].at[:, pl.ds(al((2 * group + side) * hc, 128), hc)]

    def w_cols(half, i):
        return pl.ds(half * 3 * hc + i * hc, hc)

    def wa_copy(half, i, xx):
        return remote(w_part(1 - ng, half, i), wb.at[w_rows(xx, c), w_cols(half, i)], swa.at[0], rwa.at[half, i], at.pa)

    def wo_copy(half, i, core):
        return remote(w_part(ng, half, i), wb.at[w_rows(x, core), w_cols(half, i)], swo.at[0], rwo.at[half, i], at.partner)

    def w_local(half, i):
        return pltpu.make_async_copy(w_part(ng, half, i), wb.at[w_rows(x, c), w_cols(half, i)], lw.at[half, i])

    def wp_copy(half, core):
        ref = wb.at[w_rows(at.xa, core), pl.ds(half * 3 * hc, 3 * hc)]
        return remote(ref, ref, swp.at[0], rwp.at[half], at.partner)

    o_local = pltpu.make_async_copy(wo, wob.at[:, half_cols(c)], lw.at[2, 0])
    o_pair = remote(wo, wob.at[:, half_cols(c)], so.at[0], ro.at[0], at.partner)
    pieces = [(half, i) for half in range(2) for i in range(3)]

    def WOP():
        for half, i in pieces:
            wo_copy(half, i, c).start()
        o_pair.start()

    def WA(half):
        for i in range(3):
            wa_copy(half, i, x).start()

    def WP(half):
        for i in range(3):
            wa_copy(half, i, at.xa).wait_recv()
        wp_copy(half, c).start()

    w_halves = [0, 1]

    def w_ready(half):
        if half not in w_halves:
            return
        w_halves.remove(half)
        for i in range(3):
            w_local(half, i).wait()
            wo_copy(half, i, 1 - c).wait_recv()
        wp_copy(half, 1 - c).wait_recv()
        if half:
            own_out()

    def own_out():
        for m in range(2):
            d_in(m).wait()
            d_out(m).start()
            d_pair(m, 3, c).start()

    def o_ready():
        o_local.wait()
        dst = wob.at[:, half_cols(1 - c)]
        remote(dst, dst, so.at[0], ro.at[0], at.partner).wait_recv()

    mlp_weights = (wg_t, wu_t)
    parts = ((0, f_a), (f_a, fc - f_a))

    def d_src(m, xx, p):
        return mlp_weights[m].at[pl.ds(al(xx * fc + parts[p][0], 8), parts[p][1])]

    def d_dst(m, xx, p):
        return w_all.at[m, pl.ds(*parts[p]), pl.ds(al((2 * xx + c) * kd, 128), kd)]

    def s_copy(d, m, p, xx):
        to, dev = ((at.xa, at.pa), (at.xb, at.pb))[d]
        return remote(d_src(m, to, p), d_dst(m, xx, p), sds.at[d], rds.at[d, m, p], dev)

    def o_copy(d, m):
        return remote(d_src(m, at.xo, d), (drel_a, drel_b)[d].at[m], sdo.at[d], rdo.at[d, m], (at.pa, at.pb)[d])

    def f_copy(d, m, xx):
        return remote((drel_a, drel_b)[d].at[m], d_dst(m, xx, d), sdf.at[d], rdf.at[d, m], (at.pb, at.pa)[d])

    def d_in(m):
        return pltpu.make_async_copy(mlp_weights[m].at[pl.ds(al(x * fc, 8), fc)], own.at[m], lg.at[0, m])

    def d_all(m, xx, core):
        return w_all.at[m, :, pl.ds(al((2 * xx + core) * kd, 128), kd)]

    def d_out(m):
        return pltpu.make_async_copy(own.at[m], d_all(m, x, c), lg.at[1, m])

    def d_pair(m, k, core):
        dst = d_all(m, (at.xa, at.xb, at.xo, x)[k], core)
        return remote(own.at[m] if k == 3 else dst, dst, sdp.at[0], rdp.at[m, k], at.partner)

    def S(link, m, p):
        s_copy("ab".index(link), m, p, x).start()

    def O(link, m):
        o_copy("ab".index(link), m).start()

    def F(link, m):
        d = "ba".index(link)
        o_copy(d, m).wait_recv()
        f_copy(d, m, (at.xa, at.xb)[d]).start()

    def DP(m):
        for d in range(2):
            for p in range(2):
                s_copy(d, m, p, (at.xa, at.xb)[d]).wait_recv()
            f_copy(d, m, at.xo).wait_recv()
        for k in range(3):
            d_pair(m, k, c).start()

    def pr_copy(n):
        return remote(part.at[n, :, pl.ds(0, 3 * hc)], precv.at[n], spr.at[0], rpr.at[n], at.pb)

    def project(g, first, size):
        def done(col, step, out):
            for i, (r, j) in enumerate(GROUPS[g]):
                part[r * NJ + j, :, pl.ds(al(first + col, 128), step)] = out[i * ch : (i + 1) * ch].astype(BF16)

        refs = [xg.at[gather.seqs[r], j] for r, j in GROUPS[g]]
        product(refs, wb.at[:, pl.ds(first, size)], wb.shape[0], size, done)

    split = {step[1] for step in ATTENTION_STEPS if step[0] == "Q"}

    def G(g):
        w_ready(0)
        for r, j in GROUPS[g]:
            gather.chunk_wait(r, j)
        if g in split:
            project(g, 0, 3 * hc)
        else:
            w_ready(1)
            project(g, 0, 6 * hc)
        for r, j in GROUPS[g]:
            pr_copy(r * NJ + j).start()

    def Q(g):
        w_ready(1)
        project(g, 3 * hc, 3 * hc)

    def kv_copy(r, j):
        s, n = gather.seqs[r], r * NJ + j
        return remote(kvo.at[s, j], kvp.at[s, j], skv.at[0], rkv.at[n], at.partner)

    def rotate(r, j):
        s, n = gather.seqs[r], r * NJ + j
        pr_copy(n).wait_recv()
        cos_t, sin_t = cos_all[j], sin_all[j]

        def total(col, size):
            mine = part[n, :, 3 * hc + col : 3 * hc + col + size]
            return (mine.astype(F32) + precv[n, :, col : col + size].astype(F32)).astype(BF16)

        def turned(col):
            v = total(col, HEAD_DIM).astype(F32)
            return (v * cos_t + pltpu.roll(v, HEAD_DIM // 2, axis=1) * sin_t).astype(BF16)

        for col in range(0, hc, HEAD_DIM):
            qb[n, :, col : col + HEAD_DIM] = turned(col)
            kvo[s, j, :, col : col + HEAD_DIM] = turned(hc + col)
        kvo[s, j, :, hc:] = total(2 * hc, hc)
        kv_copy(r, j).start()

    def R(g):
        for r, j in GROUPS[g]:
            rotate(r, j)

    def o_cols(xx):
        return pl.ds(al((2 * rem(div(xx + 1, 2), 2) + div(xx, 2)) * hc, 128), hc)

    cut = ch // 8

    def og_copy(kind, n):
        if kind < 2:
            ref = og.at[n, :, o_cols(x)]
        elif kind == 2:
            ref = og.at[n, pl.ds(0, cut), o_cols(at.xa)]
        else:
            ref = og.at[n, pl.ds(cut, ch - cut), o_cols(at.xb)]
        return remote(ref, ref, sog.at[kind], rog.at[kind, n], at.pa if kind in (0, 3) else at.pb)

    def og_wait(kind, n):
        xx = (at.xa, at.xb, at.xo, at.xo)[kind]
        rows = (pl.ds(0, ch), pl.ds(0, ch), pl.ds(0, cut), pl.ds(cut, ch - cut))[kind]
        dst = og.at[n, rows, o_cols(xx)]
        remote(dst, dst, sog.at[kind], rog.at[kind, n], at.pa).wait_recv()

    def attend(r, j, i):
        s, n = gather.seqs[r], r * NJ + j
        keys = (j + 1) * ch
        iq = lax.broadcasted_iota(jnp.int32, (ch, keys), 0) + j * ch
        ik = lax.broadcasted_iota(jnp.int32, (ch, keys), 1)
        own_ok = iq >= ik
        par_ok = ik < (j + c) * ch
        contract = (((1,), (1,)), ((), ()))
        cols = pl.ds(al(i * HEAD_DIM, 128), HEAD_DIM)
        v_cols = pl.ds(al(hc + i * HEAD_DIM, 128), HEAD_DIM)
        q = qb[n, :, cols]
        k_own = kvo[s, 0 : j + 1, :, cols].reshape(keys, HEAD_DIM)
        k_par = kvp[s, 0 : j + 1, :, cols].reshape(keys, HEAD_DIM)
        s_own = lax.dot_general(q, k_own, contract, preferred_element_type=F32) * HEAD_DIM**-0.5
        s_par = lax.dot_general(q, k_par, contract, preferred_element_type=F32) * HEAD_DIM**-0.5
        s_own = jnp.where(own_ok, s_own, -1e30)
        s_par = jnp.where(par_ok, s_par, -1e30)
        top = jnp.maximum(jnp.max(s_own, axis=1, keepdims=True), jnp.max(s_par, axis=1, keepdims=True))
        e_own, e_par = jnp.exp(s_own - top), jnp.exp(s_par - top)
        inv = 1.0 / (jnp.sum(e_own, axis=1, keepdims=True) + jnp.sum(e_par, axis=1, keepdims=True))
        v_own = kvo[s, 0 : j + 1, :, v_cols].reshape(keys, HEAD_DIM)
        v_par = kvp[s, 0 : j + 1, :, v_cols].reshape(keys, HEAD_DIM)
        out = jnp.dot((e_own * inv).astype(BF16), v_own, preferred_element_type=F32)
        out += jnp.dot((e_par * inv).astype(BF16), v_par, preferred_element_type=F32)
        og[n, :, pl.ds(al((2 * ng + kh) * hc + i * HEAD_DIM, 128), HEAD_DIM)] = out.astype(BF16)

    def A(g):
        for r, j in GROUPS[g]:
            kv_copy(r, j).wait_recv()

        def head(i, carry):
            for r, j in GROUPS[g]:
                attend(r, j, i)
            return carry

        lax.fori_loop(0, hc // HEAD_DIM, head, 0)
        for r, j in GROUPS[g]:
            og_copy(0, r * NJ + j).start()
            og_copy(1, r * NJ + j).start()

    def P(g):
        for r, j in GROUPS[g]:
            for kind in range(2):
                og_wait(kind, r * NJ + j)
                og_copy(kind + 2, r * NJ + j).start()

    def X(g):
        for r, j in GROUPS[g]:
            og_wait(2, r * NJ + j)
            og_wait(3, r * NJ + j)

        def done(col, size, out):
            for i, (r, j) in enumerate(GROUPS[g]):
                zb[r, j, :, pl.ds(al(col, 128), size)] = out[i * ch : (i + 1) * ch].astype(BF16)

        product([og.at[r * NJ + j] for r, j in GROUPS[g]], wob, wob.shape[0], kc, done, 512 if GROUPS[g][0][0] == 0 else 256)
        for r, j in GROUPS[g]:
            if r == 2:
                reduce.halves(j)

    def T(j):
        def done(rows, attn):
            h_ref[j, rows, :] = (xc[j, rows, :].astype(F32) + attn.astype(BF16).astype(F32)).astype(BF16)

        reduce.total(j, done)
        chunk_out(j).start()

    def chunk_out(j):
        return pltpu.make_async_copy(h_ref.at[j], h_hbm.at[j], lx.at[1 + j])

    def h_out(r, u):
        rows = pl.ds(u * (ch // 2), ch // 2)
        return pltpu.make_async_copy(hg.at[ahead.seqs[r], 0, rows], hg_all.at[ahead.seqs[r], rows], lh.at[r, u])

    kept = []

    def HF(u):
        if not kept:
            kept.append(u)
            ahead.keep_own()
        ahead.XF(0, u)

    def HY(u):
        ahead.YH(u)
        for r in (0, 1, 3):
            h_out(r, u).start()

    def HO(u):
        for d in range(2):
            ahead.yhalf_wait(d, u)
        h_out(2, u).start()

    def own_rows():
        for half, i in pieces:
            w_local(half, i).start()
        o_local.start()
        for m in range(2):
            d_in(m).start()
        x_in.wait()
        for j in range(NJ):
            xc[j, :, half_cols(c)] = x_ref[x_rows(j, c), :]

    x_in = pltpu.make_async_copy(x_hbm, x_ref, lx.at[0])
    x_in.start()
    tables = [pltpu.make_async_copy(src, dst, lx.at[1 + NJ + i]) for i, (src, dst) in enumerate(((turn_hbm, turn_ref), (base_hbm, base_ref)))]
    for copy in tables:
        copy.start()
    at.barrier(own_rows)

    def angles():
        for copy in tables:
            copy.wait()
        lane = lax.broadcasted_iota(jnp.int32, (ch, HEAD_DIM), 1)
        for j in range(NJ):
            base_cos, base_sin = base_ref[0, pl.ds(2 * j + c, 1), :], base_ref[1, pl.ds(2 * j + c, 1), :]
            cos_all[j] = base_cos * turn_ref[0] - base_sin * turn_ref[1]
            sine = base_sin * turn_ref[0] + base_cos * turn_ref[1]
            sin_all[j] = jnp.where(lane < HEAD_DIM // 2, -sine, sine)

    ops = {
        "XP": XP, "WOP": WOP, "XE": XE, "ST": ST, "N": N, "YH": gather.YH, "WA": WA, "WP": WP, "S": S, "O": O, "F": F, "DP": DP,
        "G": G, "Q": Q, "R": R, "A": A, "P": P, "X": X, "M": reduce.middle, "T": T,
        "HF": HF, "HH": lambda u: ahead.XH(0, u), "HN": lambda u: ahead.N(0, u), "HY": HY, "HO": HO,
    }
    def all_sent(ref, sem):
        remote(ref, ref, sem, ro.at[0], at.partner).wait_send()

    def sent():
        for m in range(2):
            for k in range(4):
                d_pair(m, k, 1 - c).wait_recv()
            d_out(m).wait()
        all_sent(w_all.at[:, :, pl.ds(0, 4 * kd)], sdp.at[0])
        for d in range(2):
            all_sent(w_all.at[:, :, pl.ds(0, kd)], sds.at[d])
            all_sent((drel_a, drel_b)[d], sdo.at[d])
            all_sent((drel_a, drel_b)[d], sdf.at[d])
            for u in range(len(units)):
                gather.ycopy(d, u).wait_send()
                gather.yhalf(d, u).wait_send()
        all_sent(x_ref.at[pl.ds(0, NJ * ch)], sd.at[0])
        all_sent(xc, sxe.at[0])
        all_sent(st_own, sst.at[0])
        reduce.drain()
        ahead.drain()
        for r in range(NX):
            for u in range(2):
                h_out(r, u).wait()
        o_pair.wait_send()
        for sem in (swa, swo, swp):
            all_sent(wb.at[pl.ds(0, kd)], sem.at[0])
        all_sent(part.at[:, :, pl.ds(0, 3 * hc)], spr.at[0])
        all_sent(kvo, skv.at[0])
        for kind, (lo, n) in enumerate(((0, ch), (0, ch), (0, cut), (cut, ch - cut))):
            all_sent(og.at[:, pl.ds(lo, n), o_cols(x)], sog.at[kind])

    waits = {"X": o_ready, "WP": angles}
    last = max(i for i, step in enumerate(ATTENTION_STEPS) if step[0] == "X")
    for i, step in enumerate(ATTENTION_STEPS):
        if step[0] in waits:
            waits.pop(step[0])()
        if i == last:
            sent()
        ops[step[0]](*step[1:])
    for j in range(NJ):
        chunk_out(j).wait()


def mlp_kernel(
    units, h_hbm, w_hbm, wdn, hg_hbm, y_ref,
    h_ref, xg, wt, raw, wd, ag, ar, act, s1, s2, zb, ya, yb, yfd, yfu, yst,
    sx, rx, sy, ry, syh, ryh, sa, ra, syr, ryr, sd, rd, lw, lwd, swd, rwd, lh, lo,
):
    at = Place()
    x, c, y = at.x, at.c, at.y
    ch, kc, h = h_ref.shape[1], h_ref.shape[2], h_ref.shape[1] // 2
    width = xg.shape[-1]
    kd = kc // 2
    fc, tiles = w_hbm.shape[1], wt.shape[1] // 256
    fm = (tiles - 1) * 128
    fr = fc - fm
    blocks, slots = 2 * tiles, raw.shape[0]
    gather = Spread(at, h_ref, xg, units, (s1, s2), sx, rx, sy, ry, syh, ryh)
    reduce = Reduce(at, zb, ya, yb, yfd, yfu, syr, ryr)

    def w_in(q):
        i, m = q // 2, q % 2
        n = min(128, fc - i * 128)
        return pltpu.make_async_copy(w_hbm.at[m, pl.ds(i * 128, n)], raw.at[q % slots, pl.ds(0, n)], lw.at[q])

    def WT(g):
        for q in range(g * blocks // 4, (g + 1) * blocks // 4):
            i, m, slot = q // 2, q % 2, q % slots
            w_in(q).wait()
            if fc < (i + 1) * 128:
                raw[slot, fc - i * 128 :, :] = jnp.zeros(((i + 1) * 128 - fc, width), BF16)

            def turn(k, carry, slot=slot, q=q):
                part = pl.ds(al(k * (width // 4), 128), width // 4)
                wt[part, q * 128 : (q + 1) * 128] = raw[slot, :, part].T
                return carry

            lax.fori_loop(0, 4, turn, 0)
            if q + slots < blocks:
                w_in(q + slots).start()

    def d_refs(q, core):
        cols = pl.ds(al(core * kd, 128), kd)
        main, rest = wdn.at[pl.ds(q * fc, fm)], wdn.at[pl.ds(q * fc + fm, fr)]
        return (main, wd.at[pl.ds(q * fm, fm), cols]), (rest, wd.at[pl.ds(NX * fm + q * 128, fr), cols])

    def d_own(q, k):
        src, dst = d_refs(q, c)[k]
        return pltpu.make_async_copy(src, dst, lwd.at[q, k])

    def d_pair(q, k, core):
        src, dst = d_refs(q, core)[k]
        return remote(src, dst, swd.at[q, k], rwd.at[q, k], at.partner)

    quarters = [(q, k) for q in range(NX) for k in range(2)]
    h_in_all = pltpu.make_async_copy(h_hbm, h_ref, lo.at[NJ])
    h_in_all.start()
    for q in range(slots):
        w_in(q).start()
    def h_in(s):
        return pltpu.make_async_copy(hg_hbm.at[s], xg.at[s, 0], lh.at[s])

    for s in range(NX):
        h_in(s).start()
    for q, k in quarters:
        d_own(q, k).start()
    for q in range(NX):
        wd[NX * fm + q * 128 + fr : NX * fm + (q + 1) * 128, :] = jnp.zeros((128 - fr, kc), BF16)
    at.barrier(h_in_all.wait)
    for q, k in quarters:
        d_pair(q, k, c).start()

    def a_refs(kind, n, xx):
        main, rest = pl.ds(al(xx * fm, 128), fm), pl.ds(al(xx * 128, 128), 128)
        if kind < 2:
            return ag.at[n, :, main], ar.at[n, :, rest]
        lo = (kind - 2) * h
        return ag.at[n, pl.ds(lo, h), main], ar.at[n, pl.ds(lo // 2, h // 2), rest]

    def a_copies(kind, n):
        refs = a_refs(kind, n, (x, x, at.xl, at.xr)[kind])
        return [remote(v, v, sa.at[kind, k], ra.at[kind, n, k], at.left if kind % 2 else at.right) for k, v in enumerate(refs)]

    def a_wait(kind, n):
        for k, v in enumerate(a_refs(kind, n, (at.xl, at.xr, at.xo, at.xo)[kind])):
            remote(v, v, sa.at[kind, k], ra.at[kind, n, k], at.right).wait_recv()

    def a_start(kind, n):
        for copy in a_copies(kind, n):
            copy.start()

    def G(g):
        for r, j in GROUPS[g]:
            gather.chunk_wait(r, j)

        def done(col, size, out):
            for k in range(0, size, 256):
                gate, up = out[:, k : k + 128].astype(BF16).astype(F32), out[:, k + 128 : k + 256].astype(BF16).astype(F32)
                value = (gate / (1.0 + jnp.exp(-gate)) * up).astype(BF16)
                act[0 : value.shape[0], pl.ds(al(div(col + k, 2), 128), 128)] = value

        product([xg.at[gather.seqs[r], j] for r, j in GROUPS[g]], wt, width, wt.shape[1], done)
        for i, (r, j) in enumerate(GROUPS[g]):
            n, lo = r * NJ + j, i * ch
            ag[n, :, pl.ds(al(x * fm, 128), fm)] = act[lo : lo + ch, :fm]
            below = pltpu.roll(act[lo + h : lo + ch, fm:].astype(F32), 64, axis=1)
            ar[n, :, pl.ds(al(x * 128, 128), 128)] = (act[lo : lo + h, fm:].astype(F32) + below).astype(BF16)
            for kind in range(2):
                a_start(kind, n)

    def P(g):
        for r, j in GROUPS[g]:
            for kind in range(2):
                a_wait(kind, r * NJ + j)
                a_start(kind + 2, r * NJ + j)

    def unpack(g):
        for r, j in GROUPS[g]:
            n = r * NJ + j
            for kind in (2, 3):
                a_wait(kind, n)
            lane = lax.broadcasted_iota(jnp.int32, (h, 128), 1)
            for q in range(NX):
                cols = pl.ds(NX * fm + q * 128, 128)
                rest = ar[n, :, q * 128 : (q + 1) * 128].astype(F32)
                ag[n, 0:h, cols] = jnp.where(lane < 64, rest, 0.0).astype(BF16)
                ag[n, h:, cols] = jnp.where(lane < 64, pltpu.roll(rest, 64, axis=1), 0.0).astype(BF16)

    def X(g):
        unpack(g)

        def done(col, size, out):
            for i, (r, j) in enumerate(GROUPS[g]):
                zb[r, j, :, pl.ds(al(col, 128), size)] = out[i * ch : (i + 1) * ch].astype(BF16)

        product([ag.at[r * NJ + j] for r, j in GROUPS[g]], wd, wd.shape[0], kc, done, 512 if len(GROUPS[g]) == 1 else 256)
        for r, j in GROUPS[g]:
            if r == 2:
                reduce.halves(j)

    def half_cols(core):
        return pl.ds(al(core * kd, 128), kd)

    def y_rows(j, core):
        return pl.ds(al((2 * j + core) * ch, 8), ch)

    def y_copy(j):
        return remote(yst.at[1 - c, j], y_ref.at[y_rows(j, c)], sd.at[j], rd.at[j], at.partner)

    def y_own(j):
        return pltpu.make_async_copy(yst.at[c, j], y_ref.at[y_rows(j, c)], lo.at[j])

    def y_wait(j):
        dst = y_ref.at[y_rows(j, 1 - c)]
        remote(dst, dst, sd.at[j], rd.at[j], at.partner).wait_recv()

    def T(j):
        def done(rows, mlp):
            out = (h_ref[j, rows, :].astype(F32) + mlp.astype(BF16).astype(F32)).astype(BF16)
            yst[0, j, rows, :] = out[:, :kd]
            yst[1, j, rows, :] = out[:, kd:]

        reduce.total(j, done)
        y_copy(j).start()
        y_own(j).start()

    def XT(g):
        ((_, j),) = GROUPS[g]
        unpack(g)
        reduce.wait(2, j)
        reduce.wait(3, j)

        def half(i, carry):
            core = 1 - c + i * (2 * c - 1)
            cols = half_cols(core)
            out = jnp.dot(ag[j], wd[:, cols], preferred_element_type=F32).astype(BF16).astype(F32)
            mlp = out + yfd[j, :, cols].astype(F32) + yfu[j, :, cols].astype(F32)
            yst[core, j] = (h_ref[j, :, cols].astype(F32) + mlp.astype(BF16).astype(F32)).astype(BF16)
            pl.when(i == 0)(lambda: y_copy(j).start())
            return carry

        lax.fori_loop(0, 2, half, 0)
        y_own(j).start()

    ops = {"G": G, "P": P, "X": X, "M": reduce.middle, "T": T, "XT": XT, "WT": WT}
    for name in ("YR", "YRH", "YH", "XF", "XH", "N"):
        ops[name] = getattr(gather, name)
    waits = {
        "N": gather.keep_own,
        "G": lambda: [h_in(s).wait() for s in range(NX)],
        "X": lambda: [(d_own(q, k).wait(), d_pair(q, k, 1 - c).wait_recv()) for q, k in quarters],
    }
    def sent():
        gather.drain()
        reduce.drain()
        for q, k in quarters:
            d_pair(q, k, c).wait_send()

        for kind in range(4):
            for k, every in enumerate(a_refs(kind, slice(None), x)):
                remote(every, every, sa.at[kind, k], ra.at[kind, 0, k], at.right).wait_send()

    (_, g), (_, j) = MLP_STEPS[-2:]
    assert MLP_STEPS[-2:] == (("X", g), ("T", j)) and GROUPS[g] == ((0, j),)
    for step in (*MLP_STEPS[:-2], ("XT", g)):
        if step[0] in waits:
            waits.pop(step[0])()
        ops[step[0]](*step[1:])
    sent()
    for j in range(NJ):
        y_copy(j).wait_send()
        y_own(j).wait()
        y_wait(j)


def vmem(*shape, dtype=BF16):
    return pltpu.VMEM(shape, dtype)


def sems(*shape):
    return pltpu.SemaphoreType.DMA(shape)


def solution(mesh):
    assert mesh.shape["tx"] == 2 * NX and mesh.shape["ty"] == NX
    act_spec = P(("dp", "ty"), None, "tx")
    col_spec = P("tx", "ty")
    row_spec = P("ty", "tx")
    any_spec = pl.BlockSpec(memory_space=pl.ANY)
    vmem_spec = pl.BlockSpec(memory_space=pltpu.VMEM)

    def layer(x_blk, w_q, w_k, w_v, w_o, w_gate, w_up, w_down):
        _, seq, kd = x_blk.shape
        kc, width = 2 * kd, 2 * NX * kd
        ch = seq // (2 * NJ)
        h = ch // 2
        row_heads = w_q.shape[1]
        hc = row_heads // NX
        fc = w_down.shape[0] // NX
        assert hc % HEAD_DIM == 0
        tiles = (fc + 127) // 128
        f_a = (fc // 2 + 15) // 16 * 16

        inv_freq = THETA ** (-2.0 * np.arange(HEAD_DIM // 2) / HEAD_DIM)
        inv_freq = np.concatenate([inv_freq, inv_freq])
        turn = np.arange(ch)[:, None] * inv_freq
        base = np.arange(2 * NJ)[:, None] * ch * inv_freq
        turn = jnp.asarray(np.stack([np.cos(turn), np.sin(turn)]), F32)
        base = jnp.asarray(np.stack([np.cos(base), np.sin(base)]), F32)

        reduce_scratch = [vmem(NX, NJ, ch, kc), vmem(NJ, h, kc), vmem(NJ, ch - h, kc), vmem(NJ, ch, kc), vmem(NJ, ch, kc)]
        units = ((0, 0, h, 0), (0, h, h, 0)) + tuple((j, 0, ch, 0) for j in range(1, NJ))
        n_u = len(units)
        h_blk, w_all, hg_all = pl.pallas_call(
            functools.partial(attention_kernel, units),
            out_shape=(
                jax.ShapeDtypeStruct((NJ, ch, kc), BF16),
                jax.ShapeDtypeStruct((2, fc, width), BF16),
                jax.ShapeDtypeStruct((NX, ch, width), BF16),
            ),
            in_specs=[any_spec] * 9,
            out_specs=(any_spec, any_spec, any_spec),
            scratch_shapes=[
                vmem(seq, kd), vmem(2, ch, HEAD_DIM, dtype=F32), vmem(2, 2 * NJ, HEAD_DIM, dtype=F32),
                vmem(NJ, ch, kc), vmem(NJ, ch, kc), vmem(NX, NJ, ch, 2 * kc), vmem(NX, 1, ch, width), vmem(NJ, ch, HEAD_DIM, dtype=F32), vmem(NJ, ch, HEAD_DIM, dtype=F32),
                vmem(NJ, ch // 4, 128, dtype=F32), vmem(NJ, ch // 4, 128, dtype=F32), vmem(ch, 128, dtype=F32), vmem(ch, 128, dtype=F32),
                vmem(2 * kc, 6 * hc), vmem(row_heads, kc), vmem(NCH, ch, 6 * hc), vmem(NCH, ch, 3 * hc), vmem(NCH, ch, hc),
                vmem(NX, NJ, ch, 2 * hc), vmem(NX, NJ, ch, 2 * hc), vmem(NCH, ch, row_heads), *reduce_scratch,
                vmem(2, fc, kd), vmem(2, f_a, kd), vmem(2, fc - f_a, kd),
                sems(1), sems(n_u), sems(1), sems(n_u), sems(2, n_u), sems(2, n_u), sems(2, n_u), sems(2, n_u),
                sems(1), sems(NJ), sems(1), sems(2, 3), sems(1), sems(2, 3), sems(1), sems(2), sems(3, 3), sems(1), sems(1),
                sems(1), sems(NCH), sems(1), sems(NCH), sems(4), sems(4, NCH), sems(4), sems(4, NJ),
                sems(2, 2), sems(2), sems(2, 2, 2), sems(2), sems(2, 2), sems(2), sems(2, 2), sems(1), sems(2, 4),
                sems(4, 2), sems(4, 2), sems(2, 2), sems(2, 2), sems(2, 2), sems(2, 2), sems(NX, 2), sems(3 + NJ),
            ],
            compiler_params=pltpu.CompilerParams(collective_id=0, has_side_effects=True, vmem_limit_bytes=VMEM_LIMIT),
            name="attention_part",
        )(x_blk[0], turn, base, w_q, w_k, w_v, w_o, w_gate.T, w_up.T)

        units = ((1, 0, h, 1), (1, h, h, 0)) + tuple((j, 0, ch, 0) for j in range(2, NJ))
        n_u, n_x = len(units), len(units) + 3
        y_blk = pl.pallas_call(
            functools.partial(mlp_kernel, units),
            out_shape=jax.ShapeDtypeStruct((seq, kd), BF16),
            in_specs=[any_spec] * 4,
            out_specs=any_spec,
            scratch_shapes=[
                vmem(NJ, ch, kc),
                vmem(NX, NJ, ch, width), vmem(width, tiles * 256), vmem(3, 128, width),
                vmem(NX * tiles * 128, kc), vmem(NCH, ch, NX * tiles * 128), vmem(NCH, h, NX * 128), vmem(2 * ch, tiles * 128),
                vmem(ch, 128, dtype=F32), vmem(ch, 128, dtype=F32),
                *reduce_scratch, vmem(2, NJ, ch, kd),
                sems(4, n_x), sems(4, n_x), sems(2, n_u), sems(2, n_u), sems(2, n_u), sems(2, n_u),
                sems(4, 2), sems(4, NCH, 2), sems(4), sems(4, NJ), sems(NJ), sems(NJ),
                sems(2 * tiles), sems(NX, 2), sems(NX, 2), sems(NX, 2), sems(NX), sems(NJ + 1),
            ],
            compiler_params=pltpu.CompilerParams(collective_id=1, has_side_effects=True, vmem_limit_bytes=VMEM_LIMIT),
            name="mlp_part",
        )(h_blk, w_all, w_down, hg_all)
        return y_blk[None]

    return jax.shard_map(
        layer,
        mesh=mesh,
        in_specs=(act_spec, col_spec, col_spec, col_spec, row_spec, col_spec, col_spec, row_spec),
        out_specs=act_spec,
        check_vma=False,
    )
```

```python
import functools

import jax
import jax.numpy as jnp
import numpy as np
from jax import lax
from jax.experimental import pallas as pl
from jax.experimental.pallas import tpu as pltpu
from jax.sharding import PartitionSpec as P

HEAD_DIM = 128
EPS = 1e-5
THETA = 10000.0
MESH = pl.DeviceIdType.MESH
F32 = jnp.float32
BF16 = jnp.bfloat16
NX = 4
NJ = 4
NCH = 16
VMEM_LIMIT = 67_043_328
GROUPS = (*(((0, j),) for j in range(NJ)), *(((3, j), (1, j)) for j in range(NJ)), *(((2, j),) for j in range(NJ)))


def rem(a, b):
    return lax.rem(a, jnp.int32(b))


def div(a, b):
    return lax.div(a, jnp.int32(b))


def al(v, m):
    return pl.multiple_of(v, m)


def remote(src, dst, ssem, rsem, dev):
    return pltpu.make_async_remote_copy(src_ref=src, dst_ref=dst, send_sem=ssem, recv_sem=rsem, device_id=dev, device_id_type=MESH)


ATTENTION_STEPS = (
    ("WA", 0), ("XP", 1), ("S", "b", 0, 1), ("XP", 0), ("XE", 1), ("XE", 0), ("XE", 2), ("XP", 2), ("S", "b", 0, 0), ("XP", 3),
    ("S", "b", 1, 0), ("ST", 1), ("WP", 0), ("WA", 1), ("O", "b", 1), ("ST", 0), ("N", 1), ("O", "b", 0), ("ST", 2),
    ("S", "b", 1, 1), ("WOP",), ("N", 0), ("G", 0), ("XE", 3), ("YH", 1), ("YH", 0), ("S", "a", 0, 1), ("N", 2), ("WP", 1),
    ("G", 8), ("G", 4), ("ST", 3), ("Q", 8), ("Q", 0), ("R", 8), ("XE", 4), ("A", 8), ("F", "a", 1), ("YH", 2), ("G", 5),
    ("R", 4), ("ST", 4), ("N", 3), ("P", 8), ("G", 9), ("A", 4), ("R", 0), ("S", "a", 1, 1), ("X", 8), ("G", 1), ("N", 4),
    ("R", 5), ("A", 0), ("R", 9), ("P", 4), ("A", 9), ("A", 5), ("G", 2), ("P", 0), ("X", 4), ("M", 0), ("P", 9),
    ("S", "a", 1, 0), ("YH", 3), ("G", 6), ("P", 5), ("X", 0), ("T", 0), ("HF", 1), ("HF", 0), ("R", 2), ("X", 9), ("R", 1),
    ("A", 1), ("YH", 4), ("X", 5), ("M", 1), ("HH", 1), ("O", "a", 0), ("G", 10), ("R", 6), ("HH", 0), ("G", 7), ("O", "a", 1),
    ("HN", 1), ("R", 10), ("G", 11), ("A", 10), ("A", 6), ("HN", 0), ("R", 7), ("A", 2), ("HY", 1), ("A", 7), ("R", 11),
    ("P", 10), ("A", 11), ("P", 6), ("G", 3), ("P", 7), ("P", 11), ("F", "b", 1), ("F", "a", 0), ("X", 10), ("HY", 0),
    ("S", "a", 0, 0), ("F", "b", 0), ("R", 3), ("X", 11), ("A", 3), ("X", 6), ("HO", 1), ("X", 7), ("P", 1), ("P", 2),
    ("M", 2), ("M", 3), ("DP", 1), ("DP", 0), ("P", 3), ("HO", 0), ("X", 1), ("T", 1), ("X", 2), ("T", 2), ("X", 3), ("T", 3),
)
MLP_STEPS = (
    ("XF", 0, 1), ("XF", 0, 0), ("WT", 0), ("YR", 0), ("WT", 1), ("XH", 0, 1), ("XF", 0, 3), ("YRH", 0), ("XF", 3, 0),
    ("N", 0, 1), ("XH", 0, 3), ("XF", 1, 0), ("XF", 2, 0), ("WT", 2), ("WT", 3), ("N", 0, 3), ("XF", 0, 2), ("G", 4),
    ("YH", 1), ("G", 0), ("XH", 2, 0), ("G", 8), ("XH", 1, 0), ("XH", 0, 0), ("XH", 3, 0), ("XH", 0, 2), ("G", 3), ("YH", 3),
    ("G", 7), ("N", 3, 0), ("N", 0, 2), ("N", 1, 0), ("P", 8), ("N", 2, 0), ("G", 9), ("G", 11), ("P", 4), ("G", 5), ("P", 11),
    ("X", 8), ("P", 7), ("P", 9), ("X", 4), ("YH", 2), ("G", 6), ("X", 11), ("X", 7), ("P", 5), ("X", 9), ("N", 0, 0),
    ("M", 0), ("G", 10), ("G", 1), ("M", 3), ("X", 5), ("M", 1), ("P", 10), ("P", 6), ("P", 0), ("G", 2), ("X", 10), ("P", 3),
    ("P", 1), ("X", 6), ("M", 2), ("P", 2), ("X", 0), ("T", 0), ("X", 3), ("T", 3), ("X", 1), ("T", 1), ("X", 2), ("T", 2),
)


class Place:
    def __init__(self):
        tx, ty = lax.axis_index("tx"), lax.axis_index("ty")
        self.x, self.c, self.y = div(tx, 2), rem(tx, 2), ty
        x, c, y = self.x, self.c, self.y
        self.xr, self.xl, self.xo = rem(x + 1, NX), rem(x + 3, NX), rem(x + 2, NX)
        self.yu, self.yd, self.yo = rem(y + 1, NX), rem(y + 3, NX), rem(y + 2, NX)
        self.right = {"tx": self.xr * 2 + c, "ty": y}
        self.left = {"tx": self.xl * 2 + c, "ty": y}
        self.up = {"tx": tx, "ty": self.yu}
        self.down = {"tx": tx, "ty": self.yd}
        self.partner = {"tx": x * 2 + 1 - c, "ty": y}
        self.xa, self.xb = x + 1 - 2 * rem(x, 2), rem(x + 3 + 2 * rem(x, 2), NX)
        self.pa, self.pb = {"tx": self.xa * 2 + c, "ty": y}, {"tx": self.xb * 2 + c, "ty": y}

    def barrier(self, between):
        sem = pltpu.get_barrier_semaphore()
        for dev in (self.right, self.left, self.up, self.down, self.partner):
            pl.semaphore_signal(sem, inc=1, device_id=dev, device_id_type=MESH)
        between()
        pl.semaphore_wait(sem, 5)


class Spread:
    def __init__(self, at, src, xg, units, sums, sx, rx, sy, ry, syh, ryh):
        self.sums = sums
        self.at, self.src, self.xg, self.units, self.kc = at, src, xg, units, src.shape[2]
        self.sx, self.rx, self.sy, self.ry, self.syh, self.ryh = sx, rx, sy, ry, syh, ryh
        pairs = [(r, u) for u, unit in enumerate(units) for r in ((0, 3, 1, 2) if unit[3] else (0,))]
        self.index = {pair: i for i, pair in enumerate(pairs)}
        self.seqs = (at.y, at.yu, at.yo, at.yd)

    def cols(self, x):
        return pl.ds(al(x * self.kc, 128), self.kc)

    def keep_own(self):
        for j in {unit[0]: 0 for unit in self.units}:
            self.xg[self.at.y, j, :, self.cols(self.at.x)] = self.src[j]

    def xcopy(self, kind, r, u):
        at, s = self.at, self.seqs[r]
        j, lo, n, _ = self.units[u]
        i = self.index[r, u]
        if kind < 2:
            dst = self.xg.at[s, j, pl.ds(lo, n), self.cols(at.x)]
            src = self.src.at[j, pl.ds(lo, n)] if r == 0 else dst
        elif kind == 2:
            src = dst = self.xg.at[s, j, pl.ds(lo, n // 2), self.cols(at.xl)]
        else:
            src = dst = self.xg.at[s, j, pl.ds(lo + n // 2, n // 2), self.cols(at.xr)]
        return remote(src, dst, self.sx.at[kind, i], self.rx.at[kind, i], at.left if kind % 2 else at.right)

    def xwait(self, kind, r, u):
        at = self.at
        j, lo, n, _ = self.units[u]
        i = self.index[r, u]
        x = (at.xl, at.xr, at.xo, at.xo)[kind]
        rows = (pl.ds(lo, n), pl.ds(lo, n), pl.ds(lo, n // 2), pl.ds(lo + n // 2, n // 2))[kind]
        dst = self.xg.at[self.seqs[r], j, rows, self.cols(x)]
        remote(dst, dst, self.sx.at[kind, i], self.rx.at[kind, i], at.right).wait_recv()

    def yref(self, s, u, lo, n):
        j, _, _, first = self.units[u]
        rows = pl.ds(lo, n)
        return self.xg.at[s, j, rows, self.cols(self.at.x)] if first else self.xg.at[s, j, rows]

    def ycopy(self, d, u):
        j, lo, n, first = self.units[u]
        dst = self.yref(self.at.y, u, lo, n)
        src = self.src.at[j, pl.ds(lo, n)] if first else dst
        return remote(src, dst, self.sy.at[d, u], self.ry.at[d, u], self.at.down if d else self.at.up)

    def ywait(self, d, u):
        _, lo, n, _ = self.units[u]
        dst = self.yref(self.at.yu if d else self.at.yd, u, lo, n)
        remote(dst, dst, self.sy.at[d, u], self.ry.at[d, u], self.at.up).wait_recv()

    def yhalf(self, d, u):
        _, lo, n, _ = self.units[u]
        ref = self.yref(self.at.yu if d else self.at.yd, u, lo + d * (n // 2), n // 2)
        return remote(ref, ref, self.syh.at[d, u], self.ryh.at[d, u], self.at.down if d else self.at.up)

    def yhalf_wait(self, d, u):
        _, lo, n, _ = self.units[u]
        dst = self.yref(self.at.yo, u, lo + d * (n // 2), n // 2)
        remote(dst, dst, self.syh.at[d, u], self.ryh.at[d, u], self.at.up).wait_recv()

    def YR(self, u):
        for d in range(2):
            self.ycopy(d, u).start()

    def YH(self, u):
        for d in range(2):
            self.ywait(d, u)
            self.yhalf(d, u).start()

    YRH = YH

    def XF(self, r, u):
        if r == 2:
            for d in range(2):
                self.yhalf_wait(d, u)
        for kind in range(2):
            self.xcopy(kind, r, u).start()

    def XH(self, r, u):
        for kind in range(2):
            self.xwait(kind, r, u)
            self.xcopy(kind + 2, r, u).start()

    def N(self, r, u):
        j, lo, n, first = self.units[u]
        for kind in (2, 3):
            self.xwait(kind, r, u)
            self.xcopy(kind, r, u).wait_send()
        if r:
            for kind in range(2):
                self.xcopy(kind, r, u).wait_send()
        if r % 2:
            self.yhalf(0 if r == 3 else 1, u).wait_send()
        width, ref = self.xg.shape[-1], self.xg.at[self.seqs[r], j]
        s1, s2 = self.sums
        lane_sums(ref, lo, n, s1, s2)
        mean = jnp.sum(s1[0:n, :], axis=-1, keepdims=True) / width
        var = jnp.sum(s2[0:n, :], axis=-1, keepdims=True) / width - mean * mean
        s1[0:n, :] = jnp.broadcast_to(mean, (n, 128))
        s2[0:n, :] = jnp.broadcast_to(lax.rsqrt(var + EPS), (n, 128))
        scale_rows(ref, lo, n, s1, s2)
        if not first:
            self.YR(u)

    def chunk_wait(self, r, j):
        if r == 2:
            for u, unit in enumerate(self.units):
                if unit[0] == j and not unit[3]:
                    for d in range(2):
                        self.yhalf_wait(d, u)

    def drain(self):
        for u, unit in enumerate(self.units):
            for d in range(2):
                self.xcopy(d, 0, u).wait_send()
                self.ycopy(d, u).wait_send()
                if not unit[3]:
                    self.yhalf(d, u).wait_send()


def rows_of(refs):
    return refs[0][...] if len(refs) == 1 else jnp.concatenate([ref[...] for ref in refs], axis=0)


def product(refs, weight, depth, n_cols, done, step=256):
    step = 256 if n_cols % step else step

    def columns(i, carry):
        out = jnp.dot(rows_of(refs), weight[0:depth, pl.ds(al(i * step, 128), step)], preferred_element_type=F32)
        done(i * step, step, out)
        return carry

    lax.fori_loop(0, n_cols // step, columns, 0)


def lane_sums(ref, lo, n, s1, s2):
    width, rows, wide = ref.shape[-1], 32, 512

    def some_rows(i, carry):
        def some_columns(k, sums):
            a, b = sums
            v = ref[pl.ds(al(lo + i * rows, 8), rows), pl.ds(al(k * wide, 128), wide)].astype(F32)
            for c in range(0, wide, 128):
                part = v[:, c : c + 128]
                a, b = a + part, b + part * part
            return a, b

        zero = jnp.zeros((rows, 128), F32)
        a, b = lax.fori_loop(0, width // wide, some_columns, (zero, zero))
        s1[pl.ds(al(i * rows, 8), rows), :] = a
        s2[pl.ds(al(i * rows, 8), rows), :] = b
        return carry

    lax.fori_loop(0, n // rows, some_rows, 0)


def scale_rows(ref, lo, n, means, scales):
    width, rows, wide = ref.shape[-1], 32, 512

    def some_rows(i, carry):
        mean, scale = (t[pl.ds(al(i * rows, 8), rows), :] for t in (means, scales))

        def some_columns(k, carry):
            at_rows = pl.ds(al(lo + i * rows, 8), rows)
            for c in range(0, wide, 128):
                cols = pl.ds(al(k * wide + c, 128), 128)
                ref[at_rows, cols] = ((ref[at_rows, cols].astype(F32) - mean) * scale).astype(BF16)
            return carry

        lax.fori_loop(0, width // wide, some_columns, 0)
        return carry

    lax.fori_loop(0, n // rows, some_rows, 0)


class Reduce:
    def __init__(self, at, zb, ya, yb, yfd, yfu, ss, rs):
        self.at, self.zb, self.ya, self.yb, self.yfd, self.yfu, self.ss, self.rs = at, zb, ya, yb, yfd, yfu, ss, rs
        self.ch = zb.shape[2]
        self.h = self.ch // 2

    def copy(self, kind, j):
        at, h, ch = self.at, self.h, self.ch
        src, dst = (
            lambda: (self.zb.at[2, j, pl.ds(0, h)], self.ya.at[j]),
            lambda: (self.zb.at[2, j, pl.ds(h, ch - h)], self.yb.at[j]),
            lambda: (self.zb.at[1, j], self.yfd.at[j]),
            lambda: (self.zb.at[3, j], self.yfu.at[j]),
        )[kind]()
        return remote(src, dst, self.ss.at[kind], self.rs.at[kind, j], at.down if kind % 2 else at.up)

    def wait(self, kind, j):
        self.copy(kind, j).wait_recv()

    def halves(self, j):
        self.copy(0, j).start()
        self.copy(1, j).start()

    def middle(self, j):
        h = self.h

        def add(r, lo, part):
            def some_rows(i, carry):
                rows, src = pl.ds(al(lo + i * 32, 8), 32), pl.ds(al(i * 32, 8), 32)
                self.zb[r, j, rows, :] = (self.zb[r, j, rows, :].astype(F32) + part[j, src, :].astype(F32)).astype(BF16)
                return carry

            lax.fori_loop(0, h // 32, some_rows, 0)

        self.wait(0, j)
        add(1, 0, self.ya)
        self.copy(2, j).start()
        self.wait(1, j)
        add(3, h, self.yb)
        self.copy(3, j).start()

    def total(self, j, done):
        self.wait(2, j)
        self.wait(3, j)

        def some_rows(i, carry):
            rows = pl.ds(al(i * 32, 8), 32)
            out = self.zb[0, j, rows, :].astype(F32) + self.yfd[j, rows, :].astype(F32) + self.yfu[j, rows, :].astype(F32)
            done(rows, out)
            return carry

        lax.fori_loop(0, self.ch // 32, some_rows, 0)

    def drain(self):
        h = self.h
        for kind, every in enumerate((self.zb.at[2, :, 0:h], self.zb.at[2, :, h:], self.zb.at[1], self.zb.at[3])):
            remote(every, every, self.ss.at[kind], self.rs.at[kind, 0], self.at.up).wait_send()


def attention_kernel(
    units, x_hbm, turn_hbm, base_hbm, wq, wk, wv, wo, wg_t, wu_t,
    h_hbm, w_all, hg_all,
    x_ref, turn_ref, base_ref, h_ref, xc, xg, hg, cos_all, sin_all, st_own, st_in, s1, s2, wb, wob, part, precv, qb, kvo, kvp, og, zb, ya, yb, yfd, yfu, own, drel_a, drel_b,
    sxe, rxe, sst, rst, sy, ry, syh, ryh, sd, rd, swa, rwa, swo, rwo, swp, rwp, lw, so, ro, spr, rpr, skv, rkv, sog, rog, syr, ryr,
    lg, sds, rds, sdo, rdo, sdf, rdf, sdp, rdp, shx, rhx, shy, rhy, shz, rhz, lh, lx,
):
    at = Place()
    x, c, y = at.x, at.c, at.y
    ch, kc = xc.shape[1], xc.shape[2]
    kd = wq.shape[0]
    hc = qb.shape[2]
    fc, f_a = w_all.shape[1], drel_a.shape[1]
    width = 2 * xg.shape[3]
    kh = div(x, 2)
    ng = rem(div(x + 1, 2), 2)
    gather = Spread(at, xc, xg, units, (s1, s2), None, None, sy, ry, syh, ryh)
    reduce = Reduce(at, zb, ya, yb, yfd, yfu, syr, ryr)
    ahead = Spread(at, h_ref, hg, ((0, 0, ch // 2, 0), (0, ch // 2, ch // 2, 0)), (s1, s2), shx, rhx, shy, rhy, shz, rhz)
    weights = (wq, wk, wv)

    def half_cols(core):
        return pl.ds(al(core * kd, 128), kd)

    def x_rows(j, core):
        return pl.ds(al((2 * j + core) * ch, 8), ch)

    def x_pair(j):
        return remote(x_ref.at[x_rows(j, 1 - c)], xc.at[j, :, half_cols(c)], sd.at[0], rd.at[j], at.partner)

    def pair_cols(xx):
        return pl.ds(al(rem(xx, 2) * kc, 128), kc)

    def xe_copy(u, xx):
        j, lo, n, _ = units[u]
        rows = pl.ds(lo, n)
        return remote(xc.at[j, rows], xg.at[y, j, rows, pair_cols(xx)], sxe.at[0], rxe.at[u], at.pa)

    def st_copy(u):
        j, lo, n, _ = units[u]
        rows = pl.ds(lo // 4, n // 4)
        return remote(st_own.at[j, rows], st_in.at[j, rows], sst.at[0], rst.at[u], at.pb)

    def XP(j):
        x_pair(j).start()

    arrived = []

    def XE(u):
        j, lo, n, _ = units[u]
        if j not in arrived:
            arrived.append(j)
            dst = xc.at[j, :, half_cols(1 - c)]
            remote(dst, dst, sd.at[0], rd.at[j], at.partner).wait_recv()
        xe_copy(u, x).start()
        xg[y, j, lo : lo + n, pair_cols(x)] = xc[j, lo : lo + n]

    def ST(u):
        j, lo, n, _ = units[u]
        xe_copy(u, at.xa).wait_recv()
        quarter = n // 4
        lane = lax.broadcasted_iota(jnp.int32, (quarter, 128), 1)
        lane_sums(xg.at[y, j], lo, n, s1, s2)
        packed = jnp.zeros((quarter, 128), F32)
        for g in range(4):
            rows = pl.ds(g * quarter, quarter)
            total, square = (jnp.sum(t[rows, :], axis=-1, keepdims=True) for t in (s1, s2))
            packed = jnp.where(lane // 32 == g, jnp.where(lane % 32 < 16, total, square), packed)
        st_own[j, lo // 4 : lo // 4 + quarter, :] = packed
        st_copy(u).start()

    def N(u):
        j, lo, n, _ = units[u]
        st_copy(u).wait_recv()
        quarter = n // 4
        at_rows = slice(lo // 4, lo // 4 + quarter)
        moments = (st_own[j, at_rows, :] + st_in[j, at_rows, :]) / width
        for g in range(4):
            mean = moments[:, 32 * g : 32 * g + 1]
            var = moments[:, 32 * g + 16 : 32 * g + 17] - mean * mean
            rows = pl.ds(g * quarter, quarter)
            s1[rows, :] = jnp.broadcast_to(mean, (quarter, 128))
            s2[rows, :] = jnp.broadcast_to(lax.rsqrt(var + EPS), (quarter, 128))
        scale_rows(xg.at[y, j], lo, n, s1, s2)
        gather.YR(u)

    def w_rows(xx, core):
        return pl.ds(al(rem(xx, 2) * kc + core * kd, 128), kd)

    def w_part(group, half, i):
        side = kh if half else 1 - kh
        return weights[i].at[:, pl.ds(al((2 * group + side) * hc, 128), hc)]

    def w_cols(half, i):
        return pl.ds(half * 3 * hc + i * hc, hc)

    def wa_copy(half, i, xx):
        return remote(w_part(1 - ng, half, i), wb.at[w_rows(xx, c), w_cols(half, i)], swa.at[0], rwa.at[half, i], at.pa)

    def wo_copy(half, i, core):
        return remote(w_part(ng, half, i), wb.at[w_rows(x, core), w_cols(half, i)], swo.at[0], rwo.at[half, i], at.partner)

    def w_local(half, i):
        return pltpu.make_async_copy(w_part(ng, half, i), wb.at[w_rows(x, c), w_cols(half, i)], lw.at[half, i])

    def wp_copy(half, core):
        ref = wb.at[w_rows(at.xa, core), pl.ds(half * 3 * hc, 3 * hc)]
        return remote(ref, ref, swp.at[0], rwp.at[half], at.partner)

    o_local = pltpu.make_async_copy(wo, wob.at[:, half_cols(c)], lw.at[2, 0])
    o_pair = remote(wo, wob.at[:, half_cols(c)], so.at[0], ro.at[0], at.partner)
    pieces = [(half, i) for half in range(2) for i in range(3)]

    def WOP():
        for half, i in pieces:
            wo_copy(half, i, c).start()
        o_pair.start()

    def WA(half):
        for i in range(3):
            wa_copy(half, i, x).start()

    def WP(half):
        for i in range(3):
            wa_copy(half, i, at.xa).wait_recv()
        wp_copy(half, c).start()

    w_halves = [0, 1]

    def w_ready(half):
        if half not in w_halves:
            return
        w_halves.remove(half)
        for i in range(3):
            w_local(half, i).wait()
            wo_copy(half, i, 1 - c).wait_recv()
        wp_copy(half, 1 - c).wait_recv()
        if half:
            own_out()

    def own_out():
        for m in range(2):
            d_in(m).wait()
            d_out(m).start()
            d_pair(m, 3, c).start()

    def o_ready():
        o_local.wait()
        dst = wob.at[:, half_cols(1 - c)]
        remote(dst, dst, so.at[0], ro.at[0], at.partner).wait_recv()

    mlp_weights = (wg_t, wu_t)
    parts = ((0, f_a), (f_a, fc - f_a))

    def d_src(m, xx, p):
        return mlp_weights[m].at[pl.ds(al(xx * fc + parts[p][0], 8), parts[p][1])]

    def d_dst(m, xx, p):
        return w_all.at[m, pl.ds(*parts[p]), pl.ds(al((2 * xx + c) * kd, 128), kd)]

    def s_copy(d, m, p, xx):
        to, dev = ((at.xa, at.pa), (at.xb, at.pb))[d]
        return remote(d_src(m, to, p), d_dst(m, xx, p), sds.at[d], rds.at[d, m, p], dev)

    def o_copy(d, m):
        return remote(d_src(m, at.xo, d), (drel_a, drel_b)[d].at[m], sdo.at[d], rdo.at[d, m], (at.pa, at.pb)[d])

    def f_copy(d, m, xx):
        return remote((drel_a, drel_b)[d].at[m], d_dst(m, xx, d), sdf.at[d], rdf.at[d, m], (at.pb, at.pa)[d])

    def d_in(m):
        return pltpu.make_async_copy(mlp_weights[m].at[pl.ds(al(x * fc, 8), fc)], own.at[m], lg.at[0, m])

    def d_all(m, xx, core):
        return w_all.at[m, :, pl.ds(al((2 * xx + core) * kd, 128), kd)]

    def d_out(m):
        return pltpu.make_async_copy(own.at[m], d_all(m, x, c), lg.at[1, m])

    def d_pair(m, k, core):
        dst = d_all(m, (at.xa, at.xb, at.xo, x)[k], core)
        return remote(own.at[m] if k == 3 else dst, dst, sdp.at[0], rdp.at[m, k], at.partner)

    def S(link, m, p):
        s_copy("ab".index(link), m, p, x).start()

    def O(link, m):
        o_copy("ab".index(link), m).start()

    def F(link, m):
        d = "ba".index(link)
        o_copy(d, m).wait_recv()
        f_copy(d, m, (at.xa, at.xb)[d]).start()

    def DP(m):
        for d in range(2):
            for p in range(2):
                s_copy(d, m, p, (at.xa, at.xb)[d]).wait_recv()
            f_copy(d, m, at.xo).wait_recv()
        for k in range(3):
            d_pair(m, k, c).start()

    def pr_copy(n):
        return remote(part.at[n, :, pl.ds(0, 3 * hc)], precv.at[n], spr.at[0], rpr.at[n], at.pb)

    def project(g, first, size):
        def done(col, step, out):
            for i, (r, j) in enumerate(GROUPS[g]):
                part[r * NJ + j, :, pl.ds(al(first + col, 128), step)] = out[i * ch : (i + 1) * ch].astype(BF16)

        refs = [xg.at[gather.seqs[r], j] for r, j in GROUPS[g]]
        product(refs, wb.at[:, pl.ds(first, size)], wb.shape[0], size, done)

    split = {step[1] for step in ATTENTION_STEPS if step[0] == "Q"}

    def G(g):
        w_ready(0)
        for r, j in GROUPS[g]:
            gather.chunk_wait(r, j)
        if g in split:
            project(g, 0, 3 * hc)
        else:
            w_ready(1)
            project(g, 0, 6 * hc)
        for r, j in GROUPS[g]:
            pr_copy(r * NJ + j).start()

    def Q(g):
        w_ready(1)
        project(g, 3 * hc, 3 * hc)

    def kv_copy(r, j):
        s, n = gather.seqs[r], r * NJ + j
        return remote(kvo.at[s, j], kvp.at[s, j], skv.at[0], rkv.at[n], at.partner)

    def rotate(r, j):
        s, n = gather.seqs[r], r * NJ + j
        pr_copy(n).wait_recv()
        cos_t, sin_t = cos_all[j], sin_all[j]

        def total(col, size):
            mine = part[n, :, 3 * hc + col : 3 * hc + col + size]
            return (mine.astype(F32) + precv[n, :, col : col + size].astype(F32)).astype(BF16)

        def turned(col):
            v = total(col, HEAD_DIM).astype(F32)
            return (v * cos_t + pltpu.roll(v, HEAD_DIM // 2, axis=1) * sin_t).astype(BF16)

        for col in range(0, hc, HEAD_DIM):
            qb[n, :, col : col + HEAD_DIM] = turned(col)
            kvo[s, j, :, col : col + HEAD_DIM] = turned(hc + col)
        kvo[s, j, :, hc:] = total(2 * hc, hc)
        kv_copy(r, j).start()

    def R(g):
        for r, j in GROUPS[g]:
            rotate(r, j)

    def o_cols(xx):
        return pl.ds(al((2 * rem(div(xx + 1, 2), 2) + div(xx, 2)) * hc, 128), hc)

    cut = ch // 8

    def og_copy(kind, n):
        if kind < 2:
            ref = og.at[n, :, o_cols(x)]
        elif kind == 2:
            ref = og.at[n, pl.ds(0, cut), o_cols(at.xa)]
        else:
            ref = og.at[n, pl.ds(cut, ch - cut), o_cols(at.xb)]
        return remote(ref, ref, sog.at[kind], rog.at[kind, n], at.pa if kind in (0, 3) else at.pb)

    def og_wait(kind, n):
        xx = (at.xa, at.xb, at.xo, at.xo)[kind]
        rows = (pl.ds(0, ch), pl.ds(0, ch), pl.ds(0, cut), pl.ds(cut, ch - cut))[kind]
        dst = og.at[n, rows, o_cols(xx)]
        remote(dst, dst, sog.at[kind], rog.at[kind, n], at.pa).wait_recv()

    def attend(r, j, i):
        s, n = gather.seqs[r], r * NJ + j
        keys = (j + 1) * ch
        iq = lax.broadcasted_iota(jnp.int32, (ch, keys), 0) + j * ch
        ik = lax.broadcasted_iota(jnp.int32, (ch, keys), 1)
        own_ok = iq >= ik
        par_ok = ik < (j + c) * ch
        contract = (((1,), (1,)), ((), ()))
        cols = pl.ds(al(i * HEAD_DIM, 128), HEAD_DIM)
        v_cols = pl.ds(al(hc + i * HEAD_DIM, 128), HEAD_DIM)
        q = qb[n, :, cols]
        k_own = kvo[s, 0 : j + 1, :, cols].reshape(keys, HEAD_DIM)
        k_par = kvp[s, 0 : j + 1, :, cols].reshape(keys, HEAD_DIM)
        s_own = lax.dot_general(q, k_own, contract, preferred_element_type=F32) * HEAD_DIM**-0.5
        s_par = lax.dot_general(q, k_par, contract, preferred_element_type=F32) * HEAD_DIM**-0.5
        s_own = jnp.where(own_ok, s_own, -1e30)
        s_par = jnp.where(par_ok, s_par, -1e30)
        top = jnp.maximum(jnp.max(s_own, axis=1, keepdims=True), jnp.max(s_par, axis=1, keepdims=True))
        e_own, e_par = jnp.exp(s_own - top), jnp.exp(s_par - top)
        inv = 1.0 / (jnp.sum(e_own, axis=1, keepdims=True) + jnp.sum(e_par, axis=1, keepdims=True))
        v_own = kvo[s, 0 : j + 1, :, v_cols].reshape(keys, HEAD_DIM)
        v_par = kvp[s, 0 : j + 1, :, v_cols].reshape(keys, HEAD_DIM)
        out = jnp.dot((e_own * inv).astype(BF16), v_own, preferred_element_type=F32)
        out += jnp.dot((e_par * inv).astype(BF16), v_par, preferred_element_type=F32)
        og[n, :, pl.ds(al((2 * ng + kh) * hc + i * HEAD_DIM, 128), HEAD_DIM)] = out.astype(BF16)

    def A(g):
        for r, j in GROUPS[g]:
            kv_copy(r, j).wait_recv()

        def head(i, carry):
            for r, j in GROUPS[g]:
                attend(r, j, i)
            return carry

        lax.fori_loop(0, hc // HEAD_DIM, head, 0)
        for r, j in GROUPS[g]:
            og_copy(0, r * NJ + j).start()
            og_copy(1, r * NJ + j).start()

    def P(g):
        for r, j in GROUPS[g]:
            for kind in range(2):
                og_wait(kind, r * NJ + j)
                og_copy(kind + 2, r * NJ + j).start()

    def X(g):
        for r, j in GROUPS[g]:
            og_wait(2, r * NJ + j)
            og_wait(3, r * NJ + j)

        def done(col, size, out):
            for i, (r, j) in enumerate(GROUPS[g]):
                zb[r, j, :, pl.ds(al(col, 128), size)] = out[i * ch : (i + 1) * ch].astype(BF16)

        product([og.at[r * NJ + j] for r, j in GROUPS[g]], wob, wob.shape[0], kc, done, 512 if GROUPS[g][0][0] == 0 else 256)
        for r, j in GROUPS[g]:
            if r == 2:
                reduce.halves(j)

    def T(j):
        def done(rows, attn):
            h_ref[j, rows, :] = (xc[j, rows, :].astype(F32) + attn.astype(BF16).astype(F32)).astype(BF16)

        reduce.total(j, done)
        chunk_out(j).start()

    def chunk_out(j):
        return pltpu.make_async_copy(h_ref.at[j], h_hbm.at[j], lx.at[1 + j])

    def h_out(r, u):
        rows = pl.ds(u * (ch // 2), ch // 2)
        return pltpu.make_async_copy(hg.at[ahead.seqs[r], 0, rows], hg_all.at[ahead.seqs[r], rows], lh.at[r, u])

    kept = []

    def HF(u):
        if not kept:
            kept.append(u)
            ahead.keep_own()
        ahead.XF(0, u)

    def HY(u):
        ahead.YH(u)
        for r in (0, 1, 3):
            h_out(r, u).start()

    def HO(u):
        for d in range(2):
            ahead.yhalf_wait(d, u)
        h_out(2, u).start()

    def own_rows():
        for half, i in pieces:
            w_local(half, i).start()
        o_local.start()
        for m in range(2):
            d_in(m).start()
        x_in.wait()
        for j in range(NJ):
            xc[j, :, half_cols(c)] = x_ref[x_rows(j, c), :]

    x_in = pltpu.make_async_copy(x_hbm, x_ref, lx.at[0])
    x_in.start()
    tables = [pltpu.make_async_copy(src, dst, lx.at[1 + NJ + i]) for i, (src, dst) in enumerate(((turn_hbm, turn_ref), (base_hbm, base_ref)))]
    for copy in tables:
        copy.start()
    at.barrier(own_rows)

    def angles():
        for copy in tables:
            copy.wait()
        lane = lax.broadcasted_iota(jnp.int32, (ch, HEAD_DIM), 1)
        for j in range(NJ):
            base_cos, base_sin = base_ref[0, pl.ds(2 * j + c, 1), :], base_ref[1, pl.ds(2 * j + c, 1), :]
            cos_all[j] = base_cos * turn_ref[0] - base_sin * turn_ref[1]
            sine = base_sin * turn_ref[0] + base_cos * turn_ref[1]
            sin_all[j] = jnp.where(lane < HEAD_DIM // 2, -sine, sine)

    ops = {
        "XP": XP, "WOP": WOP, "XE": XE, "ST": ST, "N": N, "YH": gather.YH, "WA": WA, "WP": WP, "S": S, "O": O, "F": F, "DP": DP,
        "G": G, "Q": Q, "R": R, "A": A, "P": P, "X": X, "M": reduce.middle, "T": T,
        "HF": HF, "HH": lambda u: ahead.XH(0, u), "HN": lambda u: ahead.N(0, u), "HY": HY, "HO": HO,
    }
    def all_sent(ref, sem):
        remote(ref, ref, sem, ro.at[0], at.partner).wait_send()

    def sent():
        for m in range(2):
            for k in range(4):
                d_pair(m, k, 1 - c).wait_recv()
            d_out(m).wait()
        all_sent(w_all.at[:, :, pl.ds(0, 4 * kd)], sdp.at[0])
        for d in range(2):
            all_sent(w_all.at[:, :, pl.ds(0, kd)], sds.at[d])
            all_sent((drel_a, drel_b)[d], sdo.at[d])
            all_sent((drel_a, drel_b)[d], sdf.at[d])
            for u in range(len(units)):
                gather.ycopy(d, u).wait_send()
                gather.yhalf(d, u).wait_send()
        all_sent(x_ref.at[pl.ds(0, NJ * ch)], sd.at[0])
        all_sent(xc, sxe.at[0])
        all_sent(st_own, sst.at[0])
        reduce.drain()
        ahead.drain()
        for r in range(NX):
            for u in range(2):
                h_out(r, u).wait()
        o_pair.wait_send()
        for sem in (swa, swo, swp):
            all_sent(wb.at[pl.ds(0, kd)], sem.at[0])
        all_sent(part.at[:, :, pl.ds(0, 3 * hc)], spr.at[0])
        all_sent(kvo, skv.at[0])
        for kind, (lo, n) in enumerate(((0, ch), (0, ch), (0, cut), (cut, ch - cut))):
            all_sent(og.at[:, pl.ds(lo, n), o_cols(x)], sog.at[kind])

    waits = {"X": o_ready, "WP": angles}
    last = max(i for i, step in enumerate(ATTENTION_STEPS) if step[0] == "X")
    for i, step in enumerate(ATTENTION_STEPS):
        if step[0] in waits:
            waits.pop(step[0])()
        if i == last:
            sent()
        ops[step[0]](*step[1:])
    for j in range(NJ):
        chunk_out(j).wait()


def mlp_kernel(
    units, h_hbm, w_hbm, wdn, hg_hbm, y_ref,
    h_ref, xg, wt, raw, wd, ag, ar, act, s1, s2, zb, ya, yb, yfd, yfu, yst,
    sx, rx, sy, ry, syh, ryh, sa, ra, syr, ryr, sd, rd, lw, lwd, swd, rwd, lh, lo,
):
    at = Place()
    x, c, y = at.x, at.c, at.y
    ch, kc, h = h_ref.shape[1], h_ref.shape[2], h_ref.shape[1] // 2
    width = xg.shape[-1]
    kd = kc // 2
    fc, tiles = w_hbm.shape[1], wt.shape[1] // 256
    fm = (tiles - 1) * 128
    fr = fc - fm
    blocks, slots = 2 * tiles, raw.shape[0]
    gather = Spread(at, h_ref, xg, units, (s1, s2), sx, rx, sy, ry, syh, ryh)
    reduce = Reduce(at, zb, ya, yb, yfd, yfu, syr, ryr)

    def w_in(q):
        i, m = q // 2, q % 2
        n = min(128, fc - i * 128)
        return pltpu.make_async_copy(w_hbm.at[m, pl.ds(i * 128, n)], raw.at[q % slots, pl.ds(0, n)], lw.at[q])

    def WT(g):
        for q in range(g * blocks // 4, (g + 1) * blocks // 4):
            i, m, slot = q // 2, q % 2, q % slots
            w_in(q).wait()
            if fc < (i + 1) * 128:
                raw[slot, fc - i * 128 :, :] = jnp.zeros(((i + 1) * 128 - fc, width), BF16)

            def turn(k, carry, slot=slot, q=q):
                part = pl.ds(al(k * (width // 4), 128), width // 4)
                wt[part, q * 128 : (q + 1) * 128] = raw[slot, :, part].T
                return carry

            lax.fori_loop(0, 4, turn, 0)
            if q + slots < blocks:
                w_in(q + slots).start()

    def d_refs(q, core):
        cols = pl.ds(al(core * kd, 128), kd)
        main, rest = wdn.at[pl.ds(q * fc, fm)], wdn.at[pl.ds(q * fc + fm, fr)]
        return (main, wd.at[pl.ds(q * fm, fm), cols]), (rest, wd.at[pl.ds(NX * fm + q * 128, fr), cols])

    def d_own(q, k):
        src, dst = d_refs(q, c)[k]
        return pltpu.make_async_copy(src, dst, lwd.at[q, k])

    def d_pair(q, k, core):
        src, dst = d_refs(q, core)[k]
        return remote(src, dst, swd.at[q, k], rwd.at[q, k], at.partner)

    quarters = [(q, k) for q in range(NX) for k in range(2)]
    h_in_all = pltpu.make_async_copy(h_hbm, h_ref, lo.at[NJ])
    h_in_all.start()
    def h_in(s):
        return pltpu.make_async_copy(hg_hbm.at[s], xg.at[s, 0], lh.at[s])

    def local_copies():
        for q in range(slots):
            w_in(q).start()
        for s in range(NX):
            h_in(s).start()
        for q, k in quarters:
            d_own(q, k).start()
        for q in range(NX):
            wd[NX * fm + q * 128 + fr : NX * fm + (q + 1) * 128, :] = jnp.zeros((128 - fr, kc), BF16)
        h_in_all.wait()

    at.barrier(local_copies)
    for q, k in quarters:
        d_pair(q, k, c).start()

    def a_refs(kind, n, xx):
        main, rest = pl.ds(al(xx * fm, 128), fm), pl.ds(al(xx * 128, 128), 128)
        if kind < 2:
            return ag.at[n, :, main], ar.at[n, :, rest]
        lo = (kind - 2) * h
        return ag.at[n, pl.ds(lo, h), main], ar.at[n, pl.ds(lo // 2, h // 2), rest]

    def a_copies(kind, n):
        refs = a_refs(kind, n, (x, x, at.xl, at.xr)[kind])
        return [remote(v, v, sa.at[kind, k], ra.at[kind, n, k], at.left if kind % 2 else at.right) for k, v in enumerate(refs)]

    def a_wait(kind, n):
        for k, v in enumerate(a_refs(kind, n, (at.xl, at.xr, at.xo, at.xo)[kind])):
            remote(v, v, sa.at[kind, k], ra.at[kind, n, k], at.right).wait_recv()

    def a_start(kind, n):
        for copy in a_copies(kind, n):
            copy.start()

    def G(g):
        for r, j in GROUPS[g]:
            gather.chunk_wait(r, j)

        def done(col, size, out):
            for k in range(0, size, 256):
                gate, up = out[:, k : k + 128].astype(BF16).astype(F32), out[:, k + 128 : k + 256].astype(BF16).astype(F32)
                value = (gate / (1.0 + jnp.exp(-gate)) * up).astype(BF16)
                act[0 : value.shape[0], pl.ds(al(div(col + k, 2), 128), 128)] = value

        product([xg.at[gather.seqs[r], j] for r, j in GROUPS[g]], wt, width, wt.shape[1], done)
        for i, (r, j) in enumerate(GROUPS[g]):
            n, lo = r * NJ + j, i * ch
            ag[n, :, pl.ds(al(x * fm, 128), fm)] = act[lo : lo + ch, :fm]
            below = pltpu.roll(act[lo + h : lo + ch, fm:].astype(F32), 64, axis=1)
            ar[n, :, pl.ds(al(x * 128, 128), 128)] = (act[lo : lo + h, fm:].astype(F32) + below).astype(BF16)
            for kind in range(2):
                a_start(kind, n)

    def P(g):
        for r, j in GROUPS[g]:
            for kind in range(2):
                a_wait(kind, r * NJ + j)
                a_start(kind + 2, r * NJ + j)

    def unpack(g):
        for r, j in GROUPS[g]:
            n = r * NJ + j
            for kind in (2, 3):
                a_wait(kind, n)
            lane = lax.broadcasted_iota(jnp.int32, (h, 128), 1)
            for q in range(NX):
                cols = pl.ds(NX * fm + q * 128, 128)
                rest = ar[n, :, q * 128 : (q + 1) * 128].astype(F32)
                ag[n, 0:h, cols] = jnp.where(lane < 64, rest, 0.0).astype(BF16)
                ag[n, h:, cols] = jnp.where(lane < 64, pltpu.roll(rest, 64, axis=1), 0.0).astype(BF16)

    def X(g):
        unpack(g)

        def done(col, size, out):
            for i, (r, j) in enumerate(GROUPS[g]):
                zb[r, j, :, pl.ds(al(col, 128), size)] = out[i * ch : (i + 1) * ch].astype(BF16)

        product([ag.at[r * NJ + j] for r, j in GROUPS[g]], wd, wd.shape[0], kc, done, 512 if len(GROUPS[g]) == 1 else 256)
        for r, j in GROUPS[g]:
            if r == 2:
                reduce.halves(j)

    def half_cols(core):
        return pl.ds(al(core * kd, 128), kd)

    def y_rows(j, core):
        return pl.ds(al((2 * j + core) * ch, 8), ch)

    def y_copy(j):
        return remote(yst.at[1 - c, j], y_ref.at[y_rows(j, c)], sd.at[j], rd.at[j], at.partner)

    def y_own(j):
        return pltpu.make_async_copy(yst.at[c, j], y_ref.at[y_rows(j, c)], lo.at[j])

    def y_wait(j):
        dst = y_ref.at[y_rows(j, 1 - c)]
        remote(dst, dst, sd.at[j], rd.at[j], at.partner).wait_recv()

    def T(j):
        def done(rows, mlp):
            out = (h_ref[j, rows, :].astype(F32) + mlp.astype(BF16).astype(F32)).astype(BF16)
            yst[0, j, rows, :] = out[:, :kd]
            yst[1, j, rows, :] = out[:, kd:]

        reduce.total(j, done)
        y_copy(j).start()
        y_own(j).start()

    def XT(g):
        ((_, j),) = GROUPS[g]
        unpack(g)
        reduce.wait(2, j)
        reduce.wait(3, j)

        def half(i, carry):
            core = 1 - c + i * (2 * c - 1)
            cols = half_cols(core)
            out = jnp.dot(ag[j], wd[:, cols], preferred_element_type=F32).astype(BF16).astype(F32)
            mlp = out + yfd[j, :, cols].astype(F32) + yfu[j, :, cols].astype(F32)
            yst[core, j] = (h_ref[j, :, cols].astype(F32) + mlp.astype(BF16).astype(F32)).astype(BF16)
            pl.when(i == 0)(lambda: y_copy(j).start())
            return carry

        lax.fori_loop(0, 2, half, 0)
        y_own(j).start()

    ops = {"G": G, "P": P, "X": X, "M": reduce.middle, "T": T, "XT": XT, "WT": WT}
    for name in ("YR", "YRH", "YH", "XF", "XH", "N"):
        ops[name] = getattr(gather, name)
    waits = {
        "N": gather.keep_own,
        "G": lambda: [h_in(s).wait() for s in range(NX)],
        "X": lambda: [(d_own(q, k).wait(), d_pair(q, k, 1 - c).wait_recv()) for q, k in quarters],
    }
    def sent():
        gather.drain()
        reduce.drain()
        for q, k in quarters:
            d_pair(q, k, c).wait_send()

        for kind in range(4):
            for k, every in enumerate(a_refs(kind, slice(None), x)):
                remote(every, every, sa.at[kind, k], ra.at[kind, 0, k], at.right).wait_send()

    (_, g), (_, j) = MLP_STEPS[-2:]
    assert MLP_STEPS[-2:] == (("X", g), ("T", j)) and GROUPS[g] == ((0, j),)
    for step in (*MLP_STEPS[:-2], ("XT", g)):
        if step[0] in waits:
            waits.pop(step[0])()
        ops[step[0]](*step[1:])
    sent()
    for j in range(NJ):
        y_copy(j).wait_send()
        y_own(j).wait()
        y_wait(j)


def vmem(*shape, dtype=BF16):
    return pltpu.VMEM(shape, dtype)


def sems(*shape):
    return pltpu.SemaphoreType.DMA(shape)


def solution(mesh):
    assert mesh.shape["tx"] == 2 * NX and mesh.shape["ty"] == NX
    act_spec = P(("dp", "ty"), None, "tx")
    col_spec = P("tx", "ty")
    row_spec = P("ty", "tx")
    any_spec = pl.BlockSpec(memory_space=pl.ANY)
    vmem_spec = pl.BlockSpec(memory_space=pltpu.VMEM)

    def layer(x_blk, w_q, w_k, w_v, w_o, w_gate, w_up, w_down):
        _, seq, kd = x_blk.shape
        kc, width = 2 * kd, 2 * NX * kd
        ch = seq // (2 * NJ)
        h = ch // 2
        row_heads = w_q.shape[1]
        hc = row_heads // NX
        fc = w_down.shape[0] // NX
        assert hc % HEAD_DIM == 0
        tiles = (fc + 127) // 128
        f_a = (fc // 2 + 15) // 16 * 16

        inv_freq = THETA ** (-2.0 * np.arange(HEAD_DIM // 2) / HEAD_DIM)
        inv_freq = np.concatenate([inv_freq, inv_freq])
        turn = np.arange(ch)[:, None] * inv_freq
        base = np.arange(2 * NJ)[:, None] * ch * inv_freq
        turn = jnp.asarray(np.stack([np.cos(turn), np.sin(turn)]), F32)
        base = jnp.asarray(np.stack([np.cos(base), np.sin(base)]), F32)

        reduce_scratch = [vmem(NX, NJ, ch, kc), vmem(NJ, h, kc), vmem(NJ, ch - h, kc), vmem(NJ, ch, kc), vmem(NJ, ch, kc)]
        units = ((0, 0, h, 0), (0, h, h, 0)) + tuple((j, 0, ch, 0) for j in range(1, NJ))
        n_u = len(units)
        h_blk, w_all, hg_all = pl.pallas_call(
            functools.partial(attention_kernel, units),
            out_shape=(
                jax.ShapeDtypeStruct((NJ, ch, kc), BF16),
                jax.ShapeDtypeStruct((2, fc, width), BF16),
                jax.ShapeDtypeStruct((NX, ch, width), BF16),
            ),
            in_specs=[any_spec] * 9,
            out_specs=(any_spec, any_spec, any_spec),
            scratch_shapes=[
                vmem(seq, kd), vmem(2, ch, HEAD_DIM, dtype=F32), vmem(2, 2 * NJ, HEAD_DIM, dtype=F32),
                vmem(NJ, ch, kc), vmem(NJ, ch, kc), vmem(NX, NJ, ch, 2 * kc), vmem(NX, 1, ch, width), vmem(NJ, ch, HEAD_DIM, dtype=F32), vmem(NJ, ch, HEAD_DIM, dtype=F32),
                vmem(NJ, ch // 4, 128, dtype=F32), vmem(NJ, ch // 4, 128, dtype=F32), vmem(ch, 128, dtype=F32), vmem(ch, 128, dtype=F32),
                vmem(2 * kc, 6 * hc), vmem(row_heads, kc), vmem(NCH, ch, 6 * hc), vmem(NCH, ch, 3 * hc), vmem(NCH, ch, hc),
                vmem(NX, NJ, ch, 2 * hc), vmem(NX, NJ, ch, 2 * hc), vmem(NCH, ch, row_heads), *reduce_scratch,
                vmem(2, fc, kd), vmem(2, f_a, kd), vmem(2, fc - f_a, kd),
                sems(1), sems(n_u), sems(1), sems(n_u), sems(2, n_u), sems(2, n_u), sems(2, n_u), sems(2, n_u),
                sems(1), sems(NJ), sems(1), sems(2, 3), sems(1), sems(2, 3), sems(1), sems(2), sems(3, 3), sems(1), sems(1),
                sems(1), sems(NCH), sems(1), sems(NCH), sems(4), sems(4, NCH), sems(4), sems(4, NJ),
                sems(2, 2), sems(2), sems(2, 2, 2), sems(2), sems(2, 2), sems(2), sems(2, 2), sems(1), sems(2, 4),
                sems(4, 2), sems(4, 2), sems(2, 2), sems(2, 2), sems(2, 2), sems(2, 2), sems(NX, 2), sems(3 + NJ),
            ],
            compiler_params=pltpu.CompilerParams(collective_id=0, has_side_effects=True, vmem_limit_bytes=VMEM_LIMIT),
            name="attention_part",
        )(x_blk[0], turn, base, w_q, w_k, w_v, w_o, w_gate.T, w_up.T)

        units = ((1, 0, h, 1), (1, h, h, 0)) + tuple((j, 0, ch, 0) for j in range(2, NJ))
        n_u, n_x = len(units), len(units) + 3
        y_blk = pl.pallas_call(
            functools.partial(mlp_kernel, units),
            out_shape=jax.ShapeDtypeStruct((seq, kd), BF16),
            in_specs=[any_spec] * 4,
            out_specs=any_spec,
            scratch_shapes=[
                vmem(NJ, ch, kc),
                vmem(NX, NJ, ch, width), vmem(width, tiles * 256), vmem(3, 128, width),
                vmem(NX * tiles * 128, kc), vmem(NCH, ch, NX * tiles * 128), vmem(NCH, h, NX * 128), vmem(2 * ch, tiles * 128),
                vmem(ch, 128, dtype=F32), vmem(ch, 128, dtype=F32),
                *reduce_scratch, vmem(2, NJ, ch, kd),
                sems(4, n_x), sems(4, n_x), sems(2, n_u), sems(2, n_u), sems(2, n_u), sems(2, n_u),
                sems(4, 2), sems(4, NCH, 2), sems(4), sems(4, NJ), sems(NJ), sems(NJ),
                sems(2 * tiles), sems(NX, 2), sems(NX, 2), sems(NX, 2), sems(NX), sems(NJ + 1),
            ],
            compiler_params=pltpu.CompilerParams(collective_id=1, has_side_effects=True, vmem_limit_bytes=VMEM_LIMIT),
            name="mlp_part",
        )(h_blk, w_all, w_down, hg_all)
        return y_blk[None]

    return jax.shard_map(
        layer,
        mesh=mesh,
        in_specs=(act_spec, col_spec, col_spec, col_spec, row_spec, col_spec, col_spec, row_spec),
        out_specs=act_spec,
        check_vma=False,
    )
```

```python
import functools

import jax
import jax.numpy as jnp
import numpy as np
from jax import lax
from jax.experimental import pallas as pl
from jax.experimental.pallas import tpu as pltpu
from jax.sharding import PartitionSpec as P

HEAD_DIM = 128
EPS = 1e-5
THETA = 10000.0
MESH = pl.DeviceIdType.MESH
F32 = jnp.float32
BF16 = jnp.bfloat16
NX = 4
NJ = 4
NCH = 16
VMEM_LIMIT = 67_043_328
GROUPS = (*(((0, j),) for j in range(NJ)), *(((3, j), (1, j)) for j in range(NJ)), *(((2, j),) for j in range(NJ)))


def rem(a, b):
    return lax.rem(a, jnp.int32(b))


def div(a, b):
    return lax.div(a, jnp.int32(b))


def al(v, m):
    return pl.multiple_of(v, m)


def remote(src, dst, ssem, rsem, dev):
    return pltpu.make_async_remote_copy(src_ref=src, dst_ref=dst, send_sem=ssem, recv_sem=rsem, device_id=dev, device_id_type=MESH)


ATTENTION_STEPS = (
    ("WA", 0), ("XP", 1), ("S", "b", 0, 1), ("XP", 0), ("XE", 1), ("XE", 0), ("XE", 2), ("XP", 2), ("S", "b", 0, 0), ("XP", 3),
    ("S", "b", 1, 0), ("ST", 1), ("WP", 0), ("WA", 1), ("O", "b", 1), ("ST", 0), ("N", 1), ("O", "b", 0), ("ST", 2),
    ("S", "b", 1, 1), ("WOP",), ("N", 0), ("G", 0), ("XE", 3), ("YH", 1), ("YH", 0), ("S", "a", 0, 1), ("N", 2), ("WP", 1),
    ("G", 8), ("G", 4), ("ST", 3), ("Q", 8), ("Q", 0), ("R", 8), ("XE", 4), ("A", 8), ("F", "a", 1), ("YH", 2), ("G", 5),
    ("R", 4), ("ST", 4), ("N", 3), ("P", 8), ("G", 9), ("A", 4), ("R", 0), ("S", "a", 1, 1), ("X", 8), ("G", 1), ("N", 4),
    ("R", 5), ("A", 0), ("R", 9), ("P", 4), ("A", 9), ("A", 5), ("G", 2), ("P", 0), ("X", 4), ("M", 0), ("P", 9),
    ("S", "a", 1, 0), ("YH", 3), ("G", 6), ("P", 5), ("X", 0), ("T", 0), ("HF", 1), ("HF", 0), ("R", 2), ("X", 9), ("R", 1),
    ("A", 1), ("YH", 4), ("X", 5), ("M", 1), ("HH", 1), ("O", "a", 0), ("G", 10), ("R", 6), ("HH", 0), ("G", 7), ("O", "a", 1),
    ("HN", 1), ("R", 10), ("G", 11), ("A", 10), ("A", 6), ("HN", 0), ("R", 7), ("A", 2), ("HY", 1), ("A", 7), ("R", 11),
    ("P", 10), ("A", 11), ("P", 6), ("G", 3), ("P", 7), ("P", 11), ("F", "b", 1), ("F", "a", 0), ("X", 10), ("HY", 0),
    ("S", "a", 0, 0), ("F", "b", 0), ("R", 3), ("X", 11), ("A", 3), ("X", 6), ("HO", 1), ("X", 7), ("P", 1), ("P", 2),
    ("M", 2), ("M", 3), ("DP", 1), ("DP", 0), ("P", 3), ("HO", 0), ("X", 1), ("T", 1), ("X", 2), ("T", 2), ("X", 3), ("T", 3),
)
MLP_STEPS = (
    ("XF", 0, 1), ("XF", 0, 0), ("WT", 0), ("YR", 0), ("WT", 1), ("XH", 0, 1), ("XF", 0, 3), ("YRH", 0), ("XF", 3, 0),
    ("N", 0, 1), ("XH", 0, 3), ("XF", 1, 0), ("XF", 2, 0), ("WT", 2), ("WT", 3), ("N", 0, 3), ("XF", 0, 2), ("G", 4),
    ("YH", 1), ("G", 0), ("XH", 2, 0), ("G", 8), ("XH", 1, 0), ("XH", 0, 0), ("XH", 3, 0), ("XH", 0, 2), ("G", 3), ("YH", 3),
    ("G", 7), ("N", 3, 0), ("N", 0, 2), ("N", 1, 0), ("P", 8), ("N", 2, 0), ("G", 9), ("G", 11), ("P", 4), ("G", 5), ("P", 11),
    ("X", 8), ("P", 7), ("P", 9), ("X", 4), ("YH", 2), ("G", 6), ("X", 11), ("X", 7), ("P", 5), ("X", 9), ("N", 0, 0),
    ("M", 0), ("G", 10), ("G", 1), ("M", 3), ("X", 5), ("M", 1), ("P", 10), ("P", 6), ("P", 0), ("G", 2), ("X", 10), ("P", 3),
    ("P", 1), ("X", 6), ("M", 2), ("P", 2), ("X", 0), ("T", 0), ("X", 3), ("T", 3), ("X", 1), ("T", 1), ("X", 2), ("T", 2),
)


class Place:
    def __init__(self):
        tx, ty = lax.axis_index("tx"), lax.axis_index("ty")
        self.x, self.c, self.y = div(tx, 2), rem(tx, 2), ty
        x, c, y = self.x, self.c, self.y
        self.xr, self.xl, self.xo = rem(x + 1, NX), rem(x + 3, NX), rem(x + 2, NX)
        self.yu, self.yd, self.yo = rem(y + 1, NX), rem(y + 3, NX), rem(y + 2, NX)
        self.right = {"tx": self.xr * 2 + c, "ty": y}
        self.left = {"tx": self.xl * 2 + c, "ty": y}
        self.up = {"tx": tx, "ty": self.yu}
        self.down = {"tx": tx, "ty": self.yd}
        self.partner = {"tx": x * 2 + 1 - c, "ty": y}
        self.xa, self.xb = x + 1 - 2 * rem(x, 2), rem(x + 3 + 2 * rem(x, 2), NX)
        self.pa, self.pb = {"tx": self.xa * 2 + c, "ty": y}, {"tx": self.xb * 2 + c, "ty": y}

    def barrier(self, between):
        sem = pltpu.get_barrier_semaphore()
        for dev in (self.right, self.left, self.up, self.down, self.partner):
            pl.semaphore_signal(sem, inc=1, device_id=dev, device_id_type=MESH)
        between()
        pl.semaphore_wait(sem, 5)


class Spread:
    def __init__(self, at, src, xg, units, sums, sx, rx, sy, ry, syh, ryh):
        self.sums = sums
        self.at, self.src, self.xg, self.units, self.kc = at, src, xg, units, src.shape[2]
        self.sx, self.rx, self.sy, self.ry, self.syh, self.ryh = sx, rx, sy, ry, syh, ryh
        pairs = [(r, u) for u, unit in enumerate(units) for r in ((0, 3, 1, 2) if unit[3] else (0,))]
        self.index = {pair: i for i, pair in enumerate(pairs)}
        self.seqs = (at.y, at.yu, at.yo, at.yd)

    def cols(self, x):
        return pl.ds(al(x * self.kc, 128), self.kc)

    def keep_own(self):
        for j in {unit[0]: 0 for unit in self.units}:
            self.xg[self.at.y, j, :, self.cols(self.at.x)] = self.src[j]

    def xcopy(self, kind, r, u):
        at, s = self.at, self.seqs[r]
        j, lo, n, _ = self.units[u]
        i = self.index[r, u]
        if kind < 2:
            dst = self.xg.at[s, j, pl.ds(lo, n), self.cols(at.x)]
            src = self.src.at[j, pl.ds(lo, n)] if r == 0 else dst
        elif kind == 2:
            src = dst = self.xg.at[s, j, pl.ds(lo, n // 2), self.cols(at.xl)]
        else:
            src = dst = self.xg.at[s, j, pl.ds(lo + n // 2, n // 2), self.cols(at.xr)]
        return remote(src, dst, self.sx.at[kind, i], self.rx.at[kind, i], at.left if kind % 2 else at.right)

    def xwait(self, kind, r, u):
        at = self.at
        j, lo, n, _ = self.units[u]
        i = self.index[r, u]
        x = (at.xl, at.xr, at.xo, at.xo)[kind]
        rows = (pl.ds(lo, n), pl.ds(lo, n), pl.ds(lo, n // 2), pl.ds(lo + n // 2, n // 2))[kind]
        dst = self.xg.at[self.seqs[r], j, rows, self.cols(x)]
        remote(dst, dst, self.sx.at[kind, i], self.rx.at[kind, i], at.right).wait_recv()

    def yref(self, s, u, lo, n):
        j, _, _, first = self.units[u]
        rows = pl.ds(lo, n)
        return self.xg.at[s, j, rows, self.cols(self.at.x)] if first else self.xg.at[s, j, rows]

    def ycopy(self, d, u):
        j, lo, n, first = self.units[u]
        dst = self.yref(self.at.y, u, lo, n)
        src = self.src.at[j, pl.ds(lo, n)] if first else dst
        return remote(src, dst, self.sy.at[d, u], self.ry.at[d, u], self.at.down if d else self.at.up)

    def ywait(self, d, u):
        _, lo, n, _ = self.units[u]
        dst = self.yref(self.at.yu if d else self.at.yd, u, lo, n)
        remote(dst, dst, self.sy.at[d, u], self.ry.at[d, u], self.at.up).wait_recv()

    def yhalf(self, d, u):
        _, lo, n, _ = self.units[u]
        ref = self.yref(self.at.yu if d else self.at.yd, u, lo + d * (n // 2), n // 2)
        return remote(ref, ref, self.syh.at[d, u], self.ryh.at[d, u], self.at.down if d else self.at.up)

    def yhalf_wait(self, d, u):
        _, lo, n, _ = self.units[u]
        dst = self.yref(self.at.yo, u, lo + d * (n // 2), n // 2)
        remote(dst, dst, self.syh.at[d, u], self.ryh.at[d, u], self.at.up).wait_recv()

    def YR(self, u):
        for d in range(2):
            self.ycopy(d, u).start()

    def YH(self, u):
        for d in range(2):
            self.ywait(d, u)
            self.yhalf(d, u).start()

    YRH = YH

    def XF(self, r, u):
        if r == 2:
            for d in range(2):
                self.yhalf_wait(d, u)
        for kind in range(2):
            self.xcopy(kind, r, u).start()

    def XH(self, r, u):
        for kind in range(2):
            self.xwait(kind, r, u)
            self.xcopy(kind + 2, r, u).start()

    def N(self, r, u):
        j, lo, n, first = self.units[u]
        for kind in (2, 3):
            self.xwait(kind, r, u)
            self.xcopy(kind, r, u).wait_send()
        if r:
            for kind in range(2):
                self.xcopy(kind, r, u).wait_send()
        if r % 2:
            self.yhalf(0 if r == 3 else 1, u).wait_send()
        width, ref = self.xg.shape[-1], self.xg.at[self.seqs[r], j]
        s1, s2 = self.sums
        lane_sums(ref, lo, n, s1, s2)
        mean = jnp.sum(s1[0:n, :], axis=-1, keepdims=True) / width
        var = jnp.sum(s2[0:n, :], axis=-1, keepdims=True) / width - mean * mean
        s1[0:n, :] = jnp.broadcast_to(mean, (n, 128))
        s2[0:n, :] = jnp.broadcast_to(lax.rsqrt(var + EPS), (n, 128))
        scale_rows(ref, lo, n, s1, s2)
        if not first:
            self.YR(u)

    def chunk_wait(self, r, j):
        if r == 2:
            for u, unit in enumerate(self.units):
                if unit[0] == j and not unit[3]:
                    for d in range(2):
                        self.yhalf_wait(d, u)

    def drain(self):
        for u, unit in enumerate(self.units):
            for d in range(2):
                self.xcopy(d, 0, u).wait_send()
                self.ycopy(d, u).wait_send()
                if not unit[3]:
                    self.yhalf(d, u).wait_send()


def rows_of(refs):
    return refs[0][...] if len(refs) == 1 else jnp.concatenate([ref[...] for ref in refs], axis=0)


def product(refs, weight, depth, n_cols, done, step=256):
    step = 256 if n_cols % step else step

    def columns(i, carry):
        out = jnp.dot(rows_of(refs), weight[0:depth, pl.ds(al(i * step, 128), step)], preferred_element_type=F32)
        done(i * step, step, out)
        return carry

    lax.fori_loop(0, n_cols // step, columns, 0)


def lane_sums(ref, lo, n, s1, s2):
    width, rows, wide = ref.shape[-1], 32, 512

    def some_rows(i, carry):
        def some_columns(k, sums):
            a, b = sums
            v = ref[pl.ds(al(lo + i * rows, 8), rows), pl.ds(al(k * wide, 128), wide)].astype(F32)
            for c in range(0, wide, 128):
                part = v[:, c : c + 128]
                a, b = a + part, b + part * part
            return a, b

        zero = jnp.zeros((rows, 128), F32)
        a, b = lax.fori_loop(0, width // wide, some_columns, (zero, zero))
        s1[pl.ds(al(i * rows, 8), rows), :] = a
        s2[pl.ds(al(i * rows, 8), rows), :] = b
        return carry

    lax.fori_loop(0, n // rows, some_rows, 0)


def scale_rows(ref, lo, n, means, scales):
    width, rows, wide = ref.shape[-1], 32, 512

    def some_rows(i, carry):
        mean, scale = (t[pl.ds(al(i * rows, 8), rows), :] for t in (means, scales))

        def some_columns(k, carry):
            at_rows = pl.ds(al(lo + i * rows, 8), rows)
            for c in range(0, wide, 128):
                cols = pl.ds(al(k * wide + c, 128), 128)
                ref[at_rows, cols] = ((ref[at_rows, cols].astype(F32) - mean) * scale).astype(BF16)
            return carry

        lax.fori_loop(0, width // wide, some_columns, 0)
        return carry

    lax.fori_loop(0, n // rows, some_rows, 0)


class Reduce:
    def __init__(self, at, zb, ya, yb, yfd, yfu, ss, rs):
        self.at, self.zb, self.ya, self.yb, self.yfd, self.yfu, self.ss, self.rs = at, zb, ya, yb, yfd, yfu, ss, rs
        self.ch = zb.shape[2]
        self.h = self.ch // 2

    def copy(self, kind, j):
        at, h, ch = self.at, self.h, self.ch
        src, dst = (
            lambda: (self.zb.at[2, j, pl.ds(0, h)], self.ya.at[j]),
            lambda: (self.zb.at[2, j, pl.ds(h, ch - h)], self.yb.at[j]),
            lambda: (self.zb.at[1, j], self.yfd.at[j]),
            lambda: (self.zb.at[3, j], self.yfu.at[j]),
        )[kind]()
        return remote(src, dst, self.ss.at[kind], self.rs.at[kind, j], at.down if kind % 2 else at.up)

    def wait(self, kind, j):
        self.copy(kind, j).wait_recv()

    def halves(self, j):
        self.copy(0, j).start()
        self.copy(1, j).start()

    def middle(self, j):
        h = self.h

        def add(r, lo, part):
            def some_rows(i, carry):
                rows, src = pl.ds(al(lo + i * 32, 8), 32), pl.ds(al(i * 32, 8), 32)
                self.zb[r, j, rows, :] = (self.zb[r, j, rows, :].astype(F32) + part[j, src, :].astype(F32)).astype(BF16)
                return carry

            lax.fori_loop(0, h // 32, some_rows, 0)

        self.wait(0, j)
        add(1, 0, self.ya)
        self.copy(2, j).start()
        self.wait(1, j)
        add(3, h, self.yb)
        self.copy(3, j).start()

    def total(self, j, done):
        self.wait(2, j)
        self.wait(3, j)

        def some_rows(i, carry):
            rows = pl.ds(al(i * 32, 8), 32)
            out = self.zb[0, j, rows, :].astype(F32) + self.yfd[j, rows, :].astype(F32) + self.yfu[j, rows, :].astype(F32)
            done(rows, out)
            return carry

        lax.fori_loop(0, self.ch // 32, some_rows, 0)

    def drain(self):
        h = self.h
        for kind, every in enumerate((self.zb.at[2, :, 0:h], self.zb.at[2, :, h:], self.zb.at[1], self.zb.at[3])):
            remote(every, every, self.ss.at[kind], self.rs.at[kind, 0], self.at.up).wait_send()


def attention_kernel(
    units, x_hbm, turn_hbm, base_hbm, wq, wk, wv, wo, wg_t, wu_t,
    h_hbm, w_all, hg_all,
    x_ref, turn_ref, base_ref, h_ref, xc, xg, hg, cos_all, sin_all, st_own, st_in, s1, s2, wb, wob, part, precv, qb, kvo, kvp, og, zb, ya, yb, yfd, yfu, own, drel_a, drel_b,
    sxe, rxe, sst, rst, sy, ry, syh, ryh, sd, rd, swa, rwa, swo, rwo, swp, rwp, lw, so, ro, spr, rpr, skv, rkv, sog, rog, syr, ryr,
    lg, sds, rds, sdo, rdo, sdf, rdf, sdp, rdp, shx, rhx, shy, rhy, shz, rhz, lh, lx,
):
    at = Place()
    x, c, y = at.x, at.c, at.y
    ch, kc = xc.shape[1], xc.shape[2]
    kd = wq.shape[0]
    hc = qb.shape[2]
    fc, f_a = w_all.shape[1], drel_a.shape[1]
    width = 2 * xg.shape[3]
    kh = div(x, 2)
    ng = rem(div(x + 1, 2), 2)
    gather = Spread(at, xc, xg, units, (s1, s2), None, None, sy, ry, syh, ryh)
    reduce = Reduce(at, zb, ya, yb, yfd, yfu, syr, ryr)
    ahead = Spread(at, h_ref, hg, ((0, 0, ch // 2, 0), (0, ch // 2, ch // 2, 0)), (s1, s2), shx, rhx, shy, rhy, shz, rhz)
    weights = (wq, wk, wv)

    def half_cols(core):
        return pl.ds(al(core * kd, 128), kd)

    def x_rows(j, core):
        return pl.ds(al((2 * j + core) * ch, 8), ch)

    def x_pair(j):
        return remote(x_ref.at[x_rows(j, 1 - c)], xc.at[j, :, half_cols(c)], sd.at[0], rd.at[j], at.partner)

    def pair_cols(xx):
        return pl.ds(al(rem(xx, 2) * kc, 128), kc)

    def xe_copy(u, xx):
        j, lo, n, _ = units[u]
        rows = pl.ds(lo, n)
        return remote(xc.at[j, rows], xg.at[y, j, rows, pair_cols(xx)], sxe.at[0], rxe.at[u], at.pa)

    def st_copy(u):
        j, lo, n, _ = units[u]
        rows = pl.ds(lo // 4, n // 4)
        return remote(st_own.at[j, rows], st_in.at[j, rows], sst.at[0], rst.at[u], at.pb)

    def XP(j):
        x_pair(j).start()

    arrived = []

    def XE(u):
        j, lo, n, _ = units[u]
        if j not in arrived:
            arrived.append(j)
            dst = xc.at[j, :, half_cols(1 - c)]
            remote(dst, dst, sd.at[0], rd.at[j], at.partner).wait_recv()
        xe_copy(u, x).start()
        xg[y, j, lo : lo + n, pair_cols(x)] = xc[j, lo : lo + n]

    def ST(u):
        j, lo, n, _ = units[u]
        xe_copy(u, at.xa).wait_recv()
        quarter = n // 4
        lane = lax.broadcasted_iota(jnp.int32, (quarter, 128), 1)
        lane_sums(xg.at[y, j], lo, n, s1, s2)
        packed = jnp.zeros((quarter, 128), F32)
        for g in range(4):
            rows = pl.ds(g * quarter, quarter)
            total, square = (jnp.sum(t[rows, :], axis=-1, keepdims=True) for t in (s1, s2))
            packed = jnp.where(lane // 32 == g, jnp.where(lane % 32 < 16, total, square), packed)
        st_own[j, lo // 4 : lo // 4 + quarter, :] = packed
        st_copy(u).start()

    def N(u):
        j, lo, n, _ = units[u]
        st_copy(u).wait_recv()
        quarter = n // 4
        at_rows = slice(lo // 4, lo // 4 + quarter)
        moments = (st_own[j, at_rows, :] + st_in[j, at_rows, :]) / width
        for g in range(4):
            mean = moments[:, 32 * g : 32 * g + 1]
            var = moments[:, 32 * g + 16 : 32 * g + 17] - mean * mean
            rows = pl.ds(g * quarter, quarter)
            s1[rows, :] = jnp.broadcast_to(mean, (quarter, 128))
            s2[rows, :] = jnp.broadcast_to(lax.rsqrt(var + EPS), (quarter, 128))
        scale_rows(xg.at[y, j], lo, n, s1, s2)
        gather.YR(u)

    def w_rows(xx, core):
        return pl.ds(al(rem(xx, 2) * kc + core * kd, 128), kd)

    def w_part(group, half, i):
        side = kh if half else 1 - kh
        return weights[i].at[:, pl.ds(al((2 * group + side) * hc, 128), hc)]

    def w_cols(half, i):
        return pl.ds(half * 3 * hc + i * hc, hc)

    def wa_copy(half, i, xx):
        return remote(w_part(1 - ng, half, i), wb.at[w_rows(xx, c), w_cols(half, i)], swa.at[0], rwa.at[half, i], at.pa)

    def wo_copy(half, i, core):
        return remote(w_part(ng, half, i), wb.at[w_rows(x, core), w_cols(half, i)], swo.at[0], rwo.at[half, i], at.partner)

    def w_local(half, i):
        return pltpu.make_async_copy(w_part(ng, half, i), wb.at[w_rows(x, c), w_cols(half, i)], lw.at[half, i])

    def wp_copy(half, core):
        ref = wb.at[w_rows(at.xa, core), pl.ds(half * 3 * hc, 3 * hc)]
        return remote(ref, ref, swp.at[0], rwp.at[half], at.partner)

    o_local = pltpu.make_async_copy(wo, wob.at[:, half_cols(c)], lw.at[2, 0])
    o_pair = remote(wo, wob.at[:, half_cols(c)], so.at[0], ro.at[0], at.partner)
    pieces = [(half, i) for half in range(2) for i in range(3)]

    def WOP():
        for half, i in pieces:
            wo_copy(half, i, c).start()
        o_pair.start()

    def WA(half):
        for i in range(3):
            wa_copy(half, i, x).start()

    def WP(half):
        for i in range(3):
            wa_copy(half, i, at.xa).wait_recv()
        wp_copy(half, c).start()

    w_halves = [0, 1]

    def w_ready(half):
        if half not in w_halves:
            return
        w_halves.remove(half)
        for i in range(3):
            w_local(half, i).wait()
            wo_copy(half, i, 1 - c).wait_recv()
        wp_copy(half, 1 - c).wait_recv()
        if half:
            own_out()

    def own_out():
        for m in range(2):
            d_in(m).wait()
            d_out(m).start()
            d_pair(m, 3, c).start()

    def o_ready():
        o_local.wait()
        dst = wob.at[:, half_cols(1 - c)]
        remote(dst, dst, so.at[0], ro.at[0], at.partner).wait_recv()

    mlp_weights = (wg_t, wu_t)
    parts = ((0, f_a), (f_a, fc - f_a))

    def d_src(m, xx, p):
        return mlp_weights[m].at[pl.ds(al(xx * fc + parts[p][0], 8), parts[p][1])]

    def d_dst(m, xx, p):
        return w_all.at[m, pl.ds(*parts[p]), pl.ds(al((2 * xx + c) * kd, 128), kd)]

    def s_copy(d, m, p, xx):
        to, dev = ((at.xa, at.pa), (at.xb, at.pb))[d]
        return remote(d_src(m, to, p), d_dst(m, xx, p), sds.at[d], rds.at[d, m, p], dev)

    def o_copy(d, m):
        return remote(d_src(m, at.xo, d), (drel_a, drel_b)[d].at[m], sdo.at[d], rdo.at[d, m], (at.pa, at.pb)[d])

    def f_copy(d, m, xx):
        return remote((drel_a, drel_b)[d].at[m], d_dst(m, xx, d), sdf.at[d], rdf.at[d, m], (at.pb, at.pa)[d])

    def d_in(m):
        return pltpu.make_async_copy(mlp_weights[m].at[pl.ds(al(x * fc, 8), fc)], own.at[m], lg.at[0, m])

    def d_all(m, xx, core):
        return w_all.at[m, :, pl.ds(al((2 * xx + core) * kd, 128), kd)]

    def d_out(m):
        return pltpu.make_async_copy(own.at[m], d_all(m, x, c), lg.at[1, m])

    def d_pair(m, k, core):
        dst = d_all(m, (at.xa, at.xb, at.xo, x)[k], core)
        return remote(own.at[m] if k == 3 else dst, dst, sdp.at[0], rdp.at[m, k], at.partner)

    def S(link, m, p):
        s_copy("ab".index(link), m, p, x).start()

    def O(link, m):
        o_copy("ab".index(link), m).start()

    def F(link, m):
        d = "ba".index(link)
        o_copy(d, m).wait_recv()
        f_copy(d, m, (at.xa, at.xb)[d]).start()

    def DP(m):
        for d in range(2):
            for p in range(2):
                s_copy(d, m, p, (at.xa, at.xb)[d]).wait_recv()
            f_copy(d, m, at.xo).wait_recv()
        for k in range(3):
            d_pair(m, k, c).start()

    def pr_copy(n):
        return remote(part.at[n, :, pl.ds(0, 3 * hc)], precv.at[n], spr.at[0], rpr.at[n], at.pb)

    def project(g, first, size):
        def done(col, step, out):
            for i, (r, j) in enumerate(GROUPS[g]):
                part[r * NJ + j, :, pl.ds(al(first + col, 128), step)] = out[i * ch : (i + 1) * ch].astype(BF16)

        refs = [xg.at[gather.seqs[r], j] for r, j in GROUPS[g]]
        product(refs, wb.at[:, pl.ds(first, size)], wb.shape[0], size, done)

    split = {step[1] for step in ATTENTION_STEPS if step[0] == "Q"}

    def G(g):
        w_ready(0)
        for r, j in GROUPS[g]:
            gather.chunk_wait(r, j)
        if g in split:
            project(g, 0, 3 * hc)
        else:
            w_ready(1)
            project(g, 0, 6 * hc)
        for r, j in GROUPS[g]:
            pr_copy(r * NJ + j).start()

    def Q(g):
        w_ready(1)
        project(g, 3 * hc, 3 * hc)

    def kv_copy(r, j):
        s, n = gather.seqs[r], r * NJ + j
        return remote(kvo.at[s, j], kvp.at[s, j], skv.at[0], rkv.at[n], at.partner)

    def rotate(r, j):
        s, n = gather.seqs[r], r * NJ + j
        pr_copy(n).wait_recv()
        cos_t, sin_t = cos_all[j], sin_all[j]

        def total(col, size):
            mine = part[n, :, 3 * hc + col : 3 * hc + col + size]
            return (mine.astype(F32) + precv[n, :, col : col + size].astype(F32)).astype(BF16)

        def turned(col):
            v = total(col, HEAD_DIM).astype(F32)
            return (v * cos_t + pltpu.roll(v, HEAD_DIM // 2, axis=1) * sin_t).astype(BF16)

        for col in range(0, hc, HEAD_DIM):
            qb[n, :, col : col + HEAD_DIM] = turned(col)
            kvo[s, j, :, col : col + HEAD_DIM] = turned(hc + col)
        kvo[s, j, :, hc:] = total(2 * hc, hc)
        kv_copy(r, j).start()

    def R(g):
        for r, j in GROUPS[g]:
            rotate(r, j)

    def o_cols(xx):
        return pl.ds(al((2 * rem(div(xx + 1, 2), 2) + div(xx, 2)) * hc, 128), hc)

    cut = ch // 8

    def og_copy(kind, n):
        if kind < 2:
            ref = og.at[n, :, o_cols(x)]
        elif kind == 2:
            ref = og.at[n, pl.ds(0, cut), o_cols(at.xa)]
        else:
            ref = og.at[n, pl.ds(cut, ch - cut), o_cols(at.xb)]
        return remote(ref, ref, sog.at[kind], rog.at[kind, n], at.pa if kind in (0, 3) else at.pb)

    def og_wait(kind, n):
        xx = (at.xa, at.xb, at.xo, at.xo)[kind]
        rows = (pl.ds(0, ch), pl.ds(0, ch), pl.ds(0, cut), pl.ds(cut, ch - cut))[kind]
        dst = og.at[n, rows, o_cols(xx)]
        remote(dst, dst, sog.at[kind], rog.at[kind, n], at.pa).wait_recv()

    def attend(r, j, i):
        s, n = gather.seqs[r], r * NJ + j
        keys = (j + 1) * ch
        iq = lax.broadcasted_iota(jnp.int32, (ch, keys), 0) + j * ch
        ik = lax.broadcasted_iota(jnp.int32, (ch, keys), 1)
        own_ok = iq >= ik
        par_ok = ik < (j + c) * ch
        contract = (((1,), (1,)), ((), ()))
        cols = pl.ds(al(i * HEAD_DIM, 128), HEAD_DIM)
        v_cols = pl.ds(al(hc + i * HEAD_DIM, 128), HEAD_DIM)
        q = qb[n, :, cols]
        k_own = kvo[s, 0 : j + 1, :, cols].reshape(keys, HEAD_DIM)
        k_par = kvp[s, 0 : j + 1, :, cols].reshape(keys, HEAD_DIM)
        s_own = lax.dot_general(q, k_own, contract, preferred_element_type=F32) * HEAD_DIM**-0.5
        s_par = lax.dot_general(q, k_par, contract, preferred_element_type=F32) * HEAD_DIM**-0.5
        s_own = jnp.where(own_ok, s_own, -1e30)
        s_par = jnp.where(par_ok, s_par, -1e30)
        top = jnp.maximum(jnp.max(s_own, axis=1, keepdims=True), jnp.max(s_par, axis=1, keepdims=True))
        e_own, e_par = jnp.exp(s_own - top), jnp.exp(s_par - top)
        inv = 1.0 / (jnp.sum(e_own, axis=1, keepdims=True) + jnp.sum(e_par, axis=1, keepdims=True))
        v_own = kvo[s, 0 : j + 1, :, v_cols].reshape(keys, HEAD_DIM)
        v_par = kvp[s, 0 : j + 1, :, v_cols].reshape(keys, HEAD_DIM)
        out = jnp.dot((e_own * inv).astype(BF16), v_own, preferred_element_type=F32)
        out += jnp.dot((e_par * inv).astype(BF16), v_par, preferred_element_type=F32)
        og[n, :, pl.ds(al((2 * ng + kh) * hc + i * HEAD_DIM, 128), HEAD_DIM)] = out.astype(BF16)

    def A(g):
        for r, j in GROUPS[g]:
            kv_copy(r, j).wait_recv()

        def head(i, carry):
            for r, j in GROUPS[g]:
                attend(r, j, i)
            return carry

        lax.fori_loop(0, hc // HEAD_DIM, head, 0)
        for r, j in GROUPS[g]:
            og_copy(0, r * NJ + j).start()
            og_copy(1, r * NJ + j).start()

    def P(g):
        for r, j in GROUPS[g]:
            for kind in range(2):
                og_wait(kind, r * NJ + j)
                og_copy(kind + 2, r * NJ + j).start()

    def X(g):
        for r, j in GROUPS[g]:
            og_wait(2, r * NJ + j)
            og_wait(3, r * NJ + j)

        def done(col, size, out):
            for i, (r, j) in enumerate(GROUPS[g]):
                zb[r, j, :, pl.ds(al(col, 128), size)] = out[i * ch : (i + 1) * ch].astype(BF16)

        product([og.at[r * NJ + j] for r, j in GROUPS[g]], wob, wob.shape[0], kc, done, 512 if GROUPS[g][0][0] == 0 else 256)
        for r, j in GROUPS[g]:
            if r == 2:
                reduce.halves(j)

    def T(j):
        def done(rows, attn):
            h_ref[j, rows, :] = (xc[j, rows, :].astype(F32) + attn.astype(BF16).astype(F32)).astype(BF16)

        reduce.total(j, done)
        chunk_out(j).start()

    def chunk_out(j):
        return pltpu.make_async_copy(h_ref.at[j], h_hbm.at[j], lx.at[1 + j])

    def h_out(r, u):
        rows = pl.ds(u * (ch // 2), ch // 2)
        return pltpu.make_async_copy(hg.at[ahead.seqs[r], 0, rows], hg_all.at[ahead.seqs[r], rows], lh.at[r, u])

    kept = []

    def HF(u):
        if not kept:
            kept.append(u)
            ahead.keep_own()
        ahead.XF(0, u)

    def HY(u):
        ahead.YH(u)
        for r in (0, 1, 3):
            h_out(r, u).start()

    def HO(u):
        for d in range(2):
            ahead.yhalf_wait(d, u)
        h_out(2, u).start()

    def local_weights():
        for half, i in pieces:
            w_local(half, i).start()
        o_local.start()
        for m in range(2):
            d_in(m).start()

    def own_rows():
        x_in.start()
        for copy in tables:
            copy.start()
        x_in.wait()
        for j in range(NJ):
            xc[j, :, half_cols(c)] = x_ref[x_rows(j, c), :]

    x_in = pltpu.make_async_copy(x_hbm, x_ref, lx.at[0])
    tables = [pltpu.make_async_copy(src, dst, lx.at[1 + NJ + i]) for i, (src, dst) in enumerate(((turn_hbm, turn_ref), (base_hbm, base_ref)))]
    at.barrier(own_rows)

    def angles():
        for copy in tables:
            copy.wait()
        lane = lax.broadcasted_iota(jnp.int32, (ch, HEAD_DIM), 1)
        for j in range(NJ):
            base_cos, base_sin = base_ref[0, pl.ds(2 * j + c, 1), :], base_ref[1, pl.ds(2 * j + c, 1), :]
            cos_all[j] = base_cos * turn_ref[0] - base_sin * turn_ref[1]
            sine = base_sin * turn_ref[0] + base_cos * turn_ref[1]
            sin_all[j] = jnp.where(lane < HEAD_DIM // 2, -sine, sine)

    ops = {
        "XP": XP, "WOP": WOP, "XE": XE, "ST": ST, "N": N, "YH": gather.YH, "WA": WA, "WP": WP, "S": S, "O": O, "F": F, "DP": DP,
        "G": G, "Q": Q, "R": R, "A": A, "P": P, "X": X, "M": reduce.middle, "T": T,
        "HF": HF, "HH": lambda u: ahead.XH(0, u), "HN": lambda u: ahead.N(0, u), "HY": HY, "HO": HO,
    }
    def all_sent(ref, sem):
        remote(ref, ref, sem, ro.at[0], at.partner).wait_send()

    def sent():
        for m in range(2):
            for k in range(4):
                d_pair(m, k, 1 - c).wait_recv()
            d_out(m).wait()
        all_sent(w_all.at[:, :, pl.ds(0, 4 * kd)], sdp.at[0])
        for d in range(2):
            all_sent(w_all.at[:, :, pl.ds(0, kd)], sds.at[d])
            all_sent((drel_a, drel_b)[d], sdo.at[d])
            all_sent((drel_a, drel_b)[d], sdf.at[d])
            for u in range(len(units)):
                gather.ycopy(d, u).wait_send()
                gather.yhalf(d, u).wait_send()
        all_sent(x_ref.at[pl.ds(0, NJ * ch)], sd.at[0])
        all_sent(xc, sxe.at[0])
        all_sent(st_own, sst.at[0])
        reduce.drain()
        ahead.drain()
        for r in range(NX):
            for u in range(2):
                h_out(r, u).wait()
        o_pair.wait_send()
        for sem in (swa, swo, swp):
            all_sent(wb.at[pl.ds(0, kd)], sem.at[0])
        all_sent(part.at[:, :, pl.ds(0, 3 * hc)], spr.at[0])
        all_sent(kvo, skv.at[0])
        for kind, (lo, n) in enumerate(((0, ch), (0, ch), (0, cut), (cut, ch - cut))):
            all_sent(og.at[:, pl.ds(lo, n), o_cols(x)], sog.at[kind])

    waits = {"X": o_ready, "WP": angles, "ST": local_weights}
    last = max(i for i, step in enumerate(ATTENTION_STEPS) if step[0] == "X")
    for i, step in enumerate(ATTENTION_STEPS):
        if step[0] in waits:
            waits.pop(step[0])()
        if i == last:
            sent()
        ops[step[0]](*step[1:])
    for j in range(NJ):
        chunk_out(j).wait()


def mlp_kernel(
    units, h_hbm, w_hbm, wdn, hg_hbm, y_ref,
    h_ref, xg, wt, raw, wd, ag, ar, act, s1, s2, zb, ya, yb, yfd, yfu, yst,
    sx, rx, sy, ry, syh, ryh, sa, ra, syr, ryr, sd, rd, lw, lwd, swd, rwd, lh, lo,
):
    at = Place()
    x, c, y = at.x, at.c, at.y
    ch, kc, h = h_ref.shape[1], h_ref.shape[2], h_ref.shape[1] // 2
    width = xg.shape[-1]
    kd = kc // 2
    fc, tiles = w_hbm.shape[1], wt.shape[1] // 256
    fm = (tiles - 1) * 128
    fr = fc - fm
    blocks, slots = 2 * tiles, raw.shape[0]
    gather = Spread(at, h_ref, xg, units, (s1, s2), sx, rx, sy, ry, syh, ryh)
    reduce = Reduce(at, zb, ya, yb, yfd, yfu, syr, ryr)

    def w_in(q):
        i, m = q // 2, q % 2
        n = min(128, fc - i * 128)
        return pltpu.make_async_copy(w_hbm.at[m, pl.ds(i * 128, n)], raw.at[q % slots, pl.ds(0, n)], lw.at[q])

    def WT(g):
        for q in range(g * blocks // 4, (g + 1) * blocks // 4):
            i, m, slot = q // 2, q % 2, q % slots
            w_in(q).wait()
            if fc < (i + 1) * 128:
                raw[slot, fc - i * 128 :, :] = jnp.zeros(((i + 1) * 128 - fc, width), BF16)

            def turn(k, carry, slot=slot, q=q):
                part = pl.ds(al(k * (width // 4), 128), width // 4)
                wt[part, q * 128 : (q + 1) * 128] = raw[slot, :, part].T
                return carry

            lax.fori_loop(0, 4, turn, 0)
            if q + slots < blocks:
                w_in(q + slots).start()

    def d_refs(q, core):
        cols = pl.ds(al(core * kd, 128), kd)
        main, rest = wdn.at[pl.ds(q * fc, fm)], wdn.at[pl.ds(q * fc + fm, fr)]
        return (main, wd.at[pl.ds(q * fm, fm), cols]), (rest, wd.at[pl.ds(NX * fm + q * 128, fr), cols])

    def d_own(q, k):
        src, dst = d_refs(q, c)[k]
        return pltpu.make_async_copy(src, dst, lwd.at[q, k])

    def d_pair(q, k, core):
        src, dst = d_refs(q, core)[k]
        return remote(src, dst, swd.at[q, k], rwd.at[q, k], at.partner)

    quarters = [(q, k) for q in range(NX) for k in range(2)]
    h_in_all = pltpu.make_async_copy(h_hbm, h_ref, lo.at[NJ])
    h_in_all.start()
    def h_in(s):
        return pltpu.make_async_copy(hg_hbm.at[s], xg.at[s, 0], lh.at[s])

    def local_copies():
        for q in range(slots):
            w_in(q).start()
        for s in range(NX):
            h_in(s).start()
        for q, k in quarters:
            d_own(q, k).start()
        for q in range(NX):
            wd[NX * fm + q * 128 + fr : NX * fm + (q + 1) * 128, :] = jnp.zeros((128 - fr, kc), BF16)
        h_in_all.wait()

    at.barrier(local_copies)
    for q, k in quarters:
        d_pair(q, k, c).start()

    def a_refs(kind, n, xx):
        main, rest = pl.ds(al(xx * fm, 128), fm), pl.ds(al(xx * 128, 128), 128)
        if kind < 2:
            return ag.at[n, :, main], ar.at[n, :, rest]
        lo = (kind - 2) * h
        return ag.at[n, pl.ds(lo, h), main], ar.at[n, pl.ds(lo // 2, h // 2), rest]

    def a_copies(kind, n):
        refs = a_refs(kind, n, (x, x, at.xl, at.xr)[kind])
        return [remote(v, v, sa.at[kind, k], ra.at[kind, n, k], at.left if kind % 2 else at.right) for k, v in enumerate(refs)]

    def a_wait(kind, n):
        for k, v in enumerate(a_refs(kind, n, (at.xl, at.xr, at.xo, at.xo)[kind])):
            remote(v, v, sa.at[kind, k], ra.at[kind, n, k], at.right).wait_recv()

    def a_start(kind, n):
        for copy in a_copies(kind, n):
            copy.start()

    def G(g):
        for r, j in GROUPS[g]:
            gather.chunk_wait(r, j)

        def done(col, size, out):
            for k in range(0, size, 256):
                gate, up = out[:, k : k + 128].astype(BF16).astype(F32), out[:, k + 128 : k + 256].astype(BF16).astype(F32)
                value = (gate / (1.0 + jnp.exp(-gate)) * up).astype(BF16)
                act[0 : value.shape[0], pl.ds(al(div(col + k, 2), 128), 128)] = value

        product([xg.at[gather.seqs[r], j] for r, j in GROUPS[g]], wt, width, wt.shape[1], done)
        for i, (r, j) in enumerate(GROUPS[g]):
            n, lo = r * NJ + j, i * ch
            ag[n, :, pl.ds(al(x * fm, 128), fm)] = act[lo : lo + ch, :fm]
            below = pltpu.roll(act[lo + h : lo + ch, fm:].astype(F32), 64, axis=1)
            ar[n, :, pl.ds(al(x * 128, 128), 128)] = (act[lo : lo + h, fm:].astype(F32) + below).astype(BF16)
            for kind in range(2):
                a_start(kind, n)

    def P(g):
        for r, j in GROUPS[g]:
            for kind in range(2):
                a_wait(kind, r * NJ + j)
                a_start(kind + 2, r * NJ + j)

    def unpack(g):
        for r, j in GROUPS[g]:
            n = r * NJ + j
            for kind in (2, 3):
                a_wait(kind, n)
            lane = lax.broadcasted_iota(jnp.int32, (h, 128), 1)
            for q in range(NX):
                cols = pl.ds(NX * fm + q * 128, 128)
                rest = ar[n, :, q * 128 : (q + 1) * 128].astype(F32)
                ag[n, 0:h, cols] = jnp.where(lane < 64, rest, 0.0).astype(BF16)
                ag[n, h:, cols] = jnp.where(lane < 64, pltpu.roll(rest, 64, axis=1), 0.0).astype(BF16)

    def X(g):
        unpack(g)

        def done(col, size, out):
            for i, (r, j) in enumerate(GROUPS[g]):
                zb[r, j, :, pl.ds(al(col, 128), size)] = out[i * ch : (i + 1) * ch].astype(BF16)

        product([ag.at[r * NJ + j] for r, j in GROUPS[g]], wd, wd.shape[0], kc, done, 512 if len(GROUPS[g]) == 1 else 256)
        for r, j in GROUPS[g]:
            if r == 2:
                reduce.halves(j)

    def half_cols(core):
        return pl.ds(al(core * kd, 128), kd)

    def y_rows(j, core):
        return pl.ds(al((2 * j + core) * ch, 8), ch)

    def y_copy(j):
        return remote(yst.at[1 - c, j], y_ref.at[y_rows(j, c)], sd.at[j], rd.at[j], at.partner)

    def y_own(j):
        return pltpu.make_async_copy(yst.at[c, j], y_ref.at[y_rows(j, c)], lo.at[j])

    def y_wait(j):
        dst = y_ref.at[y_rows(j, 1 - c)]
        remote(dst, dst, sd.at[j], rd.at[j], at.partner).wait_recv()

    def T(j):
        def done(rows, mlp):
            out = (h_ref[j, rows, :].astype(F32) + mlp.astype(BF16).astype(F32)).astype(BF16)
            yst[0, j, rows, :] = out[:, :kd]
            yst[1, j, rows, :] = out[:, kd:]

        reduce.total(j, done)
        y_copy(j).start()
        y_own(j).start()

    def XT(g):
        ((_, j),) = GROUPS[g]
        unpack(g)
        reduce.wait(2, j)
        reduce.wait(3, j)

        def half(i, carry):
            core = 1 - c + i * (2 * c - 1)
            cols = half_cols(core)
            out = jnp.dot(ag[j], wd[:, cols], preferred_element_type=F32).astype(BF16).astype(F32)
            mlp = out + yfd[j, :, cols].astype(F32) + yfu[j, :, cols].astype(F32)
            yst[core, j] = (h_ref[j, :, cols].astype(F32) + mlp.astype(BF16).astype(F32)).astype(BF16)
            pl.when(i == 0)(lambda: y_copy(j).start())
            return carry

        lax.fori_loop(0, 2, half, 0)
        y_own(j).start()

    ops = {"G": G, "P": P, "X": X, "M": reduce.middle, "T": T, "XT": XT, "WT": WT}
    for name in ("YR", "YRH", "YH", "XF", "XH", "N"):
        ops[name] = getattr(gather, name)
    waits = {
        "N": gather.keep_own,
        "G": lambda: [h_in(s).wait() for s in range(NX)],
        "X": lambda: [(d_own(q, k).wait(), d_pair(q, k, 1 - c).wait_recv()) for q, k in quarters],
    }
    def sent():
        gather.drain()
        reduce.drain()
        for q, k in quarters:
            d_pair(q, k, c).wait_send()

        for kind in range(4):
            for k, every in enumerate(a_refs(kind, slice(None), x)):
                remote(every, every, sa.at[kind, k], ra.at[kind, 0, k], at.right).wait_send()

    (_, g), (_, j) = MLP_STEPS[-2:]
    assert MLP_STEPS[-2:] == (("X", g), ("T", j)) and GROUPS[g] == ((0, j),)
    for step in (*MLP_STEPS[:-2], ("XT", g)):
        if step[0] in waits:
            waits.pop(step[0])()
        ops[step[0]](*step[1:])
    sent()
    for j in range(NJ):
        y_copy(j).wait_send()
        y_own(j).wait()
        y_wait(j)


def vmem(*shape, dtype=BF16):
    return pltpu.VMEM(shape, dtype)


def sems(*shape):
    return pltpu.SemaphoreType.DMA(shape)


def solution(mesh):
    assert mesh.shape["tx"] == 2 * NX and mesh.shape["ty"] == NX
    act_spec = P(("dp", "ty"), None, "tx")
    col_spec = P("tx", "ty")
    row_spec = P("ty", "tx")
    any_spec = pl.BlockSpec(memory_space=pl.ANY)
    vmem_spec = pl.BlockSpec(memory_space=pltpu.VMEM)

    def layer(x_blk, w_q, w_k, w_v, w_o, w_gate, w_up, w_down):
        _, seq, kd = x_blk.shape
        kc, width = 2 * kd, 2 * NX * kd
        ch = seq // (2 * NJ)
        h = ch // 2
        row_heads = w_q.shape[1]
        hc = row_heads // NX
        fc = w_down.shape[0] // NX
        assert hc % HEAD_DIM == 0
        tiles = (fc + 127) // 128
        f_a = (fc // 2 + 15) // 16 * 16

        inv_freq = THETA ** (-2.0 * np.arange(HEAD_DIM // 2) / HEAD_DIM)
        inv_freq = np.concatenate([inv_freq, inv_freq])
        turn = np.arange(ch)[:, None] * inv_freq
        base = np.arange(2 * NJ)[:, None] * ch * inv_freq
        turn = jnp.asarray(np.stack([np.cos(turn), np.sin(turn)]), F32)
        base = jnp.asarray(np.stack([np.cos(base), np.sin(base)]), F32)

        reduce_scratch = [vmem(NX, NJ, ch, kc), vmem(NJ, h, kc), vmem(NJ, ch - h, kc), vmem(NJ, ch, kc), vmem(NJ, ch, kc)]
        units = ((0, 0, h, 0), (0, h, h, 0)) + tuple((j, 0, ch, 0) for j in range(1, NJ))
        n_u = len(units)
        h_blk, w_all, hg_all = pl.pallas_call(
            functools.partial(attention_kernel, units),
            out_shape=(
                jax.ShapeDtypeStruct((NJ, ch, kc), BF16),
                jax.ShapeDtypeStruct((2, fc, width), BF16),
                jax.ShapeDtypeStruct((NX, ch, width), BF16),
            ),
            in_specs=[any_spec] * 9,
            out_specs=(any_spec, any_spec, any_spec),
            scratch_shapes=[
                vmem(seq, kd), vmem(2, ch, HEAD_DIM, dtype=F32), vmem(2, 2 * NJ, HEAD_DIM, dtype=F32),
                vmem(NJ, ch, kc), vmem(NJ, ch, kc), vmem(NX, NJ, ch, 2 * kc), vmem(NX, 1, ch, width), vmem(NJ, ch, HEAD_DIM, dtype=F32), vmem(NJ, ch, HEAD_DIM, dtype=F32),
                vmem(NJ, ch // 4, 128, dtype=F32), vmem(NJ, ch // 4, 128, dtype=F32), vmem(ch, 128, dtype=F32), vmem(ch, 128, dtype=F32),
                vmem(2 * kc, 6 * hc), vmem(row_heads, kc), vmem(NCH, ch, 6 * hc), vmem(NCH, ch, 3 * hc), vmem(NCH, ch, hc),
                vmem(NX, NJ, ch, 2 * hc), vmem(NX, NJ, ch, 2 * hc), vmem(NCH, ch, row_heads), *reduce_scratch,
                vmem(2, fc, kd), vmem(2, f_a, kd), vmem(2, fc - f_a, kd),
                sems(1), sems(n_u), sems(1), sems(n_u), sems(2, n_u), sems(2, n_u), sems(2, n_u), sems(2, n_u),
                sems(1), sems(NJ), sems(1), sems(2, 3), sems(1), sems(2, 3), sems(1), sems(2), sems(3, 3), sems(1), sems(1),
                sems(1), sems(NCH), sems(1), sems(NCH), sems(4), sems(4, NCH), sems(4), sems(4, NJ),
                sems(2, 2), sems(2), sems(2, 2, 2), sems(2), sems(2, 2), sems(2), sems(2, 2), sems(1), sems(2, 4),
                sems(4, 2), sems(4, 2), sems(2, 2), sems(2, 2), sems(2, 2), sems(2, 2), sems(NX, 2), sems(3 + NJ),
            ],
            compiler_params=pltpu.CompilerParams(collective_id=0, has_side_effects=True, vmem_limit_bytes=VMEM_LIMIT),
            name="attention_part",
        )(x_blk[0], turn, base, w_q, w_k, w_v, w_o, w_gate.T, w_up.T)

        units = ((1, 0, h, 1), (1, h, h, 0)) + tuple((j, 0, ch, 0) for j in range(2, NJ))
        n_u, n_x = len(units), len(units) + 3
        y_blk = pl.pallas_call(
            functools.partial(mlp_kernel, units),
            out_shape=jax.ShapeDtypeStruct((seq, kd), BF16),
            in_specs=[any_spec] * 4,
            out_specs=any_spec,
            scratch_shapes=[
                vmem(NJ, ch, kc),
                vmem(NX, NJ, ch, width), vmem(width, tiles * 256), vmem(3, 128, width),
                vmem(NX * tiles * 128, kc), vmem(NCH, ch, NX * tiles * 128), vmem(NCH, h, NX * 128), vmem(2 * ch, tiles * 128),
                vmem(ch, 128, dtype=F32), vmem(ch, 128, dtype=F32),
                *reduce_scratch, vmem(2, NJ, ch, kd),
                sems(4, n_x), sems(4, n_x), sems(2, n_u), sems(2, n_u), sems(2, n_u), sems(2, n_u),
                sems(4, 2), sems(4, NCH, 2), sems(4), sems(4, NJ), sems(NJ), sems(NJ),
                sems(2 * tiles), sems(NX, 2), sems(NX, 2), sems(NX, 2), sems(NX), sems(NJ + 1),
            ],
            compiler_params=pltpu.CompilerParams(collective_id=1, has_side_effects=True, vmem_limit_bytes=VMEM_LIMIT),
            name="mlp_part",
        )(h_blk, w_all, w_down, hg_all)
        return y_blk[None]

    return jax.shard_map(
        layer,
        mesh=mesh,
        in_specs=(act_spec, col_spec, col_spec, col_spec, row_spec, col_spec, col_spec, row_spec),
        out_specs=act_spec,
        check_vma=False,
    )
```
